32 devices in a mesh: pipe: 2 (over core), dp: 4 (over y, x), tensor: 4 (over z).
Axes of the slice: x: 2, y: 2, z: 4, core: 2. Of those that a mesh axis runs over, the one named last changes fastest.
Arguments:
- images: bfloat16 [4, 32, 196, 512], P(None, ('dp', 'tensor')), may hold values from -6 to 6
- cotangent: bfloat16 [4, 32, 196, 512], P(None, ('dp', 'tensor')), may hold values from -6 to 6
- counts: int32 [4, 4], P(None, 'dp'), may hold values from 4 to 8, as said below
- rel_index: int32 [49, 49], replicated, may hold values from 0 to 168, as said below
- pre_attn_gain: bfloat16 [2, 512], P('pipe', 'tensor'), may hold values from 0.25 to 1.75
- pre_attn_bias: bfloat16 [2, 512], P('pipe', 'tensor'), may hold values from -3 to 3
- qkv_weight: bfloat16 [2, 512, 1536], P('pipe', None, 'tensor'), may hold values from -0.25 to 0.25
- qv_bias: bfloat16 [2, 1024], P('pipe', 'tensor'), may hold values from -3 to 3
- bias_table: bfloat16 [2, 16, 169], P('pipe', 'tensor'), may hold values from -3 to 256
- proj_weight: bfloat16 [2, 512, 512], P('pipe', 'tensor'), may hold values from -0.75 to 0.75
- proj_bias: bfloat16 [2, 512], P('pipe', 'tensor'), may hold values from -3 to 3
- pre_mlp_gain: bfloat16 [2, 512], P('pipe', 'tensor'), may hold values from 0.25 to 1.75
- pre_mlp_bias: bfloat16 [2, 512], P('pipe', 'tensor'), may hold values from -3 to 3
- hidden_weight: bfloat16 [2, 512, 2048], P('pipe', None, 'tensor'), may hold values from -0.25 to 0.25
- hidden_bias: bfloat16 [2, 2048], P('pipe', 'tensor'), may hold values from -3 to 3
- out_weight: bfloat16 [2, 2048, 512], P('pipe', 'tensor'), may hold values from -0.125 to 0.125
- out_bias: bfloat16 [2, 512], P('pipe', 'tensor'), may hold values from -3 to 3
Outputs:
- block_out: bfloat16 [2, 4, 32, 196, 512], P('pipe', None, ('dp', 'tensor'))
- input_grad: bfloat16 [2, 4, 32, 196, 512], P('pipe', None, ('dp', 'tensor'))
- pre_attn_gain_grad: float32 [2, 512], P('pipe', 'tensor')
- pre_attn_bias_grad: float32 [2, 512], P('pipe', 'tensor')
- qkv_weight_grad: float32 [2, 512, 1536], P('pipe', None, 'tensor')
- qv_bias_grad: float32 [2, 1024], P('pipe', 'tensor')
- bias_table_grad: float32 [2, 16, 169], P('pipe', 'tensor')
- proj_weight_grad: float32 [2, 512, 512], P('pipe', 'tensor')
- proj_bias_grad: float32 [2, 512], P('pipe', 'tensor')
- pre_mlp_gain_grad: float32 [2, 512], P('pipe', 'tensor')
- pre_mlp_bias_grad: float32 [2, 512], P('pipe', 'tensor')
- hidden_weight_grad: float32 [2, 512, 2048], P('pipe', None, 'tensor')
- hidden_bias_grad: float32 [2, 2048], P('pipe', 'tensor')
- out_weight_grad: float32 [2, 2048, 512], P('pipe', 'tensor')
- out_bias_grad: float32 [2, 512], P('pipe', 'tensor')
The draws below stay inside these ranges and needn't reach their ends.
Inputs may be any that keep to these rules, and one draw needn't show every extreme that they name: Slots 0 to counts - 1 of a data shard's 8 slots hold images; both ends are reached in every draw. rel_index[a, b] depends only on the offset between positions a and b of a window; distinct offsets have distinct entries.
All inputs are finite; a program needn't handle non-finite values.
Results may differ from the reference program's by a relative error of at most 0.023.
Values may be sent and summed in bfloat16 or wider, within the bound.
A program may use at most 320 MiB of HBM per device.

```python
import math
import jax
import jax.numpy as jnp
from jax import lax

D = 512
H = 16
HD = 32
FF = 2048
WIN = 7
GRID = 14
SHIFT = 3
M = 4
TOK = 196
RELS = 169
CAP = 8
IMAGES = 32
N_DP = 4


def table_order(key):
    return jax.random.permutation(jax.random.fold_in(key, 7), RELS)


def draw_rel_index(key, part):
    span = jnp.arange(WIN * WIN, dtype=jnp.int32)
    row_pos = span // WIN
    col_pos = span % WIN
    offsets = (row_pos[:, None] - row_pos[None, :] + WIN - 1) * (2 * WIN - 1) + (col_pos[:, None] - col_pos[None, :] + WIN - 1)
    return table_order(key)[offsets].astype(jnp.int32)


def draw_bias_table(key, part):
    base = jax.random.normal(jax.random.fold_in(key, 3), (2, H, RELS), jnp.float32)
    return jnp.clip(base, -3.0, 3.0).astype(jnp.bfloat16)


def draw_counts(key, part):
    total_cells = M * N_DP
    drawn = jax.random.randint(jax.random.fold_in(key, 1), (total_cells,), CAP // 2, CAP + 1)
    spot = jax.random.randint(jax.random.fold_in(key, 2), (), 0, total_cells)
    drawn = drawn.at[spot].set(CAP)
    drawn = drawn.at[(spot + 1) % total_cells].set(CAP // 2)
    return drawn.reshape(M, N_DP).astype(jnp.int32)


def level_of(rng, dims, pieces, low, largest):
    level, own = 1.0, jax.random.fold_in(rng, 6)
    for dim, parts in pieces:
        steps = jnp.exp(jax.random.uniform(jax.random.fold_in(own, dim), (parts,), jnp.float32, low / len(pieces), largest / len(pieces)))
        level = level * jnp.repeat(steps, dims[dim] // parts).reshape([-1 if axis == dim else 1 for axis in range(len(dims))])
    return level


def bell_draw(stream_key, extent, spread, most, pieces=(), held_as=jnp.bfloat16):
    values = jax.random.normal(stream_key, extent, jnp.float32) * spread
    if len(pieces) > 0:
        values = level_of(stream_key, extent, pieces, -0.22, 0.18) * values
    return jnp.clip(values, min=-most, max=most).astype(held_as)


def setup_inputs(seed: int = 0) -> dict:
    keys = jax.random.split(jax.random.key(seed), 18)
    images = bell_draw(keys[0], (M, IMAGES, TOK, D), 1.0, 6.0, ((1, 16),))
    cotangent = bell_draw(keys[1], (M, IMAGES, TOK, D), 1.0, 6.0, ((1, 16),))
    counts = draw_counts(jax.random.fold_in(keys[17], 71), 0)
    rel_index = draw_rel_index(jax.random.fold_in(keys[17], 71), 0)
    pre_attn_gain = jnp.clip(1.0 + 0.15 * jax.random.normal(keys[4], (2, D), jnp.float32), 0.25, 1.75).astype(jnp.bfloat16)
    pre_attn_bias = bell_draw(keys[5], (2, D), 0.5, 3.0, ((0, 2), (1, 4)))
    qkv_weight = bell_draw(keys[6], (2, D, 3 * D), D ** -0.5, 0.25, ((0, 2), (2, 4)))
    qv_bias = bell_draw(keys[7], (2, 2 * D), 0.5, 3.0, ((0, 2), (1, 4)))
    bias_table = draw_bias_table(jax.random.fold_in(keys[17], 71), 0)
    proj_weight = bell_draw(keys[9], (2, D, D), (D // 7) ** -0.5, 0.75, ((0, 2), (1, 4)))
    proj_bias = bell_draw(keys[10], (2, D), 0.5, 3.0, ((0, 2), (1, 4)))
    pre_mlp_gain = jnp.clip(1.0 + 0.15 * jax.random.normal(keys[11], (2, D), jnp.float32), 0.25, 1.75).astype(jnp.bfloat16)
    pre_mlp_bias = bell_draw(keys[12], (2, D), 0.5, 3.0, ((0, 2), (1, 4)))
    hidden_weight = bell_draw(keys[13], (2, D, FF), D ** -0.5, 0.25, ((0, 2), (2, 4)))
    hidden_bias = bell_draw(keys[14], (2, FF), 0.5, 3.0, ((0, 2), (1, 4)))
    out_weight = bell_draw(keys[15], (2, FF, D), FF ** -0.5, 0.125, ((0, 2), (1, 4)))
    out_bias = bell_draw(keys[16], (2, D), 0.5, 3.0, ((0, 2), (1, 4)))
    return dict(images=images, cotangent=cotangent, counts=counts, rel_index=rel_index, pre_attn_gain=pre_attn_gain, pre_attn_bias=pre_attn_bias, qkv_weight=qkv_weight, qv_bias=qv_bias, bias_table=bias_table, proj_weight=proj_weight, proj_bias=proj_bias, pre_mlp_gain=pre_mlp_gain, pre_mlp_bias=pre_mlp_bias, hidden_weight=hidden_weight, hidden_bias=hidden_bias, out_weight=out_weight, out_bias=out_bias)


EPSILON = 1e-05
MASK_VALUE = -100.0

def cyclic(tensor, offset, which_dim):
    length = tensor.shape[which_dim]
    doubled = jnp.concatenate([tensor, tensor], which_dim)
    return lax.dynamic_slice_in_dim(doubled, offset, length, which_dim)

def to_windows(tensor, offset):
    count_img = tensor.shape[0]
    channels = tensor.shape[-1]
    per_side = GRID // WIN
    grid_view = tensor.reshape(count_img, GRID, GRID, channels)
    grid_view = cyclic(cyclic(grid_view, offset, 1), offset, 2)
    grid_view = grid_view.reshape(count_img, per_side, WIN, per_side, WIN, channels).transpose(0, 1, 3, 2, 4, 5)
    return grid_view.reshape(count_img * per_side * per_side, WIN * WIN, channels)

def from_windows(windows, offset, count_img):
    channels = windows.shape[-1]
    per_side = GRID // WIN
    grid_view = windows.reshape(count_img, per_side, per_side, WIN, WIN, channels).transpose(0, 1, 3, 2, 4, 5)
    grid_view = grid_view.reshape(count_img, GRID, GRID, channels)
    grid_view = cyclic(cyclic(grid_view, GRID - offset, 1), GRID - offset, 2)
    return grid_view.reshape(count_img, GRID * GRID, channels)

def region_labels():
    span = jnp.arange(TOK, dtype=jnp.int32)
    row_band = (span // GRID >= GRID - WIN).astype(jnp.int32) + (span // GRID >= GRID - SHIFT).astype(jnp.int32)
    col_band = (span % GRID >= GRID - WIN).astype(jnp.int32) + (span % GRID >= GRID - SHIFT).astype(jnp.int32)
    return row_band * 3 + col_band

def bias_and_mask(table, onehot, mask_on):
    flat_bias = jnp.dot(table.astype(jnp.float32), onehot.T, precision=lax.Precision.HIGHEST)
    position = flat_bias.reshape(H, WIN * WIN, WIN * WIN)
    labels = to_windows(region_labels().reshape(1, TOK, 1), 0)[:, :, 0]
    differ = (labels[:, :, None] != labels[:, None, :]).astype(jnp.float32)
    return position[None, :, :, :] + MASK_VALUE * mask_on * differ[:, None, :, :]

def norm_rows(resid, gain, shift_term):
    center = resid - lax.optimization_barrier(jnp.mean(resid, -1, keepdims=True))
    inverse = lax.rsqrt(lax.optimization_barrier(jnp.mean(center * center, -1, keepdims=True)) + EPSILON)
    normed = center * inverse
    return (normed * gain.astype(jnp.float32) + shift_term.astype(jnp.float32), normed, inverse)

def norm_back(grad_out, normed, inverse, gain):
    scaled = grad_out * gain.astype(jnp.float32)
    grad_in = inverse * (scaled - lax.optimization_barrier(jnp.mean(scaled, -1, keepdims=True)) - normed * lax.optimization_barrier(jnp.mean(scaled * normed, -1, keepdims=True)))
    return (grad_in, lax.optimization_barrier(jnp.sum(grad_out * normed, (0, 1))), lax.optimization_barrier(jnp.sum(grad_out, (0, 1))))

def gelu_slope(inputs):
    cdf_part = 0.5 * (1.0 + lax.erf(inputs * 0.5 ** 0.5))
    pdf_part = jnp.exp(-0.5 * inputs * inputs) * (2.0 * math.pi) ** (-0.5)
    return cdf_part + inputs * pdf_part

def batched(spec, left, right):
    return jnp.einsum(spec, left.astype(jnp.float32), right.astype(jnp.float32))

def matmul(left, right):
    return jnp.dot(left, right, preferred_element_type=jnp.float32)

def layer_parts(params, layer_in, alive, offset, bias_mask):
    attn_gain, attn_shift, qkv_w, qv_terms_in, table_unused, proj_w, proj_b, mlp_gain, mlp_shift, hidden_w, hidden_b, out_w, out_b = params
    count_img = layer_in.shape[0]
    query_scale = HD ** (-0.5)
    resid = layer_in.astype(jnp.float32)
    first_in, normed_a, inverse_a = norm_rows(resid, attn_gain, attn_shift)
    windows = to_windows(first_in.astype(jnp.bfloat16), offset)
    count_win = windows.shape[0]
    projected = matmul(windows.reshape(-1, D), qkv_w).reshape(count_win, WIN * WIN, H, 3, HD)
    qv_terms = qv_terms_in.astype(jnp.float32).reshape(H, 2, HD)
    queries = ((projected[:, :, :, 0] + qv_terms[:, 0]) * query_scale).astype(jnp.bfloat16)
    keys_w = projected[:, :, :, 1].astype(jnp.bfloat16)
    values = (projected[:, :, :, 2] + qv_terms[:, 1]).astype(jnp.bfloat16)
    scores = batched('bqhe,bkhe->bhqk', queries, keys_w)
    scores = scores.reshape(count_img, -1, H, WIN * WIN, WIN * WIN) + bias_mask[None]
    scores = scores.reshape(count_win, H, WIN * WIN, WIN * WIN)
    top_score = lax.optimization_barrier(jnp.max(scores, -1, keepdims=True))
    exp_scores = jnp.exp(scores - top_score)
    attn_probs = exp_scores / lax.optimization_barrier(jnp.sum(exp_scores, -1, keepdims=True))
    probs_bf = attn_probs.astype(jnp.bfloat16)
    mixed_heads = batched('bhqk,bkhe->bqhe', probs_bf, values).astype(jnp.bfloat16)
    heads_out = from_windows(mixed_heads.reshape(count_win, WIN * WIN, D), offset, count_img)
    attended = matmul(heads_out.reshape(-1, D), proj_w).reshape(resid.shape) + proj_b.astype(jnp.float32)
    middle = resid + attended
    second_in, normed_m, inverse_m = norm_rows(middle, mlp_gain, mlp_shift)
    second_bf = second_in.astype(jnp.bfloat16).reshape(-1, D)
    hidden_pre = matmul(second_bf, hidden_w) + hidden_b.astype(jnp.float32)
    activ_bf = jax.nn.gelu(hidden_pre, approximate=False).astype(jnp.bfloat16)
    mlp_out = matmul(activ_bf, out_w).reshape(resid.shape) + out_b.astype(jnp.float32)
    result = ((middle + mlp_out) * alive).astype(jnp.bfloat16)
    kept_state = (normed_a, inverse_a, windows, queries, keys_w, values, attn_probs, probs_bf, heads_out, normed_m, inverse_m, second_bf, hidden_pre, activ_bf)
    return (result, kept_state)

def layer_back(params, kept_state, cotan, alive, offset, onehot):
    attn_gain, attn_shift, qkv_w, qv_terms_in, table_unused, proj_w, proj_b, mlp_gain, mlp_shift, hidden_w, hidden_b, out_w, out_b = params
    normed_a, inverse_a, windows, queries, keys_w, values, attn_probs, probs_bf, heads_out, normed_m, inverse_m, second_bf, hidden_pre, activ_bf = kept_state
    count_img = cotan.shape[0]
    count_win = windows.shape[0]
    query_scale = HD ** (-0.5)
    grad_rows = (cotan.astype(jnp.float32) * alive).reshape(-1, D)
    grad_rows_bf = grad_rows.astype(jnp.bfloat16)
    out_w_grad = matmul(activ_bf.T, grad_rows_bf)
    out_b_grad = lax.optimization_barrier(jnp.sum(grad_rows, 0))
    grad_pre = matmul(grad_rows_bf, out_w.T) * gelu_slope(hidden_pre)
    grad_pre_bf = grad_pre.astype(jnp.bfloat16)
    hidden_w_grad = matmul(second_bf.T, grad_pre_bf)
    hidden_b_grad = lax.optimization_barrier(jnp.sum(grad_pre, 0))
    grad_second = matmul(grad_pre_bf, hidden_w.T).reshape(count_img, TOK, D)
    grad_norm_m, mlp_gain_grad, mlp_shift_grad = norm_back(grad_second, normed_m, inverse_m, mlp_gain)
    grad_middle = grad_rows.reshape(count_img, TOK, D) + grad_norm_m
    middle_rows = grad_middle.reshape(-1, D)
    middle_bf = middle_rows.astype(jnp.bfloat16)
    proj_w_grad = matmul(heads_out.reshape(-1, D).T, middle_bf)
    proj_b_grad = lax.optimization_barrier(jnp.sum(middle_rows, 0))
    grad_heads = matmul(middle_bf, proj_w.T).astype(jnp.bfloat16).reshape(count_img, TOK, D)
    grad_win = to_windows(grad_heads, offset).reshape(count_win, WIN * WIN, H, HD)
    grad_probs = batched('bqhe,bkhe->bhqk', grad_win, values)
    grad_values = batched('bhqk,bqhe->bkhe', probs_bf, grad_win)
    grad_scores = attn_probs * (grad_probs - lax.optimization_barrier(jnp.sum(grad_probs * attn_probs, -1, keepdims=True)))
    table_grad = jnp.dot(lax.optimization_barrier(jnp.sum(grad_scores, 0)).reshape(H, -1), onehot, precision=lax.Precision.HIGHEST)
    scores_bf = grad_scores.astype(jnp.bfloat16)
    grad_queries = batched('bhqk,bkhe->bqhe', scores_bf, keys_w) * query_scale
    grad_keys = batched('bhqk,bqhe->bkhe', scores_bf, queries)
    qv_grad = jnp.stack([lax.optimization_barrier(jnp.sum(grad_queries, (0, 1))), lax.optimization_barrier(jnp.sum(grad_values, (0, 1)))], 1).reshape(-1)
    grad_proj = jnp.stack([grad_queries, grad_keys, grad_values], 3).astype(jnp.bfloat16).reshape(-1, 3 * D)
    qkv_w_grad = matmul(windows.reshape(-1, D).T, grad_proj)
    grad_first = from_windows(matmul(grad_proj, qkv_w.T).reshape(count_win, WIN * WIN, D), offset, count_img)
    grad_norm_a, attn_gain_grad, attn_shift_grad = norm_back(grad_first, normed_a, inverse_a, attn_gain)
    grad_in = (grad_middle + grad_norm_a).astype(jnp.bfloat16)
    return (grad_in, (attn_gain_grad, attn_shift_grad, qkv_w_grad, qv_grad, table_grad, proj_w_grad, proj_b_grad, mlp_gain_grad, mlp_shift_grad, hidden_w_grad, hidden_b_grad, out_w_grad, out_b_grad))

def reference(images, cotangent, counts, rel_index, pre_attn_gain, pre_attn_bias, qkv_weight, qv_bias, bias_table, proj_weight, proj_bias, pre_mlp_gain, pre_mlp_bias, hidden_weight, hidden_bias, out_weight, out_bias):
    stacked = (pre_attn_gain, pre_attn_bias, qkv_weight, qv_bias, bias_table, proj_weight, proj_bias, pre_mlp_gain, pre_mlp_bias, hidden_weight, hidden_bias, out_weight, out_bias)
    onehot = (rel_index.reshape(-1)[:, None] == jnp.arange(RELS, dtype=jnp.int32)[None, :]).astype(jnp.float32)
    first_params = tuple((member[0] for member in stacked))
    second_params = tuple((member[1] for member in stacked))
    first_mask = bias_and_mask(first_params[4], onehot, 0.0)
    second_mask = bias_and_mask(second_params[4], onehot, 1.0)
    positions = jnp.arange(IMAGES, dtype=jnp.int32)
    alive_all = ((positions % CAP)[None, :] < counts[:, positions // CAP]).astype(jnp.float32)

    def one_batch(totals, inputs):
        batch_in, batch_cot, alive_row = inputs
        alive = alive_row[:, None, None]
        first_out, first_kept = layer_parts(first_params, batch_in, alive, 0, first_mask)
        second_out, second_kept = layer_parts(second_params, first_out, alive, SHIFT, second_mask)
        second_grad, second_terms = layer_back(second_params, second_kept, batch_cot, alive, SHIFT, onehot)
        first_grad, first_terms = layer_back(first_params, first_kept, second_grad, alive, 0, onehot)
        totals = tuple((total + jnp.stack([term_a, term_b]) for total, term_a, term_b in zip(totals, first_terms, second_terms)))
        return (totals, (first_out, second_out, first_grad, second_grad))
    zero_grads = tuple((jnp.zeros(member.shape, jnp.float32) for member in stacked))
    totals, outputs = lax.scan(one_batch, zero_grads, (images, cotangent, alive_all))
    block_out = jnp.stack([outputs[0], outputs[1]])
    input_grad = jnp.stack([outputs[2], outputs[3]])
    return (block_out, input_grad, totals[0], totals[1], totals[2], totals[3], totals[4], totals[5], totals[6], totals[7], totals[8], totals[9], totals[10], totals[11], totals[12])
```

```python
import functools
import math

import jax
import jax.numpy as jnp
from jax import lax
from jax.experimental import pallas as pl
from jax.experimental.pallas import tpu as pltpu
from jax.sharding import PartitionSpec as P

D = 512
H = 16
HD = 32
WIN = 7
GRID = 14
SHIFT = 3
TOK = 196
RELS = 169
POS = WIN * WIN
NW = 4
WP = 64
TP = 208
ROWS = NW * WP
GH = 4
GL = GH * HD
EPSILON = 1e-05
MASK_VALUE = -100.0
F32 = jnp.float32
BF = jnp.bfloat16


def dot_nn(a, b):
    return lax.dot_general(a, b, (((1,), (0,)), ((), ())), preferred_element_type=F32)


def dot_nt(a, b):
    return lax.dot_general(a, b, (((1,), (1,)), ((), ())), preferred_element_type=F32)


def dot_tn(a, b):
    return lax.dot_general(a, b, (((0,), (0,)), ((), ())), preferred_element_type=F32)


def normalize(rows):
    center = rows - jnp.mean(rows, -1, keepdims=True)
    inverse = lax.rsqrt(jnp.mean(center * center, -1, keepdims=True) + EPSILON)
    return center * inverse, inverse


def norm_back(grad_out, normed, inverse, gain):
    scaled = grad_out * gain
    return inverse * (
        scaled
        - jnp.mean(scaled, -1, keepdims=True)
        - normed * jnp.mean(scaled * normed, -1, keepdims=True)
    )


def block_diagonal(rows, head_mask):
    return jnp.concatenate([rows] * GH, axis=0) * head_mask


def pick_diagonal(full):
    head = lax.broadcasted_iota(jnp.int32, (WP, GL), 1) // HD
    out = full[0:WP]
    for h in range(1, GH):
        out = jnp.where(head == h, full[h * WP : (h + 1) * WP], out)
    return out


def attn_fwd_body(
    x_ref, gain_ref, shift_ref, spread_ref, gather_ref, head_mask_ref, wqkv_ref, qkv_scale_ref, qkv_shift_ref,
    bias_ref, wproj_ref, bproj_ref, fw_ref, qkv_ref, p_ref, ho_ref, mid_ref, how_ref,
):
    x = x_ref[0].astype(F32)
    normed, _ = normalize(x)
    first = (normed * gain_ref[...] + shift_ref[...]).astype(BF)
    fw = dot_nn(spread_ref[...], first).astype(BF)
    fw_ref[0] = fw
    for g in range(4):
        projected = dot_nn(fw, wqkv_ref[g])
        qkv_ref[0, g] = (projected * qkv_scale_ref[...] + qkv_shift_ref[g]).astype(BF)

    def window(w, carry):
        rows = pl.ds(pl.multiple_of(w * WP, WP), WP)
        for g in range(4):
            q = qkv_ref[0, g, rows, 0:GL]
            k = qkv_ref[0, g, rows, GL : 2 * GL]
            v = qkv_ref[0, g, rows, 2 * GL : 3 * GL]
            st = dot_nt(k, block_diagonal(q, head_mask_ref[...])) + bias_ref[w, g]
            e = jnp.exp(st - jnp.max(st, 0, keepdims=True))
            pt = (e * (1.0 / jnp.sum(e, 0, keepdims=True))).astype(BF)
            p_ref[0, w, g] = pt
            how_ref[rows, g * GL : (g + 1) * GL] = pick_diagonal(dot_tn(pt, v)).astype(BF)
        return carry

    lax.fori_loop(0, NW, window, 0)
    ho = dot_nn(gather_ref[...], how_ref[...]).astype(BF)
    ho_ref[0] = ho
    mid_ref[0] = x + (dot_nn(ho, wproj_ref[...]) + bproj_ref[...])


def whole(shape):
    return pl.BlockSpec(shape, lambda i: (0,) * len(shape))


def per(shape):
    return pl.BlockSpec((1,) + shape, lambda i: (i,) + (0,) * len(shape))


def attn_fwd(x, gain, shift, spread, gather, head_mask, wqkv, qkv_scale, qkv_shift, bias, wproj, bproj):
    n = x.shape[0]
    return pl.pallas_call(
        attn_fwd_body,
        grid=(n,),
        in_specs=[
            per((TP, D)), whole((1, D)), whole((1, D)), whole((ROWS, TP)), whole((TP, ROWS)), whole((GH * WP, GL)),
            whole((4, D, 3 * GL)), whole((1, 3 * GL)), whole((4, 1, 3 * GL)), whole((NW, 4, WP, GH * WP)),
            whole((D, D)), whole((1, D)),
        ],
        out_specs=[per((ROWS, D)), per((4, ROWS, 3 * GL)), per((NW, 4, WP, GH * WP)), per((TP, D)), per((TP, D))],
        out_shape=[
            jax.ShapeDtypeStruct((n, ROWS, D), BF),
            jax.ShapeDtypeStruct((n, 4, ROWS, 3 * GL), BF),
            jax.ShapeDtypeStruct((n, NW, 4, WP, GH * WP), BF),
            jax.ShapeDtypeStruct((n, TP, D), BF),
            jax.ShapeDtypeStruct((n, TP, D), F32),
        ],
        scratch_shapes=[pltpu.VMEM((ROWS, D), BF)],
        name="attn_fwd",
        compiler_params=pltpu.CompilerParams(vmem_limit_bytes=48 << 20),
        cost_estimate=pl.CostEstimate(flops=n * 2 * 256 * 512 * 2600, bytes_accessed=n * 2 << 20, transcendentals=0),
    )(x, gain, shift, spread, gather, head_mask, wqkv, qkv_scale, qkv_shift, bias, wproj, bproj)


def gelu_parts(v):
    cdf = 0.5 * (1.0 + lax.erf(v * 0.5**0.5))
    pdf = jnp.exp(-0.5 * v * v) * (2.0 * math.pi) ** (-0.5)
    return v * cdf, cdf + v * pdf


BLK = 416


def mlp_fwd_body(mid_ref, gain_ref, shift_ref, hw_ref, hb_ref, ow_ref, ob_ref, alive_ref, second_ref, act_ref, slope_ref, y_ref, acc_ref):
    c = pl.program_id(0)
    rows_total = mid_ref.shape[0]

    @pl.when(c == 0)
    def _():
        mid = mid_ref[...]
        normed, _ = normalize(mid)
        second_ref[...] = (normed * gain_ref[...] + shift_ref[...]).astype(BF)
        acc_ref[...] = mid + ob_ref[...]

    def block(b, carry):
        rows = pl.ds(pl.multiple_of(b * BLK, BLK), BLK)
        pre = dot_nn(second_ref[rows, :], hw_ref[0]) + hb_ref[0]
        act, slope = gelu_parts(pre)
        act = act.astype(BF)
        act_ref[0, rows, :] = act
        slope_ref[0, rows, :] = slope.astype(BF)
        acc_ref[rows, :] += dot_nn(act, ow_ref[0])
        return carry

    lax.fori_loop(0, rows_total // BLK, block, 0)

    @pl.when(c == pl.num_programs(0) - 1)
    def _():
        y_ref[...] = (acc_ref[...] * alive_ref[...]).astype(BF)


def mlp_fwd(mid, gain, shift, hw, hb, ow, ob, alive):
    r = mid.shape[0]
    nc, _, fc = hw.shape
    return pl.pallas_call(
        mlp_fwd_body,
        grid=(nc,),
        in_specs=[
            whole((r, D)), whole((1, D)), whole((1, D)), per((D, fc)), per((1, fc)), per((fc, D)), whole((1, D)), whole((r, 1)),
        ],
        out_specs=[whole((r, D)), per((r, fc)), per((r, fc)), whole((r, D))],
        out_shape=[
            jax.ShapeDtypeStruct((r, D), BF),
            jax.ShapeDtypeStruct((nc, r, fc), BF),
            jax.ShapeDtypeStruct((nc, r, fc), BF),
            jax.ShapeDtypeStruct((r, D), BF),
        ],
        scratch_shapes=[pltpu.VMEM((r, D), F32)],
        name="mlp_fwd",
        compiler_params=pltpu.CompilerParams(vmem_limit_bytes=48 << 20),
        cost_estimate=pl.CostEstimate(flops=4 * r * D * 2048, bytes_accessed=12 << 20, transcendentals=0),
    )(mid, gain, shift, hw, hb, ow, ob, alive)


def mlp_bwd_body(
    g_ref, alive_ref, act_ref, slope_ref, hw_ref, ow_ref, second_ref, mid_ref, gain_ref,
    ghw_ref, gow_ref, ghb_ref, gmid_ref, small_ref, gy_ref, gyt_ref, sect_ref, gp_ref, acc_ref,
):
    c = pl.program_id(0)
    rows_total = mid_ref.shape[0]

    @pl.when(c == 0)
    def _():
        gy = g_ref[...].astype(F32) * alive_ref[...]
        small_ref[0:1] = jnp.sum(gy, 0, keepdims=True)
        gy = gy.astype(BF)
        gy_ref[...] = gy
        gyt_ref[...] = gy.T
        sect_ref[...] = second_ref[...].T
        acc_ref[...] = jnp.zeros_like(acc_ref)

    ghb_ref[0] = jnp.zeros_like(ghb_ref[0])

    def block(b, carry):
        rows = pl.ds(pl.multiple_of(b * BLK, BLK), BLK)
        gp = dot_nt(gy_ref[rows, :], ow_ref[0]) * slope_ref[0, rows, :].astype(F32)
        ghb_ref[0] += jnp.sum(gp, 0, keepdims=True)
        gp = gp.astype(BF)
        gp_ref[rows, :] = gp
        acc_ref[rows, :] += dot_nt(gp, hw_ref[0])
        return carry

    lax.fori_loop(0, rows_total // BLK, block, 0)
    ghw_ref[0] = dot_nn(sect_ref[...], gp_ref[...]).astype(BF)
    gow_ref[0] = dot_nn(gyt_ref[...], act_ref[0]).astype(BF)

    @pl.when(c == pl.num_programs(0) - 1)
    def _():
        e = acc_ref[...]
        normed, inverse = normalize(mid_ref[...])
        small_ref[2:3] = jnp.sum(e * normed, 0, keepdims=True)
        small_ref[3:4] = jnp.sum(e, 0, keepdims=True)
        gmid = gy_ref[...].astype(F32) + norm_back(e, normed, inverse, gain_ref[...])
        small_ref[1:2] = jnp.sum(gmid, 0, keepdims=True)
        gmid_ref[...] = gmid


def mlp_bwd(g, alive, act, slope, hw, ow, second, mid, gain):
    r = mid.shape[0]
    nc, _, fc = hw.shape
    return pl.pallas_call(
        mlp_bwd_body,
        grid=(nc,),
        in_specs=[
            whole((r, D)), whole((r, 1)), per((r, fc)), per((r, fc)), per((D, fc)), per((fc, D)), whole((r, D)), whole((r, D)), whole((1, D)),
        ],
        out_specs=[per((D, fc)), per((D, fc)), per((1, fc)), whole((r, D)), whole((4, D))],
        out_shape=[
            jax.ShapeDtypeStruct((nc, D, fc), BF),
            jax.ShapeDtypeStruct((nc, D, fc), BF),
            jax.ShapeDtypeStruct((nc, 1, fc), F32),
            jax.ShapeDtypeStruct((r, D), F32),
            jax.ShapeDtypeStruct((4, D), F32),
        ],
        scratch_shapes=[
            pltpu.VMEM((r, D), BF), pltpu.VMEM((D, r), BF), pltpu.VMEM((D, r), BF), pltpu.VMEM((r, fc), BF), pltpu.VMEM((r, D), F32),
        ],
        name="mlp_bwd",
        compiler_params=pltpu.CompilerParams(vmem_limit_bytes=48 << 20),
        cost_estimate=pl.CostEstimate(flops=8 * r * D * 2048, bytes_accessed=16 << 20, transcendentals=0),
    )(g, alive, act, slope, hw, ow, second, mid, gain)


def attn_bwd_body(
    x_ref, gmid_ref, fw_ref, qkv_ref, p_ref, ho_ref, gain_ref, spread_ref, gather_ref, head_mask_ref, wqkv_ref, wproj_ref,
    gin_ref, gqkv_ref, gproj_ref, gqv_ref, gtab_ref, small_ref, gw_ref, dq_ref, fwt_ref, hot_ref, gmb_ref,
):
    i = pl.program_id(0)
    last = pl.num_programs(0) - 1

    @pl.when(i == 0)
    def _():
        gqv_ref[...] = jnp.zeros_like(gqv_ref)
        gtab_ref[...] = jnp.zeros_like(gtab_ref)
        small_ref[...] = jnp.zeros_like(small_ref)

    gmid = gmid_ref[0]
    gmb = gmid.astype(BF)
    gmb_ref[i] = gmb
    heads = dot_nt(gmb, wproj_ref[...]).astype(BF)
    gw_ref[...] = dot_nn(spread_ref[...], heads).astype(BF)
    base = pl.multiple_of(i * ROWS, ROWS)
    fwt_ref[:, pl.ds(base, ROWS)] = fw_ref[0].T
    scale = HD ** (-0.5)

    def window(w, carry):
        rows = pl.ds(pl.multiple_of(w * WP, WP), WP)
        out_rows = pl.ds(pl.multiple_of(base + w * WP, WP), WP)
        for g in range(4):
            q = qkv_ref[0, g, rows, 0:GL]
            k = qkv_ref[0, g, rows, GL : 2 * GL]
            v = qkv_ref[0, g, rows, 2 * GL : 3 * GL]
            pt = p_ref[0, w, g]
            head_mask = head_mask_ref[...]
            bd_grad = block_diagonal(gw_ref[rows, g * GL : (g + 1) * GL], head_mask)
            ptf = pt.astype(F32)
            t = dot_nt(v, bd_grad)
            pd = t * ptf
            ds = pd - ptf * jnp.sum(pd, 0, keepdims=True)
            gtab_ref[g] += ds
            dsb = ds.astype(BF)
            dv = dot_nn(pt, bd_grad)
            dk = dot_nn(dsb, block_diagonal(q, head_mask))
            dq = pick_diagonal(dot_tn(dsb, k)) * scale
            gqv_ref[g, 0:1] += jnp.sum(dq, 0, keepdims=True)
            gqv_ref[g, 1:2] += jnp.sum(dv, 0, keepdims=True)
            dq_ref[g, out_rows, 0:GL] = dq.astype(BF)
            dq_ref[g, out_rows, GL : 2 * GL] = dk.astype(BF)
            dq_ref[g, out_rows, 2 * GL : 3 * GL] = dv.astype(BF)
        return carry

    lax.fori_loop(0, NW, window, 0)
    image_rows = pl.ds(base, ROWS)
    e = dot_nt(dq_ref[0, image_rows, :], wqkv_ref[0])
    for g in range(1, 4):
        e += dot_nt(dq_ref[g, image_rows, :], wqkv_ref[g])
    e = dot_nn(gather_ref[...], e.astype(BF))
    normed, inverse = normalize(x_ref[0].astype(F32))
    small_ref[0:1] += jnp.sum(e * normed, 0, keepdims=True)
    small_ref[1:2] += jnp.sum(e, 0, keepdims=True)
    gin_ref[0] = (gmid + norm_back(e, normed, inverse, gain_ref[...])).astype(BF)

    hot_ref[i] = ho_ref[0].T

    @pl.when(i == last)
    def _():
        for g in range(4):
            gqkv_ref[g] = dot_nn(fwt_ref[...], dq_ref[g]).astype(BF)
        acc = dot_nn(hot_ref[0], gmb_ref[0])
        for b in range(1, hot_ref.shape[0]):
            acc += dot_nn(hot_ref[b], gmb_ref[b])
        gproj_ref[...] = acc.astype(BF)


def attn_bwd(x, gmid, fw, qkv, p, ho, gain, spread, gather, head_mask, wqkv, wproj):
    n = x.shape[0]
    return pl.pallas_call(
        attn_bwd_body,
        grid=(n,),
        in_specs=[
            per((TP, D)), per((TP, D)), per((ROWS, D)), per((4, ROWS, 3 * GL)), per((NW, 4, WP, GH * WP)), per((TP, D)),
            whole((1, D)), whole((ROWS, TP)), whole((TP, ROWS)), whole((GH * WP, GL)), whole((4, D, 3 * GL)), whole((D, D)),
        ],
        out_specs=[
            per((TP, D)), whole((4, D, 3 * GL)), whole((D, D)), whole((4, 2, GL)), whole((4, WP, GH * WP)), whole((2, D)),
        ],
        out_shape=[
            jax.ShapeDtypeStruct((n, TP, D), BF),
            jax.ShapeDtypeStruct((4, D, 3 * GL), BF),
            jax.ShapeDtypeStruct((D, D), BF),
            jax.ShapeDtypeStruct((4, 2, GL), F32),
            jax.ShapeDtypeStruct((4, WP, GH * WP), F32),
            jax.ShapeDtypeStruct((2, D), F32),
        ],
        scratch_shapes=[
            pltpu.VMEM((ROWS, D), BF), pltpu.VMEM((4, n * ROWS, 3 * GL), BF), pltpu.VMEM((D, n * ROWS), BF),
            pltpu.VMEM((n, D, TP), BF), pltpu.VMEM((n, TP, D), BF),
        ],
        name="attn_bwd",
        compiler_params=pltpu.CompilerParams(vmem_limit_bytes=48 << 20),
        cost_estimate=pl.CostEstimate(flops=n * 4 * 256 * 512 * 2600, bytes_accessed=n * 3 << 20, transcendentals=0),
    )(x, gmid, fw, qkv, p, ho, gain, spread, gather, head_mask, wqkv, wproj)


def window_maps(offset):
    token = jnp.arange(TP, dtype=jnp.int32)
    r = (token // GRID - offset) % GRID
    c = (token % GRID - offset) % GRID
    slot = ((r // WIN) * 2 + c // WIN) * WP + (r % WIN) * WIN + c % WIN
    slot = jnp.where(token < TOK, slot, -1)
    spread = (jnp.arange(ROWS, dtype=jnp.int32)[:, None] == slot[None, :]).astype(BF)
    return spread, spread.T


def region_differs():
    w = jnp.arange(NW, dtype=jnp.int32)
    a = jnp.arange(WP, dtype=jnp.int32)
    r = (w // 2)[:, None] * WIN + (a // WIN)[None, :]
    c = (w % 2)[:, None] * WIN + (a % WIN)[None, :]

    def band(t):
        return (t >= GRID - WIN).astype(jnp.int32) + (t >= GRID - SHIFT).astype(jnp.int32)

    label = band(r) * 3 + band(c)
    return (label[:, :, None] != label[:, None, :]).astype(F32)


def bias_tables(table, rel_index, masked):
    rel = jnp.pad(rel_index.T, ((0, WP - POS), (0, WP - POS)), constant_values=-1).reshape(-1)
    onehot = (jnp.arange(RELS, dtype=jnp.int32)[:, None] == rel[None, :]).astype(BF)
    flat = jnp.dot(table, onehot, preferred_element_type=F32)
    position = flat.reshape(4, GH, WP, WP).transpose(0, 2, 1, 3)
    key_pad = jnp.where(jnp.arange(WP) < POS, 0.0, -1e30).astype(F32)[:, None]
    extra = key_pad + (MASK_VALUE * region_differs() if masked else jnp.zeros((NW, WP, WP), F32))
    return (position[None] + extra[:, None, :, None, :]).reshape(NW, 4, WP, GH * WP)


def table_grad(gtab, rel_index):
    rel = jnp.pad(rel_index.T, ((0, WP - POS), (0, WP - POS)), constant_values=-1).reshape(-1)
    onehot = (rel[:, None] == jnp.arange(RELS, dtype=jnp.int32)[None, :]).astype(F32)
    flat = gtab.reshape(4, WP, GH, WP).transpose(0, 2, 1, 3).reshape(H, WP * WP)
    return jnp.dot(flat, onehot, precision=lax.Precision.HIGHEST)


def qkv_order(w):
    lead = w.shape[:-1]
    return jnp.swapaxes(w.reshape(*lead, GH, 3, HD), -3, -2).reshape(*lead, 3 * GL)


def head_masks():
    row = jnp.arange(GH * WP, dtype=jnp.int32) // WP
    lane = jnp.arange(GL, dtype=jnp.int32) // HD
    return (row[:, None] == lane[None, :]).astype(BF)


def rows_of(vector):
    return vector.astype(F32).reshape(1, -1)


SMALL = ("gain", "shift", "qv", "table", "bproj", "mgain", "mshift", "hb", "ob")


def pack_small(parts):
    return jnp.concatenate([part.reshape(-1) for part in parts])


def unpack_small(packed, shapes):
    out, at = [], 0
    for shape in shapes:
        size = math.prod(shape)
        piece = packed[:, at : at + size]
        out.append(piece.reshape((piece.shape[0] * shape[0],) + tuple(shape[1:])))
        at += size
    return out


def qkv_terms(qv):
    qv = qv.astype(F32).reshape(4, GH, 2, HD)
    shift = jnp.concatenate(
        [
            qv[:, :, 0].reshape(4, 1, GL) * HD ** (-0.5),
            jnp.zeros((4, 1, GL), F32),
            qv[:, :, 1].reshape(4, 1, GL),
        ],
        2,
    )
    scale = jnp.concatenate([jnp.full((1, GL), HD ** (-0.5), F32), jnp.ones((1, 2 * GL), F32)], 1)
    return scale, shift


def qkv_unorder(w):
    lead = w.shape[:-1]
    return jnp.swapaxes(w.reshape(*lead, 3, GH, HD), -3, -2).reshape(*lead, 3 * GL)


def layer_forward(x, weights, alive_rows, maps, head_mask):
    count = x.shape[0]
    spread, gather = maps
    fw, qkv, p, ho, mid = attn_fwd(
        x, weights["gain"], weights["shift"], spread, gather, head_mask, weights["wqkv"], weights["qkv_scale"],
        weights["qkv_shift"], weights["bias"], weights["wproj"], weights["bproj"],
    )
    mid = mid.reshape(count * TP, D)
    second, act, slope, y = mlp_fwd(
        mid, weights["mgain"], weights["mshift"], weights["hw"], weights["hb"], weights["ow"], weights["ob"], alive_rows
    )
    return y.reshape(count, TP, D), (x, fw, qkv, p, ho, mid, second, act, slope)


def layer_backward(cot, kept, weights, alive_rows, maps, head_mask):
    x, fw, qkv, p, ho, mid, second, act, slope = kept
    count = x.shape[0]
    ghw, gow, ghb, gmid, small_m = mlp_bwd(
        cot.reshape(count * TP, D), alive_rows, act, slope, weights["hw"], weights["ow"], second, mid, weights["mgain"]
    )
    gin, gqkv, gproj, gqv, gtab, small_a = attn_bwd(
        x, gmid.reshape(count, TP, D), fw, qkv, p, ho, weights["gain"], maps[0], maps[1], head_mask, weights["wqkv"], weights["wproj"]
    )
    return gin, (ghw, gow, gqkv, gproj), (ghb, small_m, gqv, gtab, small_a)


def local(
    images, cotangent, counts, rel_index, pre_attn_gain, pre_attn_bias, qkv_weight, qv_bias, bias_table, proj_weight, proj_bias,
    pre_mlp_gain, pre_mlp_bias, hidden_weight, hidden_bias, out_weight, out_bias,
):
    core = lax.axis_index("pipe")
    first_core = core == 0
    batches, slots = images.shape[:2]
    half = slots // 2

    def own_slots(array):
        mine = lax.dynamic_slice_in_dim(array, core * half, half, 1).reshape(batches * half, TOK, D)
        return jnp.pad(mine, ((0, 0), (0, TP - TOK), (0, 0)))

    x0 = own_slots(images)
    cot = own_slots(cotangent)
    slot_ids = lax.axis_index("tensor") * slots + core * half + jnp.arange(half, dtype=jnp.int32)
    alive = (slot_ids[None, :] < counts).astype(F32).reshape(-1)
    alive_rows = (alive[:, None] * (jnp.arange(TP) < TOK).astype(F32)[None, :]).reshape(-1, 1)

    small_in = (pre_attn_gain, pre_attn_bias, qv_bias, bias_table, proj_bias, pre_mlp_gain, pre_mlp_bias, hidden_bias, out_bias)
    shapes = [member.shape[1:] for member in small_in]
    packed = lax.all_gather(lax.all_gather(pack_small(small_in), "tensor"), "pipe")

    def both(member, axis):
        return lax.all_gather(lax.all_gather(member[0], "tensor", axis=axis, tiled=True), "pipe")

    wqkv2, wproj2, hw2, ow2 = both(qkv_weight, 1), both(proj_weight, 0), both(hidden_weight, 1), both(out_weight, 0)
    layers = []
    for l in range(2):
        small = dict(zip(SMALL, unpack_small(packed[l], shapes)))
        scale, shift = qkv_terms(small["qv"])
        layers.append(
            dict(
                gain=rows_of(small["gain"]), shift=rows_of(small["shift"]), bproj=rows_of(small["bproj"]),
                mgain=rows_of(small["mgain"]), mshift=rows_of(small["mshift"]), ob=rows_of(small["ob"]),
                hb=small["hb"].astype(F32).reshape(4, 1, -1), qkv_scale=scale, qkv_shift=shift,
                bias=bias_tables(small["table"], rel_index, l == 1),
                wqkv=qkv_order(wqkv2[l].reshape(D, 4, 3 * GL).transpose(1, 0, 2)), wproj=wproj2[l],
                hw=hw2[l].reshape(D, 4, -1).transpose(1, 0, 2), ow=ow2[l].reshape(4, -1, D),
            )
        )
    head_mask = head_masks()
    maps = [window_maps(l * SHIFT) for l in range(2)]
    y0, kept0 = layer_forward(x0, layers[0], alive_rows, maps[0], head_mask)
    y1, kept1 = layer_forward(y0, layers[1], alive_rows, maps[1], head_mask)
    g1, big1, little1 = layer_backward(cot, kept1, layers[1], alive_rows, maps[1], head_mask)
    g0, big0, little0 = layer_backward(g1, kept0, layers[0], alive_rows, maps[0], head_mask)

    def assemble(mine0, mine1):
        sent = lax.ppermute(jnp.where(first_core, mine1, mine0), "pipe", [(0, 1), (1, 0)])
        mine = jnp.where(first_core, mine0, mine1)
        mine, sent = (part[:, :TOK].reshape(batches, half, TOK, D) for part in (mine, sent))
        low, high = jnp.where(first_core, mine, sent), jnp.where(first_core, sent, mine)
        return jnp.concatenate([low, high], 1)[None]

    block_out = assemble(y0, y1)
    input_grad = assemble(g0, g1)

    def full(big):
        ghw, gow, gqkv, gproj = big
        return (
            qkv_unorder(gqkv).transpose(1, 0, 2).reshape(D, 3 * D), gproj,
            ghw.transpose(1, 0, 2).reshape(D, -1), gow.transpose(0, 2, 1).reshape(-1, D),
        )

    def reduced(pair, axis):
        mine = lax.psum_scatter(jnp.stack(pair), "pipe", scatter_dimension=0, tiled=False)
        mine = lax.psum_scatter(mine, "tensor", scatter_dimension=axis, tiled=True)
        return lax.psum(mine, "dp").astype(F32)[None]

    gqkv, gproj, ghw, gow = (reduced(pair, axis) for pair, axis in zip(zip(full(big0), full(big1)), (1, 0, 1, 0)))

    def little(terms):
        ghb, small_m, gqv, gtab, small_a = terms
        qv = jnp.swapaxes(gqv.reshape(4, 2, GH, HD), 1, 2).reshape(-1)
        return (
            small_a[0], small_a[1], qv, table_grad(gtab, rel_index), small_m[1], small_m[2], small_m[3], ghb.reshape(-1), small_m[0],
        )

    totals = lax.psum(jnp.stack([pack_small(little(little0)), pack_small(little(little1))]), ("pipe", "dp", "tensor"))
    mine = jnp.where(first_core, totals[0], totals[1])
    shards = lax.axis_size("tensor")
    outs, at = [], 0
    for shape in shapes:
        whole_shape = (shape[0] * shards,) + tuple(shape[1:])
        size = math.prod(whole_shape)
        piece = mine[at : at + size].reshape(whole_shape)
        outs.append(lax.dynamic_slice_in_dim(piece, lax.axis_index("tensor") * shape[0], shape[0], 0)[None])
        at += size
    gain_g, shift_g, qv_g, table_g, bproj_g, mgain_g, mshift_g, hb_g, ob_g = outs
    return (
        block_out, input_grad, gain_g, shift_g, gqkv, qv_g, table_g, gproj, bproj_g, mgain_g, mshift_g, ghw, hb_g, gow, ob_g,
    )


def solution(mesh):
    return jax.shard_map(
        local,
        mesh=mesh,
        in_specs=(
            P(None, ("dp", "tensor"), None, None),
            P(None, ("dp", "tensor"), None, None),
            P(None, "dp"),
            P(),
            P("pipe", "tensor"),
            P("pipe", "tensor"),
            P("pipe", None, "tensor"),
            P("pipe", "tensor"),
            P("pipe", "tensor", None),
            P("pipe", "tensor", None),
            P("pipe", "tensor"),
            P("pipe", "tensor"),
            P("pipe", "tensor"),
            P("pipe", None, "tensor"),
            P("pipe", "tensor"),
            P("pipe", "tensor", None),
            P("pipe", "tensor"),
        ),
        out_specs=(
            P("pipe", None, ("dp", "tensor"), None, None),
            P("pipe", None, ("dp", "tensor"), None, None),
            P("pipe", "tensor"),
            P("pipe", "tensor"),
            P("pipe", None, "tensor"),
            P("pipe", "tensor"),
            P("pipe", "tensor", None),
            P("pipe", "tensor", None),
            P("pipe", "tensor"),
            P("pipe", "tensor"),
            P("pipe", "tensor"),
            P("pipe", None, "tensor"),
            P("pipe", "tensor"),
            P("pipe", "tensor", None),
            P("pipe", "tensor"),
        ),
        check_vma=False,
    )
```

```python
import functools
import math

import jax
import jax.numpy as jnp
from jax import lax
from jax.experimental import pallas as pl
from jax.experimental.pallas import tpu as pltpu
from jax.sharding import PartitionSpec as P

D = 512
H = 16
HD = 32
WIN = 7
GRID = 14
SHIFT = 3
TOK = 196
RELS = 169
POS = WIN * WIN
NW = 4
WP = 64
TP = 208
ROWS = NW * WP
GH = 4
GL = GH * HD
EPSILON = 1e-05
MASK_VALUE = -100.0
F32 = jnp.float32
BF = jnp.bfloat16


def dot_nn(a, b):
    return lax.dot_general(a, b, (((1,), (0,)), ((), ())), preferred_element_type=F32)


def dot_nt(a, b):
    return lax.dot_general(a, b, (((1,), (1,)), ((), ())), preferred_element_type=F32)


def dot_tn(a, b):
    return lax.dot_general(a, b, (((0,), (0,)), ((), ())), preferred_element_type=F32)


def normalize(rows):
    center = rows - jnp.mean(rows, -1, keepdims=True)
    inverse = lax.rsqrt(jnp.mean(center * center, -1, keepdims=True) + EPSILON)
    return center * inverse, inverse


def norm_back(grad_out, normed, inverse, gain):
    scaled = grad_out * gain
    return inverse * (
        scaled
        - jnp.mean(scaled, -1, keepdims=True)
        - normed * jnp.mean(scaled * normed, -1, keepdims=True)
    )


def block_diagonal(rows, head_mask):
    return jnp.concatenate([rows] * GH, axis=0) * head_mask


def pick_diagonal(full):
    head = lax.broadcasted_iota(jnp.int32, (WP, GL), 1) // HD
    out = full[0:WP]
    for h in range(1, GH):
        out = jnp.where(head == h, full[h * WP : (h + 1) * WP], out)
    return out


ANY = pl.BlockSpec(memory_space=pl.ANY)
CHUNK = 64


def remote(source, target, sems, axis, index):
    return pltpu.make_async_remote_copy(
        src_ref=source, dst_ref=target, send_sem=sems[0], recv_sem=sems[1], device_id={axis: index},
        device_id_type=pl.DeviceIdType.MESH,
    )


def place_in_mesh():
    return lax.axis_index("pipe"), lax.axis_index("dp"), lax.axis_index("tensor")


def greet():
    core, dp, shard = place_in_mesh()
    barrier = pltpu.get_barrier_semaphore()

    def signal(axis, index):
        pl.semaphore_signal(barrier, inc=1, device_id={axis: index}, device_id_type=pl.DeviceIdType.MESH)

    signal("pipe", 1 - core)
    for k in (1, 2, 3):
        signal("dp", dp ^ k)
        signal("tensor", lax.rem(shard + k, 4))
    pl.semaphore_wait(barrier, 7)


def quarter(half, j):
    core, dp, _ = place_in_mesh()
    return pl.ds(pl.multiple_of((core ^ half) * 256 + (dp ^ j) * CHUNK, CHUNK), CHUNK)


class Part:
    def __init__(self, inputs=(), outputs=(), scratch=()):
        self.inputs, self.outputs, self.scratch = list(inputs), list(outputs), list(scratch)

    def bind(self, ins, outs, scratch):
        self.ins, self.outs, self.kept = ins, outs, scratch


def sems(*shape):
    return [pltpu.SemaphoreType.DMA(shape), pltpu.SemaphoreType.DMA(shape)]


class Weights(Part):
    def __init__(self, count, layer, whole=None, own=None, other=None, pieces=None):
        self.count, self.layer, self.whole = count, layer, whole
        inputs = [whole] if whole is not None else [*own, *other, *pieces]
        copies = 1 if whole is not None else 9
        super().__init__(inputs, (), [pltpu.VMEM((count, 4, D, D), BF), pltpu.SemaphoreType.DMA((copies * count,))])

    def shard(self, mine, b):
        store, sem = self.kept
        owns, others = self.ins[: self.count], self.ins[self.count : 2 * self.count]
        return pltpu.make_async_copy((owns if mine else others)[b], store.at[b, 0], sem.at[b * 9])

    def piece(self, b, half, j):
        store, sem = self.kept
        source = self.ins[2 * self.count + half * 4 + j].at[:, b]
        target = store.at[b, pl.ds(1, 3), quarter(half, j), :]
        return pltpu.make_async_copy(source, target, sem.at[b * 9 + half * 4 + j + 1])

    def load(self):
        store, sem = self.kept
        count = self.count
        if self.whole is not None:
            copies = [pltpu.make_async_copy(self.ins[0].at[b], store.at[b], sem.at[b]) for b in range(count)]
            for copy in copies:
                copy.start()
            for copy in copies:
                copy.wait()
            return
        core = lax.axis_index("pipe")

        @pl.when(core == self.layer)
        def _():
            for b in range(count):
                self.shard(True, b).start()

        @pl.when(core != self.layer)
        def _():
            for b in range(count):
                self.shard(False, b).start()

        copies = [self.piece(b, half, j) for b in range(count) for half in range(2) for j in range(4)]
        for copy in copies:
            copy.start()
        for b in range(count):
            self.shard(True, b).wait()
        for copy in copies:
            copy.wait()


class Near(Part):
    def __init__(self, count, layer, own, other):
        self.count, self.layer = count, layer
        super().__init__([*own, *other], [jax.ShapeDtypeStruct((3, count, CHUNK, D), BF)], sems(3, count))

    def copy(self, mine, k, b):
        _, _, shard = place_in_mesh()
        source = self.ins[b if mine else self.count + b]
        return remote(
            source.at[quarter(0, 0), :], self.outs[0].at[k - 1, b], [sem.at[k - 1, b] for sem in self.kept], "tensor",
            lax.rem(shard + 4 - k, 4),
        )

    def each(self, mine):
        return [self.copy(mine, k, b) for b in range(self.count) for k in (1, 2, 3)]

    def start(self):
        core = lax.axis_index("pipe")

        @pl.when(core == self.layer)
        def _():
            for copy in self.each(True):
                copy.start()

        @pl.when(core != self.layer)
        def _():
            for copy in self.each(False):
                copy.start()

    def middle(self):
        pass

    def end(self):
        for copy in self.each(True):
            copy.wait()


class Far(Part):
    def __init__(self, count, near):
        shape = jax.ShapeDtypeStruct((3, count, CHUNK, D), BF)
        super().__init__([near], [shape] * 7, sems(3) + sems(4))

    def across(self, j):
        _, dp, _ = place_in_mesh()
        return remote(self.ins[0], self.outs[j - 1], [sem.at[j - 1] for sem in self.kept[:2]], "dp", dp ^ j)

    def over(self, j):
        core, _, _ = place_in_mesh()
        source = self.ins[0] if j == 0 else self.outs[j - 1]
        return remote(source, self.outs[3 + j], [sem.at[j] for sem in self.kept[2:]], "pipe", 1 - core)

    def start(self):
        for j in (1, 2, 3):
            self.across(j).start()
        self.over(0).start()

    def middle(self):
        pass

    def end(self):
        for j in (1, 2, 3):
            self.across(j).wait()
            self.over(j).start()
        for j in range(4):
            self.over(j).wait()

    def pieces(self, near, outs):
        return [near, *outs[:3], *outs[3:]]


def carried_call(body, parts, collective_id, *, grid, in_specs, inputs, out_specs, out_shape, scratch_shapes, name, cost, scalars=()):
    n_in, n_out, n_scratch, n_scalar = len(inputs), len(out_shape), len(scratch_shapes), len(scalars)

    def whole_body(*refs):
        refs = list(refs)
        own = [refs.pop(0) for _ in range(n_scalar)]

        def take(count, groups):
            mine = [refs.pop(0) for _ in range(count)]
            return mine, [[refs.pop(0) for _ in range(n)] for n in groups]

        mine, part_ins = take(n_in, [len(part.inputs) for part in parts])
        outs, part_outs = take(n_out, [len(part.outputs) for part in parts])
        kept, part_kept = take(n_scratch, [len(part.scratch) for part in parts])
        for part, a, b, c in zip(parts, part_ins, part_outs, part_kept):
            part.bind(a, b, c)
        body(*own, *mine, *outs, *kept)

    extra_in = [x for part in parts for x in part.inputs]
    extra_out = [x for part in parts for x in part.outputs]
    extra_scratch = [x for part in parts for x in part.scratch]
    params = dict(vmem_limit_bytes=60 << 20)
    if collective_id is not None:
        params.update(collective_id=collective_id, has_side_effects=True)
    results = pl.pallas_call(
        whole_body,
        grid_spec=pltpu.PrefetchScalarGridSpec(
            num_scalar_prefetch=n_scalar,
            grid=grid,
            in_specs=list(in_specs) + [ANY] * len(extra_in),
            out_specs=list(out_specs) + [ANY] * len(extra_out),
            scratch_shapes=list(scratch_shapes) + extra_scratch,
        ),
        out_shape=list(out_shape) + extra_out,
        name=name,
        compiler_params=pltpu.CompilerParams(**params),
        cost_estimate=cost,
    )(*scalars, *inputs, *extra_in)
    own, rest = results[:n_out], results[n_out:]
    given = []
    for part in parts:
        given.append(rest[: len(part.outputs)])
        rest = rest[len(part.outputs) :]
    return own, given


def at_step(step, tasks, method):
    tasks = [task for task in tasks if task is not None]
    if tasks:

        @pl.when(pl.program_id(0) == step)
        def _():
            if method == "start":
                greet()
            for task in tasks:
                getattr(task, method)()


def attn_fwd_body(
    weights, tasks, x_ref, gain_ref, shift_ref, spread_ref, gather_ref, head_mask_ref, qkv_scale_ref, qkv_shift_ref,
    bias_ref, bproj_ref, fw_ref, qkv_ref, p_ref, ho_ref, mid_ref, how_ref, wpt_ref,
):
    at_step(0, tasks, "start")
    wa_ref = weights.kept[0].at[0]

    @pl.when(pl.program_id(0) == 0)
    def _():
        weights.load()
        for g in range(4):
            wpt_ref[:, g * GL : (g + 1) * GL] = wa_ref[g, :, 3 * GL :]

    x = x_ref[0].astype(F32)
    normed, _ = normalize(x)
    first = (normed * gain_ref[...] + shift_ref[...]).astype(BF)
    fw = dot_nn(spread_ref[...], first).astype(BF)
    fw_ref[0] = fw
    for g in range(4):
        projected = dot_nn(fw, wa_ref[g, :, : 3 * GL])
        qkv_ref[0, g] = (projected * qkv_scale_ref[...] + qkv_shift_ref[g]).astype(BF)

    def window(w, carry):
        rows = pl.ds(pl.multiple_of(w * WP, WP), WP)
        for g in range(4):
            q = qkv_ref[0, g, rows, 0:GL]
            k = qkv_ref[0, g, rows, GL : 2 * GL]
            v = qkv_ref[0, g, rows, 2 * GL : 3 * GL]
            st = dot_nt(k, block_diagonal(q, head_mask_ref[...])) + bias_ref[w, g]
            e = jnp.exp(st - jnp.max(st, 0, keepdims=True))
            pt = (e * (1.0 / jnp.sum(e, 0, keepdims=True))).astype(BF)
            p_ref[0, w, g] = pt
            how_ref[rows, g * GL : (g + 1) * GL] = pick_diagonal(dot_tn(pt, v)).astype(BF)
        return carry

    lax.fori_loop(0, NW, window, 0)
    ho = dot_nn(gather_ref[...], how_ref[...]).astype(BF)
    ho_ref[0] = ho
    mid_ref[0] = x + (dot_nt(ho, wpt_ref[...]) + bproj_ref[...])
    at_step(pl.num_programs(0) - 1, tasks, "end")


def whole(shape):
    return pl.BlockSpec(shape, lambda i, *_: (0,) * len(shape))


def per(shape):
    return pl.BlockSpec((1,) + shape, lambda i, *_: (i,) + (0,) * len(shape))


def matrix(which):
    return pl.BlockSpec((1, 1, D, D), lambda i, *_: (which, i, 0, 0))


def attn_fwd(x, gain, shift, spread, gather, head_mask, qkv_scale, qkv_shift, bias, bproj, weights, tasks=(), collective_id=None):
    n = x.shape[0]
    return carried_call(
        functools.partial(attn_fwd_body, weights, tasks),
        [weights, *tasks],
        collective_id,
        grid=(n,),
        in_specs=[
            per((TP, D)), whole((1, D)), whole((1, D)), whole((ROWS, TP)), whole((TP, ROWS)), whole((GH * WP, GL)),
            whole((1, 3 * GL)), whole((4, 1, 3 * GL)), whole((NW, 4, WP, GH * WP)), whole((1, D)),
        ],
        inputs=(x, gain, shift, spread, gather, head_mask, qkv_scale, qkv_shift, bias, bproj),
        out_specs=[per((ROWS, D)), per((4, ROWS, 3 * GL)), per((NW, 4, WP, GH * WP)), per((TP, D)), per((TP, D))],
        out_shape=[
            jax.ShapeDtypeStruct((n, ROWS, D), BF),
            jax.ShapeDtypeStruct((n, 4, ROWS, 3 * GL), BF),
            jax.ShapeDtypeStruct((n, NW, 4, WP, GH * WP), BF),
            jax.ShapeDtypeStruct((n, TP, D), BF),
            jax.ShapeDtypeStruct((n, TP, D), F32),
        ],
        scratch_shapes=[pltpu.VMEM((ROWS, D), BF), pltpu.VMEM((D, D), BF)],
        name="attn_fwd",
        cost=pl.CostEstimate(flops=n * 2 * 256 * 512 * 2600, bytes_accessed=n * 2 << 20, transcendentals=0),
    )


def gelu_parts(v):
    cdf = 0.5 * (1.0 + lax.erf(v * 0.5**0.5))
    pdf = jnp.exp(-0.5 * v * v) * (2.0 * math.pi) ** (-0.5)
    return v * cdf, cdf + v * pdf


BLK = 416


def mlp_fwd_body(
    weights, tasks, mid_ref, gain_ref, shift_ref, hb_ref, ob_ref, alive_ref, second_ref, act_ref, slope_ref, y_ref, acc_ref
):
    c = pl.program_id(0)
    at_step(0, tasks, "start")
    pl.when(c == 0)(weights.load)
    wm_ref = weights.kept[0]
    rows_total = mid_ref.shape[0]

    @pl.when(c == 0)
    def _():
        mid = mid_ref[...]
        normed, _ = normalize(mid)
        second_ref[...] = (normed * gain_ref[...] + shift_ref[...]).astype(BF)
        acc_ref[...] = mid + ob_ref[...]

    def block(b, carry):
        rows = pl.ds(pl.multiple_of(b * BLK, BLK), BLK)
        pre = dot_nn(second_ref[rows, :], wm_ref[0, c]) + hb_ref[0]
        act, slope = gelu_parts(pre)
        act = act.astype(BF)
        act_ref[0, rows, :] = act
        slope_ref[0, rows, :] = slope.astype(BF)
        acc_ref[rows, :] += dot_nn(act, wm_ref[1, c])
        return carry

    lax.fori_loop(0, rows_total // BLK, block, 0)

    @pl.when(c == pl.num_programs(0) - 1)
    def _():
        y_ref[...] = (acc_ref[...] * alive_ref[...]).astype(BF)

    at_step(pl.num_programs(0) - 1, tasks, "end")


def mlp_fwd(mid, gain, shift, hb, ob, alive, weights, tasks=(), collective_id=None):
    r = mid.shape[0]
    nc, fc = 4, D
    return carried_call(
        functools.partial(mlp_fwd_body, weights, tasks),
        [weights, *tasks],
        collective_id,
        grid=(nc,),
        in_specs=[whole((r, D)), whole((1, D)), whole((1, D)), per((1, fc)), whole((1, D)), whole((r, 1))],
        inputs=(mid, gain, shift, hb, ob, alive),
        out_specs=[whole((r, D)), per((r, fc)), per((r, fc)), whole((r, D))],
        out_shape=[
            jax.ShapeDtypeStruct((r, D), BF),
            jax.ShapeDtypeStruct((nc, r, fc), BF),
            jax.ShapeDtypeStruct((nc, r, fc), BF),
            jax.ShapeDtypeStruct((r, D), BF),
        ],
        scratch_shapes=[pltpu.VMEM((r, D), F32)],
        name="mlp_fwd",
        cost=pl.CostEstimate(flops=4 * r * D * 2048, bytes_accessed=12 << 20, transcendentals=0),
    )


def scatter_rows(place_ref, value_ref, mine_ref, theirs_ref, index):
    for half, out_ref in enumerate((mine_ref, theirs_ref)):
        for j in range(4):
            start = (place_ref[0] ^ half) * 256 + (place_ref[1] ^ j) * 64
            out_ref[j, index] = value_ref[pl.ds(pl.multiple_of(start, 64), 64), :]


def mlp_bwd_body(
    weights, tasks, place_ref, g_ref, alive_ref, act_ref, slope_ref, second_ref, mid_ref, gain_ref,
    ghw_ref, ghw_away_ref, gow_ref, gow_away_ref, ghb_ref, gmid_ref, small_ref,
    gy_ref, gyt_ref, sect_ref, gp_ref, acc_ref, value_ref,
):
    c = pl.program_id(0)
    at_step(0, tasks, "start")
    pl.when(c == 0)(weights.load)
    wm_ref = weights.kept[0]
    rows_total = mid_ref.shape[0]

    @pl.when(c == 0)
    def _():
        gy = g_ref[...].astype(F32) * alive_ref[...]
        small_ref[0:1] = jnp.sum(gy, 0, keepdims=True)
        gy = gy.astype(BF)
        gy_ref[...] = gy
        gyt_ref[...] = gy.T
        sect_ref[...] = second_ref[...].T
        acc_ref[...] = jnp.zeros_like(acc_ref)

    ghb_ref[0] = jnp.zeros_like(ghb_ref[0])

    def block(b, carry):
        rows = pl.ds(pl.multiple_of(b * BLK, BLK), BLK)
        gp = dot_nt(gy_ref[rows, :], wm_ref[1, c]) * slope_ref[0, rows, :].astype(F32)
        ghb_ref[0] += jnp.sum(gp, 0, keepdims=True)
        gp = gp.astype(BF)
        gp_ref[rows, :] = gp
        acc_ref[rows, :] += dot_nt(gp, wm_ref[0, c])
        return carry

    lax.fori_loop(0, rows_total // BLK, block, 0)
    value_ref[0] = dot_nn(sect_ref[...], gp_ref[...]).astype(BF)
    value_ref[1] = dot_nn(gyt_ref[...], act_ref[0]).astype(BF)
    scatter_rows(place_ref, value_ref.at[0], ghw_ref, ghw_away_ref, 0)
    scatter_rows(place_ref, value_ref.at[1], gow_ref, gow_away_ref, 0)
    at_step(1, tasks, "middle")

    @pl.when(c == pl.num_programs(0) - 1)
    def _():
        e = acc_ref[...]
        normed, inverse = normalize(mid_ref[...])
        small_ref[2:3] = jnp.sum(e * normed, 0, keepdims=True)
        small_ref[3:4] = jnp.sum(e, 0, keepdims=True)
        gmid = gy_ref[...].astype(F32) + norm_back(e, normed, inverse, gain_ref[...])
        small_ref[1:2] = jnp.sum(gmid, 0, keepdims=True)
        gmid_ref[...] = gmid

    at_step(pl.num_programs(0) - 1, tasks, "end")


PIECES = jax.ShapeDtypeStruct((4, 4, 64, D), BF)


def mlp_bwd(place, g, alive, act, slope, second, mid, gain, weights, tasks=(), collective_id=None):
    r = mid.shape[0]
    nc, fc = 4, D
    pieces = pl.BlockSpec((4, 1, 64, D), lambda i, *_: (0, i, 0, 0))
    return carried_call(
        functools.partial(mlp_bwd_body, weights, tasks),
        [weights, *tasks],
        collective_id,
        grid=(nc,),
        in_specs=[
            pl.BlockSpec(memory_space=pltpu.SMEM),
            whole((r, D)), whole((r, 1)), per((r, fc)), per((r, fc)), whole((r, D)), whole((r, D)), whole((1, D)),
        ],
        inputs=(place, g, alive, act, slope, second, mid, gain),
        out_specs=[pieces, pieces, pieces, pieces, per((1, fc)), whole((r, D)), whole((4, D))],
        out_shape=[
            PIECES, PIECES, PIECES, PIECES,
            jax.ShapeDtypeStruct((nc, 1, fc), F32),
            jax.ShapeDtypeStruct((r, D), F32),
            jax.ShapeDtypeStruct((4, D), F32),
        ],
        scratch_shapes=[
            pltpu.VMEM((r, D), BF), pltpu.VMEM((D, r), BF), pltpu.VMEM((D, r), BF), pltpu.VMEM((r, fc), BF),
            pltpu.VMEM((r, D), F32), pltpu.VMEM((2, D, D), BF),
        ],
        name="mlp_bwd",
        cost=pl.CostEstimate(flops=8 * r * D * 2048, bytes_accessed=16 << 20, transcendentals=0),
    )


def attn_bwd_body(
    weights, tasks, place_ref, x_ref, gmid_ref, fw_ref, qkv_ref, p_ref, ho_ref, gain_ref, spread_ref, gather_ref, head_mask_ref,
    gin_ref, ga_ref, ga_away_ref, gqv_ref, gtab_ref, small_ref,
    gw_ref, dq_ref, fwt_ref, hos_ref, gmt_ref, wpt_ref, value_ref,
):
    i = pl.program_id(0)
    last = pl.num_programs(0) - 1
    at_step(0, tasks, "start")
    wa_ref = weights.kept[0].at[0]

    @pl.when(i == 0)
    def _():
        weights.load()
        gqv_ref[...] = jnp.zeros_like(gqv_ref)
        gtab_ref[...] = jnp.zeros_like(gtab_ref)
        small_ref[...] = jnp.zeros_like(small_ref)
        for g in range(4):
            wpt_ref[:, g * GL : (g + 1) * GL] = wa_ref[g, :, 3 * GL :]

    gmid = gmid_ref[0]
    gmb = gmid.astype(BF)
    gmt_ref[i] = gmb.T
    hos_ref[i] = ho_ref[0]
    heads = dot_nn(gmb, wpt_ref[...]).astype(BF)
    gw_ref[...] = dot_nn(spread_ref[...], heads).astype(BF)
    base = pl.multiple_of(i * ROWS, ROWS)
    fwt_ref[:, pl.ds(base, ROWS)] = fw_ref[0].T
    scale = HD ** (-0.5)

    def window(w, carry):
        rows = pl.ds(pl.multiple_of(w * WP, WP), WP)
        out_rows = pl.ds(pl.multiple_of(base + w * WP, WP), WP)
        for g in range(4):
            q = qkv_ref[0, g, rows, 0:GL]
            k = qkv_ref[0, g, rows, GL : 2 * GL]
            v = qkv_ref[0, g, rows, 2 * GL : 3 * GL]
            pt = p_ref[0, w, g]
            head_mask = head_mask_ref[...]
            bd_grad = block_diagonal(gw_ref[rows, g * GL : (g + 1) * GL], head_mask)
            ptf = pt.astype(F32)
            t = dot_nt(v, bd_grad)
            pd = t * ptf
            ds = pd - ptf * jnp.sum(pd, 0, keepdims=True)
            gtab_ref[g] += ds
            dsb = ds.astype(BF)
            dv = dot_nn(pt, bd_grad)
            dk = dot_nn(dsb, block_diagonal(q, head_mask))
            dq = pick_diagonal(dot_tn(dsb, k)) * scale
            gqv_ref[g, 0:1] += jnp.sum(dq, 0, keepdims=True)
            gqv_ref[g, 1:2] += jnp.sum(dv, 0, keepdims=True)
            dq_ref[g, out_rows, 0:GL] = dq.astype(BF)
            dq_ref[g, out_rows, GL : 2 * GL] = dk.astype(BF)
            dq_ref[g, out_rows, 2 * GL : 3 * GL] = dv.astype(BF)
        return carry

    lax.fori_loop(0, NW, window, 0)
    image_rows = pl.ds(base, ROWS)
    e = dot_nt(dq_ref[0, image_rows, :], wa_ref[0, :, : 3 * GL])
    for g in range(1, 4):
        e += dot_nt(dq_ref[g, image_rows, :], wa_ref[g, :, : 3 * GL])
    e = dot_nn(gather_ref[...], e.astype(BF))
    normed, inverse = normalize(x_ref[0].astype(F32))
    small_ref[0:1] += jnp.sum(e * normed, 0, keepdims=True)
    small_ref[1:2] += jnp.sum(e, 0, keepdims=True)
    gin_ref[0] = (gmid + norm_back(e, normed, inverse, gain_ref[...])).astype(BF)

    @pl.when(i == last)
    def _():
        for g in range(4):
            value_ref[:, : 3 * GL] = dot_nn(fwt_ref[...], dq_ref[g]).astype(BF)
            acc = dot_nn(gmt_ref[0], hos_ref[0, :, g * GL : (g + 1) * GL])
            for b in range(1, hos_ref.shape[0]):
                acc += dot_nn(gmt_ref[b], hos_ref[b, :, g * GL : (g + 1) * GL])
            value_ref[:, 3 * GL :] = acc.astype(BF)
            scatter_rows(place_ref, value_ref, ga_ref, ga_away_ref, g)

    at_step(1, tasks, "middle")
    at_step(last, tasks, "end")


def attn_bwd(place, x, gmid, fw, qkv, p, ho, gain, spread, gather, head_mask, weights, tasks=(), collective_id=None):
    n = x.shape[0]
    return carried_call(
        functools.partial(attn_bwd_body, weights, tasks),
        [weights, *tasks],
        collective_id,
        grid=(n,),
        in_specs=[
            pl.BlockSpec(memory_space=pltpu.SMEM),
            per((TP, D)), per((TP, D)), per((ROWS, D)), per((4, ROWS, 3 * GL)), per((NW, 4, WP, GH * WP)), per((TP, D)),
            whole((1, D)), whole((ROWS, TP)), whole((TP, ROWS)), whole((GH * WP, GL)),
        ],
        inputs=(place, x, gmid, fw, qkv, p, ho, gain, spread, gather, head_mask),
        out_specs=[
            per((TP, D)), whole((4, 4, 64, D)), whole((4, 4, 64, D)), whole((4, 2, GL)), whole((4, WP, GH * WP)), whole((2, D)),
        ],
        out_shape=[
            jax.ShapeDtypeStruct((n, TP, D), BF),
            PIECES, PIECES,
            jax.ShapeDtypeStruct((4, 2, GL), F32),
            jax.ShapeDtypeStruct((4, WP, GH * WP), F32),
            jax.ShapeDtypeStruct((2, D), F32),
        ],
        scratch_shapes=[
            pltpu.VMEM((ROWS, D), BF), pltpu.VMEM((4, n * ROWS, 3 * GL), BF), pltpu.VMEM((D, n * ROWS), BF),
            pltpu.VMEM((n, TP, D), BF), pltpu.VMEM((n, D, TP), BF), pltpu.VMEM((D, D), BF), pltpu.VMEM((D, D), BF),
        ],
        name="attn_bwd",
        cost=pl.CostEstimate(flops=n * 4 * 256 * 512 * 2600, bytes_accessed=n * 3 << 20, transcendentals=0),
    )


def window_maps(offset):
    token = jnp.arange(TP, dtype=jnp.int32)
    r = (token // GRID - offset) % GRID
    c = (token % GRID - offset) % GRID
    slot = ((r // WIN) * 2 + c // WIN) * WP + (r % WIN) * WIN + c % WIN
    slot = jnp.where(token < TOK, slot, -1)
    spread = (jnp.arange(ROWS, dtype=jnp.int32)[:, None] == slot[None, :]).astype(BF)
    return spread, spread.T


def region_differs():
    w = jnp.arange(NW, dtype=jnp.int32)
    a = jnp.arange(WP, dtype=jnp.int32)
    r = (w // 2)[:, None] * WIN + (a // WIN)[None, :]
    c = (w % 2)[:, None] * WIN + (a % WIN)[None, :]

    def band(t):
        return (t >= GRID - WIN).astype(jnp.int32) + (t >= GRID - SHIFT).astype(jnp.int32)

    label = band(r) * 3 + band(c)
    return (label[:, :, None] != label[:, None, :]).astype(F32)


def bias_tables(table, rel_index, masked):
    rel = jnp.pad(rel_index.T, ((0, WP - POS), (0, WP - POS)), constant_values=-1).reshape(-1)
    onehot = (jnp.arange(RELS, dtype=jnp.int32)[:, None] == rel[None, :]).astype(BF)
    flat = jnp.dot(table, onehot, preferred_element_type=F32)
    position = flat.reshape(4, GH, WP, WP).transpose(0, 2, 1, 3)
    key_pad = jnp.where(jnp.arange(WP) < POS, 0.0, -1e30).astype(F32)[:, None]
    extra = key_pad + (MASK_VALUE * region_differs() if masked else jnp.zeros((NW, WP, WP), F32))
    return (position[None] + extra[:, None, :, None, :]).reshape(NW, 4, WP, GH * WP)


def table_grad(gtab, rel_index):
    rel = jnp.pad(rel_index.T, ((0, WP - POS), (0, WP - POS)), constant_values=-1).reshape(-1)
    onehot = (rel[:, None] == jnp.arange(RELS, dtype=jnp.int32)[None, :]).astype(F32)
    flat = gtab.reshape(4, WP, GH, WP).transpose(0, 2, 1, 3).reshape(H, WP * WP)
    return jnp.dot(flat, onehot, precision=lax.Precision.HIGHEST)


def qkv_order(w):
    lead = w.shape[:-1]
    return jnp.swapaxes(w.reshape(*lead, GH, 3, HD), -3, -2).reshape(*lead, 3 * GL)


def head_masks():
    row = jnp.arange(GH * WP, dtype=jnp.int32) // WP
    lane = jnp.arange(GL, dtype=jnp.int32) // HD
    return (row[:, None] == lane[None, :]).astype(BF)


def vmem():
    return pl.BlockSpec(memory_space=pltpu.VMEM)


def plain_call(body, out_shape, name, inputs, scalars=(), bytes_accessed=4 << 20):
    return pl.pallas_call(
        body,
        out_shape=out_shape,
        in_specs=[pl.BlockSpec(memory_space=pltpu.SMEM)] * len(scalars) + [vmem()] * len(inputs),
        out_specs=jax.tree.map(lambda _: vmem(), out_shape),
        name=name,
        compiler_params=pltpu.CompilerParams(vmem_limit_bytes=48 << 20),
        cost_estimate=pl.CostEstimate(flops=bytes_accessed, bytes_accessed=bytes_accessed, transcendentals=0),
    )(*scalars, *inputs)


def column_order(inverse):
    rows = lax.broadcasted_iota(jnp.int32, (3 * GL, 3 * GL), 1 if inverse else 0)
    cols = lax.broadcasted_iota(jnp.int32, (3 * GL, 3 * GL), 0 if inverse else 1)
    which, head, feature = cols // GL, (cols % GL) // HD, cols % HD
    return (rows == head * (3 * HD) + which * HD + feature).astype(BF)


def pack_attention(wqkv, wproj):
    def body(wqkv_ref, wproj_ref, out_ref):
        out_ref[:, : 3 * GL] = dot_nn(wqkv_ref[...], column_order(False)).astype(BF)
        out_ref[:, 3 * GL :] = wproj_ref[...].T

    return plain_call(body, jax.ShapeDtypeStruct((D, D), BF), "pack_attention", (wqkv, wproj))


def swap(value):
    return lax.ppermute(value, "pipe", [(0, 1), (1, 0)])


def across(value, j):
    return lax.ppermute(value, "dp", [(i, i ^ j) for i in range(4)])


def along(value, k):
    return lax.ppermute(value, "tensor", [(i, (i + k) % 4) for i in range(4)])


class Exchange(Part):
    def __init__(self, own, small):
        shapes = [jax.ShapeDtypeStruct(part.shape, part.dtype) for part in own]
        shapes.append(jax.ShapeDtypeStruct((4, 2) + small.shape, small.dtype))
        super().__init__([*own, small], shapes, sems(4) + sems(3) + [pltpu.SemaphoreType.DMA(())])

    def swap(self, n):
        core, _, _ = place_in_mesh()
        target = self.outs[n] if n < 3 else self.outs[3].at[0, core]
        return remote(self.ins[n], target, [sem.at[n] for sem in self.kept[:2]], "pipe", 1 - core)

    def keep(self):
        core, _, _ = place_in_mesh()
        return pltpu.make_async_copy(self.ins[3], self.outs[3].at[0, core], self.kept[4])

    def spread(self, k):
        _, _, shard = place_in_mesh()
        table = self.outs[3]
        return remote(table.at[0], table.at[k], [sem.at[k - 1] for sem in self.kept[2:4]], "tensor", lax.rem(shard + 4 - k, 4))


def gather_start(own, small):
    exchange = Exchange(own, small)
    near_a, near_m, far_a = Near(1, 0, (), ()), Near(2, 0, (), ()), Far(1, None)
    far_a.inputs = []

    def body():
        near_a.ins = [exchange.ins[0], exchange.outs[0]]
        near_m.ins = [*exchange.ins[1:3], *exchange.outs[1:3]]
        far_a.ins = [near_a.outs[0]]
        greet()
        for n in (0, 3, 1, 2):
            exchange.swap(n).start()
        exchange.keep().start()
        exchange.swap(0).wait()
        near_a.start()
        exchange.keep().wait()
        exchange.swap(3).wait()
        for k in (1, 2, 3):
            exchange.spread(k).start()
        exchange.swap(1).wait()
        exchange.swap(2).wait()
        near_m.start()
        near_a.end()
        far_a.start()
        far_a.end()
        for k in (1, 2, 3):
            exchange.spread(k).wait()
        near_m.end()

    _, given = carried_call(
        body, [exchange, near_a, near_m, far_a], 0, grid=(), in_specs=[], inputs=(), out_specs=[], out_shape=[], scratch_shapes=[],
        name="gather_start", cost=pl.CostEstimate(flops=1 << 24, bytes_accessed=8 << 20, transcendentals=0),
    )
    others, pieces_a, near_m, far = given[0], given[1], given[2][0], given[3]
    return others[:3], others[3], [pieces_a[0], *far], near_m


def reduce_pieces(pairs):
    count = len(pairs)
    received = [swap(away) for _, away in pairs]

    def first_body(*refs):
        mine, came, outs = refs[:count], refs[count : 2 * count], refs[2 * count :]
        for j in range(4):
            for b in range(count):
                outs[j][b] = (mine[b][j].astype(F32) + came[b][j].astype(F32)).astype(BF)

    part = jax.ShapeDtypeStruct((count, 4, 64, D), BF)
    parts = plain_call(first_body, [part] * 4, "add_cores", (*[mine for mine, _ in pairs], *received), (), count * 6 << 20)
    came = [across(parts[j], j) for j in (1, 2, 3)]

    def second_body(*refs):
        for k in range(4):
            total = refs[0][:, k].astype(F32)
            for j in range(1, 4):
                total += refs[j][:, k].astype(F32)
            refs[4 + k][...] = total.astype(BF)

    part = jax.ShapeDtypeStruct((count, 64, D), BF)
    parts = plain_call(second_body, [part] * 4, "add_dp", (parts[0], *came), (), count * 2 << 20)
    came = [along(parts[k], k) for k in (1, 2, 3)]
    total = parts[0].astype(F32)
    for part in came:
        total += part.astype(F32)
    total = total.astype(BF)
    return jnp.stack([total] + [across(total, j) for j in (1, 2, 3)])


def finish_body(kind, place_ref, keep_ref, came_ref, *refs):
    outs, value_ref = refs[:-1], refs[-1]
    for b in range(keep_ref.shape[1]):
        for half, source in enumerate((keep_ref, came_ref)):
            for j in range(4):
                start = (place_ref[0] ^ half) * 256 + (place_ref[1] ^ j) * 64
                value_ref[pl.ds(pl.multiple_of(start, 64), 64), :] = source[j, b]
        if kind == "attn":
            outs[0][...] = dot_nn(value_ref[:, : 3 * GL], column_order(True))
            outs[1][...] = value_ref[:, 3 * GL :].T.astype(F32)
        elif b == 0:
            outs[0][...] = value_ref[...].astype(F32)
        else:
            outs[1][...] = value_ref[...].T.astype(F32)


def finish(kind, place, first_core, reduced0, reduced1):
    keep = jnp.where(first_core, reduced0, reduced1)
    came = swap(jnp.where(first_core, reduced1, reduced0))
    shapes = ((D, 3 * GL), (GL, D)) if kind == "attn" else ((D, D), (D, D))
    return pl.pallas_call(
        functools.partial(finish_body, kind),
        out_shape=[jax.ShapeDtypeStruct(shape, F32) for shape in shapes],
        in_specs=[pl.BlockSpec(memory_space=pltpu.SMEM), vmem(), vmem()],
        out_specs=[vmem(), vmem()],
        scratch_shapes=[pltpu.VMEM((D, D), BF)],
        name="finish_" + kind,
        compiler_params=pltpu.CompilerParams(vmem_limit_bytes=48 << 20),
        cost_estimate=pl.CostEstimate(flops=1 << 22, bytes_accessed=1 << 22, transcendentals=0),
    )(place, keep, came)


def rows_of(vector):
    return vector.astype(F32).reshape(1, -1)


SMALL = ("gain", "shift", "qv", "table", "bproj", "mgain", "mshift", "hb", "ob")
ALONG_MODEL = (True, True, False, False, True, True, True, False, True)


def pack_small(parts):
    return jnp.concatenate([part.reshape(-1) for part in parts])


def unpack_small(packed, shapes):
    out, at = [], 0
    for shape in shapes:
        size = math.prod(shape)
        piece = packed[:, at : at + size]
        out.append(piece.reshape((piece.shape[0] * shape[0],) + tuple(shape[1:])))
        at += size
    return out


def qkv_terms(qv):
    qv = qv.astype(F32).reshape(4, GH, 2, HD)
    shift = jnp.concatenate(
        [
            qv[:, :, 0].reshape(4, 1, GL) * HD ** (-0.5),
            jnp.zeros((4, 1, GL), F32),
            qv[:, :, 1].reshape(4, 1, GL),
        ],
        2,
    )
    scale = jnp.concatenate([jnp.full((1, GL), HD ** (-0.5), F32), jnp.ones((1, 2 * GL), F32)], 1)
    return scale, shift


def layer_forward(x, small, weights, tasks, ids, alive_rows, maps, head_mask):
    count = x.shape[0]
    spread, gather = maps
    (fw, qkv, p, ho, mid), given = attn_fwd(
        x, small["gain"], small["shift"], spread, gather, head_mask, small["qkv_scale"], small["qkv_shift"], small["bias"],
        small["bproj"], weights[0](), tasks[0](), ids[0],
    )
    mid = mid.reshape(count * TP, D)
    (second, act, slope, y), more = mlp_fwd(
        mid, small["mgain"], small["mshift"], small["hb"], small["ob"], alive_rows, weights[1](given), tasks[1](given), ids[1]
    )
    return y.reshape(count, TP, D), (x, fw, qkv, p, ho, mid, second, act, slope), given, more


def layer_backward(place, cot, kept, small, weights, alive_rows, maps, head_mask):
    x, fw, qkv, p, ho, mid, second, act, slope = kept
    count = x.shape[0]
    (ghw, ghw_away, gow, gow_away, ghb, gmid, small_m), _ = mlp_bwd(
        place, cot.reshape(count * TP, D), alive_rows, act, slope, second, mid, small["mgain"], weights[1]
    )
    (gin, ga, ga_away, gqv, gtab, small_a), _ = attn_bwd(
        place, x, gmid.reshape(count, TP, D), fw, qkv, p, ho, small["gain"], maps[0], maps[1], head_mask, weights[0]
    )
    return gin, ((ga, ga_away), (ghw, ghw_away), (gow, gow_away)), (ghb, small_m, gqv, gtab, small_a)


def local(
    images, cotangent, counts, rel_index, pre_attn_gain, pre_attn_bias, qkv_weight, qv_bias, bias_table, proj_weight, proj_bias,
    pre_mlp_gain, pre_mlp_bias, hidden_weight, hidden_bias, out_weight, out_bias,
):
    core = lax.axis_index("pipe")
    first_core = core == 0
    batches, slots = images.shape[:2]
    half = slots // 2
    shards = lax.axis_size("tensor")
    shard = lax.axis_index("tensor")
    fast = shards == 4 and lax.axis_size("dp") == 4
    place = jnp.stack([core, lax.axis_index("dp")]).astype(jnp.int32) if fast else jnp.zeros((2,), jnp.int32)

    small_in = (pre_attn_gain, pre_attn_bias, qv_bias, bias_table, proj_bias, pre_mlp_gain, pre_mlp_bias, hidden_bias, out_bias)
    shapes = [member.shape[1:] for member in small_in]
    if fast:
        own = (pack_attention(qkv_weight[0], proj_weight[0]), hidden_weight[0], out_weight[0])
        table_rows = jnp.pad(bias_table[0], ((0, 0), (0, 2 * GL - RELS))).reshape(-1, GL)
        lines = [table_rows if n == 3 else member.reshape(-1, GL) for n, member in enumerate(small_in)]
        counts_of = [line.shape[0] for line in lines]
        other, table, pieces_a0, near_m0 = gather_start(own, jnp.pad(jnp.concatenate(lines), ((0, 32 - sum(counts_of)), (0, 0))))
        packed, ordered = [], []
        doubled = jnp.concatenate([table, table])
        rolled = lax.dynamic_slice_in_dim(doubled, (4 - shard) % 4, 4, 0)
        for l in range(2):
            for source, out in ((table, packed), (rolled, ordered)):
                values, at = {}, 0
                for name, count in zip(SMALL, counts_of):
                    line = source[:, l, at : at + count]
                    if name == "table":
                        line = line.reshape(H, 2 * GL)[:, :RELS]
                    values[name] = line if name == "table" else line.reshape(-1)
                    at += count
                out.append(values)
    else:
        packed = pack_small(small_in)
        gathered = lax.all_gather(lax.all_gather(packed, "tensor"), "pipe")
        ordered = packed = [dict(zip(SMALL, unpack_small(gathered[l], shapes))) for l in range(2)]

        def both(member, axis):
            return lax.all_gather(lax.all_gather(member[0], "tensor", axis=axis, tiled=True), "pipe")

        gathered = both(qkv_weight, 1), both(proj_weight, 0), both(hidden_weight, 1), both(out_weight, 0)
        matrices = []
        for l in range(2):
            wqkv, wproj, hw, ow = (pair[l] for pair in gathered)
            wqkv = qkv_order(wqkv.reshape(D, 4, 3 * GL).transpose(1, 0, 2))
            wa = jnp.concatenate([wqkv, wproj.reshape(4, GL, D).transpose(0, 2, 1)], 2)
            wm = jnp.stack([hw.reshape(D, 4, -1).transpose(1, 0, 2), ow.reshape(4, -1, D)])
            matrices.append((wa[None], wm))

    def own_slots(array):
        mine = lax.dynamic_slice_in_dim(array, core * half, half, 1).reshape(batches * half, TOK, D)
        return jnp.pad(mine, ((0, 0), (0, TP - TOK), (0, 0)))

    x0 = own_slots(images)
    cot = own_slots(cotangent)
    slot_ids = shard * slots + core * half + jnp.arange(half, dtype=jnp.int32)
    alive = (slot_ids[None, :] < counts).astype(F32).reshape(-1)
    alive_rows = (alive[:, None] * (jnp.arange(TP) < TOK).astype(F32)[None, :]).reshape(-1, 1)

    layers = []
    for l in range(2):
        by_shard, small = packed[l], ordered[l]
        scale, shift = qkv_terms(by_shard["qv"])
        layers.append(
            dict(
                gain=rows_of(small["gain"]), shift=rows_of(small["shift"]), bproj=rows_of(small["bproj"]),
                mgain=rows_of(small["mgain"]), mshift=rows_of(small["mshift"]), ob=rows_of(small["ob"]),
                hb=by_shard["hb"].astype(F32).reshape(4, 1, -1), qkv_scale=scale, qkv_shift=shift,
                bias=bias_tables(by_shard["table"], rel_index, l == 1),
            )
        )
    head_mask = head_masks()
    maps = [window_maps(l * SHIFT) for l in range(2)]
    if fast:
        own_a, own_m, other_a, other_m = own[:1], own[1:], other[:1], other[1:]

        def weights_a(layer, pieces):
            return lambda *_: Weights(1, layer, own=own_a, other=other_a, pieces=pieces)

        def weights_m(layer, pieces):
            return lambda *_: Weights(2, layer, own=own_m, other=other_m, pieces=pieces)

        def fars(near, far):
            return [near, *far]

        y0, kept0, given, more = layer_forward(
            x0, layers[0],
            (weights_a(0, pieces_a0), lambda given: weights_m(0, fars(near_m0, given[1]))()),
            (lambda: [Far(2, near_m0), Near(1, 1, own_a, other_a)], lambda given: [Far(1, given[2][0]), Near(2, 1, own_m, other_m)]),
            (1, 2), alive_rows, maps[0], head_mask,
        )
        pieces_m0, near_a1 = fars(near_m0, given[1]), given[2][0]
        pieces_a1, near_m1 = fars(near_a1, more[1]), more[2][0]
        y1, kept1, given, _ = layer_forward(
            y0, layers[1],
            (weights_a(1, pieces_a1), lambda given: weights_m(1, fars(near_m1, given[1]))()),
            (lambda: [Far(2, near_m1)], lambda given: []),
            (3, None), alive_rows, maps[1], head_mask,
        )
        pieces_m1 = fars(near_m1, given[1])
        weights = [(weights_a(0, pieces_a0), weights_m(0, pieces_m0)), (weights_a(1, pieces_a1), weights_m(1, pieces_m1))]
    else:
        weights = [
            (lambda *_, wa=wa: Weights(1, 0, whole=wa), lambda *_, wm=wm: Weights(2, 0, whole=wm)) for wa, wm in matrices
        ]
        none = (lambda: [], lambda given: [])
        y0, kept0, _, _ = layer_forward(x0, layers[0], weights[0], none, (None, None), alive_rows, maps[0], head_mask)
        y1, kept1, _, _ = layer_forward(y0, layers[1], weights[1], none, (None, None), alive_rows, maps[1], head_mask)
    g1, big1, little1 = layer_backward(place, cot, kept1, layers[1], [w() for w in weights[1]], alive_rows, maps[1], head_mask)
    g0, big0, little0 = layer_backward(place, g1, kept0, layers[0], [w() for w in weights[0]], alive_rows, maps[0], head_mask)

    def assemble(mine0, mine1):
        sent = swap(jnp.where(first_core, mine1, mine0))
        mine = jnp.where(first_core, mine0, mine1)
        mine, sent = (part[:, :TOK].reshape(batches, half, TOK, D) for part in (mine, sent))
        low, high = jnp.where(first_core, mine, sent), jnp.where(first_core, sent, mine)
        return jnp.concatenate([low, high], 1)[None]

    block_out = assemble(y0, y1)
    input_grad = assemble(g0, g1)

    def little(terms):
        ghb, small_m, gqv, gtab, small_a = terms
        qv = jnp.swapaxes(gqv.reshape(4, 2, GH, HD), 1, 2).reshape(-1)
        return (
            small_a[0], small_a[1], qv, table_grad(gtab, rel_index), small_m[1], small_m[2], small_m[3], ghb.reshape(-1), small_m[0],
        )

    if fast:
        reduced = [[reduce_pieces(big[:1]), reduce_pieces(big[1:])] for big in (big0, big1)]
        gqkv, gproj = finish("attn", place, first_core, reduced[0][0], reduced[1][0])
        ghw, gow = finish("mlp", place, first_core, reduced[0][1], reduced[1][1])
        gqkv, gproj, ghw, gow = (part[None] for part in (gqkv, gproj, ghw, gow))

        def by_distance(part, along_model):
            part = part.reshape(4, -1)
            if along_model:
                part = lax.dynamic_slice_in_dim(jnp.concatenate([part, part]), shard, 4, 0)
            return part

        sums = jnp.stack(
            [
                jnp.concatenate([by_distance(part, flag) for part, flag in zip(little(terms), ALONG_MODEL)], 1)
                for terms in (little0, little1)
            ]
        )
        sums = sums + swap(sums)
        sums = jnp.where(first_core, sums[0], sums[1])
        sums = sums + across(sums, 1) + across(sums, 2) + across(sums, 3)
        mine = sums[0] + along(sums[1], 1) + along(sums[2], 2) + along(sums[3], 3)
        outs, at = [], 0
        for shape in shapes:
            size = math.prod(shape)
            outs.append(mine[at : at + size].reshape(shape)[None])
            at += size
    else:

        def matrix_of(pair):
            return jnp.concatenate(pair).transpose(1, 0, 2, 3).reshape(4, D, D)

        def full(big):
            ga, ghw, gow = (matrix_of(pair) for pair in big)
            gqkv = jnp.swapaxes(ga[:, :, : 3 * GL].reshape(4, D, 3, GH, HD), 2, 3).reshape(4, D, 3 * GL)
            return (
                gqkv.transpose(1, 0, 2).reshape(D, 3 * D), ga[:, :, 3 * GL :].transpose(0, 2, 1).reshape(D, D),
                ghw.transpose(1, 0, 2).reshape(D, -1), gow.transpose(0, 2, 1).reshape(-1, D),
            )

        def reduced(pair, axis):
            mine = lax.psum_scatter(jnp.stack(pair), "pipe", scatter_dimension=0, tiled=False)
            mine = lax.psum_scatter(mine, "tensor", scatter_dimension=axis, tiled=True)
            return lax.psum(mine, "dp").astype(F32)[None]

        gqkv, gproj, ghw, gow = (reduced(pair, axis) for pair, axis in zip(zip(full(big0), full(big1)), (1, 0, 1, 0)))
        totals = lax.psum(jnp.stack([pack_small(little(little0)), pack_small(little(little1))]), ("pipe", "dp", "tensor"))
        mine = jnp.where(first_core, totals[0], totals[1])
        outs, at = [], 0
        for shape in shapes:
            whole_shape = (shape[0] * shards,) + tuple(shape[1:])
            size = math.prod(whole_shape)
            piece = mine[at : at + size].reshape(whole_shape)
            outs.append(lax.dynamic_slice_in_dim(piece, shard * shape[0], shape[0], 0)[None])
            at += size
    gain_g, shift_g, qv_g, table_g, bproj_g, mgain_g, mshift_g, hb_g, ob_g = outs
    return (
        block_out, input_grad, gain_g, shift_g, gqkv, qv_g, table_g, gproj, bproj_g, mgain_g, mshift_g, ghw, hb_g, gow, ob_g,
    )


def solution(mesh):
    return jax.shard_map(
        local,
        mesh=mesh,
        in_specs=(
            P(None, ("dp", "tensor"), None, None),
            P(None, ("dp", "tensor"), None, None),
            P(None, "dp"),
            P(),
            P("pipe", "tensor"),
            P("pipe", "tensor"),
            P("pipe", None, "tensor"),
            P("pipe", "tensor"),
            P("pipe", "tensor", None),
            P("pipe", "tensor", None),
            P("pipe", "tensor"),
            P("pipe", "tensor"),
            P("pipe", "tensor"),
            P("pipe", None, "tensor"),
            P("pipe", "tensor"),
            P("pipe", "tensor", None),
            P("pipe", "tensor"),
        ),
        out_specs=(
            P("pipe", None, ("dp", "tensor"), None, None),
            P("pipe", None, ("dp", "tensor"), None, None),
            P("pipe", "tensor"),
            P("pipe", "tensor"),
            P("pipe", None, "tensor"),
            P("pipe", "tensor"),
            P("pipe", "tensor", None),
            P("pipe", "tensor", None),
            P("pipe", "tensor"),
            P("pipe", "tensor"),
            P("pipe", "tensor"),
            P("pipe", None, "tensor"),
            P("pipe", "tensor"),
            P("pipe", "tensor", None),
            P("pipe", "tensor"),
        ),
        check_vma=False,
    )
```

```python
import functools
import math

import jax
import jax.numpy as jnp
from jax import lax
from jax.experimental import pallas as pl
from jax.experimental.pallas import tpu as pltpu
from jax.sharding import PartitionSpec as P

D = 512
H = 16
HD = 32
WIN = 7
GRID = 14
SHIFT = 3
TOK = 196
RELS = 169
POS = WIN * WIN
NW = 4
WP = 64
TP = 208
ROWS = NW * WP
GH = 4
GL = GH * HD
BLK = 832
SUB_FWD = 208
SUB_BWD = 416
CHUNK = 64
AT_ONCE = 2
LATE = "late"
LINES = 32
GAIN, SHIFT_ROW, QV, TABLE, BPROJ, MGAIN, MSHIFT, HB, OB = 0, 1, 2, 4, 12, 13, 14, 15, 19
PLACES = (1, 3, 2, 0)
EPSILON = 1e-05
MASK_VALUE = -100.0
SHUT = -1e30
F32 = jnp.float32
BF = jnp.bfloat16
ANY = pl.BlockSpec(memory_space=pl.ANY)
VMEM_LIMIT = 60 << 20


def dot_nn(a, b):
    return lax.dot_general(a, b, (((1,), (0,)), ((), ())), preferred_element_type=F32)


def dot_nt(a, b):
    return lax.dot_general(a, b, (((1,), (1,)), ((), ())), preferred_element_type=F32)


def dot_tn(a, b):
    return lax.dot_general(a, b, (((0,), (0,)), ((), ())), preferred_element_type=F32)


def iota(shape, axis):
    return lax.broadcasted_iota(jnp.int32, shape, axis)


def normalize(rows):
    center = rows - jnp.mean(rows, -1, keepdims=True)
    inverse = lax.rsqrt(jnp.mean(center * center, -1, keepdims=True) + EPSILON)
    return center * inverse, inverse


def norm_back(grad_out, normed, inverse, gain):
    scaled = grad_out * gain
    return inverse * (
        scaled
        - jnp.mean(scaled, -1, keepdims=True)
        - normed * jnp.mean(scaled * normed, -1, keepdims=True)
    )


def remote(source, target, sems, axis, index):
    return pltpu.make_async_remote_copy(
        src_ref=source, dst_ref=target, send_sem=sems[0], recv_sem=sems[1], device_id={axis: index},
        device_id_type=pl.DeviceIdType.MESH,
    )


def place_in_mesh():
    return lax.axis_index("pipe"), lax.axis_index("dp"), lax.axis_index("tensor")


def greet():
    core, dp, shard = place_in_mesh()
    barrier = pltpu.get_barrier_semaphore()

    def signal(axis, index):
        pl.semaphore_signal(barrier, inc=1, device_id={axis: index}, device_id_type=pl.DeviceIdType.MESH)

    signal("pipe", 1 - core)
    for k in (1, 2, 3):
        signal("dp", dp ^ k)
        signal("tensor", lax.rem(shard + k, 4))
    pl.semaphore_wait(barrier, 7)


def quarter(half, j):
    core, dp, _ = place_in_mesh()
    return pl.ds(pl.multiple_of((core ^ half) * 256 + (dp ^ j) * CHUNK, CHUNK), CHUNK)


def by_core(action):
    for which in (0, 1):

        @pl.when(lax.axis_index("pipe") == which)
        def _():
            action(which)


def sems(*shape):
    return [pltpu.SemaphoreType.DMA(shape), pltpu.SemaphoreType.DMA(shape)]


class Part:
    plan = ()
    deferred = False

    def __init__(self, inputs=(), outputs=(), scratch=()):
        self.inputs, self.outputs, self.scratch = list(inputs), list(outputs), list(scratch)

    def bind(self, ins, outs, kept):
        self.ins, self.outs, self.kept = ins, outs, kept


class Weights(Part):
    def __init__(self, count, layer, whole=None, own=None, other=None, pieces=None):
        self.count, self.layer, self.whole = count, layer, whole
        inputs = [whole] if whole is not None else [*own, *other, *[piece for group in pieces for piece in group]]
        super().__init__(inputs, (), [pltpu.VMEM((count, 4, D, D), BF), pltpu.SemaphoreType.DMA((9 * count,))])

    def shard(self, mine, b):
        store, sem = self.kept
        if self.whole is not None:
            return pltpu.make_async_copy(self.ins[0].at[b, 0], store.at[b, 0], sem.at[b * 9])
        owns, others = self.ins[: self.count], self.ins[self.count : 2 * self.count]
        return pltpu.make_async_copy((owns if mine else others)[b], store.at[b, 0], sem.at[b * 9])

    def rest(self):
        store, sem = self.kept
        if self.whole is not None:
            return [
                pltpu.make_async_copy(self.ins[0].at[b, pl.ds(1, 3)], store.at[b, pl.ds(1, 3)], sem.at[b * 9 + 1])
                for b in range(self.count)
            ]
        return [
            pltpu.make_async_copy(
                self.ins[2 * self.count + b * 8 + half * 4 + j], store.at[b, pl.ds(1, 3), quarter(half, j), :],
                sem.at[b * 9 + half * 4 + j + 1],
            )
            for b in range(self.count)
            for half in range(2)
            for j in range(4)
        ]

    def load(self):
        if self.whole is not None:
            for b in range(self.count):
                self.shard(True, b).start()
        else:

            def shards(core):
                for b in range(self.count):
                    self.shard(core == self.layer, b).start()

            by_core(shards)
        for copy in self.rest():
            copy.start()

    def wait_shard(self):
        for b in range(self.count):
            self.shard(True, b).wait()

    def wait_rest(self):
        for copy in self.rest():
            copy.wait()


class Stored(Part):
    def __init__(self, *arrays):
        super().__init__(arrays, (), [pltpu.VMEM(a.shape, a.dtype) for a in arrays] + [pltpu.SemaphoreType.DMA((len(arrays),))])

    def copies(self):
        return [pltpu.make_async_copy(ref, kept, self.kept[-1].at[n]) for n, (ref, kept) in enumerate(zip(self.ins, self.kept))]

    def load(self):
        for copy in self.copies():
            copy.start()

    def wait(self):
        for copy in self.copies():
            copy.wait()


class Keep(Part):
    def __init__(self, *shapes):
        super().__init__((), [jax.ShapeDtypeStruct(shape, BF) for shape in shapes], [pltpu.SemaphoreType.DMA((len(shapes),))])

    def copies(self, refs):
        return [pltpu.make_async_copy(ref, out, self.kept[0].at[n]) for n, (ref, out) in enumerate(zip(refs, self.outs))]

    def start(self, *refs):
        for copy in self.copies(refs):
            copy.start()

    def wait(self, *refs):
        for copy in self.copies(refs):
            copy.wait()


class Near(Part):
    def __init__(self, layer, own, other, plan=(), deferred=False):
        self.layer, self.plan, self.deferred = layer, plan, deferred
        inputs = [] if own is None else [own, other]
        super().__init__(inputs, [jax.ShapeDtypeStruct((3, CHUNK, D), BF)], sems(3))

    def copy(self, mine, k):
        _, _, shard = place_in_mesh()
        source = self.ins[0 if mine else 1].at[quarter(0, 0), :]
        return remote(source, self.outs[0].at[k - 1], [sem.at[k - 1] for sem in self.kept], "tensor", lax.rem(shard + 4 - k, 4))

    def start(self):
        def sends(core):
            for k in (2, 1, 3):
                self.copy(core == self.layer, k).start()

        by_core(sends)

    def finish(self):
        for k in (1, 2, 3):
            self.copy(True, k).wait()

    def end(self):
        if not any(what == "finish" for _, what in self.plan):
            self.finish()


class Far(Part):
    def __init__(self, near, plan=(), source=None, deferred=False):
        self.plan, self.source, self.deferred = plan, source, deferred
        shape = jax.ShapeDtypeStruct((3, CHUNK, D), BF)
        super().__init__([] if near is None else [near], [shape] * 7, sems(2, 2) + sems(2) + sems(4))

    def rows(self, j):
        return pl.ds((j - 1) * 32, 32)

    def across(self, j, half):
        _, dp, _ = place_in_mesh()
        rows = self.rows(j if half == 0 else 3 - j)
        return remote(
            self.ins[0].at[:, rows], self.outs[j - 1].at[:, rows], [sem.at[j - 1, half] for sem in self.kept[:2]], "dp", dp ^ j
        )

    def onward(self, j):
        _, dp, _ = place_in_mesh()
        rows = self.rows(j)
        return remote(
            self.outs[j - 1].at[:, rows], self.outs[2].at[:, rows], [sem.at[j - 1] for sem in self.kept[2:4]], "dp", dp ^ (3 - j)
        )

    def over(self, j):
        core, _, _ = place_in_mesh()
        source = self.ins[0] if j == 0 else self.outs[j - 1]
        return remote(source, self.outs[3 + j], [sem.at[j] for sem in self.kept[4:]], "pipe", 1 - core)

    def start(self):
        for half in (0, 1):
            for j in (1, 2):
                self.across(j, half).start()
        self.over(0).start()

    def turn(self):
        for j in (1, 2):
            self.across(j, 0).wait()
        for j in (1, 2):
            self.onward(j).start()

    def rest(self):
        for j in (1, 2):
            self.across(j, 1).wait()
            self.over(j).start()

    def last(self):
        for j in (1, 2):
            self.onward(j).wait()
        self.over(3).start()

    def end(self):
        for j in range(4):
            self.over(j).wait()


class FarFirst(Part):
    def __init__(self, near, plan=(), source=None, deferred=False):
        self.plan, self.source, self.deferred = plan, source, deferred
        shape = jax.ShapeDtypeStruct((3, CHUNK, D), BF)
        super().__init__([] if near is None else [near], [shape] * 5, sems(2) + sems(3))

    def across(self, j):
        _, dp, _ = place_in_mesh()
        return remote(self.ins[0], self.outs[j - 1], [sem.at[j - 1] for sem in self.kept[:2]], "dp", dp ^ j)

    def over(self, j):
        core, _, _ = place_in_mesh()
        source = self.ins[0] if j == 0 else self.outs[j - 1]
        return remote(source, self.outs[2 + j], [sem.at[j] for sem in self.kept[2:]], "pipe", 1 - core)

    def start(self):
        for j in (1, 2):
            self.across(j).start()
        self.over(0).start()

    def end(self):
        for j in (1, 2):
            self.across(j).wait()
            self.over(j).start()
        for j in range(3):
            self.over(j).wait()


class FarSecond(Part):
    def __init__(self, first, plan=()):
        self.plan = plan
        shape = jax.ShapeDtypeStruct((3, CHUNK, D), BF)
        super().__init__(first[:2], [shape] * 2, sems(2) + sems())

    def onward(self, j):
        _, dp, _ = place_in_mesh()
        rows = pl.ds((j - 1) * 32, 32)
        return remote(
            self.ins[j - 1].at[:, rows], self.outs[0].at[:, rows], [sem.at[j - 1] for sem in self.kept[:2]], "dp", dp ^ (3 - j)
        )

    def over(self):
        core, _, _ = place_in_mesh()
        return remote(self.outs[0], self.outs[1], self.kept[2:], "pipe", 1 - core)

    def start(self):
        for j in (1, 2):
            self.onward(j).start()

    def last(self):
        for j in (1, 2):
            self.onward(j).wait()
        self.over().start()

    def end(self):
        if not any(what == "last" for _, what in self.plan):
            self.last()
        self.over().wait()


def gathered(near, first, second):
    return [near, *first[:2], second[0], *first[2:], second[1]]


class ReduceFirst(Part):
    def __init__(self, pair, plan=(), rows=(0, CHUNK)):
        self.plan, (self.start_row, self.size) = plan, rows
        size = self.size
        half = pltpu.VMEM((4, 4, size, D), BF)
        super().__init__(
            pair,
            [jax.ShapeDtypeStruct((4, size, D), BF)],
            [half, half, pltpu.VMEM((2, 2, 2, size, D), BF), pltpu.VMEM((2, 2, size, D), BF), pltpu.VMEM((4, size, D), BF)]
            + sems() + sems(2) + sems(2) + [pltpu.SemaphoreType.DMA(()), pltpu.SemaphoreType.DMA(())],
        )

    def bind(self, ins, outs, kept):
        super().bind(ins, outs, kept)
        self.mine, self.came, self.first, self.second, self.total = kept[:5]

    def over(self):
        core, _, _ = place_in_mesh()
        source = self.ins[1].at[:, :, pl.ds(self.start_row, self.size)]
        return remote(source, self.came, self.kept[5:7], "pipe", 1 - core)

    def load(self):
        return pltpu.make_async_copy(self.ins[0].at[:, :, pl.ds(self.start_row, self.size)], self.mine, self.kept[11])

    def across(self, j):
        _, dp, _ = place_in_mesh()
        source = self.mine.at[pl.ds(j - 1, 2), pl.ds(2 * j - 2, 2)]
        return remote(source, self.first.at[j - 1], [sem.at[j - 1] for sem in self.kept[7:9]], "dp", dp ^ j)

    def onward(self, j):
        _, dp, _ = place_in_mesh()
        source = self.mine.at[2 if j == 1 else 0, pl.ds(2 * j - 2, 2)]
        return remote(source, self.second.at[j - 1], [sem.at[j - 1] for sem in self.kept[9:11]], "dp", dp ^ (3 - j))

    def start(self):
        self.over().start()
        self.load().start()

    def cores(self):
        self.over().wait()
        self.load().wait()

        def add(place, k):
            self.mine[place, k] = (self.mine[place, k].astype(F32) + self.came[place, k].astype(F32)).astype(BF)

        def sent(n, carry):
            add(n // 2, n % 2)
            add(n // 2 + 1, n % 2 + 2)
            return carry

        def kept(n, carry):
            add(3, n)
            add(2 - n // 2 * 2, n)
            return carry

        lax.fori_loop(0, 4, sent, 0)
        for j in (1, 2):
            self.across(j).start()
        lax.fori_loop(0, 4, kept, 0)

    def turn(self):
        for j in (1, 2):
            self.across(j).wait()

        def add(n, carry):
            self.mine[2, n] = (self.mine[2, n].astype(F32) + self.first[0, 1, n].astype(F32)).astype(BF)
            self.mine[0, n + 2] = (self.mine[0, n + 2].astype(F32) + self.first[1, 0, n].astype(F32)).astype(BF)
            return carry

        lax.fori_loop(0, 2, add, 0)
        for j in (1, 2):
            self.onward(j).start()

    def close(self):
        for j in (1, 2):
            self.onward(j).wait()

        def add(n, carry):
            for j in (1, 2):
                k = n + 2 * j - 2
                total = self.mine[3, k].astype(F32) + self.first[j - 1, j - 1, n].astype(F32)
                self.total[k] = (total + self.second[j - 1, n].astype(F32)).astype(BF)
            return carry

        lax.fori_loop(0, 2, add, 0)

    def end(self):
        self.close()
        copy = pltpu.make_async_copy(self.total, self.outs[0], self.kept[12])
        copy.start()
        copy.wait()


class ReduceTurn(ReduceFirst):
    def __init__(self, pair, plan=()):
        super().__init__(pair, plan)
        self.outputs = [jax.ShapeDtypeStruct((2, 2, CHUNK, D), BF), jax.ShapeDtypeStruct((4, CHUNK, D), BF)]
        self.scratch.append(pltpu.SemaphoreType.DMA((3,)))

    def end(self):
        for j in (1, 2):
            self.across(j).wait()

        def add(n, carry):
            self.mine[2, n] = (self.mine[2, n].astype(F32) + self.first[0, 1, n].astype(F32)).astype(BF)
            self.mine[0, n + 2] = (self.mine[0, n + 2].astype(F32) + self.first[1, 0, n].astype(F32)).astype(BF)
            for j in (1, 2):
                k = n + 2 * j - 2
                self.mine[3, k] = (self.mine[3, k].astype(F32) + self.first[j - 1, j - 1, n].astype(F32)).astype(BF)
            return carry

        lax.fori_loop(0, 2, add, 0)
        sem = self.kept[13]
        copies = [
            pltpu.make_async_copy(self.mine.at[2, pl.ds(0, 2)], self.outs[0].at[0], sem.at[0]),
            pltpu.make_async_copy(self.mine.at[0, pl.ds(2, 2)], self.outs[0].at[1], sem.at[1]),
            pltpu.make_async_copy(self.mine.at[3], self.outs[1], sem.at[2]),
        ]
        for copy in copies:
            copy.start()
        for copy in copies:
            copy.wait()


class ReduceOnward(Part):
    def __init__(self, given, plan=()):
        self.plan = plan
        base = pltpu.VMEM((4, CHUNK, D), BF)
        super().__init__(
            given, [jax.ShapeDtypeStruct((4, CHUNK, D), BF)],
            [base, pltpu.VMEM((2, 2, CHUNK, D), BF)] + sems(2) + [pltpu.SemaphoreType.DMA(()), pltpu.SemaphoreType.DMA(())],
        )

    def onward(self, j):
        _, dp, _ = place_in_mesh()
        return remote(self.ins[0].at[j - 1], self.kept[1].at[j - 1], [sem.at[j - 1] for sem in self.kept[2:4]], "dp", dp ^ (3 - j))

    def load(self):
        return pltpu.make_async_copy(self.ins[1], self.kept[0], self.kept[4])

    def start(self):
        for j in (1, 2):
            self.onward(j).start()
        self.load().start()

    def close(self):
        self.load().wait()
        for j in (1, 2):
            self.onward(j).wait()
        total = self.kept[0]

        def add(n, carry):
            for j in (1, 2):
                k = n + 2 * j - 2
                total[k] = (total[k].astype(F32) + self.kept[1][j - 1, n].astype(F32)).astype(BF)
            return carry

        lax.fori_loop(0, 2, add, 0)

    def end(self):
        self.close()
        copy = pltpu.make_async_copy(self.kept[0], self.outs[0], self.kept[5])
        copy.start()
        copy.wait()


class ReduceSecond(Part):
    def __init__(self, totals=None, size=CHUNK, plan=()):
        self.plan = plan
        line = pltpu.VMEM((size, D), BF)
        super().__init__(
            [totals] if totals is not None else [],
            [jax.ShapeDtypeStruct((size, D), BF)],
            [line, pltpu.VMEM((3, size, D), BF)] + sems(3) + [pltpu.SemaphoreType.DMA(()), pltpu.SemaphoreType.DMA(())],
        )

    def own(self):
        return pltpu.make_async_copy(self.ins[0].at[0], self.kept[0], self.kept[4])

    def along(self, k):
        _, _, shard = place_in_mesh()
        return remote(
            self.ins[0].at[k], self.kept[1].at[k - 1], [sem.at[k - 1] for sem in self.kept[2:4]], "tensor", lax.rem(shard + k, 4)
        )

    def start(self):
        for k in (2, 1, 3):
            self.along(k).start()
        self.own().start()

    def close(self):
        self.own().wait()
        for k in (1, 2, 3):
            self.along(k).wait()
        total = self.kept[0][...].astype(F32)
        for k in range(3):
            total += self.kept[1][k].astype(F32)
        self.kept[0][...] = total.astype(BF)

    def end(self):
        if not any(what == "close" for _, what in self.plan):
            self.close()
        copy = pltpu.make_async_copy(self.kept[0], self.outs[0], self.kept[5])
        copy.start()
        copy.wait()


class Share(Part):
    def __init__(self, piece=None, rows=(0, CHUNK), target=None, source=None, plan=()):
        self.start_row, self.size = rows
        self.target, self.after, self.plan, self.deferred = target, source, plan, source is not None
        super().__init__(
            [piece] if piece is not None else [],
            [jax.ShapeDtypeStruct((D, D), BF)] if target is None else [],
            [pltpu.VMEM((self.size, D), BF)] + sems(3) + [pltpu.SemaphoreType.DMA(()), pltpu.SemaphoreType.DMA(())],
        )

    def place(self):
        core, dp, _ = place_in_mesh()
        start = pl.multiple_of(core * 256 + dp * CHUNK, CHUNK) + self.start_row
        out = self.outs[0] if self.target is None else self.target.outs[0]
        return out.at[pl.ds(pl.multiple_of(start, self.size), self.size), :]

    def across(self, j):
        _, dp, _ = place_in_mesh()
        return remote(self.ins[0], self.place(), [sem.at[j - 1] for sem in self.kept[1:3]], "dp", dp ^ j)

    def load(self):
        return pltpu.make_async_copy(self.ins[0], self.kept[0], self.kept[3])

    def keep(self):
        return pltpu.make_async_copy(self.kept[0], self.place(), self.kept[4])

    def start(self):
        if self.after is not None:
            self.ins = [self.after.kept[0]]
        for j in (3, 1, 2):
            self.across(j).start()
        self.load().start()

    def end(self):
        self.load().wait()
        self.keep().start()
        for j in (1, 2, 3):
            self.across(j).wait()
        self.keep().wait()


class Deliver(Part):
    def __init__(self, of_layers):
        super().__init__(of_layers, [jax.ShapeDtypeStruct(of_layers[0].shape, BF)], sems())

    def send(self, core):
        return remote(self.ins[1 - core], self.outs[0], self.kept, "pipe", 1 - core)

    def start(self):
        by_core(lambda core: self.send(core).start())

    def end(self):
        self.send(0).wait()


def carried_call(body, parts, collective_id, *, grid, in_specs, inputs, out_specs, out_shape, scratch_shapes, name, cost):
    n_in, n_out, n_scratch = len(inputs), len(out_shape), len(scratch_shapes)
    counts = [(len(part.inputs), len(part.outputs), len(part.scratch)) for part in parts]

    def whole_body(*refs):
        refs = list(refs)

        def take(count, groups):
            mine = [refs.pop(0) for _ in range(count)]
            return mine, [[refs.pop(0) for _ in range(n)] for n in groups]

        mine, part_ins = take(n_in, [n for n, _, _ in counts])
        outs, part_outs = take(n_out, [n for _, n, _ in counts])
        kept, part_kept = take(n_scratch, [n for _, _, n in counts])
        for part, a, b, c in zip(parts, part_ins, part_outs, part_kept):
            part.bind(a, b, c)
        for part in parts:
            if getattr(part, "source", None) is not None:
                part.ins = [part.source.outs[0]]
        body(*mine, *outs, *kept)

    extra_in = [x for part in parts for x in part.inputs]
    extra_out = [x for part in parts for x in part.outputs]
    params = dict(vmem_limit_bytes=VMEM_LIMIT)
    if collective_id is not None:
        params.update(collective_id=collective_id, has_side_effects=True)
    results = pl.pallas_call(
        whole_body,
        grid_spec=pltpu.PrefetchScalarGridSpec(
            num_scalar_prefetch=0,
            grid=grid,
            in_specs=list(in_specs) + [ANY] * len(extra_in),
            out_specs=list(out_specs) + [ANY] * len(extra_out),
            scratch_shapes=list(scratch_shapes) + [x for part in parts for x in part.scratch],
        ),
        out_shape=list(out_shape) + extra_out,
        name=name,
        compiler_params=pltpu.CompilerParams(**params),
        cost_estimate=cost,
    )(*inputs, *extra_in)
    own, rest = results[:n_out], results[n_out:]
    given = []
    for _, n, _ in counts:
        given.append(rest[:n])
        rest = rest[n:]
    return own, given


def begin(weights, tasks):
    pl.when(pl.program_id(0) == 0)(weights.load)
    if tasks:

        @pl.when(pl.program_id(0) == 0)
        def _():
            greet()
            for task in tasks:
                if not task.deferred:
                    task.start()


def planned(tasks, point):
    return [getattr(task, what) for task in tasks for at, what in task.plan if at == point]


def step_end(tasks, steps):
    for step in range(steps):
        calls = planned(tasks, step)
        if step == steps - 1:
            calls += [task.end for task in tasks]
        if calls:

            @pl.when(pl.program_id(0) == step)
            def _():
                for call in calls:
                    call()


def whole(shape):
    return pl.BlockSpec(shape, lambda i: (0,) * len(shape))


def per(shape):
    return pl.BlockSpec((1,) + shape, lambda i: (i,) + (0,) * len(shape))


SMEM = pl.BlockSpec(memory_space=pltpu.SMEM)


def along_model(table_ref, layer, row, rolled):
    shard = lax.axis_index("tensor") if rolled else 0
    return jnp.concatenate([table_ref[(z - shard + 4) % 4, layer, row : row + 1, :].astype(F32) for z in range(4)], 1)


def window_token(shape, axis, offset):
    s = iota(shape, axis)
    w, a = s // WP, s % WP
    r = (w // 2) * WIN + a // WIN + offset
    c = (w % 2) * WIN + a % WIN + offset
    r, c = jnp.where(r >= GRID, r - GRID, r), jnp.where(c >= GRID, c - GRID, c)
    return jnp.where(a < POS, r * GRID + c, -1)


def spread_map(offset):
    return (window_token((ROWS, 1), 0, offset) == iota((ROWS, TP), 1)).astype(F32).astype(BF)


def gather_map(offset):
    return (window_token((1, ROWS), 1, offset) == iota((TP, ROWS), 0)).astype(F32).astype(BF)


def head_mask():
    return (iota((GH * WP, GL), 0) // WP == iota((GH * WP, GL), 1) // HD).astype(F32).astype(BF)


def region_mask(w):
    def band(a, which):
        place = which * WIN + a
        return (place >= GRID - WIN).astype(jnp.int32) + (place >= GRID - SHIFT).astype(jnp.int32)

    def label(a):
        return band(a // WIN, w // 2) * 3 + band(a % WIN, w % 2)

    keys = label(iota((WP, 1), 0))
    queries = label(iota((1, GH * WP), 1) % WP)
    return jnp.where(keys != queries, MASK_VALUE, 0.0).astype(F32)


def block_diagonal(rows, mask):
    return jnp.concatenate([rows] * GH, axis=0) * mask


def query_major(pt):
    turned = pt.T
    return jnp.concatenate([turned[h * WP : (h + 1) * WP] for h in range(GH)], axis=1)


def pick_diagonal(full):
    head = iota((WP, GL), 1) // HD
    out = full[0:WP]
    for h in range(1, GH):
        out = jnp.where(head == h, full[h * WP : (h + 1) * WP], out)
    return out


def permutation(size, source_of, inverse):
    rows = iota((size, size), 1 if inverse else 0)
    cols = iota((size, size), 0 if inverse else 1)
    return (rows == source_of(cols)).astype(F32).astype(BF)


def qkv_source(col):
    return (col % GL) // HD * (3 * HD) + col // GL * HD + col % HD


def qv_source(col):
    return (col % GL) // HD * (2 * HD) + col // GL * HD + col % HD


def attn_fwd_body(
    layer, rolled, weights, keep, tasks, x_ref, table_ref, bias_ref, fw_ref, qkv_ref, p_ref, ho_ref, mid_ref,
    xs_ref, how_ref, wq_ref, wpt_ref, vec_ref, shift_ref, spread_ref, gather_ref, mask_ref, region_ref,
):
    begin(weights, tasks)
    wa_ref = weights.kept[0].at[0]
    first_step = pl.program_id(0) == 0

    @pl.when(first_step)
    def _():
        for n, row in enumerate((GAIN, SHIFT_ROW, BPROJ)):
            vec_ref[n : n + 1, :] = along_model(table_ref, layer, row, rolled)
        for g in range(4):
            qv = table_ref[g, layer, QV : QV + 2, :].astype(F32)
            at = 3 * GL * g
            for n, (scale, shift) in enumerate(((HD ** (-0.5), qv[0:1] * HD ** (-0.5)), (1.0, 0.0), (1.0, qv[1:2]))):
                lanes = slice(at + n * GL, at + (n + 1) * GL)
                shift_ref[0:1, lanes] = jnp.full((1, GL), scale, F32)
                shift_ref[1:2, lanes] = shift + jnp.zeros((1, GL), F32)
        spread_ref[...] = spread_map(layer * SHIFT)
        gather_ref[...] = gather_map(layer * SHIFT)
        mask_ref[...] = head_mask()
        if layer:
            for w in range(NW):
                region_ref[w] = region_mask(w)
        else:
            xs_ref[...] = jnp.zeros_like(xs_ref)

    if layer:
        x = x_ref[0].astype(F32)
    else:
        xs_ref[0:TOK, :] = x_ref[0, lax.axis_index("pipe")]
        x = xs_ref[...].astype(F32)
    normed, _ = normalize(x)
    first = (normed * vec_ref[0:1, :] + vec_ref[1:2, :]).astype(BF)
    fw = dot_nn(spread_ref[...], first).astype(BF)
    fw_ref[0] = fw

    @pl.when(first_step)
    def _():
        weights.wait_shard()
        weights.wait_rest()
        for g in range(4):
            wq_ref[:, 3 * GL * g : 3 * GL * (g + 1)] = wa_ref[g, :, : 3 * GL]
            wpt_ref[:, g * GL : (g + 1) * GL] = wa_ref[g, :, 3 * GL :]
        keep.start(wq_ref, wpt_ref)

    for n in range(3):
        lanes = slice(n * D, (n + 1) * D)
        projected = dot_nn(fw, wq_ref[:, lanes])
        qkv_ref[0, :, lanes] = (projected * shift_ref[0:1, lanes] + shift_ref[1:2, lanes]).astype(BF)

    def windows(n, carry):
        chains = [(n * AT_ONCE + w, g) for w in range(AT_ONCE) for g in range(4)]

        def rows(w):
            return pl.ds(pl.multiple_of(w * WP, WP), WP)

        def part(w, g, n):
            return qkv_ref[0, rows(w), (3 * g + n) * GL : (3 * g + n + 1) * GL]

        scores = [dot_nt(part(w, g, 1), block_diagonal(part(w, g, 0), mask_ref[...])) for w, g in chains]
        probs = []
        for (w, g), st in zip(chains, scores):
            st = st + bias_ref[g]
            if layer:
                st = st + region_ref[w]
            e = jnp.exp(st - jnp.max(st, 0, keepdims=True))
            pt = (e * (1.0 / jnp.sum(e, 0, keepdims=True))).astype(BF)
            p_ref[0, w, g] = pt
            probs.append(pt)
        mixed = [dot_tn(pt, part(w, g, 2)) for (w, g), pt in zip(chains, probs)]
        for (w, g), out in zip(chains, mixed):
            how_ref[rows(w), g * GL : (g + 1) * GL] = pick_diagonal(out).astype(BF)
        return carry

    lax.fori_loop(0, NW // AT_ONCE, windows, 0)
    ho = dot_nn(gather_ref[...], how_ref[...]).astype(BF)
    ho_ref[0] = ho
    mid_ref[0] = x + (dot_nt(ho, wpt_ref[...]) + vec_ref[2:3, :])
    step_end(tasks, 4)

    @pl.when(pl.program_id(0) == pl.num_programs(0) - 1)
    def _():
        keep.wait(wq_ref, wpt_ref)


def attn_fwd(layer, rolled, x, table, bias, weights, tasks=(), collective_id=None):
    n = x.shape[0]
    keep = Keep((D, 3 * D), (D, D))
    return carried_call(
        functools.partial(attn_fwd_body, layer, rolled, weights, keep, tasks),
        [keep, weights, *tasks],
        collective_id,
        grid=(n,),
        in_specs=[per(x.shape[1:]), whole(table.shape), whole((4, WP, GH * WP))],
        inputs=(x, table, bias),
        out_specs=[per((ROWS, D)), per((ROWS, 3 * D)), per((NW, 4, WP, GH * WP)), per((TP, D)), per((TP, D))],
        out_shape=[
            jax.ShapeDtypeStruct((n, ROWS, D), BF),
            jax.ShapeDtypeStruct((n, ROWS, 3 * D), BF),
            jax.ShapeDtypeStruct((n, NW, 4, WP, GH * WP), BF),
            jax.ShapeDtypeStruct((n, TP, D), BF),
            jax.ShapeDtypeStruct((n, TP, D), F32),
        ],
        scratch_shapes=[
            pltpu.VMEM((TP, D), BF), pltpu.VMEM((ROWS, D), BF), pltpu.VMEM((D, 3 * D), BF), pltpu.VMEM((D, D), BF), pltpu.VMEM((8, D), F32),
            pltpu.VMEM((8, 3 * D), F32), pltpu.VMEM((ROWS, TP), BF), pltpu.VMEM((TP, ROWS), BF), pltpu.VMEM((GH * WP, GL), BF),
            pltpu.VMEM((NW, WP, GH * WP), F32),
        ],
        name="attn_fwd",
        cost=pl.CostEstimate(flops=n * 2 * 256 * 512 * 2600, bytes_accessed=n * 2 << 20, transcendentals=0),
    )


def gelu_parts(v):
    cdf = 0.5 * (1.0 + lax.erf(v * 0.5**0.5))
    pdf = jnp.exp(-0.5 * v * v) * (2.0 * math.pi) ** (-0.5)
    return v * cdf, cdf + v * pdf


def alive_of(counts_ref, m):
    slot = lax.axis_index("tensor") * 2 + lax.axis_index("pipe")
    return (slot < counts_ref[m, 0]).astype(F32)


def live_rows(counts_ref, m):
    return jnp.where(iota((TP, 1), 0) < TOK, alive_of(counts_ref, m), 0.0)


def mlp_fwd_body(
    layer, rolled, weights, keep, tasks, counts_ref, mid_ref, table_ref, second_ref, act_ref, slope_ref, y_ref, out_ref, acc_ref, hb_ref
):
    c = pl.program_id(0)
    rows_total = mid_ref.shape[0]
    begin(weights, tasks)
    wm_ref = weights.kept[0]

    @pl.when(c == 0)
    def _():
        for k in range(4):
            hb_ref[k] = jnp.concatenate([table_ref[k, layer, HB + n : HB + n + 1, :].astype(F32) for n in range(4)], 1)
        gain = along_model(table_ref, layer, MGAIN, rolled)
        shift = along_model(table_ref, layer, MSHIFT, rolled)
        mid = mid_ref[...]
        normed, _ = normalize(mid)
        second_ref[...] = (normed * gain + shift).astype(BF)
        acc_ref[...] = mid + along_model(table_ref, layer, OB, rolled)
        weights.wait_shard()

    @pl.when(c == 1)
    def _():
        weights.wait_rest()
        keep.start(wm_ref)

    def block(b, carry):
        parts = [pl.ds(pl.multiple_of(b * BLK + n * SUB_FWD, SUB_FWD), SUB_FWD) for n in range(BLK // SUB_FWD)]
        acts = []
        pre = [dot_nn(second_ref[rows, :], wm_ref[0, c]) for rows in parts]
        for rows, value in zip(parts, pre):
            act, slope = gelu_parts(value + hb_ref[c])
            act = act.astype(BF)
            act_ref[0, rows, :] = act
            slope_ref[0, rows, :] = slope.astype(BF)
            acts.append(act)
        outs = [dot_nn(act, wm_ref[1, c]) for act in acts]
        for rows, out in zip(parts, outs):
            acc_ref[rows, :] += out
        return carry

    lax.fori_loop(0, rows_total // BLK, block, 0)

    @pl.when(c == pl.num_programs(0) - 1)
    def _():
        for m in range(rows_total // TP):
            y = (acc_ref[m * TP : (m + 1) * TP, :] * live_rows(counts_ref, m)).astype(BF)
            y_ref[m] = y
            out_ref[m] = y[:TOK]
        keep.wait(wm_ref)

    step_end(tasks, 4)


def mlp_fwd(layer, rolled, counts, mid, table, weights, tasks=(), collective_id=None):
    r = mid.shape[0]
    n = r // TP
    keep = Keep((2, 4, D, D))
    return carried_call(
        functools.partial(mlp_fwd_body, layer, rolled, weights, keep, tasks),
        [keep, weights, *tasks],
        collective_id,
        grid=(4,),
        in_specs=[SMEM, whole((r, D)), whole(table.shape)],
        inputs=(counts, mid, table),
        out_specs=[whole((r, D)), per((r, D)), per((r, D)), whole((n, TP, D)), whole((n, TOK, D))],
        out_shape=[
            jax.ShapeDtypeStruct((r, D), BF),
            jax.ShapeDtypeStruct((4, r, D), BF),
            jax.ShapeDtypeStruct((4, r, D), BF),
            jax.ShapeDtypeStruct((n, TP, D), BF),
            jax.ShapeDtypeStruct((n, TOK, D), BF),
        ],
        scratch_shapes=[pltpu.VMEM((r, D), F32), pltpu.VMEM((4, 1, D), F32)],
        name="mlp_fwd",
        cost=pl.CostEstimate(flops=4 * r * D * 2048, bytes_accessed=12 << 20, transcendentals=0),
    )


def scatter_rows(place, value_ref, mine_ref, away_ref, index):
    core, dp = place
    for half, out_ref in enumerate((mine_ref, away_ref)):
        for n, j in enumerate(PLACES):
            start = (core ^ half) * 256 + (dp ^ j) * CHUNK
            out_ref[n, index] = value_ref[pl.ds(pl.multiple_of(start, CHUNK), CHUNK), :]


def where_in_plane(rolled):
    return (lax.axis_index("pipe"), lax.axis_index("dp")) if rolled else (jnp.int32(0), jnp.int32(0))


def by_shard(row):
    return jnp.concatenate([row[None, :, z * GL : (z + 1) * GL] for z in range(4)], 0)


def mlp_bwd_body(
    layer, rolled, weights, tasks, counts_ref, g_ref, act_ref, slope_ref, second_ref, mid_ref, table_ref,
    ghw_ref, ghw_away_ref, gow_ref, gow_away_ref, ghb_ref, gmid_ref, small_ref,
    gy_ref, gyt_ref, sect_ref, gp_ref, acc_ref, value_ref,
):
    c = pl.program_id(0)
    rows_total = mid_ref.shape[0]
    begin(weights, tasks)
    wm_ref = weights.kept[0]

    @pl.when(c == 0)
    def _():
        total = jnp.zeros((1, D), F32)
        for m in range(rows_total // TP):
            rows = slice(m * TP, (m + 1) * TP)
            if layer:
                gy_ref[rows, :] = jnp.zeros((TP, D), BF)
                gy = g_ref[m, lax.axis_index("pipe")].astype(F32) * alive_of(counts_ref, m)
                gy_ref[m * TP : m * TP + TOK, :] = gy.astype(BF)
            else:
                gy = g_ref[m].astype(F32) * live_rows(counts_ref, m)
                gy_ref[rows, :] = gy.astype(BF)
            total += jnp.sum(gy, 0, keepdims=True)
        small_ref[:, 0:1] = by_shard(total)
        gyt_ref[...] = gy_ref[...].T
        sect_ref[...] = second_ref[...].T
        acc_ref[...] = jnp.zeros_like(acc_ref)
        weights.wait()

    ghb_ref[0] = jnp.zeros_like(ghb_ref[0])

    def block(b, carry):
        parts = [pl.ds(pl.multiple_of(b * BLK + n * SUB_BWD, SUB_BWD), SUB_BWD) for n in range(BLK // SUB_BWD)]
        slopes = [dot_nt(gy_ref[rows, :], wm_ref[1, c]) for rows in parts]
        pres = []
        for rows, value in zip(parts, slopes):
            gp = value * slope_ref[0, rows, :].astype(F32)
            total = jnp.sum(gp, 0, keepdims=True)
            for n in range(4):
                ghb_ref[0, n : n + 1, :] += total[:, n * GL : (n + 1) * GL]
            gp = gp.astype(BF)
            gp_ref[rows, :] = gp
            pres.append(gp)
        outs = [dot_nt(gp, wm_ref[0, c]) for gp in pres]
        for rows, out in zip(parts, outs):
            acc_ref[rows, :] += out
        return carry

    lax.fori_loop(0, rows_total // BLK, block, 0)
    place = where_in_plane(rolled)
    value_ref[0] = dot_nn(sect_ref[...], gp_ref[...]).astype(BF)
    value_ref[1] = dot_nn(gyt_ref[...], act_ref[0]).astype(BF)
    scatter_rows(place, value_ref.at[0], ghw_ref, ghw_away_ref, 0)
    scatter_rows(place, value_ref.at[1], gow_ref, gow_away_ref, 0)

    @pl.when(c == pl.num_programs(0) - 1)
    def _():
        for call in planned(tasks, LATE):
            call()
        e = acc_ref[...]
        normed, inverse = normalize(mid_ref[...])
        small_ref[:, 2:3] = by_shard(jnp.sum(e * normed, 0, keepdims=True))
        small_ref[:, 3:4] = by_shard(jnp.sum(e, 0, keepdims=True))
        gmid = gy_ref[...].astype(F32) + norm_back(e, normed, inverse, along_model(table_ref, layer, MGAIN, rolled))
        small_ref[:, 1:2] = by_shard(jnp.sum(gmid, 0, keepdims=True))
        gmid_ref[...] = gmid

    step_end(tasks, 4)


PIECES = jax.ShapeDtypeStruct((4, 4, CHUNK, D), BF)


def mlp_bwd(layer, rolled, counts, g, act, slope, second, mid, table, weights, tasks=(), collective_id=None):
    r = mid.shape[0]
    pieces = pl.BlockSpec((4, 1, CHUNK, D), lambda i: (0, i, 0, 0))
    return carried_call(
        functools.partial(mlp_bwd_body, layer, rolled, weights, tasks),
        [weights, *tasks],
        collective_id,
        grid=(4,),
        in_specs=[SMEM, whole(g.shape), per((r, D)), per((r, D)), whole((r, D)), whole((r, D)), whole(table.shape)],
        inputs=(counts, g, act, slope, second, mid, table),
        out_specs=[pieces, pieces, pieces, pieces, per((4, GL)), whole((r, D)), whole((4, 4, GL))],
        out_shape=[
            PIECES, PIECES, PIECES, PIECES,
            jax.ShapeDtypeStruct((4, 4, GL), F32),
            jax.ShapeDtypeStruct((r, D), F32),
            jax.ShapeDtypeStruct((4, 4, GL), F32),
        ],
        scratch_shapes=[
            pltpu.VMEM((r, D), BF), pltpu.VMEM((D, r), BF), pltpu.VMEM((D, r), BF), pltpu.VMEM((r, D), BF),
            pltpu.VMEM((r, D), F32), pltpu.VMEM((2, D, D), BF),
        ],
        name="mlp_bwd",
        cost=pl.CostEstimate(flops=8 * r * D * 2048, bytes_accessed=16 << 20, transcendentals=0),
    )


def attn_bwd_body(
    layer, rolled, weights, tasks, x_ref, gmid_ref, fw_ref, qkv_ref, p_ref, ho_ref, table_ref,
    gin_ref, out_ref, ga_ref, ga_away_ref, gqv_ref, gtab_ref, small_ref,
    xs_ref, gw_ref, dq_ref, fwt_ref, hos_ref, gms_ref, value_ref, spread_ref, gather_ref, mask_ref, gain_ref,
):
    i = pl.program_id(0)
    last = pl.num_programs(0) - 1
    begin(weights, tasks)
    wq_ref, wpt_ref = weights.kept[:2]

    @pl.when(i == 0)
    def _():
        gqv_ref[...] = jnp.zeros_like(gqv_ref)
        gtab_ref[...] = jnp.zeros_like(gtab_ref)
        small_ref[...] = jnp.zeros_like(small_ref)
        spread_ref[...] = spread_map(layer * SHIFT)
        gather_ref[...] = gather_map(layer * SHIFT)
        mask_ref[...] = head_mask()
        gain_ref[...] = along_model(table_ref, layer, GAIN, rolled)
        if not layer:
            xs_ref[...] = jnp.zeros_like(xs_ref)

    gmid = gmid_ref[0]
    gmb = gmid.astype(BF)
    image = pl.ds(pl.multiple_of(i * TP, 16), TP)
    gms_ref[image, :] = gmb
    hos_ref[image, :] = ho_ref[0]
    base = pl.multiple_of(i * ROWS, ROWS)
    fwt_ref[:, pl.ds(base, ROWS)] = fw_ref[0].T

    @pl.when(i == 0)
    def _():
        weights.wait()

    heads = dot_nn(gmb, wpt_ref[...]).astype(BF)
    gw_ref[...] = dot_nn(spread_ref[...], heads).astype(BF)
    scale = HD ** (-0.5)

    def windows(n, carry):
        chains = [(n * AT_ONCE + w, g) for w in range(AT_ONCE) for g in range(4)]
        mask = mask_ref[...]

        def rows(w):
            return pl.ds(pl.multiple_of(w * WP, WP), WP)

        def part(w, g, n):
            return qkv_ref[0, rows(w), (3 * g + n) * GL : (3 * g + n + 1) * GL]

        bd_grads = [block_diagonal(gw_ref[rows(w), g * GL : (g + 1) * GL], mask) for w, g in chains]
        terms = [dot_nt(part(w, g, 2), bd_grad) for (w, g), bd_grad in zip(chains, bd_grads)]
        dvs = [dot_nn(p_ref[0, w, g], bd_grad) for (w, g), bd_grad in zip(chains, bd_grads)]
        scores = []
        for (w, g), term in zip(chains, terms):
            ptf = p_ref[0, w, g].astype(F32)
            pd = term * ptf
            ds = pd - ptf * jnp.sum(pd, 0, keepdims=True)
            gtab_ref[g] += ds
            scores.append(ds.astype(BF))
        dks = [dot_nn(ds, block_diagonal(part(w, g, 0), mask)) for (w, g), ds in zip(chains, scores)]
        dqs = [dot_tn(ds, part(w, g, 1)) for (w, g), ds in zip(chains, scores)]
        for (w, g), full, dk, dv in zip(chains, dqs, dks, dvs):
            dq = pick_diagonal(full) * scale
            out_rows = pl.ds(pl.multiple_of(base + w * WP, WP), WP)
            gqv_ref[g, 0:1] += jnp.sum(dq, 0, keepdims=True)
            gqv_ref[g, 1:2] += jnp.sum(dv, 0, keepdims=True)
            for n, value in enumerate((dq, dk, dv)):
                dq_ref[out_rows, (3 * g + n) * GL : (3 * g + n + 1) * GL] = value.astype(BF)
        return carry

    lax.fori_loop(0, NW // AT_ONCE, windows, 0)
    image_rows = pl.ds(base, ROWS)
    e = dot_nt(dq_ref[image_rows, :], wq_ref[...])
    e = dot_nn(gather_ref[...], e.astype(BF))
    if layer:
        x = x_ref[0].astype(F32)
    else:
        xs_ref[0:TOK, :] = x_ref[0, lax.axis_index("pipe")]
        x = xs_ref[...].astype(F32)
    normed, inverse = normalize(x)
    small_ref[:, 0:1] += by_shard(jnp.sum(e * normed, 0, keepdims=True))
    small_ref[:, 1:2] += by_shard(jnp.sum(e, 0, keepdims=True))
    gin = (gmid + norm_back(e, normed, inverse, gain_ref[...])).astype(BF)
    gin_ref[0] = gin
    out_ref[0] = gin[:TOK]

    @pl.when(i == last)
    def _():
        for call in planned(tasks, LATE):
            call()

        def chunk(n, carry):
            lanes = pl.ds(pl.multiple_of(n * D, D), D)
            value_ref[:, lanes] = dot_nn(fwt_ref[...], dq_ref[:, lanes]).astype(BF)
            return carry

        lax.fori_loop(0, 3, chunk, 0)
        value_ref[:, 3 * D :] = dot_nn(gms_ref[...].T, hos_ref[...]).astype(BF)
        core, dp = where_in_plane(rolled)
        for half, group_ref in enumerate((ga_ref, ga_away_ref)):
            for n, j in enumerate(PLACES):
                rows = pl.ds(pl.multiple_of((core ^ half) * 256 + (dp ^ j) * CHUNK, CHUNK), CHUNK)
                for g in range(4):
                    group_ref[n, g, :, : 3 * GL] = value_ref[rows, 3 * GL * g : 3 * GL * (g + 1)]
                    group_ref[n, g, :, 3 * GL :] = value_ref[rows, 3 * D + GL * g : 3 * D + GL * (g + 1)]

    step_end(tasks, 4)


def attn_bwd(layer, rolled, x, gmid, fw, qkv, p, ho, table, weights, tasks=(), collective_id=None):
    n = x.shape[0]
    return carried_call(
        functools.partial(attn_bwd_body, layer, rolled, weights, tasks),
        [weights, *tasks],
        collective_id,
        grid=(n,),
        in_specs=[
            per(x.shape[1:]), per((TP, D)), per((ROWS, D)), per((ROWS, 3 * D)), per((NW, 4, WP, GH * WP)), per((TP, D)),
            whole(table.shape),
        ],
        inputs=(x, gmid, fw, qkv, p, ho, table),
        out_specs=[
            per((TP, D)), per((TOK, D)), whole(PIECES.shape), whole(PIECES.shape), whole((4, 2, GL)), whole((4, WP, GH * WP)),
            whole((4, 2, GL)),
        ],
        out_shape=[
            jax.ShapeDtypeStruct((n, TP, D), BF),
            jax.ShapeDtypeStruct((n, TOK, D), BF),
            PIECES, PIECES,
            jax.ShapeDtypeStruct((4, 2, GL), F32),
            jax.ShapeDtypeStruct((4, WP, GH * WP), F32),
            jax.ShapeDtypeStruct((4, 2, GL), F32),
        ],
        scratch_shapes=[
            pltpu.VMEM((TP, D), BF), pltpu.VMEM((ROWS, D), BF), pltpu.VMEM((n * ROWS, 3 * D), BF), pltpu.VMEM((D, n * ROWS), BF),
            pltpu.VMEM((n * TP, D), BF), pltpu.VMEM((n * TP, D), BF), pltpu.VMEM((D, 4 * D), BF),
            pltpu.VMEM((ROWS, TP), BF), pltpu.VMEM((TP, ROWS), BF), pltpu.VMEM((GH * WP, GL), BF), pltpu.VMEM((1, D), F32),
        ],
        name="attn_bwd",
        cost=pl.CostEstimate(flops=n * 4 * 256 * 512 * 2600, bytes_accessed=n * 3 << 20, transcendentals=0),
    )


def plain_call(body, name, inputs, out_shape, scratch_shapes=(), grid=(), in_specs=None, out_specs=None, bytes_accessed=4 << 20):
    return pl.pallas_call(
        body,
        grid=grid,
        out_shape=out_shape,
        in_specs=in_specs or [pl.BlockSpec(memory_space=pltpu.VMEM)] * len(inputs),
        out_specs=out_specs or jax.tree.map(lambda _: pl.BlockSpec(memory_space=pltpu.VMEM), out_shape),
        scratch_shapes=list(scratch_shapes),
        name=name,
        compiler_params=pltpu.CompilerParams(vmem_limit_bytes=VMEM_LIMIT),
        cost_estimate=pl.CostEstimate(flops=bytes_accessed, bytes_accessed=bytes_accessed, transcendentals=0),
    )(*inputs)


def prepare_body(wqkv, wproj, gain, shift, qv, table, bproj, mgain, mshift, hb, ob, own_a_ref, lines_ref, rows_ref):
    own_a_ref[:, : 3 * GL] = dot_nn(wqkv[...], permutation(3 * GL, qkv_source, False)).astype(BF)
    own_a_ref[:, 3 * GL :] = wproj[...].T
    rows_ref[...] = jnp.zeros_like(rows_ref)
    for row, ref in ((GAIN, gain), (SHIFT_ROW, shift), (BPROJ, bproj), (MGAIN, mgain), (MSHIFT, mshift), (OB, ob)):
        rows_ref[row : row + 1, :] = ref[...].astype(F32)
    terms = dot_nn(jnp.broadcast_to(qv[...], (16, 2 * GL)), permutation(2 * GL, qv_source, False))
    hidden, places = hb[...].astype(F32), table[...].astype(F32)
    for n in range(2):
        rows_ref[QV + n : QV + n + 1, :] = terms[0:1, n * GL : (n + 1) * GL]
    for n in range(4):
        rows_ref[HB + n : HB + n + 1, :] = hidden[:, n * GL : (n + 1) * GL]
    rows_ref[TABLE : TABLE + 4, :] = places[:, :GL]
    rows_ref[TABLE + 4 : TABLE + 8, 0 : RELS - GL] = places[:, GL:]
    lines_ref[...] = rows_ref[...].astype(BF)


def prepare(wqkv, wproj, *small):
    return plain_call(
        prepare_body, "prepare", (wqkv, wproj, *small),
        [jax.ShapeDtypeStruct((D, D), BF), jax.ShapeDtypeStruct((LINES, GL), BF)], [pltpu.VMEM((LINES, GL), F32)],
    )


class Exchange(Part):
    def __init__(self, own, lines):
        shapes = [jax.ShapeDtypeStruct(part.shape, part.dtype) for part in own]
        shapes.append(jax.ShapeDtypeStruct((4, 2) + lines.shape, lines.dtype))
        super().__init__([*own, lines], shapes, sems(4) + sems(3) + [pltpu.SemaphoreType.DMA(())])

    def swap(self, n):
        core, _, _ = place_in_mesh()
        target = self.outs[n] if n < 3 else self.outs[3].at[0, core]
        return remote(self.ins[n], target, [sem.at[n] for sem in self.kept[:2]], "pipe", 1 - core)

    def keep(self):
        core, _, _ = place_in_mesh()
        return pltpu.make_async_copy(self.ins[3], self.outs[3].at[0, core], self.kept[4])

    def spread(self, k):
        _, _, shard = place_in_mesh()
        table = self.outs[3]
        return remote(table.at[0], table.at[k], [sem.at[k - 1] for sem in self.kept[2:4]], "tensor", lax.rem(shard + 4 - k, 4))


def gather_start(own, lines):
    exchange = Exchange(own, lines)
    near_a, near_h, far_a, far_h = Near(0, None, None), Near(0, None, None), Far(None), FarFirst(None)

    def body():
        for n, task in enumerate((near_a, near_h)):
            task.ins = [exchange.ins[n], exchange.outs[n]]
        far_a.ins, far_h.ins = [near_a.outs[0]], [near_h.outs[0]]
        greet()
        for n in (0, 3, 1, 2):
            exchange.swap(n).start()
        exchange.keep().start()
        exchange.swap(0).wait()
        near_a.start()
        exchange.keep().wait()
        exchange.swap(3).wait()
        for k in (1, 2, 3):
            exchange.spread(k).start()
        near_a.end()
        far_a.start()
        exchange.swap(1).wait()
        near_h.start()
        far_a.turn()
        far_a.rest()
        far_a.last()
        exchange.swap(2).wait()
        for k in (1, 2, 3):
            exchange.spread(k).wait()
        near_h.end()
        far_h.start()
        far_a.end()
        far_h.end()

    parts = [exchange, near_a, near_h, far_a, far_h]
    _, given = carried_call(
        body, parts, 0, grid=(), in_specs=[], inputs=(), out_specs=[], out_shape=[], scratch_shapes=[],
        name="gather_start", cost=pl.CostEstimate(flops=1 << 24, bytes_accessed=8 << 20, transcendentals=0),
    )
    others, given_a, given_h, far, first_h = given
    return others[:3], others[3], [given_a[0], *far], (given_h[0], first_h)


def onehot_of(rel_index):
    rel = jnp.pad(rel_index.T, ((0, WP - POS), (0, WP - POS)), constant_values=-1).reshape(-1)
    return (jnp.arange(2 * GL, dtype=jnp.int32)[:, None] == rel[None, :]).astype(BF)


def bias_tables(table, onehot):
    rows = table[:, :, TABLE : TABLE + 8].reshape(4, 2, 2, GH, GL).transpose(1, 0, 3, 2, 4).reshape(2 * H, 2 * GL)
    flat = jnp.dot(rows, onehot, preferred_element_type=F32)
    position = flat.reshape(2, 4, GH, WP, WP).transpose(0, 1, 3, 2, 4)
    shut = jnp.where(jnp.arange(WP) < POS, 0.0, SHUT).astype(F32)[:, None, None]
    return (position + shut).reshape(2, 4, WP, GH * WP)


def table_grad(gtab, rel_index):
    rel = jnp.pad(rel_index.T, ((0, WP - POS), (0, WP - POS)), constant_values=-1).reshape(-1)
    onehot = (rel[:, None] == jnp.arange(RELS, dtype=jnp.int32)[None, :]).astype(F32)
    flat = gtab.reshape(4, WP, GH, WP).transpose(0, 2, 1, 3).reshape(H, WP * WP)
    return jnp.dot(flat, onehot, precision=lax.Precision.HIGHEST).reshape(4, GH, RELS)


class Little(Part):
    def __init__(self, rows):
        self.rows = rows
        super().__init__(
            [],
            [jax.ShapeDtypeStruct((rows, GL), F32)],
            [pltpu.VMEM((2, 4, rows, GL), F32), pltpu.VMEM((4, rows, GL), F32), pltpu.VMEM((3, 4, rows, GL), F32),
             pltpu.VMEM((3, rows, GL), F32)]
            + sems() + sems(3) + sems(3) + [pltpu.SemaphoreType.DMA(())],
        )

    def pack(self, layers, tabs):
        _, _, shard = place_in_mesh()
        sums = self.kept[0]
        sums[...] = jnp.zeros_like(sums)
        for layer, (ghb, small_m, gqv, _, small_a) in enumerate(layers):
            for k in range(4):
                z = lax.rem(shard + k, 4)
                for row, source, n in (
                    (GAIN, small_a, 0), (SHIFT_ROW, small_a, 1), (OB, small_m, 0), (BPROJ, small_m, 1), (MGAIN, small_m, 2),
                    (MSHIFT, small_m, 3),
                ):
                    sums[layer, k, row : row + 1, :] = source[z, n : n + 1, :]
                sums[layer, k, QV : QV + 2, :] = gqv[k]
                sums[layer, k, HB : HB + 4, :] = ghb[k]
                rows = tabs[layer][GH * k : GH * (k + 1)]
                sums[layer, k, TABLE : TABLE + 4, :] = rows[:, 0:GL]
                sums[layer, k, TABLE + 4 : TABLE + 8, :] = rows[:, GL:]

    def over(self):
        core, _, _ = place_in_mesh()
        return remote(self.kept[0].at[1 - core], self.kept[1], self.kept[4:6], "pipe", 1 - core)

    def across(self, j):
        _, dp, _ = place_in_mesh()
        return remote(self.kept[1], self.kept[2].at[j - 1], [sem.at[j - 1] for sem in self.kept[6:8]], "dp", dp ^ j)

    def along(self, k):
        _, _, shard = place_in_mesh()
        return remote(
            self.kept[1].at[k], self.kept[3].at[k - 1], [sem.at[k - 1] for sem in self.kept[8:10]], "tensor", lax.rem(shard + k, 4)
        )

    def start(self):
        self.over().start()

    def second(self):
        core, _, _ = place_in_mesh()
        self.over().wait()
        self.kept[1][...] += self.kept[0][core]
        for j in (1, 2, 3):
            self.across(j).start()

    def third(self):
        for j in (1, 2, 3):
            self.across(j).wait()
        self.kept[1][...] += self.kept[2][0] + self.kept[2][1] + self.kept[2][2]
        for k in (1, 2, 3):
            self.along(k).start()

    def end(self):
        for k in (1, 2, 3):
            self.along(k).wait()
        self.kept[2][0, 0] = self.kept[1][0] + self.kept[3][0] + self.kept[3][1] + self.kept[3][2]
        copy = pltpu.make_async_copy(self.kept[2].at[0, 0], self.outs[0], self.kept[10])
        copy.start()
        copy.wait()


class Settle(Part):
    def __init__(self):
        super().__init__(
            [],
            [jax.ShapeDtypeStruct((3, D, D), BF)],
            [pltpu.VMEM((3, D, D), BF)] + sems(3) + [pltpu.SemaphoreType.DMA((3,)), pltpu.SemaphoreType.DMA((3,))],
        )

    def rows(self, core):
        return pl.ds(core * 256, 256)

    def send(self, source, n, core):
        return remote(source.at[self.rows(core)], self.outs[0].at[n, self.rows(core)], [sem.at[n] for sem in self.kept[1:3]], "pipe", 1 - core)

    def load(self, source, n, core):
        return pltpu.make_async_copy(source.at[self.rows(core)], self.kept[0].at[n, self.rows(core)], self.kept[3].at[n])

    def store(self, n, core):
        return pltpu.make_async_copy(self.kept[0].at[n, self.rows(core)], self.outs[0].at[n, self.rows(core)], self.kept[4].at[n])

    def start(self, matrices, layer, which):
        def action(core):
            for n in which:
                (self.load if core == layer else self.send)(matrices[n], n, core).start()

        by_core(action)

    def pass_on(self, matrices, layer, which):
        @pl.when(lax.axis_index("pipe") == layer)
        def _():
            for n in which:
                self.load(matrices[n], n, layer).wait()
                self.store(n, layer).start()

    def end(self, matrices):
        def action(core):
            for n in range(3):
                self.store(n, core).wait()
                self.send(matrices[1 - core][n], n, core).wait()

        by_core(action)


def table_sums(gtab_ref, onehot_ref, half_ref, pairs_ref, out_ref):
    for g in range(4):
        for n in range(2):
            half_ref[...] = gtab_ref[g, :, n * GL : (n + 1) * GL]
            even = half_ref[pl.ds(0, WP // 2, 2), :]
            odd = half_ref[pl.ds(1, WP // 2, 2), :]
            for m in range(2):
                lanes = slice(m * WP, (m + 1) * WP)
                pairs_ref[:, g * GH + 2 * n + m, :] = jnp.concatenate([even[:, lanes], odd[:, lanes]], 1)

    def add(n, total):
        pair = pairs_ref[n]
        high = pair.astype(BF)
        low = (pair - high.astype(F32)).astype(BF)
        places = onehot_ref[:, pl.ds(pl.multiple_of(n * GL, GL), GL)]
        return total + (dot_nt(high, places) + dot_nt(low, places))

    out_ref[...] = lax.fori_loop(0, WP // 2, add, jnp.zeros((H, 2 * GL), F32))


def reduce_end(attention0, turned0, totals_a1, shared1, grads_in, small, onehot):
    halves = ((0, 32), (32, 32))
    first = [ReduceFirst(attention0, rows=rows) for rows in halves]
    second = [ReduceSecond(size=32) for _ in halves]
    share = [Share(rows=halves[0])]
    share.append(Share(rows=halves[1], target=share[0]))
    onward_m = [ReduceOnward(given) for given in turned0]
    second_m, share_m = [ReduceSecond(), ReduceSecond()], [Share(), Share()]
    second_a1, share_a1, done_m1 = ReduceSecond(totals_a1), Share(), Part(shared1)
    settle, little, deliver, places = Settle(), Little(24), Deliver(grads_in), Stored(onehot)

    def body(*refs):
        layers, (tabs_ref, pairs_ref, half_ref) = (refs[:5], refs[5:10]), refs[10:]
        for n in range(2):
            second[n].ins, share[n].ins = [first[n].total], [second[n].kept[0]]
            second_m[n].ins, share_m[n].ins = [onward_m[n].kept[0]], [second_m[n].kept[0]]
        share_a1.ins = [second_a1.kept[0]]
        done = (
            [share[0].outs[0], share_m[0].outs[0], share_m[1].outs[0]],
            [share_a1.outs[0], done_m1.ins[0], done_m1.ins[1]],
        )

        def tab(layer):
            table_sums(layers[layer][3], places.kept[0], half_ref, pairs_ref, tabs_ref.at[layer])

        greet()
        for task in (*first, *onward_m):
            task.start()
        places.load()
        first[0].cores()
        first[1].cores()
        second_a1.start()
        settle.start(done[1], 1, (1, 2))
        deliver.start()
        places.wait()
        tab(1)
        for n in range(2):
            onward_m[n].close()
            second_m[n].start()
        first[0].turn()
        tab(0)
        little.pack(layers, tabs_ref)
        little.start()
        first[1].turn()
        second_a1.close()
        share_a1.start()
        settle.pass_on(done[1], 1, (1, 2))
        first[0].close()
        second[0].start()
        little.second()
        first[1].close()
        second[1].start()
        for n in range(2):
            second_m[n].close()
            share_m[n].start()
        share_a1.end()
        settle.start(done[1], 1, (0,))
        little.third()
        settle.pass_on(done[1], 1, (0,))
        for n in range(2):
            second[n].close()
            share[n].start()
        for n in range(2):
            share_m[n].end()
        settle.start(done[0], 0, (1, 2))
        little.end()
        deliver.end()
        settle.pass_on(done[0], 0, (1, 2))
        for n in range(2):
            share[n].end()
        settle.start(done[0], 0, (0,))
        settle.pass_on(done[0], 0, (0,))
        settle.end(done)

    parts = [*first, *second, *share, *onward_m, *second_m, *share_m, second_a1, share_a1, done_m1, settle, little, deliver, places]
    _, given = carried_call(
        body, parts, 7, grid=(), in_specs=[pl.BlockSpec(memory_space=pltpu.VMEM)] * 10, inputs=small, out_specs=[], out_shape=[],
        scratch_shapes=[pltpu.VMEM((2, H, 2 * GL), F32), pltpu.VMEM((WP // 2, H, GL), F32), pltpu.VMEM((WP, GL), F32)],
        name="reduce_end", cost=pl.CostEstimate(flops=1 << 24, bytes_accessed=8 << 20, transcendentals=0),
    )
    by_part = dict(zip(map(id, parts), given))
    return by_part[id(settle)][0], by_part[id(little)][0], by_part[id(deliver)][0]


def finish_body(
    matrix_ref, lines_ref, out0_ref, out1_ref, out_came_ref, gin0_ref, gin1_ref, gin_came_ref,
    block_out_ref, input_grad_ref, gqkv_ref, gproj_ref, ghw_ref, gow_ref, gain_ref, shift_ref, qv_ref, table_ref, bproj_ref,
    mgain_ref, mshift_ref, hb_ref, ob_ref,
):
    def images(core):
        for ref, own, came in (
            (block_out_ref, (out0_ref, out1_ref), out_came_ref), (input_grad_ref, (gin0_ref, gin1_ref), gin_came_ref)
        ):
            ref[0, 0, core] = own[core][0]
            ref[0, 0, 1 - core] = came[0]

    by_core(images)

    @pl.when(pl.program_id(0) == 0)
    def _():
        gqkv_ref[0] = dot_nn(matrix_ref[0, :, : 3 * GL], permutation(3 * GL, qkv_source, True))
        gproj_ref[0] = matrix_ref[0, :, 3 * GL :].T.astype(F32)
        lines = lines_ref[...]
        for row, ref in (
            (GAIN, gain_ref), (SHIFT_ROW, shift_ref), (BPROJ, bproj_ref), (MGAIN, mgain_ref), (MSHIFT, mshift_ref), (OB, ob_ref)
        ):
            ref[...] = lines[row : row + 1]
        qv_ref[...] = jnp.concatenate(
            [lines[QV + n : QV + n + 1, h * HD : (h + 1) * HD] for h in range(GH) for n in range(2)], 1
        )
        table_ref[0] = jnp.concatenate([lines[TABLE : TABLE + 4], lines[TABLE + 4 : TABLE + 8, : RELS - GL]], 1)
        hb_ref[...] = jnp.concatenate([lines[HB + n : HB + n + 1] for n in range(4)], 1)

    @pl.when(pl.program_id(0) == 1)
    def _():
        ghw_ref[0] = matrix_ref[1].astype(F32)
        gow_ref[0] = matrix_ref[2].T.astype(F32)


def finish(matrices, lines, out0, out1, out_came, gin0, gin1, gin_came):
    n = out0.shape[0]
    image = per((TOK, D))
    both = pl.BlockSpec((1, 1, 2, TOK, D), lambda i: (0, i, 0, 0, 0))
    shapes = [
        (1, D, 3 * GL), (1, GL, D), (1, D, D), (1, D, D), (1, GL), (1, GL), (1, 2 * GL), (1, GH, RELS), (1, GL), (1, GL), (1, GL),
        (1, D), (1, GL),
    ]
    return plain_call(
        finish_body, "finish", (matrices, lines, out0, out1, out_came, gin0, gin1, gin_came),
        [jax.ShapeDtypeStruct((1, n, 2, TOK, D), BF)] * 2 + [jax.ShapeDtypeStruct(shape, F32) for shape in shapes],
        grid=(n,),
        in_specs=[whole(matrices.shape), whole(lines.shape)] + [image] * 6,
        out_specs=[both, both] + [whole(shape) for shape in shapes],
    )


def layer_forward(layer, rolled, x, counts, table, bias, weights, tasks, ids):
    (fw, qkv, p, ho, mid), given = attn_fwd(layer, rolled, x, table, bias, weights[0](), tasks[0](), ids[0])
    mid = mid.reshape(-1, D)
    kept_a, given = given[0], given[1:]
    (second, act, slope, y, out), more = mlp_fwd(layer, rolled, counts, mid, table, weights[1](given), tasks[1](given), ids[1])
    return y, out, (x, fw, qkv, p, ho, mid, second, act, slope, kept_a, more[0]), given, more[1:]


def layer_backward(layer, rolled, cot, kept, counts, table, tasks, ids):
    x, fw, qkv, p, ho, mid, second, act, slope, kept_a, kept_m = kept
    if not layer:
        cot = cot.reshape(-1, TP, D)
    (ghw, ghw_away, gow, gow_away, ghb, gmid, small_m), given = mlp_bwd(
        layer, rolled, counts, cot, act, slope, second, mid, table, Stored(*kept_m), tasks[0](), ids[0]
    )
    big_m = ((ghw, ghw_away), (gow, gow_away))
    (gin, out, ga, ga_away, gqv, gtab, small_a), more = attn_bwd(
        layer, rolled, x, gmid.reshape(-1, TP, D), fw, qkv, p, ho, table, Stored(*kept_a), tasks[1](big_m, given), ids[1]
    )
    return gin, out, ((ga, ga_away), *big_m), (ghb, small_m, gqv, gtab, small_a), given, more


SMALL_ROWS = ((GAIN, 1), (SHIFT_ROW, 1), (QV, 2), (TABLE, 8), (BPROJ, 1), (MGAIN, 1), (MSHIFT, 1), (HB, 4), (OB, 1))


def on_lines(small_in):
    whole_of = [lax.all_gather(lax.all_gather(member[0], "tensor", axis=0, tiled=True), "pipe") for member in small_in]
    gain, shift, qv, table, bproj, mgain, mshift, hb, ob = whole_of

    def lines(member):
        return member.reshape(2, 4, -1, GL)

    qv = qv.reshape(2, 4, GH, 2, HD).transpose(0, 1, 3, 2, 4)
    table = jnp.pad(table, ((0, 0), (0, 0), (0, 2 * GL - RELS))).reshape(2, 4, GH, 2, GL).transpose(0, 1, 3, 2, 4)
    rows = jnp.concatenate([lines(part) for part in (gain, shift, qv, table, bproj, mgain, mshift, hb, ob)], 2)
    return jnp.pad(rows, ((0, 0), (0, 0), (0, LINES - rows.shape[2]), (0, 0))).transpose(1, 0, 2, 3)


def qkv_order(w):
    lead = w.shape[:-1]
    return jnp.swapaxes(w.reshape(*lead, GH, 3, HD), -3, -2).reshape(*lead, 3 * GL)


def general(core, images, cotangent, counts, rel_index, small_in, big_in):
    def both(member, axis):
        return lax.all_gather(lax.all_gather(member[0], "tensor", axis=axis, tiled=True), "pipe")

    table = on_lines(small_in)
    bias = bias_tables(table, onehot_of(rel_index))
    gathered = [both(member, axis) for member, axis in zip(big_in, (1, 0, 1, 0))]
    weights = []
    for l in range(2):
        wqkv, wproj, hw, ow = (pair[l] for pair in gathered)
        wqkv = qkv_order(wqkv.reshape(D, 4, 3 * GL).transpose(1, 0, 2))
        wa = jnp.concatenate([wqkv, wproj.reshape(4, GL, D).transpose(0, 2, 1)], 2)[None]
        wm = jnp.stack([hw.reshape(D, 4, -1).transpose(1, 0, 2), ow.reshape(4, -1, D)])
        weights.append((lambda *_, wa=wa: Weights(1, 0, whole=wa), lambda *_, wm=wm: Weights(2, 0, whole=wm)))
    none, back_none, ids = (lambda: [], lambda given: []), (lambda: [], lambda *_: []), (None, None)
    y0, out0, kept0, _, _ = layer_forward(0, False, images, counts, table, bias[0], weights[0], none, ids)
    _, out1, kept1, _, _ = layer_forward(1, False, y0, counts, table, bias[1], weights[1], none, ids)
    g1, gin1, big1, small1, _, _ = layer_backward(1, False, cotangent, kept1, counts, table, back_none, ids)
    _, gin0, big0, small0, _, _ = layer_backward(0, False, g1, kept0, counts, table, back_none, ids)
    first_core = core == 0

    def deliver(mine0, mine1):
        came = lax.ppermute(jnp.where(first_core, mine1, mine0), "pipe", [(0, 1), (1, 0)])
        mine = jnp.where(first_core, mine0, mine1)
        return jnp.stack([jnp.where(first_core, mine, came), jnp.where(first_core, came, mine)], 1)[None]

    def matrix_of(pair):
        parts = [part[jnp.array([PLACES.index(j) for j in range(4)])] for part in pair]
        return jnp.concatenate(parts).transpose(1, 0, 2, 3).reshape(4, D, D)

    def full(big):
        ga, ghw, gow = (matrix_of(pair) for pair in big)
        gqkv = jnp.swapaxes(ga[:, :, : 3 * GL].reshape(4, D, 3, GH, HD), 2, 3).reshape(4, D, 3 * GL)
        return (
            gqkv.transpose(1, 0, 2).reshape(D, 3 * D), ga[:, :, 3 * GL :].transpose(0, 2, 1).reshape(D, D),
            ghw.transpose(1, 0, 2).reshape(D, -1), gow.transpose(0, 2, 1).reshape(-1, D),
        )

    def reduced(pair, axis):
        mine = lax.psum_scatter(jnp.stack(pair), "pipe", scatter_dimension=0, tiled=False)
        mine = lax.psum_scatter(mine, "tensor", scatter_dimension=axis, tiled=True)
        return lax.psum(mine, "dp").astype(F32)[None]

    gqkv, gproj, ghw, gow = (reduced(pair, axis) for pair, axis in zip(zip(full(big0), full(big1)), (1, 0, 1, 0)))

    def vectors(terms):
        ghb, small_m, gqv, gtab, small_a = terms
        qv = jnp.swapaxes(gqv.reshape(4, 2, GH, HD), 1, 2).reshape(-1)
        tab = table_grad(gtab, rel_index).reshape(H, RELS)
        parts = (small_a[:, 0], small_a[:, 1], qv, tab, small_m[:, 1], small_m[:, 2], small_m[:, 3], ghb, small_m[:, 0])
        return jnp.concatenate([part.reshape(-1) for part in parts])

    totals = lax.psum(jnp.stack([vectors(small0), vectors(small1)]), ("pipe", "dp", "tensor"))
    mine = jnp.where(first_core, totals[0], totals[1])
    outs, at = [], 0
    for member in small_in:
        shape = member.shape[1:]
        whole_shape = (shape[0] * lax.axis_size("tensor"),) + tuple(shape[1:])
        size = math.prod(whole_shape)
        piece = mine[at : at + size].reshape(whole_shape)
        outs.append(lax.dynamic_slice_in_dim(piece, lax.axis_index("tensor") * shape[0], shape[0], 0)[None])
        at += size
    return deliver(out0, out1), deliver(gin0, gin1), (gqkv, gproj, ghw, gow), outs


def four_by_four(images, cotangent, counts, rel_index, small_in, big_in):
    own_a, lines = prepare(big_in[0][0], big_in[1][0], *[member[0] if member.ndim == 3 else member for member in small_in])
    own = (own_a, big_in[2][0], big_in[3][0])
    onehot = onehot_of(rel_index)
    other, table, pieces_a0, hidden0 = gather_start(own, lines)
    bias = bias_tables(table, onehot)

    def near(n, layer, **how):
        return Near(layer, own[n], other[n], **how)

    def weights(layer, which, pieces):
        return Weights(len(which), layer, own=[own[n] for n in which], other=[other[n] for n in which], pieces=pieces)

    def out_tasks(layer):
        near_o = near(2, layer, plan=((1, "finish"),))
        far_o = Far(None, source=near_o, deferred=True, plan=((1, "start"), (2, "turn"), (3, "rest"), (3, "last")))
        return [near_o, far_o]

    def weights_of_first(layer, pieces):
        return lambda: weights(layer, (0,), [pieces])

    y0, out0, kept0, given, more = layer_forward(
        0, True, images, counts, table, bias[0],
        (weights_of_first(0, pieces_a0),
         lambda given: weights(0, (1, 2), [gathered(*hidden0, given[1]), [given[2][0], *given[3]]])),
        (lambda: [FarSecond(hidden0[1], plan=((1, "last"),)), *out_tasks(0), near(0, 1, deferred=True, plan=((2, "start"),))],
         lambda given: [Far(given[4][0], plan=((1, "turn"), (3, "rest"), (3, "last"))), near(1, 1, deferred=True, plan=((1, "start"),))]),
        (1, 2),
    )
    pieces_a1, near_h1 = [given[4][0], *more[1]], more[2][0]
    _, out1, kept1, _, _ = layer_forward(
        1, True, y0, counts, table, bias[1],
        (weights_of_first(1, pieces_a1),
         lambda given: weights(1, (1, 2), [[near_h1, *given[1]], [given[2][0], *given[3]]])),
        (lambda: [Far(near_h1, plan=((1, "turn"), (2, "rest"), (2, "last"))), *out_tasks(1)], lambda given: []), (3, None),
    )

    def mlp_reduce(big_m):
        return [ReduceTurn(big_m[0], plan=((0, "cores"),)), ReduceTurn(big_m[1], plan=((1, "cores"),))]

    g1, gin1, big1, small1, given, more = layer_backward(
        1, True, cotangent, kept1, counts, table, (lambda: [Deliver([out0, out1])], lambda big_m, given: mlp_reduce(big_m)), (4, 5)
    )
    out_came, turned1 = given[1][0], more[1:3]

    def last_tasks(big_m, given):
        seconds = [ReduceSecond(given[2][0], plan=((1, "close"),)), ReduceSecond(given[3][0], plan=((LATE, "close"),))]
        shares = [Share(source=seconds[0], plan=((1, "start"),)), Share(source=seconds[1], plan=((LATE, "start"),))]
        return [*mlp_reduce(big_m), ReduceOnward(given[1]), *seconds, *shares]

    _, gin0, big0, small0, given, more = layer_backward(
        0, True, g1, kept0, counts, table,
        (
            lambda: [ReduceTurn(big1[0], plan=((0, "cores"),)), *[ReduceOnward(turned) for turned in turned1]],
            last_tasks,
        ),
        (6, 8),
    )
    turned0, totals_a1, shared1 = more[1:3], more[3][0], (more[6][0], more[7][0])
    matrices, lines, gin_came = reduce_end(big0[0], turned0, totals_a1, shared1, [gin0, gin1], [*small0, *small1], onehot)
    block_out, input_grad, gqkv, gproj, ghw, gow, *outs = finish(matrices, lines, out0, out1, out_came, gin0, gin1, gin_came)
    return block_out, input_grad, (gqkv, gproj, ghw, gow), outs


def local(
    images, cotangent, counts, rel_index, pre_attn_gain, pre_attn_bias, qkv_weight, qv_bias, bias_table, proj_weight, proj_bias,
    pre_mlp_gain, pre_mlp_bias, hidden_weight, hidden_bias, out_weight, out_bias,
):
    assert images.shape[1] == 2, images.shape
    small_in = (pre_attn_gain, pre_attn_bias, qv_bias, bias_table, proj_bias, pre_mlp_gain, pre_mlp_bias, hidden_bias, out_bias)
    big_in = (qkv_weight, proj_weight, hidden_weight, out_weight)
    if lax.axis_size("tensor") == 4 and lax.axis_size("dp") == 4:
        block_out, input_grad, big, small = four_by_four(images, cotangent, counts, rel_index, small_in, big_in)
    else:
        block_out, input_grad, big, small = general(
            lax.axis_index("pipe"), images, cotangent, counts, rel_index, small_in, big_in
        )
    gqkv, gproj, ghw, gow = big
    gain_g, shift_g, qv_g, table_g, bproj_g, mgain_g, mshift_g, hb_g, ob_g = small
    return (
        block_out, input_grad, gain_g, shift_g, gqkv, qv_g, table_g, gproj, bproj_g, mgain_g, mshift_g, ghw, hb_g, gow, ob_g,
    )


def solution(mesh):
    return jax.shard_map(
        local,
        mesh=mesh,
        in_specs=(
            P(None, ("dp", "tensor"), None, None),
            P(None, ("dp", "tensor"), None, None),
            P(None, "dp"),
            P(),
            P("pipe", "tensor"),
            P("pipe", "tensor"),
            P("pipe", None, "tensor"),
            P("pipe", "tensor"),
            P("pipe", "tensor", None),
            P("pipe", "tensor", None),
            P("pipe", "tensor"),
            P("pipe", "tensor"),
            P("pipe", "tensor"),
            P("pipe", None, "tensor"),
            P("pipe", "tensor"),
            P("pipe", "tensor", None),
            P("pipe", "tensor"),
        ),
        out_specs=(
            P("pipe", None, ("dp", "tensor"), None, None),
            P("pipe", None, ("dp", "tensor"), None, None),
            P("pipe", "tensor"),
            P("pipe", "tensor"),
            P("pipe", None, "tensor"),
            P("pipe", "tensor"),
            P("pipe", "tensor", None),
            P("pipe", "tensor", None),
            P("pipe", "tensor"),
            P("pipe", "tensor"),
            P("pipe", "tensor"),
            P("pipe", None, "tensor"),
            P("pipe", "tensor"),
            P("pipe", "tensor", None),
            P("pipe", "tensor"),
        ),
        check_vma=False,
    )
```

```python
import functools
import math

import jax
import jax.numpy as jnp
from jax import lax
from jax.experimental import pallas as pl
from jax.experimental.pallas import tpu as pltpu
from jax.sharding import PartitionSpec as P

D = 512
H = 16
HD = 32
WIN = 7
GRID = 14
SHIFT = 3
TOK = 196
RELS = 169
POS = WIN * WIN
NW = 4
WP = 64
TP = 208
ROWS = NW * WP
GH = 4
GL = GH * HD
BLK = 832
SUB_FWD = 208
SUB_BWD = 416
CHUNK = 64
AT_ONCE = 2
LATE = "late"
LINES = 32
GAIN, SHIFT_ROW, QV, TABLE, BPROJ, MGAIN, MSHIFT, HB, OB = 0, 1, 2, 4, 12, 13, 14, 15, 19
PLACES = (1, 3, 2, 0)
EPSILON = 1e-05
MASK_VALUE = -100.0
SHUT = -1e30
F32 = jnp.float32
BF = jnp.bfloat16
ANY = pl.BlockSpec(memory_space=pl.ANY)
VMEM_LIMIT = 60 << 20


def dot_nn(a, b):
    return lax.dot_general(a, b, (((1,), (0,)), ((), ())), preferred_element_type=F32)


def dot_nt(a, b):
    return lax.dot_general(a, b, (((1,), (1,)), ((), ())), preferred_element_type=F32)


def dot_tn(a, b):
    return lax.dot_general(a, b, (((0,), (0,)), ((), ())), preferred_element_type=F32)


def iota(shape, axis):
    return lax.broadcasted_iota(jnp.int32, shape, axis)


def normalize(rows):
    center = rows - jnp.mean(rows, -1, keepdims=True)
    inverse = lax.rsqrt(jnp.mean(center * center, -1, keepdims=True) + EPSILON)
    return center * inverse, inverse


def norm_back(grad_out, normed, inverse, gain):
    scaled = grad_out * gain
    return inverse * (
        scaled
        - jnp.mean(scaled, -1, keepdims=True)
        - normed * jnp.mean(scaled * normed, -1, keepdims=True)
    )


def remote(source, target, sems, axis, index):
    return pltpu.make_async_remote_copy(
        src_ref=source, dst_ref=target, send_sem=sems[0], recv_sem=sems[1], device_id={axis: index},
        device_id_type=pl.DeviceIdType.MESH,
    )


def place_in_mesh():
    return lax.axis_index("pipe"), lax.axis_index("dp"), lax.axis_index("tensor")


def greet():
    core, dp, shard = place_in_mesh()
    barrier = pltpu.get_barrier_semaphore()

    def signal(axis, index):
        pl.semaphore_signal(barrier, inc=1, device_id={axis: index}, device_id_type=pl.DeviceIdType.MESH)

    signal("pipe", 1 - core)
    for k in (1, 2, 3):
        signal("dp", dp ^ k)
        signal("tensor", lax.rem(shard + k, 4))
    pl.semaphore_wait(barrier, 7)


def quarter(half, j):
    core, dp, _ = place_in_mesh()
    return pl.ds(pl.multiple_of((core ^ half) * 256 + (dp ^ j) * CHUNK, CHUNK), CHUNK)


def by_core(action):
    for which in (0, 1):

        @pl.when(lax.axis_index("pipe") == which)
        def _():
            action(which)


def sems(*shape):
    return [pltpu.SemaphoreType.DMA(shape), pltpu.SemaphoreType.DMA(shape)]


class Part:
    plan = ()
    deferred = False

    def flush(self):
        pass

    def __init__(self, inputs=(), outputs=(), scratch=()):
        self.inputs, self.outputs, self.scratch = list(inputs), list(outputs), list(scratch)

    def bind(self, ins, outs, kept):
        self.ins, self.outs, self.kept = ins, outs, kept


class Weights(Part):
    def __init__(self, count, layer, whole=None, own=None, other=None, pieces=None):
        self.count, self.layer, self.whole = count, layer, whole
        inputs = [whole] if whole is not None else [*own, *other, *[piece for group in pieces for piece in group]]
        super().__init__(inputs, (), [pltpu.VMEM((count, 4, D, D), BF), pltpu.SemaphoreType.DMA((9 * count,))])

    def shard(self, mine, b):
        store, sem = self.kept
        if self.whole is not None:
            return pltpu.make_async_copy(self.ins[0].at[b, 0], store.at[b, 0], sem.at[b * 9])
        owns, others = self.ins[: self.count], self.ins[self.count : 2 * self.count]
        return pltpu.make_async_copy((owns if mine else others)[b], store.at[b, 0], sem.at[b * 9])

    def rest(self):
        store, sem = self.kept
        if self.whole is not None:
            return [
                pltpu.make_async_copy(self.ins[0].at[b, pl.ds(1, 3)], store.at[b, pl.ds(1, 3)], sem.at[b * 9 + 1])
                for b in range(self.count)
            ]
        return [
            pltpu.make_async_copy(
                self.ins[2 * self.count + b * 8 + half * 4 + j], store.at[b, pl.ds(1, 3), quarter(half, j), :],
                sem.at[b * 9 + half * 4 + j + 1],
            )
            for b in range(self.count)
            for half in range(2)
            for j in range(4)
        ]

    def load(self):
        if self.whole is not None:
            for b in range(self.count):
                self.shard(True, b).start()
        else:

            def shards(core):
                for b in range(self.count):
                    self.shard(core == self.layer, b).start()

            by_core(shards)
        if self.count == 1:
            self.load_rest()

    def load_rest(self):
        for copy in self.rest():
            copy.start()

    def wait_shard(self):
        for b in range(self.count):
            self.shard(True, b).wait()

    def wait_rest(self):
        for copy in self.rest():
            copy.wait()


class Stored(Part):
    def __init__(self, *arrays):
        super().__init__(arrays, (), [pltpu.VMEM(a.shape, a.dtype) for a in arrays] + [pltpu.SemaphoreType.DMA((len(arrays),))])

    def copies(self):
        return [pltpu.make_async_copy(ref, kept, self.kept[-1].at[n]) for n, (ref, kept) in enumerate(zip(self.ins, self.kept))]

    def load(self):
        for copy in self.copies():
            copy.start()

    def wait(self):
        for copy in self.copies():
            copy.wait()


class Keep(Part):
    def __init__(self, *shapes):
        super().__init__((), [jax.ShapeDtypeStruct(shape, BF) for shape in shapes], [pltpu.SemaphoreType.DMA((len(shapes),))])

    def copies(self, refs):
        return [pltpu.make_async_copy(ref, out, self.kept[0].at[n]) for n, (ref, out) in enumerate(zip(refs, self.outs))]

    def start(self, *refs):
        for copy in self.copies(refs):
            copy.start()

    def wait(self, *refs):
        for copy in self.copies(refs):
            copy.wait()


class Near(Part):
    def __init__(self, layer, own, other, plan=(), deferred=False):
        self.layer, self.plan, self.deferred = layer, plan, deferred
        inputs = [] if own is None else [own, other]
        super().__init__(inputs, [jax.ShapeDtypeStruct((3, CHUNK, D), BF)], sems(3))

    def copy(self, mine, k):
        _, _, shard = place_in_mesh()
        source = self.ins[0 if mine else 1].at[quarter(0, 0), :]
        return remote(source, self.outs[0].at[k - 1], [sem.at[k - 1] for sem in self.kept], "tensor", lax.rem(shard + 4 - k, 4))

    def start(self):
        def sends(core):
            for k in (2, 1, 3):
                self.copy(core == self.layer, k).start()

        by_core(sends)

    def finish(self):
        for k in (1, 2, 3):
            self.copy(True, k).wait()

    def end(self):
        if not any(what == "finish" for _, what in self.plan):
            self.finish()


class Far(Part):
    def __init__(self, near, plan=(), source=None, deferred=False):
        self.plan, self.source, self.deferred = plan, source, deferred
        shape = jax.ShapeDtypeStruct((3, CHUNK, D), BF)
        super().__init__([] if near is None else [near], [shape] * 7, sems(2, 2) + sems(2) + sems(4))

    def rows(self, j):
        return pl.ds((j - 1) * 32, 32)

    def across(self, j, half):
        _, dp, _ = place_in_mesh()
        rows = self.rows(j if half == 0 else 3 - j)
        return remote(
            self.ins[0].at[:, rows], self.outs[j - 1].at[:, rows], [sem.at[j - 1, half] for sem in self.kept[:2]], "dp", dp ^ j
        )

    def onward(self, j):
        _, dp, _ = place_in_mesh()
        rows = self.rows(j)
        return remote(
            self.outs[j - 1].at[:, rows], self.outs[2].at[:, rows], [sem.at[j - 1] for sem in self.kept[2:4]], "dp", dp ^ (3 - j)
        )

    def over(self, j):
        core, _, _ = place_in_mesh()
        source = self.ins[0] if j == 0 else self.outs[j - 1]
        return remote(source, self.outs[3 + j], [sem.at[j] for sem in self.kept[4:]], "pipe", 1 - core)

    def start(self):
        for half in (0, 1):
            for j in (1, 2):
                self.across(j, half).start()
        self.over(0).start()

    def turn(self):
        for j in (1, 2):
            self.across(j, 0).wait()
        for j in (1, 2):
            self.onward(j).start()

    def rest(self):
        for j in (1, 2):
            self.across(j, 1).wait()
            self.over(j).start()

    def last(self):
        for j in (1, 2):
            self.onward(j).wait()
        self.over(3).start()

    def end(self):
        for j in range(4):
            self.over(j).wait()


class ReduceFirst(Part):
    def __init__(self, pair, plan=(), rows=(0, CHUNK)):
        self.plan, (self.start_row, self.size) = plan, rows
        size = self.size
        half = pltpu.VMEM((4, 4, size, D), BF)
        super().__init__(
            pair,
            [jax.ShapeDtypeStruct((4, size, D), BF)],
            [half, half, pltpu.VMEM((2, 2, 2, size, D), BF), pltpu.VMEM((2, 2, size, D), BF), pltpu.VMEM((4, size, D), BF)]
            + sems() + sems(2) + sems(2) + [pltpu.SemaphoreType.DMA(()), pltpu.SemaphoreType.DMA(())],
        )

    def bind(self, ins, outs, kept):
        super().bind(ins, outs, kept)
        self.mine, self.came, self.first, self.second, self.total = kept[:5]

    def over(self):
        core, _, _ = place_in_mesh()
        source = self.ins[1].at[:, :, pl.ds(self.start_row, self.size)]
        return remote(source, self.came, self.kept[5:7], "pipe", 1 - core)

    def load(self):
        return pltpu.make_async_copy(self.ins[0].at[:, :, pl.ds(self.start_row, self.size)], self.mine, self.kept[11])

    def across(self, j):
        _, dp, _ = place_in_mesh()
        source = self.mine.at[pl.ds(j - 1, 2), pl.ds(2 * j - 2, 2)]
        return remote(source, self.first.at[j - 1], [sem.at[j - 1] for sem in self.kept[7:9]], "dp", dp ^ j)

    def onward(self, j):
        _, dp, _ = place_in_mesh()
        source = self.mine.at[2 if j == 1 else 0, pl.ds(2 * j - 2, 2)]
        return remote(source, self.second.at[j - 1], [sem.at[j - 1] for sem in self.kept[9:11]], "dp", dp ^ (3 - j))

    def start(self):
        self.over().start()
        self.load().start()

    def cores(self):
        self.over().wait()
        self.load().wait()

        def add(place, k):
            self.mine[place, k] += self.came[place, k]

        def sent(n, carry):
            add(n // 2, n % 2)
            add(n // 2 + 1, n % 2 + 2)
            return carry

        def kept(n, carry):
            add(3, n)
            add(2 - n // 2 * 2, n)
            return carry

        lax.fori_loop(0, 4, sent, 0)
        for j in (1, 2):
            self.across(j).start()
        lax.fori_loop(0, 4, kept, 0)

    def turn(self):
        for j in (1, 2):
            self.across(j).wait()

        def add(n, carry):
            self.mine[2, n] += self.first[0, 1, n]
            self.mine[0, n + 2] += self.first[1, 0, n]
            return carry

        lax.fori_loop(0, 2, add, 0)
        for j in (1, 2):
            self.onward(j).start()

    def close(self):
        for j in (1, 2):
            self.onward(j).wait()

        def add(n, carry):
            for j in (1, 2):
                k = n + 2 * j - 2
                total = self.mine[3, k].astype(F32) + self.first[j - 1, j - 1, n].astype(F32)
                self.total[k] = (total + self.second[j - 1, n].astype(F32)).astype(BF)
            return carry

        lax.fori_loop(0, 2, add, 0)

    def out(self):
        return pltpu.make_async_copy(self.total, self.outs[0], self.kept[12])

    def end(self):
        self.close()
        self.out().start()

    def flush(self):
        self.out().wait()


class ReduceTurn(ReduceFirst):
    def __init__(self, pair, plan=()):
        super().__init__(pair, plan)
        self.outputs = [jax.ShapeDtypeStruct((2, 2, CHUNK, D), BF), jax.ShapeDtypeStruct((4, CHUNK, D), BF)]
        self.scratch.append(pltpu.SemaphoreType.DMA((3,)))

    def end(self):
        for j in (1, 2):
            self.across(j).wait()

        def add(n, carry):
            self.mine[2, n] += self.first[0, 1, n]
            self.mine[0, n + 2] += self.first[1, 0, n]
            for j in (1, 2):
                self.mine[3, n + 2 * j - 2] += self.first[j - 1, j - 1, n]
            return carry

        lax.fori_loop(0, 2, add, 0)
        for copy in self.copies():
            copy.start()

    def copies(self):
        sem = self.kept[13]
        return [
            pltpu.make_async_copy(self.mine.at[2, pl.ds(0, 2)], self.outs[0].at[0], sem.at[0]),
            pltpu.make_async_copy(self.mine.at[0, pl.ds(2, 2)], self.outs[0].at[1], sem.at[1]),
            pltpu.make_async_copy(self.mine.at[3], self.outs[1], sem.at[2]),
        ]

    def flush(self):
        for copy in self.copies():
            copy.wait()


class ReduceOnward(Part):
    def __init__(self, given, plan=()):
        self.plan = plan
        base = pltpu.VMEM((4, CHUNK, D), BF)
        super().__init__(
            given, [jax.ShapeDtypeStruct((4, CHUNK, D), BF)],
            [base, pltpu.VMEM((2, 2, CHUNK, D), BF)] + sems(2) + [pltpu.SemaphoreType.DMA(()), pltpu.SemaphoreType.DMA(())],
        )

    def onward(self, j):
        _, dp, _ = place_in_mesh()
        return remote(self.ins[0].at[j - 1], self.kept[1].at[j - 1], [sem.at[j - 1] for sem in self.kept[2:4]], "dp", dp ^ (3 - j))

    def load(self):
        return pltpu.make_async_copy(self.ins[1], self.kept[0], self.kept[4])

    def start(self):
        for j in (1, 2):
            self.onward(j).start()
        self.load().start()

    def close(self):
        self.load().wait()
        for j in (1, 2):
            self.onward(j).wait()
        total = self.kept[0]

        def add(n, carry):
            for j in (1, 2):
                total[n + 2 * j - 2] += self.kept[1][j - 1, n]
            return carry

        lax.fori_loop(0, 2, add, 0)

    def out(self):
        return pltpu.make_async_copy(self.kept[0], self.outs[0], self.kept[5])

    def end(self):
        if not any(what == "close" for _, what in self.plan):
            self.close()
        self.out().start()

    def flush(self):
        self.out().wait()


class ReduceSecond(Part):
    def __init__(self, totals=None, size=CHUNK, plan=(), source=None, deferred=False):
        self.plan, self.after, self.deferred = plan, source, deferred
        line = pltpu.VMEM((size, D), BF)
        super().__init__(
            [totals] if totals is not None else [],
            [jax.ShapeDtypeStruct((size, D), BF)],
            [line, pltpu.VMEM((3, size, D), BF)] + sems(3) + [pltpu.SemaphoreType.DMA(()), pltpu.SemaphoreType.DMA(())],
        )

    def own(self):
        return pltpu.make_async_copy(self.ins[0].at[0], self.kept[0], self.kept[4])

    def along(self, k):
        _, _, shard = place_in_mesh()
        return remote(
            self.ins[0].at[k], self.kept[1].at[k - 1], [sem.at[k - 1] for sem in self.kept[2:4]], "tensor", lax.rem(shard + k, 4)
        )

    def start(self):
        if self.after is not None:
            self.ins = [self.after.kept[0]]
        for k in (2, 1, 3):
            self.along(k).start()
        self.own().start()

    def close(self):
        self.own().wait()
        for k in (1, 2, 3):
            self.along(k).wait()
        total = self.kept[0][...].astype(F32)
        for k in range(3):
            total += self.kept[1][k].astype(F32)
        self.kept[0][...] = total.astype(BF)

    def end(self):
        if not any(what == "close" for _, what in self.plan):
            self.close()
        self.out().start()

    def out(self):
        return pltpu.make_async_copy(self.kept[0], self.outs[0], self.kept[5])

    def flush(self):
        self.out().wait()


class Share(Part):
    def __init__(self, piece=None, rows=(0, CHUNK), target=None, source=None, plan=()):
        self.start_row, self.size = rows
        self.target, self.after, self.plan, self.deferred = target, source, plan, source is not None
        super().__init__(
            [piece] if piece is not None else [],
            [jax.ShapeDtypeStruct((D, D), BF)] if target is None else [],
            [pltpu.VMEM((self.size, D), BF)] + sems(3) + [pltpu.SemaphoreType.DMA(()), pltpu.SemaphoreType.DMA(())],
        )

    def place(self):
        core, dp, _ = place_in_mesh()
        start = pl.multiple_of(core * 256 + dp * CHUNK, CHUNK) + self.start_row
        out = self.outs[0] if self.target is None else self.target.outs[0]
        return out.at[pl.ds(pl.multiple_of(start, self.size), self.size), :]

    def across(self, j):
        _, dp, _ = place_in_mesh()
        return remote(self.ins[0], self.place(), [sem.at[j - 1] for sem in self.kept[1:3]], "dp", dp ^ j)

    def load(self):
        return pltpu.make_async_copy(self.ins[0], self.kept[0], self.kept[3])

    def keep(self):
        return pltpu.make_async_copy(self.kept[0], self.place(), self.kept[4])

    def start(self):
        if self.after is not None:
            self.ins = [self.after.kept[0]]
        for j in (3, 1, 2):
            self.across(j).start()
        self.load().start()

    def end(self):
        self.load().wait()
        self.keep().start()
        for j in (1, 2, 3):
            self.across(j).wait()
        self.keep().wait()


class Deliver(Part):
    def __init__(self, of_layers):
        super().__init__(of_layers, [jax.ShapeDtypeStruct(of_layers[0].shape, BF)], sems())

    def send(self, core):
        return remote(self.ins[1 - core], self.outs[0], self.kept, "pipe", 1 - core)

    def start(self):
        by_core(lambda core: self.send(core).start())

    def end(self):
        self.send(0).wait()


class Weave(Part):
    def __init__(self, of_layers, came=None, plan=()):
        self.plan = plan
        count = of_layers[0].shape[0]
        images = pltpu.VMEM((count, TOK, D), BF)
        self.count = count
        super().__init__(
            [*of_layers] + ([] if came is None else [came]), [jax.ShapeDtypeStruct((count, TOK, 2, D), BF)],
            [images, images, pltpu.VMEM((count, TOK, 2, D), BF)] + sems()
            + [pltpu.SemaphoreType.DMA(()), pltpu.SemaphoreType.DMA(()), pltpu.SemaphoreType.DMA((count,))],
        )

    def send(self, core):
        return remote(self.ins[1 - core], self.kept[1], self.kept[3:5], "pipe", 1 - core)

    def own(self, core):
        return pltpu.make_async_copy(self.ins[core], self.kept[0], self.kept[5])

    def came(self):
        return pltpu.make_async_copy(self.ins[2], self.kept[1], self.kept[6])

    def store(self, m):
        return pltpu.make_async_copy(self.kept[2].at[m], self.outs[0].at[m], self.kept[7].at[m])

    def start(self):
        by_core(lambda core: self.own(core).start())
        if len(self.ins) > 2:
            self.came().start()
        else:
            by_core(lambda core: self.send(core).start())

    def wait(self):
        self.own(0).wait()
        (self.came() if len(self.ins) > 2 else self.send(0)).wait()

    def weave(self, first, last):
        first_core = lax.axis_index("pipe") == 0

        def image(m, carry):
            mine, theirs = self.kept[0][m], self.kept[1][m]
            pair = [jnp.where(first_core, mine, theirs), jnp.where(first_core, theirs, mine)]
            self.kept[2][m] = jnp.stack(pair, axis=1)
            return carry

        lax.fori_loop(first, last, image, 0)
        for m in range(first, last):
            self.store(m).start()

    def all(self):
        self.wait()
        self.weave(0, self.count)

    def end(self):
        for m in range(self.count):
            self.store(m).wait()


def carried_call(body, parts, collective_id, *, grid, in_specs, inputs, out_specs, out_shape, scratch_shapes, name, cost):
    n_in, n_out, n_scratch = len(inputs), len(out_shape), len(scratch_shapes)
    counts = [(len(part.inputs), len(part.outputs), len(part.scratch)) for part in parts]

    def whole_body(*refs):
        refs = list(refs)

        def take(count, groups):
            mine = [refs.pop(0) for _ in range(count)]
            return mine, [[refs.pop(0) for _ in range(n)] for n in groups]

        mine, part_ins = take(n_in, [n for n, _, _ in counts])
        outs, part_outs = take(n_out, [n for _, n, _ in counts])
        kept, part_kept = take(n_scratch, [n for _, _, n in counts])
        for part, a, b, c in zip(parts, part_ins, part_outs, part_kept):
            part.bind(a, b, c)
        for part in parts:
            if getattr(part, "source", None) is not None:
                part.ins = [part.source.outs[0]]
        body(*mine, *outs, *kept)

    extra_in = [x for part in parts for x in part.inputs]
    extra_out = [x for part in parts for x in part.outputs]
    params = dict(vmem_limit_bytes=VMEM_LIMIT)
    if collective_id is not None:
        params.update(collective_id=collective_id, has_side_effects=True)
    results = pl.pallas_call(
        whole_body,
        grid_spec=pltpu.PrefetchScalarGridSpec(
            num_scalar_prefetch=0,
            grid=grid,
            in_specs=list(in_specs) + [ANY] * len(extra_in),
            out_specs=list(out_specs) + [ANY] * len(extra_out),
            scratch_shapes=list(scratch_shapes) + [x for part in parts for x in part.scratch],
        ),
        out_shape=list(out_shape) + extra_out,
        name=name,
        compiler_params=pltpu.CompilerParams(**params),
        cost_estimate=cost,
    )(*inputs, *extra_in)
    own, rest = results[:n_out], results[n_out:]
    given = []
    for _, n, _ in counts:
        given.append(rest[:n])
        rest = rest[n:]
    return own, given


def begin(weights, tasks):
    pl.when(pl.program_id(0) == 0)(weights.load)
    if tasks:

        @pl.when(pl.program_id(0) == 0)
        def _():
            greet()
            for task in tasks:
                if not task.deferred:
                    task.start()

    if isinstance(weights, Weights) and weights.count > 1:
        pl.when(pl.program_id(0) == 0)(weights.load_rest)


def planned(tasks, point):
    return [getattr(task, what) for task in tasks for at, what in task.plan if at == point]


def step_end(tasks, steps):
    for step in range(steps):
        calls = planned(tasks, step)
        if step == steps - 1:
            calls += [task.end for task in tasks] + [task.flush for task in tasks]
        if calls:

            @pl.when(pl.program_id(0) == step)
            def _():
                for call in calls:
                    call()


def whole(shape):
    return pl.BlockSpec(shape, lambda i: (0,) * len(shape))


def per(shape):
    return pl.BlockSpec((1,) + shape, lambda i: (i,) + (0,) * len(shape))


SMEM = pl.BlockSpec(memory_space=pltpu.SMEM)


def along_model(table_ref, layer, row, rolled):
    shard = lax.axis_index("tensor") if rolled else 0
    return jnp.concatenate([table_ref[(z - shard + 4) % 4, layer, row : row + 1, :].astype(F32) for z in range(4)], 1)


def window_token(shape, axis, offset):
    s = iota(shape, axis)
    w, a = s // WP, s % WP
    r = (w // 2) * WIN + a // WIN + offset
    c = (w % 2) * WIN + a % WIN + offset
    r, c = jnp.where(r >= GRID, r - GRID, r), jnp.where(c >= GRID, c - GRID, c)
    return jnp.where(a < POS, r * GRID + c, -1)


def spread_map(offset):
    return (window_token((ROWS, 1), 0, offset) == iota((ROWS, TP), 1)).astype(F32).astype(BF)


def gather_map(offset):
    return (window_token((1, ROWS), 1, offset) == iota((TP, ROWS), 0)).astype(F32).astype(BF)


def head_mask():
    return (iota((GH * WP, GL), 0) // WP == iota((GH * WP, GL), 1) // HD).astype(F32).astype(BF)


def region_mask(w):
    def band(a, which):
        place = which * WIN + a
        return (place >= GRID - WIN).astype(jnp.int32) + (place >= GRID - SHIFT).astype(jnp.int32)

    def label(a):
        return band(a // WIN, w // 2) * 3 + band(a % WIN, w % 2)

    keys = label(iota((WP, 1), 0))
    queries = label(iota((1, GH * WP), 1) % WP)
    return jnp.where(keys != queries, MASK_VALUE, 0.0).astype(F32)


def block_diagonal(rows, mask):
    return jnp.concatenate([rows] * GH, axis=0) * mask


def query_major(pt):
    turned = pt.T
    return jnp.concatenate([turned[h * WP : (h + 1) * WP] for h in range(GH)], axis=1)


def pick_diagonal(full):
    head = iota((WP, GL), 1) // HD
    out = full[0:WP]
    for h in range(1, GH):
        out = jnp.where(head == h, full[h * WP : (h + 1) * WP], out)
    return out


def permutation(size, source_of, inverse):
    rows = iota((size, size), 1 if inverse else 0)
    cols = iota((size, size), 0 if inverse else 1)
    return (rows == source_of(cols)).astype(F32).astype(BF)


def qkv_source(col):
    return (col % GL) // HD * (3 * HD) + col // GL * HD + col % HD


def qv_source(col):
    return (col % GL) // HD * (2 * HD) + col // GL * HD + col % HD


def attn_fwd_body(
    layer, rolled, weights, keep, tasks, x_ref, table_ref, bias_ref, fw_ref, qkv_ref, p_ref, ho_ref, mid_ref,
    how_ref, wq_ref, wpt_ref, vec_ref, shift_ref, spread_ref, gather_ref, mask_ref, region_ref,
):
    begin(weights, tasks)
    wa_ref = weights.kept[0].at[0]
    first_step = pl.program_id(0) == 0

    @pl.when(first_step)
    def _():
        for n, row in enumerate((GAIN, SHIFT_ROW, BPROJ)):
            vec_ref[n : n + 1, :] = along_model(table_ref, layer, row, rolled)
        for g in range(4):
            qv = table_ref[g, layer, QV : QV + 2, :].astype(F32)
            at = 3 * GL * g
            for n, (scale, shift) in enumerate(((HD ** (-0.5), qv[0:1] * HD ** (-0.5)), (1.0, 0.0), (1.0, qv[1:2]))):
                lanes = slice(at + n * GL, at + (n + 1) * GL)
                shift_ref[0:1, lanes] = jnp.full((1, GL), scale, F32)
                shift_ref[1:2, lanes] = shift + jnp.zeros((1, GL), F32)
        spread_ref[...] = spread_map(layer * SHIFT)
        gather_ref[...] = gather_map(layer * SHIFT)
        mask_ref[...] = head_mask()
        if layer:
            for w in range(NW):
                region_ref[w] = region_mask(w)

    x = x_ref[0].astype(F32)
    normed, _ = normalize(x)
    first = (normed * vec_ref[0:1, :] + vec_ref[1:2, :]).astype(BF)
    fw = dot_nn(spread_ref[...], first).astype(BF)
    fw_ref[0] = fw

    @pl.when(first_step)
    def _():
        weights.wait_shard()
        weights.wait_rest()
        for g in range(4):
            wq_ref[:, 3 * GL * g : 3 * GL * (g + 1)] = wa_ref[g, :, : 3 * GL]
            wpt_ref[:, g * GL : (g + 1) * GL] = wa_ref[g, :, 3 * GL :]
        keep.start(wq_ref, wpt_ref)

    for n in range(3):
        lanes = slice(n * D, (n + 1) * D)
        projected = dot_nn(fw, wq_ref[:, lanes])
        qkv_ref[0, :, lanes] = (projected * shift_ref[0:1, lanes] + shift_ref[1:2, lanes]).astype(BF)

    def windows(n, carry):
        chains = [(n * AT_ONCE + w, g) for w in range(AT_ONCE) for g in range(4)]

        def rows(w):
            return pl.ds(pl.multiple_of(w * WP, WP), WP)

        def part(w, g, n):
            return qkv_ref[0, rows(w), (3 * g + n) * GL : (3 * g + n + 1) * GL]

        scores = [dot_nt(part(w, g, 1), block_diagonal(part(w, g, 0), mask_ref[...])) for w, g in chains]
        probs = []
        for (w, g), st in zip(chains, scores):
            st = st + bias_ref[0, g]
            if layer:
                st = st + region_ref[w]
            e = jnp.exp(st - jnp.max(st, 0, keepdims=True))
            pt = (e * (1.0 / jnp.sum(e, 0, keepdims=True))).astype(BF)
            p_ref[0, w, g] = pt
            probs.append(pt)
        mixed = [dot_tn(pt, part(w, g, 2)) for (w, g), pt in zip(chains, probs)]
        for (w, g), out in zip(chains, mixed):
            how_ref[rows(w), g * GL : (g + 1) * GL] = pick_diagonal(out).astype(BF)
        return carry

    lax.fori_loop(0, NW // AT_ONCE, windows, 0)
    ho = dot_nn(gather_ref[...], how_ref[...]).astype(BF)
    ho_ref[0] = ho
    mid_ref[0] = x + (dot_nt(ho, wpt_ref[...]) + vec_ref[2:3, :])
    step_end(tasks, 4)

    @pl.when(pl.program_id(0) == pl.num_programs(0) - 1)
    def _():
        keep.wait(wq_ref, wpt_ref)


def attn_fwd(layer, rolled, x, table, bias, weights, tasks=(), collective_id=None):
    n = x.shape[0]
    keep = Keep((D, 3 * D), (D, D))
    return carried_call(
        functools.partial(attn_fwd_body, layer, rolled, weights, keep, tasks),
        [keep, weights, *tasks],
        collective_id,
        grid=(n,),
        in_specs=[
            per(x.shape[1:]), whole(table.shape), pl.BlockSpec((1, 4, WP, GH * WP), lambda i: (layer, 0, 0, 0)),
        ],
        inputs=(x, table, bias),
        out_specs=[per((ROWS, D)), per((ROWS, 3 * D)), per((NW, 4, WP, GH * WP)), per((TP, D)), per((TP, D))],
        out_shape=[
            jax.ShapeDtypeStruct((n, ROWS, D), BF),
            jax.ShapeDtypeStruct((n, ROWS, 3 * D), BF),
            jax.ShapeDtypeStruct((n, NW, 4, WP, GH * WP), BF),
            jax.ShapeDtypeStruct((n, TP, D), BF),
            jax.ShapeDtypeStruct((n, TP, D), F32),
        ],
        scratch_shapes=[
            pltpu.VMEM((ROWS, D), BF), pltpu.VMEM((D, 3 * D), BF), pltpu.VMEM((D, D), BF), pltpu.VMEM((8, D), F32),
            pltpu.VMEM((8, 3 * D), F32), pltpu.VMEM((ROWS, TP), BF), pltpu.VMEM((TP, ROWS), BF), pltpu.VMEM((GH * WP, GL), BF),
            pltpu.VMEM((NW, WP, GH * WP), F32),
        ],
        name="attn_fwd",
        cost=pl.CostEstimate(flops=n * 2 * 256 * 512 * 2600, bytes_accessed=n * 2 << 20, transcendentals=0),
    )


def gelu_parts(v):
    cdf = 0.5 * (1.0 + lax.erf(v * 0.5**0.5))
    pdf = jnp.exp(-0.5 * v * v) * (2.0 * math.pi) ** (-0.5)
    return v * cdf, cdf + v * pdf


def alive_of(counts_ref, m):
    slot = lax.axis_index("tensor") * 2 + lax.axis_index("pipe")
    return (slot < counts_ref[0, m]).astype(F32)


def live_rows(counts_ref, m):
    return jnp.where(iota((TP, 1), 0) < TOK, alive_of(counts_ref, m), 0.0)


def mlp_fwd_body(
    layer, rolled, weights, keep, tasks, counts_ref, mid_ref, table_ref, second_ref, act_ref, slope_ref, y_ref, out_ref, acc_ref, hb_ref
):
    c = pl.program_id(0)
    rows_total = mid_ref.shape[0]
    begin(weights, tasks)
    wm_ref = weights.kept[0]

    @pl.when(c == 0)
    def _():
        for k in range(4):
            hb_ref[k] = jnp.concatenate([table_ref[k, layer, HB + n : HB + n + 1, :].astype(F32) for n in range(4)], 1)
        gain = along_model(table_ref, layer, MGAIN, rolled)
        shift = along_model(table_ref, layer, MSHIFT, rolled)
        mid = mid_ref[...]
        normed, _ = normalize(mid)
        second_ref[...] = (normed * gain + shift).astype(BF)
        acc_ref[...] = mid + along_model(table_ref, layer, OB, rolled)
        weights.wait_shard()

    @pl.when(c == 1)
    def _():
        weights.wait_rest()
        keep.start(wm_ref)

    def block(b, carry):
        parts = [pl.ds(pl.multiple_of(b * BLK + n * SUB_FWD, SUB_FWD), SUB_FWD) for n in range(BLK // SUB_FWD)]
        acts = []
        pre = [dot_nn(second_ref[rows, :], wm_ref[0, c]) for rows in parts]
        for rows, value in zip(parts, pre):
            act, slope = gelu_parts(value + hb_ref[c])
            act = act.astype(BF)
            act_ref[0, rows, :] = act
            slope_ref[0, rows, :] = slope.astype(BF)
            acts.append(act)
        outs = [dot_nn(act, wm_ref[1, c]) for act in acts]
        for rows, out in zip(parts, outs):
            acc_ref[rows, :] += out
        return carry

    lax.fori_loop(0, rows_total // BLK, block, 0)

    @pl.when(c == pl.num_programs(0) - 1)
    def _():
        for m in range(rows_total // TP):
            y = (acc_ref[m * TP : (m + 1) * TP, :] * live_rows(counts_ref, m)).astype(BF)
            y_ref[m] = y
            out_ref[m] = y[:TOK]
        keep.wait(wm_ref)

    step_end(tasks, 4)


def mlp_fwd(layer, rolled, counts, mid, table, weights, tasks=(), collective_id=None):
    r = mid.shape[0]
    n = r // TP
    keep = Keep((2, 4, D, D))
    return carried_call(
        functools.partial(mlp_fwd_body, layer, rolled, weights, keep, tasks),
        [keep, weights, *tasks],
        collective_id,
        grid=(4,),
        in_specs=[SMEM, whole((r, D)), whole(table.shape)],
        inputs=(counts, mid, table),
        out_specs=[whole((r, D)), per((r, D)), per((r, D)), whole((n, TP, D)), whole((n, TOK, D))],
        out_shape=[
            jax.ShapeDtypeStruct((r, D), BF),
            jax.ShapeDtypeStruct((4, r, D), BF),
            jax.ShapeDtypeStruct((4, r, D), BF),
            jax.ShapeDtypeStruct((n, TP, D), BF),
            jax.ShapeDtypeStruct((n, TOK, D), BF),
        ],
        scratch_shapes=[pltpu.VMEM((r, D), F32), pltpu.VMEM((4, 1, D), F32)],
        name="mlp_fwd",
        cost=pl.CostEstimate(flops=4 * r * D * 2048, bytes_accessed=12 << 20, transcendentals=0),
    )


def scatter_rows(place, value_ref, mine_ref, away_ref, index):
    core, dp = place
    for half, out_ref in enumerate((mine_ref, away_ref)):
        for n, j in enumerate(PLACES):
            start = (core ^ half) * 256 + (dp ^ j) * CHUNK
            out_ref[n, index] = value_ref[pl.ds(pl.multiple_of(start, CHUNK), CHUNK), :]


def where_in_plane(rolled):
    return (lax.axis_index("pipe"), lax.axis_index("dp")) if rolled else (jnp.int32(0), jnp.int32(0))


def by_shard(row):
    return jnp.concatenate([row[None, :, z * GL : (z + 1) * GL] for z in range(4)], 0)


def mlp_bwd_body(
    layer, rolled, weights, tasks, counts_ref, g_ref, act_ref, slope_ref, second_ref, mid_ref, table_ref,
    ghw_ref, ghw_away_ref, gow_ref, gow_away_ref, ghb_ref, gmid_ref, small_ref,
    gy_ref, gyt_ref, sect_ref, gp_ref, acc_ref, value_ref,
):
    c = pl.program_id(0)
    rows_total = mid_ref.shape[0]
    begin(weights, tasks)
    wm_ref = weights.kept[0]

    @pl.when(c == 0)
    def _():
        total = jnp.zeros((1, D), F32)
        for m in range(rows_total // TP):
            rows = slice(m * TP, (m + 1) * TP)
            gy = g_ref[m].astype(F32) * live_rows(counts_ref, m)
            gy_ref[rows, :] = gy.astype(BF)
            total += jnp.sum(gy, 0, keepdims=True)
        small_ref[:, 0:1] = by_shard(total)
        gyt_ref[...] = gy_ref[...].T
        sect_ref[...] = second_ref[...].T
        acc_ref[...] = jnp.zeros_like(acc_ref)
        weights.wait()

    ghb_ref[0] = jnp.zeros_like(ghb_ref[0])

    def block(b, carry):
        parts = [pl.ds(pl.multiple_of(b * BLK + n * SUB_BWD, SUB_BWD), SUB_BWD) for n in range(BLK // SUB_BWD)]
        slopes = [dot_nt(gy_ref[rows, :], wm_ref[1, c]) for rows in parts]
        pres = []
        for rows, value in zip(parts, slopes):
            gp = value * slope_ref[0, rows, :].astype(F32)
            total = jnp.sum(gp, 0, keepdims=True)
            for n in range(4):
                ghb_ref[0, n : n + 1, :] += total[:, n * GL : (n + 1) * GL]
            gp = gp.astype(BF)
            gp_ref[rows, :] = gp
            pres.append(gp)
        outs = [dot_nt(gp, wm_ref[0, c]) for gp in pres]
        for rows, out in zip(parts, outs):
            acc_ref[rows, :] += out
        return carry

    lax.fori_loop(0, rows_total // BLK, block, 0)
    place = where_in_plane(rolled)
    value_ref[0] = dot_nn(sect_ref[...], gp_ref[...]).astype(BF)
    value_ref[1] = dot_nn(gyt_ref[...], act_ref[0]).astype(BF)
    scatter_rows(place, value_ref.at[0], ghw_ref, ghw_away_ref, 0)
    scatter_rows(place, value_ref.at[1], gow_ref, gow_away_ref, 0)

    @pl.when(c == pl.num_programs(0) - 1)
    def _():
        for call in planned(tasks, LATE):
            call()
        e = acc_ref[...]
        normed, inverse = normalize(mid_ref[...])
        small_ref[:, 2:3] = by_shard(jnp.sum(e * normed, 0, keepdims=True))
        small_ref[:, 3:4] = by_shard(jnp.sum(e, 0, keepdims=True))
        gmid = gy_ref[...].astype(F32) + norm_back(e, normed, inverse, along_model(table_ref, layer, MGAIN, rolled))
        small_ref[:, 1:2] = by_shard(jnp.sum(gmid, 0, keepdims=True))
        gmid_ref[...] = gmid

    step_end(tasks, 4)


PIECES = jax.ShapeDtypeStruct((4, 4, CHUNK, D), BF)


def mlp_bwd(layer, rolled, counts, g, act, slope, second, mid, table, weights, tasks=(), collective_id=None):
    r = mid.shape[0]
    pieces = pl.BlockSpec((4, 1, CHUNK, D), lambda i: (0, i, 0, 0))
    return carried_call(
        functools.partial(mlp_bwd_body, layer, rolled, weights, tasks),
        [weights, *tasks],
        collective_id,
        grid=(4,),
        in_specs=[SMEM, whole(g.shape), per((r, D)), per((r, D)), whole((r, D)), whole((r, D)), whole(table.shape)],
        inputs=(counts, g, act, slope, second, mid, table),
        out_specs=[pieces, pieces, pieces, pieces, per((4, GL)), whole((r, D)), whole((4, 4, GL))],
        out_shape=[
            PIECES, PIECES, PIECES, PIECES,
            jax.ShapeDtypeStruct((4, 4, GL), F32),
            jax.ShapeDtypeStruct((r, D), F32),
            jax.ShapeDtypeStruct((4, 4, GL), F32),
        ],
        scratch_shapes=[
            pltpu.VMEM((r, D), BF), pltpu.VMEM((D, r), BF), pltpu.VMEM((D, r), BF), pltpu.VMEM((r, D), BF),
            pltpu.VMEM((r, D), F32), pltpu.VMEM((2, D, D), BF),
        ],
        name="mlp_bwd",
        cost=pl.CostEstimate(flops=8 * r * D * 2048, bytes_accessed=16 << 20, transcendentals=0),
    )


def attn_bwd_body(
    layer, rolled, weights, tasks, x_ref, gmid_ref, fw_ref, qkv_ref, p_ref, ho_ref, table_ref,
    gin_ref, out_ref, ga_ref, ga_away_ref, gqv_ref, gtab_ref, small_ref,
    gw_ref, dq_ref, fwt_ref, hos_ref, gms_ref, value_ref, spread_ref, gather_ref, mask_ref, gain_ref,
):
    i = pl.program_id(0)
    last = pl.num_programs(0) - 1
    begin(weights, tasks)
    wq_ref, wpt_ref = weights.kept[:2]

    @pl.when(i == 0)
    def _():
        gqv_ref[...] = jnp.zeros_like(gqv_ref)
        gtab_ref[...] = jnp.zeros_like(gtab_ref)
        small_ref[...] = jnp.zeros_like(small_ref)
        spread_ref[...] = spread_map(layer * SHIFT)
        gather_ref[...] = gather_map(layer * SHIFT)
        mask_ref[...] = head_mask()
        gain_ref[...] = along_model(table_ref, layer, GAIN, rolled)

    gmid = gmid_ref[0]
    gmb = gmid.astype(BF)
    image = pl.ds(pl.multiple_of(i * TP, 16), TP)
    gms_ref[image, :] = gmb
    hos_ref[image, :] = ho_ref[0]
    base = pl.multiple_of(i * ROWS, ROWS)
    fwt_ref[:, pl.ds(base, ROWS)] = fw_ref[0].T

    @pl.when(i == 0)
    def _():
        weights.wait()

    heads = dot_nn(gmb, wpt_ref[...]).astype(BF)
    gw_ref[...] = dot_nn(spread_ref[...], heads).astype(BF)
    scale = HD ** (-0.5)

    def windows(n, carry):
        chains = [(n * AT_ONCE + w, g) for w in range(AT_ONCE) for g in range(4)]
        mask = mask_ref[...]

        def rows(w):
            return pl.ds(pl.multiple_of(w * WP, WP), WP)

        def part(w, g, n):
            return qkv_ref[0, rows(w), (3 * g + n) * GL : (3 * g + n + 1) * GL]

        bd_grads = [block_diagonal(gw_ref[rows(w), g * GL : (g + 1) * GL], mask) for w, g in chains]
        terms = [dot_nt(part(w, g, 2), bd_grad) for (w, g), bd_grad in zip(chains, bd_grads)]
        dvs = [dot_nn(p_ref[0, w, g], bd_grad) for (w, g), bd_grad in zip(chains, bd_grads)]
        scores = []
        for (w, g), term in zip(chains, terms):
            ptf = p_ref[0, w, g].astype(F32)
            pd = term * ptf
            ds = pd - ptf * jnp.sum(pd, 0, keepdims=True)
            gtab_ref[g] += ds
            scores.append(ds.astype(BF))
        dks = [dot_nn(ds, block_diagonal(part(w, g, 0), mask)) for (w, g), ds in zip(chains, scores)]
        dqs = [dot_tn(ds, part(w, g, 1)) for (w, g), ds in zip(chains, scores)]
        for (w, g), full, dk, dv in zip(chains, dqs, dks, dvs):
            dq = pick_diagonal(full) * scale
            out_rows = pl.ds(pl.multiple_of(base + w * WP, WP), WP)
            gqv_ref[g, 0:1] += jnp.sum(dq, 0, keepdims=True)
            gqv_ref[g, 1:2] += jnp.sum(dv, 0, keepdims=True)
            for n, value in enumerate((dq, dk, dv)):
                dq_ref[out_rows, (3 * g + n) * GL : (3 * g + n + 1) * GL] = value.astype(BF)
        return carry

    lax.fori_loop(0, NW // AT_ONCE, windows, 0)
    image_rows = pl.ds(base, ROWS)
    e = dot_nt(dq_ref[image_rows, :], wq_ref[...])
    e = dot_nn(gather_ref[...], e.astype(BF))
    normed, inverse = normalize(x_ref[0].astype(F32))
    small_ref[:, 0:1] += by_shard(jnp.sum(e * normed, 0, keepdims=True))
    small_ref[:, 1:2] += by_shard(jnp.sum(e, 0, keepdims=True))
    gin = (gmid + norm_back(e, normed, inverse, gain_ref[...])).astype(BF)
    gin_ref[0] = gin
    out_ref[0] = gin[:TOK]

    @pl.when(i == last)
    def _():
        for call in planned(tasks, LATE):
            call()

        def chunk(n, carry):
            lanes = pl.ds(pl.multiple_of(n * D, D), D)
            value_ref[:, lanes] = dot_nn(fwt_ref[...], dq_ref[:, lanes]).astype(BF)
            return carry

        lax.fori_loop(0, 3, chunk, 0)
        value_ref[:, 3 * D :] = dot_nn(gms_ref[...].T, hos_ref[...]).astype(BF)
        core, dp = where_in_plane(rolled)
        for half, group_ref in enumerate((ga_ref, ga_away_ref)):
            for n, j in enumerate(PLACES):
                rows = pl.ds(pl.multiple_of((core ^ half) * 256 + (dp ^ j) * CHUNK, CHUNK), CHUNK)
                for g in range(4):
                    group_ref[n, g, :, : 3 * GL] = value_ref[rows, 3 * GL * g : 3 * GL * (g + 1)]
                    group_ref[n, g, :, 3 * GL :] = value_ref[rows, 3 * D + GL * g : 3 * D + GL * (g + 1)]

    step_end(tasks, 4)


def attn_bwd(layer, rolled, x, gmid, fw, qkv, p, ho, table, weights, tasks=(), collective_id=None):
    n = x.shape[0]
    return carried_call(
        functools.partial(attn_bwd_body, layer, rolled, weights, tasks),
        [weights, *tasks],
        collective_id,
        grid=(n,),
        in_specs=[
            per(x.shape[1:]), per((TP, D)), per((ROWS, D)), per((ROWS, 3 * D)), per((NW, 4, WP, GH * WP)), per((TP, D)),
            whole(table.shape),
        ],
        inputs=(x, gmid, fw, qkv, p, ho, table),
        out_specs=[
            per((TP, D)), per((TOK, D)), whole(PIECES.shape), whole(PIECES.shape), whole((4, 2, GL)), whole((4, WP, GH * WP)),
            whole((4, 2, GL)),
        ],
        out_shape=[
            jax.ShapeDtypeStruct((n, TP, D), BF),
            jax.ShapeDtypeStruct((n, TOK, D), BF),
            PIECES, PIECES,
            jax.ShapeDtypeStruct((4, 2, GL), F32),
            jax.ShapeDtypeStruct((4, WP, GH * WP), F32),
            jax.ShapeDtypeStruct((4, 2, GL), F32),
        ],
        scratch_shapes=[
            pltpu.VMEM((ROWS, D), BF), pltpu.VMEM((n * ROWS, 3 * D), BF), pltpu.VMEM((D, n * ROWS), BF),
            pltpu.VMEM((n * TP, D), BF), pltpu.VMEM((n * TP, D), BF), pltpu.VMEM((D, 4 * D), BF),
            pltpu.VMEM((ROWS, TP), BF), pltpu.VMEM((TP, ROWS), BF), pltpu.VMEM((GH * WP, GL), BF), pltpu.VMEM((1, D), F32),
        ],
        name="attn_bwd",
        cost=pl.CostEstimate(flops=n * 4 * 256 * 512 * 2600, bytes_accessed=n * 3 << 20, transcendentals=0),
    )


def plain_call(body, name, inputs, out_shape, scratch_shapes=(), grid=(), in_specs=None, out_specs=None, bytes_accessed=4 << 20):
    return pl.pallas_call(
        body,
        grid=grid,
        out_shape=out_shape,
        in_specs=in_specs or [pl.BlockSpec(memory_space=pltpu.VMEM)] * len(inputs),
        out_specs=out_specs or jax.tree.map(lambda _: pl.BlockSpec(memory_space=pltpu.VMEM), out_shape),
        scratch_shapes=list(scratch_shapes),
        name=name,
        compiler_params=pltpu.CompilerParams(vmem_limit_bytes=VMEM_LIMIT),
        cost_estimate=pl.CostEstimate(flops=bytes_accessed, bytes_accessed=bytes_accessed, transcendentals=0),
    )(*inputs)


def prepare_body(turned, wqkv, wproj, gain, shift, qv, table, bproj, mgain, mshift, hb, ob, own_a_ref, lines_ref, index_ref, rows_ref, keys_ref):
    own_a_ref[:, : 3 * GL] = dot_nn(wqkv[...], permutation(3 * GL, qkv_source, False)).astype(BF)
    own_a_ref[:, 3 * GL :] = wproj[...].T
    rows_ref[...] = jnp.zeros_like(rows_ref)
    for row, ref in ((GAIN, gain), (SHIFT_ROW, shift), (BPROJ, bproj), (MGAIN, mgain), (MSHIFT, mshift), (OB, ob)):
        rows_ref[row : row + 1, :] = ref[...].astype(F32)
    terms = dot_nn(jnp.broadcast_to(qv[...], (16, 2 * GL)), permutation(2 * GL, qv_source, False))
    hidden, places = hb[...].astype(F32), table[...].astype(F32)
    for n in range(2):
        rows_ref[QV + n : QV + n + 1, :] = terms[0:1, n * GL : (n + 1) * GL]
    for n in range(4):
        rows_ref[HB + n : HB + n + 1, :] = hidden[:, n * GL : (n + 1) * GL]
    rows_ref[TABLE : TABLE + 4, :] = places[:, :GL]
    rows_ref[TABLE + 4 : TABLE + 8, 0 : RELS - GL] = places[:, GL:]
    lines_ref[...] = rows_ref[...].astype(BF)
    keys_ref[...] = jnp.full((WP, GL), -1, jnp.int32)
    keys_ref[0:POS, 0:POS] = turned[...]
    pair = [keys_ref[pl.ds(odd, WP // 2, 2), :][:, :WP] for odd in range(2)]
    index_ref[...] = jnp.concatenate(pair, 1)


def prepare(turned, wqkv, wproj, *small):
    return plain_call(
        prepare_body, "prepare", (turned, wqkv, wproj, *small),
        [
            jax.ShapeDtypeStruct((D, D), BF), jax.ShapeDtypeStruct((LINES, GL), BF),
            jax.ShapeDtypeStruct((WP // 2, GL), jnp.int32),
        ],
        [pltpu.VMEM((LINES, GL), F32), pltpu.VMEM((WP, GL), jnp.int32)],
    )


class Exchange(Part):
    def __init__(self, own, lines):
        shapes = [jax.ShapeDtypeStruct(part.shape, part.dtype) for part in own]
        shapes.append(jax.ShapeDtypeStruct((4, 2) + lines.shape, lines.dtype))
        super().__init__([*own, lines], shapes, sems(4) + sems(3) + [pltpu.SemaphoreType.DMA(())])

    def swap(self, n):
        core, _, _ = place_in_mesh()
        target = self.outs[n] if n < 3 else self.outs[3].at[0, core]
        return remote(self.ins[n], target, [sem.at[n] for sem in self.kept[:2]], "pipe", 1 - core)

    def keep(self):
        core, _, _ = place_in_mesh()
        return pltpu.make_async_copy(self.ins[3], self.outs[3].at[0, core], self.kept[4])

    def spread(self, k):
        _, _, shard = place_in_mesh()
        table = self.outs[3]
        return remote(table.at[0], table.at[k], [sem.at[k - 1] for sem in self.kept[2:4]], "tensor", lax.rem(shard + 4 - k, 4))


def gather_start(own, lines, index, view):
    exchange = Exchange(own, lines)
    near_a, near_h, near_o, far_a, bias = Near(0, None, None), Near(0, None, None), Near(0, None, None), Far(None), Bias(index)
    pick = Own(view)

    def body():
        for n, task in enumerate((near_a, near_h, near_o)):
            task.ins = [exchange.ins[n], exchange.outs[n]]
        far_a.ins = [near_a.outs[0]]
        greet()
        for n in (0, 3, 1, 2):
            exchange.swap(n).start()
        exchange.keep().start()
        pick.start()
        exchange.swap(0).wait()
        near_a.start()
        exchange.keep().wait()
        exchange.swap(3).wait()
        for k in (1, 2, 3):
            exchange.spread(k).start()
        pick.pick()
        near_a.end()
        far_a.start()
        exchange.swap(1).wait()
        near_h.start()
        for k in (1, 2, 3):
            exchange.spread(k).wait()
        bias.build(exchange.outs[3])
        far_a.turn()
        exchange.swap(2).wait()
        near_o.start()
        far_a.rest()
        far_a.last()
        far_a.end()
        bias.end()
        pick.end()
        near_h.end()
        near_o.end()

    parts = [exchange, near_a, near_h, near_o, far_a, bias, pick]
    _, given = carried_call(
        body, parts, 0, grid=(), in_specs=[], inputs=(), out_specs=[], out_shape=[], scratch_shapes=[],
        name="gather_start", cost=pl.CostEstimate(flops=1 << 24, bytes_accessed=8 << 20, transcendentals=0),
    )
    others, given_a, given_h, given_o, far, *rest = given
    return others[:3], others[3], [given_a[0], *far], given_h[0], given_o[0], *[part[0] for part in rest]


def turned_index(rel_index):
    return jnp.pad(rel_index.T, ((0, WP - POS), (0, WP - POS)), constant_values=-1)


def places_of(pairs):
    return (iota((2 * GL, pairs.shape[1]), 0) == pairs).astype(F32).astype(BF)


class Own(Part):
    def __init__(self, view, plan=()):
        count = view.shape[0]
        self.count, self.plan = count, plan
        super().__init__(
            [view], [jax.ShapeDtypeStruct((count, TP, D), BF)],
            [pltpu.VMEM(view.shape, BF), pltpu.VMEM((count, TP, D), BF), pltpu.SemaphoreType.DMA((2,))],
        )

    def load(self):
        return pltpu.make_async_copy(self.ins[0], self.kept[0], self.kept[2].at[0])

    def out(self):
        return pltpu.make_async_copy(self.kept[1], self.outs[0], self.kept[2].at[1])

    def start(self):
        self.load().start()

    def pick(self):
        self.load().wait()
        first_core = lax.axis_index("pipe") == 0

        def image(m, carry):
            both = self.kept[0][m]
            self.kept[1][m] = jnp.zeros((TP, D), BF)
            self.kept[1][m, 0:TOK, :] = jnp.where(first_core, both[:, 0, :], both[:, 1, :])
            return carry

        lax.fori_loop(0, self.count, image, 0)
        self.out().start()

    def end(self):
        self.out().wait()


class Bias(Part):
    def __init__(self, index):
        super().__init__(
            [index], [jax.ShapeDtypeStruct((2, 4, WP, GH * WP), F32)],
            [pltpu.VMEM((4, 2, LINES, GL), BF), pltpu.VMEM((WP // 2, GL), jnp.int32), pltpu.VMEM((2 * H, 2 * GL), F32),
             pltpu.VMEM((WP // 2, 2 * H, GL), F32), pltpu.VMEM((WP, GL), F32), pltpu.VMEM((2, 4, WP, GH * WP), F32),
             pltpu.SemaphoreType.DMA((3,))],
        )

    def loads(self, table):
        return [pltpu.make_async_copy(table, self.kept[0], self.kept[6].at[0]), self.index()]

    def index(self):
        return pltpu.make_async_copy(self.ins[0], self.kept[1], self.kept[6].at[1])

    def out(self):
        return pltpu.make_async_copy(self.kept[5], self.outs[0], self.kept[6].at[2])

    def build(self, table):
        lines, index, rows, pairs, half, whole_ref, _ = self.kept
        for copy in self.loads(table):
            copy.start()
        for copy in self.loads(table):
            copy.wait()
        for l in range(2):
            for k in range(4):
                values = lines[k, l].astype(F32)
                at = l * H + k * GH
                rows[at : at + GH, :GL] = values[TABLE : TABLE + GH]
                rows[at : at + GH, GL:] = values[TABLE + GH : TABLE + 2 * GH]
        tables = rows[...].astype(BF)

        def product(n, carry):
            pairs[n] = dot_nn(tables, places_of(index[pl.ds(n, 1), :]))
            return carry

        lax.fori_loop(0, WP // 2, product, 0)
        shut = jnp.where(iota((WP, GL), 0) < POS, 0.0, SHUT).astype(F32)
        for l in range(2):
            for g in range(4):
                for n in range(2):
                    heads = [pairs[:, l * H + g * GH + 2 * n + m, :] for m in range(2)]
                    for odd in range(2):
                        lanes = slice(odd * WP, (odd + 1) * WP)
                        half[pl.ds(odd, WP // 2, 2), :] = jnp.concatenate([head[:, lanes] for head in heads], 1)
                    whole_ref[l, g, :, n * GL : (n + 1) * GL] = half[...] + shut
        self.out().start()

    def end(self):
        self.out().wait()


def bias_tables(table, rel_index):
    rows = table[:, :, TABLE : TABLE + 8].reshape(4, 2, 2, GH, GL).transpose(1, 0, 3, 2, 4).reshape(2 * H, 2 * GL)
    onehot = (jnp.arange(2 * GL, dtype=jnp.int32)[:, None] == turned_index(rel_index).reshape(1, -1)).astype(BF)
    flat = jnp.dot(rows, onehot, preferred_element_type=F32)
    position = flat.reshape(2, 4, GH, WP, WP).transpose(0, 1, 3, 2, 4)
    shut = jnp.where(jnp.arange(WP) < POS, 0.0, SHUT).astype(F32)[:, None, None]
    return (position + shut).reshape(2, 4, WP, GH * WP)


def table_grad(gtab, rel_index):
    rel = jnp.pad(rel_index.T, ((0, WP - POS), (0, WP - POS)), constant_values=-1).reshape(-1)
    onehot = (rel[:, None] == jnp.arange(RELS, dtype=jnp.int32)[None, :]).astype(F32)
    flat = gtab.reshape(4, WP, GH, WP).transpose(0, 2, 1, 3).reshape(H, WP * WP)
    return jnp.dot(flat, onehot, precision=lax.Precision.HIGHEST).reshape(4, GH, RELS)


class Little(Part):
    def __init__(self, rows):
        self.rows = rows
        super().__init__(
            [],
            [jax.ShapeDtypeStruct((rows, GL), F32)],
            [pltpu.VMEM((2, 4, rows, GL), F32), pltpu.VMEM((4, rows, GL), F32), pltpu.VMEM((3, 4, rows, GL), F32),
             pltpu.VMEM((3, rows, GL), F32)]
            + sems() + sems(3) + sems(3) + [pltpu.SemaphoreType.DMA(())],
        )

    def pack(self, layers, tabs):
        _, _, shard = place_in_mesh()
        sums = self.kept[0]
        sums[...] = jnp.zeros_like(sums)
        for layer, (ghb, small_m, gqv, _, small_a) in enumerate(layers):
            for k in range(4):
                z = lax.rem(shard + k, 4)
                for row, source, n in (
                    (GAIN, small_a, 0), (SHIFT_ROW, small_a, 1), (OB, small_m, 0), (BPROJ, small_m, 1), (MGAIN, small_m, 2),
                    (MSHIFT, small_m, 3),
                ):
                    sums[layer, k, row : row + 1, :] = source[z, n : n + 1, :]
                sums[layer, k, QV : QV + 2, :] = gqv[k]
                sums[layer, k, HB : HB + 4, :] = ghb[k]
                rows = tabs[layer][GH * k : GH * (k + 1)]
                sums[layer, k, TABLE : TABLE + 4, :] = rows[:, 0:GL]
                sums[layer, k, TABLE + 4 : TABLE + 8, :] = rows[:, GL:]

    def over(self):
        core, _, _ = place_in_mesh()
        return remote(self.kept[0].at[1 - core], self.kept[1], self.kept[4:6], "pipe", 1 - core)

    def across(self, j):
        _, dp, _ = place_in_mesh()
        return remote(self.kept[1], self.kept[2].at[j - 1], [sem.at[j - 1] for sem in self.kept[6:8]], "dp", dp ^ j)

    def along(self, k):
        _, _, shard = place_in_mesh()
        return remote(
            self.kept[1].at[k], self.kept[3].at[k - 1], [sem.at[k - 1] for sem in self.kept[8:10]], "tensor", lax.rem(shard + k, 4)
        )

    def start(self):
        self.over().start()

    def second(self):
        core, _, _ = place_in_mesh()
        self.over().wait()
        self.kept[1][...] += self.kept[0][core]
        for j in (1, 2, 3):
            self.across(j).start()

    def third(self):
        for j in (1, 2, 3):
            self.across(j).wait()
        self.kept[1][...] += self.kept[2][0] + self.kept[2][1] + self.kept[2][2]
        for k in (1, 2, 3):
            self.along(k).start()

    def end(self):
        for k in (1, 2, 3):
            self.along(k).wait()
        self.kept[2][0, 0] = self.kept[1][0] + self.kept[3][0] + self.kept[3][1] + self.kept[3][2]
        copy = pltpu.make_async_copy(self.kept[2].at[0, 0], self.outs[0], self.kept[10])
        copy.start()
        copy.wait()


class Settle(Part):
    def __init__(self):
        super().__init__(
            [],
            [jax.ShapeDtypeStruct((3, D, D), BF)],
            [pltpu.VMEM((3, D, D), BF)] + sems(3) + [pltpu.SemaphoreType.DMA((3,)), pltpu.SemaphoreType.DMA((3,))],
        )

    def rows(self, core):
        return pl.ds(core * 256, 256)

    def send(self, source, n, core):
        return remote(source.at[self.rows(core)], self.outs[0].at[n, self.rows(core)], [sem.at[n] for sem in self.kept[1:3]], "pipe", 1 - core)

    def load(self, source, n, core):
        return pltpu.make_async_copy(source.at[self.rows(core)], self.kept[0].at[n, self.rows(core)], self.kept[3].at[n])

    def store(self, n, core):
        return pltpu.make_async_copy(self.kept[0].at[n, self.rows(core)], self.outs[0].at[n, self.rows(core)], self.kept[4].at[n])

    def start(self, matrices, layer, which):
        def action(core):
            for n in which:
                (self.load if core == layer else self.send)(matrices[n], n, core).start()

        by_core(action)

    def pass_on(self, matrices, layer, which):
        @pl.when(lax.axis_index("pipe") == layer)
        def _():
            for n in which:
                self.load(matrices[n], n, layer).wait()
                self.store(n, layer).start()

    def end(self, matrices):
        def action(core):
            for n in range(3):
                self.store(n, core).wait()
                self.send(matrices[1 - core][n], n, core).wait()

        by_core(action)


def table_sums(gtab_ref, index_ref, half_ref, pairs_ref, out_ref):
    for g in range(4):
        for n in range(2):
            half_ref[...] = gtab_ref[g, :, n * GL : (n + 1) * GL]
            even = half_ref[pl.ds(0, WP // 2, 2), :]
            odd = half_ref[pl.ds(1, WP // 2, 2), :]
            for m in range(2):
                lanes = slice(m * WP, (m + 1) * WP)
                pairs_ref[:, g * GH + 2 * n + m, :] = jnp.concatenate([even[:, lanes], odd[:, lanes]], 1)

    def add(n, total):
        pair = pairs_ref[n]
        high = pair.astype(BF)
        low = (pair - high.astype(F32)).astype(BF)
        places = places_of(index_ref[pl.ds(n, 1), :])
        return total + (dot_nt(high, places) + dot_nt(low, places))

    out_ref[...] = lax.fori_loop(0, WP // 2, add, jnp.zeros((H, 2 * GL), F32))


def reduce_end(attention0, totals_h0, turned_o0, piece_a1, shared1, grads_in, small, index):
    halves = ((0, 32), (32, 32))
    first = [ReduceFirst(attention0, rows=rows) for rows in halves]
    second = [ReduceSecond(size=32) for _ in halves]
    share = [Share(rows=halves[0])]
    share.append(Share(rows=halves[1], target=share[0]))
    onward_o = ReduceOnward(turned_o0)
    second_m, share_m = [ReduceSecond(totals_h0), ReduceSecond()], [Share(), Share()]
    share_a1, done_m1 = Share(piece_a1), Part(shared1)
    settle, little, places = Settle(), Little(24), Stored(index)
    input_grad = Weave(grads_in)

    def body(*refs):
        layers, (tabs_ref, pairs_ref, half_ref) = (refs[:5], refs[5:10]), refs[10:]
        for n in range(2):
            second[n].ins, share[n].ins, share_m[n].ins = [first[n].total], [second[n].kept[0]], [second_m[n].kept[0]]
        second_m[1].ins = [onward_o.kept[0]]
        done = (
            [share[0].outs[0], share_m[0].outs[0], share_m[1].outs[0]],
            [share_a1.outs[0], done_m1.ins[0], done_m1.ins[1]],
        )

        def tab(layer):
            table_sums(layers[layer][3], places.kept[0], half_ref, pairs_ref, tabs_ref.at[layer])

        greet()
        for task in (*first, onward_o, second_m[0]):
            task.start()
        places.load()
        first[0].cores()
        first[1].cores()
        settle.start(done[1], 1, (1, 2))
        input_grad.start()
        places.wait()
        tab(1)
        onward_o.close()
        second_m[1].start()
        second_m[0].close()
        share_m[0].start()
        first[0].turn()
        first[1].turn()
        tab(0)
        little.pack(layers, tabs_ref)
        little.start()
        share_a1.start()
        settle.pass_on(done[1], 1, (1, 2))
        first[0].close()
        second[0].start()
        little.second()
        first[1].close()
        second[1].start()
        second_m[1].close()
        share_m[1].start()
        share_m[0].end()
        share_a1.end()
        settle.start(done[1], 1, (0,))
        settle.start(done[0], 0, (1,))
        little.third()
        input_grad.wait()
        input_grad.weave(0, 2)
        for n in range(2):
            second[n].close()
            share[n].start()
        settle.pass_on(done[1], 1, (0,))
        settle.pass_on(done[0], 0, (1,))
        share_m[1].end()
        settle.start(done[0], 0, (2,))
        little.end()
        input_grad.weave(2, 4)
        settle.pass_on(done[0], 0, (2,))
        for n in range(2):
            share[n].end()
        settle.start(done[0], 0, (0,))
        settle.pass_on(done[0], 0, (0,))
        input_grad.end()
        settle.end(done)

    parts = [
        *first, *second, *share, onward_o, *second_m, *share_m, share_a1, done_m1, settle, little, input_grad, places
    ]
    _, given = carried_call(
        body, parts, 7, grid=(), in_specs=[pl.BlockSpec(memory_space=pltpu.VMEM)] * 10, inputs=small, out_specs=[], out_shape=[],
        scratch_shapes=[pltpu.VMEM((2, H, 2 * GL), F32), pltpu.VMEM((WP // 2, H, GL), F32), pltpu.VMEM((WP, GL), F32)],
        name="reduce_end", cost=pl.CostEstimate(flops=1 << 24, bytes_accessed=8 << 20, transcendentals=0),
    )
    by_part = dict(zip(map(id, parts), given))
    return by_part[id(settle)][0], by_part[id(little)][0], by_part[id(input_grad)][0]


def finish_body(
    matrix_ref, lines_ref, gqkv_ref, gproj_ref, ghw_ref, gow_ref, gain_ref, shift_ref, qv_ref, table_ref, bproj_ref, mgain_ref,
    mshift_ref, hb_ref, ob_ref,
):
    gqkv_ref[0] = dot_nn(matrix_ref[0, :, : 3 * GL], permutation(3 * GL, qkv_source, True))
    gproj_ref[0] = matrix_ref[0, :, 3 * GL :].T.astype(F32)
    ghw_ref[0] = matrix_ref[1].astype(F32)
    gow_ref[0] = matrix_ref[2].T.astype(F32)
    lines = lines_ref[...]
    for row, ref in (
        (GAIN, gain_ref), (SHIFT_ROW, shift_ref), (BPROJ, bproj_ref), (MGAIN, mgain_ref), (MSHIFT, mshift_ref), (OB, ob_ref)
    ):
        ref[...] = lines[row : row + 1]
    qv_ref[...] = jnp.concatenate([lines[QV + n : QV + n + 1, h * HD : (h + 1) * HD] for h in range(GH) for n in range(2)], 1)
    table_ref[0] = jnp.concatenate([lines[TABLE : TABLE + 4], lines[TABLE + 4 : TABLE + 8, : RELS - GL]], 1)
    hb_ref[...] = jnp.concatenate([lines[HB + n : HB + n + 1] for n in range(4)], 1)


def finish(matrices, lines):
    shapes = [
        (1, D, 3 * GL), (1, GL, D), (1, D, D), (1, D, D), (1, GL), (1, GL), (1, 2 * GL), (1, GH, RELS), (1, GL), (1, GL), (1, GL),
        (1, D), (1, GL),
    ]
    return plain_call(finish_body, "finish", (matrices, lines), [jax.ShapeDtypeStruct(shape, F32) for shape in shapes])


def layer_forward(layer, rolled, x, counts, table, bias, weights, tasks, ids):
    (fw, qkv, p, ho, mid), given = attn_fwd(layer, rolled, x, table, bias, weights[0](), tasks[0](), ids[0])
    mid = mid.reshape(-1, D)
    kept_a, given = given[0], given[1:]
    (second, act, slope, y, out), more = mlp_fwd(layer, rolled, counts, mid, table, weights[1](given), tasks[1](given), ids[1])
    return y, out, (x, fw, qkv, p, ho, mid, second, act, slope, kept_a, more[0]), given, more[1:]


def layer_backward(layer, rolled, cot, kept, counts, table, tasks, ids):
    x, fw, qkv, p, ho, mid, second, act, slope, kept_a, kept_m = kept
    (ghw, ghw_away, gow, gow_away, ghb, gmid, small_m), given = mlp_bwd(
        layer, rolled, counts, cot, act, slope, second, mid, table, Stored(*kept_m), tasks[0](), ids[0]
    )
    big_m = ((ghw, ghw_away), (gow, gow_away))
    (gin, out, ga, ga_away, gqv, gtab, small_a), more = attn_bwd(
        layer, rolled, x, gmid.reshape(-1, TP, D), fw, qkv, p, ho, table, Stored(*kept_a), tasks[1](big_m, given), ids[1]
    )
    return gin, out, ((ga, ga_away), *big_m), (ghb, small_m, gqv, gtab, small_a), given, more


SMALL_ROWS = ((GAIN, 1), (SHIFT_ROW, 1), (QV, 2), (TABLE, 8), (BPROJ, 1), (MGAIN, 1), (MSHIFT, 1), (HB, 4), (OB, 1))


def on_lines(small_in):
    whole_of = [lax.all_gather(lax.all_gather(member[0], "tensor", axis=0, tiled=True), "pipe") for member in small_in]
    gain, shift, qv, table, bproj, mgain, mshift, hb, ob = whole_of

    def lines(member):
        return member.reshape(2, 4, -1, GL)

    qv = qv.reshape(2, 4, GH, 2, HD).transpose(0, 1, 3, 2, 4)
    table = jnp.pad(table, ((0, 0), (0, 0), (0, 2 * GL - RELS))).reshape(2, 4, GH, 2, GL).transpose(0, 1, 3, 2, 4)
    rows = jnp.concatenate([lines(part) for part in (gain, shift, qv, table, bproj, mgain, mshift, hb, ob)], 2)
    return jnp.pad(rows, ((0, 0), (0, 0), (0, LINES - rows.shape[2]), (0, 0))).transpose(1, 0, 2, 3)


def qkv_order(w):
    lead = w.shape[:-1]
    return jnp.swapaxes(w.reshape(*lead, GH, 3, HD), -3, -2).reshape(*lead, 3 * GL)


def general(core, images, cotangent, counts, rel_index, small_in, big_in):
    def both(member, axis):
        return lax.all_gather(lax.all_gather(member[0], "tensor", axis=axis, tiled=True), "pipe")

    table = on_lines(small_in)
    bias = bias_tables(table, rel_index)
    gathered = [both(member, axis) for member, axis in zip(big_in, (1, 0, 1, 0))]
    weights = []
    for l in range(2):
        wqkv, wproj, hw, ow = (pair[l] for pair in gathered)
        wqkv = qkv_order(wqkv.reshape(D, 4, 3 * GL).transpose(1, 0, 2))
        wa = jnp.concatenate([wqkv, wproj.reshape(4, GL, D).transpose(0, 2, 1)], 2)[None]
        wm = jnp.stack([hw.reshape(D, 4, -1).transpose(1, 0, 2), ow.reshape(4, -1, D)])
        weights.append((lambda *_, wa=wa: Weights(1, 0, whole=wa), lambda *_, wm=wm: Weights(2, 0, whole=wm)))
    none, back_none, ids = (lambda: [], lambda given: []), (lambda: [], lambda *_: []), (None, None)
    images, cotangent = (
        jnp.pad(lax.dynamic_index_in_dim(array, core, 1, False), ((0, 0), (0, TP - TOK), (0, 0))) for array in (images, cotangent)
    )
    y0, out0, kept0, _, _ = layer_forward(0, False, images, counts, table, bias, weights[0], none, ids)
    _, out1, kept1, _, _ = layer_forward(1, False, y0, counts, table, bias, weights[1], none, ids)
    g1, gin1, big1, small1, _, _ = layer_backward(1, False, cotangent, kept1, counts, table, back_none, ids)
    _, gin0, big0, small0, _, _ = layer_backward(0, False, g1, kept0, counts, table, back_none, ids)
    first_core = core == 0

    def deliver(mine0, mine1):
        came = lax.ppermute(jnp.where(first_core, mine1, mine0), "pipe", [(0, 1), (1, 0)])
        mine = jnp.where(first_core, mine0, mine1)
        return jnp.stack([jnp.where(first_core, mine, came), jnp.where(first_core, came, mine)], 1)[None]

    def matrix_of(pair):
        parts = [part[jnp.array([PLACES.index(j) for j in range(4)])] for part in pair]
        return jnp.concatenate(parts).transpose(1, 0, 2, 3).reshape(4, D, D)

    def full(big):
        ga, ghw, gow = (matrix_of(pair) for pair in big)
        gqkv = jnp.swapaxes(ga[:, :, : 3 * GL].reshape(4, D, 3, GH, HD), 2, 3).reshape(4, D, 3 * GL)
        return (
            gqkv.transpose(1, 0, 2).reshape(D, 3 * D), ga[:, :, 3 * GL :].transpose(0, 2, 1).reshape(D, D),
            ghw.transpose(1, 0, 2).reshape(D, -1), gow.transpose(0, 2, 1).reshape(-1, D),
        )

    def reduced(pair, axis):
        mine = lax.psum_scatter(jnp.stack(pair), "pipe", scatter_dimension=0, tiled=False)
        mine = lax.psum_scatter(mine, "tensor", scatter_dimension=axis, tiled=True)
        return lax.psum(mine, "dp").astype(F32)[None]

    gqkv, gproj, ghw, gow = (reduced(pair, axis) for pair, axis in zip(zip(full(big0), full(big1)), (1, 0, 1, 0)))

    def vectors(terms):
        ghb, small_m, gqv, gtab, small_a = terms
        qv = jnp.swapaxes(gqv.reshape(4, 2, GH, HD), 1, 2).reshape(-1)
        tab = table_grad(gtab, rel_index).reshape(H, RELS)
        parts = (small_a[:, 0], small_a[:, 1], qv, tab, small_m[:, 1], small_m[:, 2], small_m[:, 3], ghb, small_m[:, 0])
        return jnp.concatenate([part.reshape(-1) for part in parts])

    totals = lax.psum(jnp.stack([vectors(small0), vectors(small1)]), ("pipe", "dp", "tensor"))
    mine = jnp.where(first_core, totals[0], totals[1])
    outs, at = [], 0
    for member in small_in:
        shape = member.shape[1:]
        whole_shape = (shape[0] * lax.axis_size("tensor"),) + tuple(shape[1:])
        size = math.prod(whole_shape)
        piece = mine[at : at + size].reshape(whole_shape)
        outs.append(lax.dynamic_slice_in_dim(piece, lax.axis_index("tensor") * shape[0], shape[0], 0)[None])
        at += size
    return deliver(out0, out1), deliver(gin0, gin1), (gqkv, gproj, ghw, gow), outs


def four_by_four(images, cotangent, counts, rel_index, small_in, big_in):
    own_a, lines, index = prepare(rel_index.T, big_in[0][0], big_in[1][0], *[member[0] if member.ndim == 3 else member for member in small_in])
    own = (own_a, big_in[2][0], big_in[3][0])
    other, table, pieces_a0, near_h0, near_o0, bias, x0 = gather_start(own, lines, index, jnp.swapaxes(images, 1, 2))
    pick_cot = Own(jnp.swapaxes(cotangent, 1, 2), plan=((2, "pick"),))

    def near(n, layer, **how):
        return Near(layer, own[n], other[n], **how)

    def weights(layer, which, pieces):
        return Weights(len(which), layer, own=[own[n] for n in which], other=[other[n] for n in which], pieces=pieces)

    def mlp_tasks(near_h, near_o):
        return [Far(near_h, plan=((1, "turn"), (2, "rest"), (3, "last"))), Far(near_o, plan=((2, "turn"), (3, "rest"), (3, "last")))]

    def forward_weights(layer, pieces, near_h, near_o):
        return (
            lambda: weights(layer, (0,), [pieces]),
            lambda given: weights(layer, (1, 2), [[near_h, *given[1]], [near_o, *given[2]]]),
        )

    y0, out0, kept0, given, more = layer_forward(
        0, True, x0, counts, table, bias, forward_weights(0, pieces_a0, near_h0, near_o0),
        (lambda: [*mlp_tasks(near_h0, near_o0), near(0, 1), near(1, 1, deferred=True, plan=((1, "start"),))],
         lambda given: [Far(given[3][0], plan=((1, "turn"), (2, "rest"), (3, "last"))), near(2, 1)]),
        (1, 2),
    )
    pieces_a1, near_h1, near_o1 = [given[3][0], *more[1]], given[4][0], more[2][0]
    _, out1, kept1, given, _ = layer_forward(
        1, True, y0, counts, table, bias, forward_weights(1, pieces_a1, near_h1, near_o1),
        (lambda: [*mlp_tasks(near_h1, near_o1), pick_cot], lambda given: []), (3, None),
    )
    cot = given[3][0]

    def mlp_reduce(big_m):
        return [ReduceTurn(big_m[0], plan=((0, "cores"),)), ReduceTurn(big_m[1], plan=((1, "cores"),))]

    g1, gin1, big1, small1, given, more = layer_backward(
        1, True, cot, kept1, counts, table, (lambda: [Deliver([out0, out1])], lambda big_m, given: mlp_reduce(big_m)), (4, 5)
    )
    out_came, turned1 = given[1][0], more[1:3]

    def last_tasks(big_m, given):
        onward = ReduceOnward(given[1], plan=((1, "close"),))
        second_h = ReduceSecond(given[2][0], plan=((1, "close"),))
        second_o = ReduceSecond(given[3][0], deferred=True, plan=((1, "start"), (LATE, "close")))
        second_a = ReduceSecond(source=onward, deferred=True, plan=((2, "start"),))
        shares = [Share(source=second_h, plan=((1, "start"),)), Share(source=second_o, plan=((LATE, "start"),))]
        return [
            ReduceFirst(big_m[0], plan=((0, "cores"), (LATE, "turn"))), ReduceTurn(big_m[1], plan=((1, "cores"),)), onward, second_h,
            *shares[:1], second_o, second_a, *shares[1:], Weave([out0, out1], out_came, plan=((3, "all"),)),
        ]

    _, gin0, big0, small0, given, more = layer_backward(
        0, True, g1, kept0, counts, table,
        (
            lambda: [ReduceTurn(big1[0], plan=((0, "cores"),)), *[ReduceOnward(turned) for turned in turned1]],
            last_tasks,
        ),
        (6, 8),
    )
    totals_h0, turned_o0, piece_a1, shared1 = more[1][0], more[2], more[7][0], (more[5][0], more[8][0])
    block_out = more[9][0]
    matrices, lines, input_grad = reduce_end(
        big0[0], totals_h0, turned_o0, piece_a1, shared1, [gin0, gin1], [*small0, *small1], index
    )
    gqkv, gproj, ghw, gow, *outs = finish(matrices, lines)
    return jnp.swapaxes(block_out, 1, 2)[None], jnp.swapaxes(input_grad, 1, 2)[None], (gqkv, gproj, ghw, gow), outs


def local(
    images, cotangent, counts, rel_index, pre_attn_gain, pre_attn_bias, qkv_weight, qv_bias, bias_table, proj_weight, proj_bias,
    pre_mlp_gain, pre_mlp_bias, hidden_weight, hidden_bias, out_weight, out_bias,
):
    assert images.shape[1] == 2, images.shape
    counts = counts.T
    small_in = (pre_attn_gain, pre_attn_bias, qv_bias, bias_table, proj_bias, pre_mlp_gain, pre_mlp_bias, hidden_bias, out_bias)
    big_in = (qkv_weight, proj_weight, hidden_weight, out_weight)
    if lax.axis_size("tensor") == 4 and lax.axis_size("dp") == 4:
        block_out, input_grad, big, small = four_by_four(images, cotangent, counts, rel_index, small_in, big_in)
    else:
        block_out, input_grad, big, small = general(
            lax.axis_index("pipe"), images, cotangent, counts, rel_index, small_in, big_in
        )
    gqkv, gproj, ghw, gow = big
    gain_g, shift_g, qv_g, table_g, bproj_g, mgain_g, mshift_g, hb_g, ob_g = small
    return (
        block_out, input_grad, gain_g, shift_g, gqkv, qv_g, table_g, gproj, bproj_g, mgain_g, mshift_g, ghw, hb_g, gow, ob_g,
    )


def solution(mesh):
    return jax.shard_map(
        local,
        mesh=mesh,
        in_specs=(
            P(None, ("dp", "tensor"), None, None),
            P(None, ("dp", "tensor"), None, None),
            P(None, "dp"),
            P(),
            P("pipe", "tensor"),
            P("pipe", "tensor"),
            P("pipe", None, "tensor"),
            P("pipe", "tensor"),
            P("pipe", "tensor", None),
            P("pipe", "tensor", None),
            P("pipe", "tensor"),
            P("pipe", "tensor"),
            P("pipe", "tensor"),
            P("pipe", None, "tensor"),
            P("pipe", "tensor"),
            P("pipe", "tensor", None),
            P("pipe", "tensor"),
        ),
        out_specs=(
            P("pipe", None, ("dp", "tensor"), None, None),
            P("pipe", None, ("dp", "tensor"), None, None),
            P("pipe", "tensor"),
            P("pipe", "tensor"),
            P("pipe", None, "tensor"),
            P("pipe", "tensor"),
            P("pipe", "tensor", None),
            P("pipe", "tensor", None),
            P("pipe", "tensor"),
            P("pipe", "tensor"),
            P("pipe", "tensor"),
            P("pipe", None, "tensor"),
            P("pipe", "tensor"),
            P("pipe", "tensor", None),
            P("pipe", "tensor"),
        ),
        check_vma=False,
    )
```

```python
import functools
import math

import jax
import jax.numpy as jnp
from jax import lax
from jax.experimental import pallas as pl
from jax.experimental.pallas import tpu as pltpu
from jax.sharding import PartitionSpec as P

D = 512
H = 16
HD = 32
WIN = 7
GRID = 14
SHIFT = 3
TOK = 196
RELS = 169
POS = WIN * WIN
NW = 4
WP = 64
TP = 208
ROWS = NW * WP
GH = 4
GL = GH * HD
BLK = 832
SUB_FWD = 208
SUB_BWD = 416
CHUNK = 64
AT_ONCE = 2
LATE = "late"
LINES = 32
GAIN, SHIFT_ROW, QV, TABLE, BPROJ, MGAIN, MSHIFT, HB, OB = 0, 1, 2, 4, 12, 13, 14, 15, 19
PLACES = (1, 3, 2, 0)
EPSILON = 1e-05
MASK_VALUE = -100.0
SHUT = -1e30
F32 = jnp.float32
BF = jnp.bfloat16
ANY = pl.BlockSpec(memory_space=pl.ANY)
VMEM_LIMIT = 60 << 20


def dot_nn(a, b):
    return lax.dot_general(a, b, (((1,), (0,)), ((), ())), preferred_element_type=F32)


def dot_nt(a, b):
    return lax.dot_general(a, b, (((1,), (1,)), ((), ())), preferred_element_type=F32)


def dot_tn(a, b):
    return lax.dot_general(a, b, (((0,), (0,)), ((), ())), preferred_element_type=F32)


def iota(shape, axis):
    return lax.broadcasted_iota(jnp.int32, shape, axis)


def normalize(rows):
    center = rows - jnp.mean(rows, -1, keepdims=True)
    inverse = lax.rsqrt(jnp.mean(center * center, -1, keepdims=True) + EPSILON)
    return center * inverse, inverse


def norm_back(grad_out, normed, inverse, gain):
    scaled = grad_out * gain
    return inverse * (
        scaled
        - jnp.mean(scaled, -1, keepdims=True)
        - normed * jnp.mean(scaled * normed, -1, keepdims=True)
    )


def remote(source, target, sems, axis, index):
    return pltpu.make_async_remote_copy(
        src_ref=source, dst_ref=target, send_sem=sems[0], recv_sem=sems[1], device_id={axis: index},
        device_id_type=pl.DeviceIdType.MESH,
    )


def place_in_mesh():
    return lax.axis_index("pipe"), lax.axis_index("dp"), lax.axis_index("tensor")


def greet():
    core, dp, shard = place_in_mesh()
    barrier = pltpu.get_barrier_semaphore()

    def signal(axis, index):
        pl.semaphore_signal(barrier, inc=1, device_id={axis: index}, device_id_type=pl.DeviceIdType.MESH)

    signal("pipe", 1 - core)
    for k in (1, 2, 3):
        signal("dp", dp ^ k)
        signal("tensor", lax.rem(shard + k, 4))
    pl.semaphore_wait(barrier, 7)


def quarter(half, j):
    core, dp, _ = place_in_mesh()
    return pl.ds(pl.multiple_of((core ^ half) * 256 + (dp ^ j) * CHUNK, CHUNK), CHUNK)


def by_core(action):
    for which in (0, 1):

        @pl.when(lax.axis_index("pipe") == which)
        def _():
            action(which)


def sems(*shape):
    return [pltpu.SemaphoreType.DMA(shape), pltpu.SemaphoreType.DMA(shape)]


class Part:
    plan = ()
    deferred = False

    def flush(self):
        pass

    def __init__(self, inputs=(), outputs=(), scratch=()):
        self.inputs, self.outputs, self.scratch = list(inputs), list(outputs), list(scratch)

    def bind(self, ins, outs, kept):
        self.ins, self.outs, self.kept = ins, outs, kept


class Weights(Part):
    def __init__(self, count, layer, whole=None, own=None, other=None, pieces=None):
        self.count, self.layer, self.whole = count, layer, whole
        inputs = [whole] if whole is not None else [*own, *other, *[piece for group in pieces for piece in group]]
        super().__init__(inputs, (), [pltpu.VMEM((count, 4, D, D), BF), pltpu.SemaphoreType.DMA((9 * count,))])

    def shard(self, mine, b):
        store, sem = self.kept
        if self.whole is not None:
            return pltpu.make_async_copy(self.ins[0].at[b, 0], store.at[b, 0], sem.at[b * 9])
        owns, others = self.ins[: self.count], self.ins[self.count : 2 * self.count]
        return pltpu.make_async_copy((owns if mine else others)[b], store.at[b, 0], sem.at[b * 9])

    def rest(self):
        store, sem = self.kept
        if self.whole is not None:
            return [
                pltpu.make_async_copy(self.ins[0].at[b, pl.ds(1, 3)], store.at[b, pl.ds(1, 3)], sem.at[b * 9 + 1])
                for b in range(self.count)
            ]
        return [
            pltpu.make_async_copy(
                self.ins[2 * self.count + b * 8 + half * 4 + j], store.at[b, pl.ds(1, 3), quarter(half, j), :],
                sem.at[b * 9 + half * 4 + j + 1],
            )
            for b in range(self.count)
            for half in range(2)
            for j in range(4)
        ]

    def load(self):
        if self.whole is not None:
            for b in range(self.count):
                self.shard(True, b).start()
        else:

            def shards(core):
                for b in range(self.count):
                    self.shard(core == self.layer, b).start()

            by_core(shards)
        if self.count == 1:
            self.load_rest()

    def load_rest(self):
        for copy in self.rest():
            copy.start()

    def wait_shard(self):
        for b in range(self.count):
            self.shard(True, b).wait()

    def wait_rest(self):
        for copy in self.rest():
            copy.wait()


class Stored(Part):
    def __init__(self, *arrays):
        super().__init__(arrays, (), [pltpu.VMEM(a.shape, a.dtype) for a in arrays] + [pltpu.SemaphoreType.DMA((len(arrays),))])

    def copies(self):
        return [pltpu.make_async_copy(ref, kept, self.kept[-1].at[n]) for n, (ref, kept) in enumerate(zip(self.ins, self.kept))]

    def load(self):
        for copy in self.copies():
            copy.start()

    def wait(self):
        for copy in self.copies():
            copy.wait()


class Keep(Part):
    def __init__(self, *shapes):
        super().__init__((), [jax.ShapeDtypeStruct(shape, BF) for shape in shapes], [pltpu.SemaphoreType.DMA((len(shapes),))])

    def copies(self, refs):
        return [pltpu.make_async_copy(ref, out, self.kept[0].at[n]) for n, (ref, out) in enumerate(zip(refs, self.outs))]

    def start(self, *refs):
        for copy in self.copies(refs):
            copy.start()

    def wait(self, *refs):
        for copy in self.copies(refs):
            copy.wait()


class Near(Part):
    def __init__(self, layer, own, other, plan=(), deferred=False):
        self.layer, self.plan, self.deferred = layer, plan, deferred
        inputs = [] if own is None else [own, other]
        super().__init__(inputs, [jax.ShapeDtypeStruct((3, CHUNK, D), BF)], sems(3))

    def copy(self, mine, k):
        _, _, shard = place_in_mesh()
        source = self.ins[0 if mine else 1].at[quarter(0, 0), :]
        return remote(source, self.outs[0].at[k - 1], [sem.at[k - 1] for sem in self.kept], "tensor", lax.rem(shard + 4 - k, 4))

    def start(self):
        def sends(core):
            for k in (2, 1, 3):
                self.copy(core == self.layer, k).start()

        by_core(sends)

    def finish(self):
        for k in (1, 2, 3):
            self.copy(True, k).wait()

    def end(self):
        if not any(what == "finish" for _, what in self.plan):
            self.finish()


class Far(Part):
    def __init__(self, near, plan=(), source=None, deferred=False):
        self.plan, self.source, self.deferred = plan, source, deferred
        shape = jax.ShapeDtypeStruct((3, CHUNK, D), BF)
        super().__init__([] if near is None else [near], [shape] * 7, sems(2, 2) + sems(2) + sems(4))

    def rows(self, j):
        return pl.ds((j - 1) * 32, 32)

    def across(self, j, half):
        _, dp, _ = place_in_mesh()
        rows = self.rows(j if half == 0 else 3 - j)
        return remote(
            self.ins[0].at[:, rows], self.outs[j - 1].at[:, rows], [sem.at[j - 1, half] for sem in self.kept[:2]], "dp", dp ^ j
        )

    def onward(self, j):
        _, dp, _ = place_in_mesh()
        rows = self.rows(j)
        return remote(
            self.outs[j - 1].at[:, rows], self.outs[2].at[:, rows], [sem.at[j - 1] for sem in self.kept[2:4]], "dp", dp ^ (3 - j)
        )

    def over(self, j):
        core, _, _ = place_in_mesh()
        source = self.ins[0] if j == 0 else self.outs[j - 1]
        return remote(source, self.outs[3 + j], [sem.at[j] for sem in self.kept[4:]], "pipe", 1 - core)

    def start(self):
        for half in (0, 1):
            for j in (1, 2):
                self.across(j, half).start()
        self.over(0).start()

    def turn(self):
        for j in (1, 2):
            self.across(j, 0).wait()
        for j in (1, 2):
            self.onward(j).start()

    def rest(self):
        for j in (1, 2):
            self.across(j, 1).wait()
            self.over(j).start()

    def last(self):
        for j in (1, 2):
            self.onward(j).wait()
        self.over(3).start()

    def end(self):
        for j in range(4):
            self.over(j).wait()


class ReduceFirst(Part):
    def __init__(self, pair, plan=(), rows=(0, CHUNK)):
        self.plan, (self.start_row, self.size) = plan, rows
        size = self.size
        half = pltpu.VMEM((4, 4, size, D), BF)
        super().__init__(
            pair,
            [jax.ShapeDtypeStruct((4, size, D), BF)],
            [half, half, pltpu.VMEM((2, 2, 2, size, D), BF), pltpu.VMEM((2, 2, size, D), BF), pltpu.VMEM((4, size, D), BF)]
            + sems() + sems(2) + sems(2) + [pltpu.SemaphoreType.DMA(()), pltpu.SemaphoreType.DMA(())],
        )

    def bind(self, ins, outs, kept):
        super().bind(ins, outs, kept)
        self.mine, self.came, self.first, self.second, self.total = kept[:5]

    def over(self):
        core, _, _ = place_in_mesh()
        source = self.ins[1].at[:, :, pl.ds(self.start_row, self.size)]
        return remote(source, self.came, self.kept[5:7], "pipe", 1 - core)

    def load(self):
        return pltpu.make_async_copy(self.ins[0].at[:, :, pl.ds(self.start_row, self.size)], self.mine, self.kept[11])

    def across(self, j):
        _, dp, _ = place_in_mesh()
        source = self.mine.at[pl.ds(j - 1, 2), pl.ds(2 * j - 2, 2)]
        return remote(source, self.first.at[j - 1], [sem.at[j - 1] for sem in self.kept[7:9]], "dp", dp ^ j)

    def onward(self, j):
        _, dp, _ = place_in_mesh()
        source = self.mine.at[2 if j == 1 else 0, pl.ds(2 * j - 2, 2)]
        return remote(source, self.second.at[j - 1], [sem.at[j - 1] for sem in self.kept[9:11]], "dp", dp ^ (3 - j))

    def start(self):
        self.over().start()
        self.load().start()

    def cores(self):
        self.over().wait()
        self.load().wait()

        def add(place, k):
            self.mine[place, k] += self.came[place, k]

        def sent(n, carry):
            add(n // 2, n % 2)
            add(n // 2 + 1, n % 2 + 2)
            return carry

        def kept(n, carry):
            add(3, n)
            add(2 - n // 2 * 2, n)
            return carry

        lax.fori_loop(0, 4, sent, 0)
        for j in (1, 2):
            self.across(j).start()
        lax.fori_loop(0, 4, kept, 0)

    def turn(self):
        for j in (1, 2):
            self.across(j).wait()

        def add(n, carry):
            self.mine[2, n] += self.first[0, 1, n]
            self.mine[0, n + 2] += self.first[1, 0, n]
            return carry

        lax.fori_loop(0, 2, add, 0)
        for j in (1, 2):
            self.onward(j).start()

    def close(self):
        for j in (1, 2):
            self.onward(j).wait()

        def add(n, carry):
            for j in (1, 2):
                k = n + 2 * j - 2
                total = self.mine[3, k].astype(F32) + self.first[j - 1, j - 1, n].astype(F32)
                self.total[k] = (total + self.second[j - 1, n].astype(F32)).astype(BF)
            return carry

        lax.fori_loop(0, 2, add, 0)

    def out(self):
        return pltpu.make_async_copy(self.total, self.outs[0], self.kept[12])

    def end(self):
        self.close()
        self.out().start()

    def flush(self):
        self.out().wait()


class ReduceTurn(ReduceFirst):
    def __init__(self, pair, plan=()):
        super().__init__(pair, plan)
        self.outputs = [jax.ShapeDtypeStruct((2, 2, CHUNK, D), BF), jax.ShapeDtypeStruct((4, CHUNK, D), BF)]
        self.scratch.append(pltpu.SemaphoreType.DMA((3,)))

    def end(self):
        for j in (1, 2):
            self.across(j).wait()

        def add(n, carry):
            self.mine[2, n] += self.first[0, 1, n]
            self.mine[0, n + 2] += self.first[1, 0, n]
            for j in (1, 2):
                self.mine[3, n + 2 * j - 2] += self.first[j - 1, j - 1, n]
            return carry

        lax.fori_loop(0, 2, add, 0)
        for copy in self.copies():
            copy.start()

    def copies(self):
        sem = self.kept[13]
        return [
            pltpu.make_async_copy(self.mine.at[2, pl.ds(0, 2)], self.outs[0].at[0], sem.at[0]),
            pltpu.make_async_copy(self.mine.at[0, pl.ds(2, 2)], self.outs[0].at[1], sem.at[1]),
            pltpu.make_async_copy(self.mine.at[3], self.outs[1], sem.at[2]),
        ]

    def flush(self):
        for copy in self.copies():
            copy.wait()


class ReduceOnward(Part):
    def __init__(self, given, plan=()):
        self.plan = plan
        base = pltpu.VMEM((4, CHUNK, D), BF)
        super().__init__(
            given, [jax.ShapeDtypeStruct((4, CHUNK, D), BF)],
            [base, pltpu.VMEM((2, 2, CHUNK, D), BF)] + sems(2) + [pltpu.SemaphoreType.DMA(()), pltpu.SemaphoreType.DMA(())],
        )

    def onward(self, j):
        _, dp, _ = place_in_mesh()
        return remote(self.ins[0].at[j - 1], self.kept[1].at[j - 1], [sem.at[j - 1] for sem in self.kept[2:4]], "dp", dp ^ (3 - j))

    def load(self):
        return pltpu.make_async_copy(self.ins[1], self.kept[0], self.kept[4])

    def start(self):
        for j in (1, 2):
            self.onward(j).start()
        self.load().start()

    def close(self):
        self.load().wait()
        for j in (1, 2):
            self.onward(j).wait()
        total = self.kept[0]

        def add(n, carry):
            for j in (1, 2):
                total[n + 2 * j - 2] += self.kept[1][j - 1, n]
            return carry

        lax.fori_loop(0, 2, add, 0)

    def out(self):
        return pltpu.make_async_copy(self.kept[0], self.outs[0], self.kept[5])

    def end(self):
        if not any(what == "close" for _, what in self.plan):
            self.close()
        self.out().start()

    def flush(self):
        self.out().wait()


class ReduceSecond(Part):
    def __init__(self, totals=None, size=CHUNK, plan=(), source=None, deferred=False):
        self.plan, self.after, self.deferred = plan, source, deferred
        line = pltpu.VMEM((size, D), BF)
        super().__init__(
            [totals] if totals is not None else [],
            [jax.ShapeDtypeStruct((size, D), BF)],
            [line, pltpu.VMEM((3, size, D), BF)] + sems(3) + [pltpu.SemaphoreType.DMA(()), pltpu.SemaphoreType.DMA(())],
        )

    def own(self):
        return pltpu.make_async_copy(self.ins[0].at[0], self.kept[0], self.kept[4])

    def along(self, k):
        _, _, shard = place_in_mesh()
        return remote(
            self.ins[0].at[k], self.kept[1].at[k - 1], [sem.at[k - 1] for sem in self.kept[2:4]], "tensor", lax.rem(shard + k, 4)
        )

    def start(self):
        if self.after is not None:
            self.ins = [self.after.kept[0]]
        for k in (2, 1, 3):
            self.along(k).start()
        self.own().start()

    def close(self):
        self.own().wait()
        for k in (1, 2, 3):
            self.along(k).wait()
        total = self.kept[0][...].astype(F32)
        for k in range(3):
            total += self.kept[1][k].astype(F32)
        self.kept[0][...] = total.astype(BF)

    def end(self):
        if not any(what == "close" for _, what in self.plan):
            self.close()
        self.out().start()

    def out(self):
        return pltpu.make_async_copy(self.kept[0], self.outs[0], self.kept[5])

    def flush(self):
        self.out().wait()


class Share(Part):
    def __init__(self, piece=None, rows=(0, CHUNK), target=None, source=None, plan=(), in_vmem=False):
        self.start_row, self.size = rows
        self.target, self.after, self.plan, self.deferred = target, source, plan, source is not None
        super().__init__(
            [piece] if piece is not None else [],
            [jax.ShapeDtypeStruct((D, D), BF)] if target is None and not in_vmem else [],
            [pltpu.VMEM((self.size, D), BF)] + sems(3) + [pltpu.SemaphoreType.DMA(()), pltpu.SemaphoreType.DMA(())]
            + ([pltpu.VMEM((D, D), BF)] if in_vmem else []),
        )
        self.in_vmem = in_vmem

    def whole(self):
        return self.kept[5] if self.in_vmem else self.outs[0]

    def place(self):
        core, dp, _ = place_in_mesh()
        start = pl.multiple_of(core * 256 + dp * CHUNK, CHUNK) + self.start_row
        out = (self.target or self).whole()
        return out.at[pl.ds(pl.multiple_of(start, self.size), self.size), :]

    def across(self, j):
        _, dp, _ = place_in_mesh()
        return remote(self.ins[0], self.place(), [sem.at[j - 1] for sem in self.kept[1:3]], "dp", dp ^ j)

    def load(self):
        return pltpu.make_async_copy(self.ins[0], self.kept[0], self.kept[3])

    def keep(self):
        return pltpu.make_async_copy(self.kept[0], self.place(), self.kept[4])

    def start(self):
        if self.after is not None:
            self.ins = [self.after.kept[0]]
        for j in (3, 1, 2):
            self.across(j).start()
        self.load().start()

    def end(self):
        self.load().wait()
        self.keep().start()
        for j in (1, 2, 3):
            self.across(j).wait()

    def flush(self):
        self.keep().wait()


class Deliver(Part):
    def __init__(self, of_layers):
        super().__init__(of_layers, [jax.ShapeDtypeStruct(of_layers[0].shape, BF)], sems())

    def send(self, core):
        return remote(self.ins[1 - core], self.outs[0], self.kept, "pipe", 1 - core)

    def start(self):
        by_core(lambda core: self.send(core).start())

    def end(self):
        self.send(0).wait()


class Weave(Part):
    def __init__(self, of_layers, came=None, plan=()):
        self.plan = plan
        count = of_layers[0].shape[0]
        images = pltpu.VMEM((count, TOK, D), BF)
        self.count = count
        super().__init__(
            [*of_layers] + ([] if came is None else [came]), [jax.ShapeDtypeStruct((count, TOK, 2, D), BF)],
            [images, images, pltpu.VMEM((count, TOK, 2, D), BF)] + sems()
            + [pltpu.SemaphoreType.DMA(()), pltpu.SemaphoreType.DMA(()), pltpu.SemaphoreType.DMA((count,))],
        )

    def send(self, core):
        return remote(self.ins[1 - core], self.kept[1], self.kept[3:5], "pipe", 1 - core)

    def own(self, core):
        return pltpu.make_async_copy(self.ins[core], self.kept[0], self.kept[5])

    def came(self):
        return pltpu.make_async_copy(self.ins[2], self.kept[1], self.kept[6])

    def store(self, m):
        return pltpu.make_async_copy(self.kept[2].at[m], self.outs[0].at[m], self.kept[7].at[m])

    def start(self):
        by_core(lambda core: self.own(core).start())
        if len(self.ins) > 2:
            self.came().start()
        else:
            by_core(lambda core: self.send(core).start())

    def wait(self):
        self.own(0).wait()
        (self.came() if len(self.ins) > 2 else self.send(0)).wait()

    def weave(self, first, last):
        first_core = lax.axis_index("pipe") == 0

        def image(m, carry):
            mine, theirs = self.kept[0][m], self.kept[1][m]
            pair = [jnp.where(first_core, mine, theirs), jnp.where(first_core, theirs, mine)]
            self.kept[2][m] = jnp.stack(pair, axis=1)
            return carry

        lax.fori_loop(first, last, image, 0)
        for m in range(first, last):
            self.store(m).start()

    def all(self):
        self.wait()
        self.weave(0, self.count)

    def end(self):
        for m in range(self.count):
            self.store(m).wait()


def carried_call(body, parts, collective_id, *, grid, in_specs, inputs, out_specs, out_shape, scratch_shapes, name, cost):
    n_in, n_out, n_scratch = len(inputs), len(out_shape), len(scratch_shapes)
    counts = [(len(part.inputs), len(part.outputs), len(part.scratch)) for part in parts]

    def whole_body(*refs):
        refs = list(refs)

        def take(count, groups):
            mine = [refs.pop(0) for _ in range(count)]
            return mine, [[refs.pop(0) for _ in range(n)] for n in groups]

        mine, part_ins = take(n_in, [n for n, _, _ in counts])
        outs, part_outs = take(n_out, [n for _, n, _ in counts])
        kept, part_kept = take(n_scratch, [n for _, _, n in counts])
        for part, a, b, c in zip(parts, part_ins, part_outs, part_kept):
            part.bind(a, b, c)
        for part in parts:
            if getattr(part, "source", None) is not None:
                part.ins = [part.source.outs[0]]
        body(*mine, *outs, *kept)

    extra_in = [x for part in parts for x in part.inputs]
    extra_out = [x for part in parts for x in part.outputs]
    params = dict(vmem_limit_bytes=VMEM_LIMIT)
    if collective_id is not None:
        params.update(collective_id=collective_id, has_side_effects=True)
    results = pl.pallas_call(
        whole_body,
        grid_spec=pltpu.PrefetchScalarGridSpec(
            num_scalar_prefetch=0,
            grid=grid,
            in_specs=list(in_specs) + [ANY] * len(extra_in),
            out_specs=list(out_specs) + [ANY] * len(extra_out),
            scratch_shapes=list(scratch_shapes) + [x for part in parts for x in part.scratch],
        ),
        out_shape=list(out_shape) + extra_out,
        name=name,
        compiler_params=pltpu.CompilerParams(**params),
        cost_estimate=cost,
    )(*inputs, *extra_in)
    own, rest = results[:n_out], results[n_out:]
    given = []
    for _, n, _ in counts:
        given.append(rest[:n])
        rest = rest[n:]
    return own, given


def begin(weights, tasks):
    pl.when(pl.program_id(0) == 0)(weights.load)
    if tasks:

        @pl.when(pl.program_id(0) == 0)
        def _():
            greet()
            for task in tasks:
                if not task.deferred:
                    task.start()

    if isinstance(weights, Weights) and weights.count > 1:
        pl.when(pl.program_id(0) == 0)(weights.load_rest)


def planned(tasks, point):
    return [getattr(task, what) for task in tasks for at, what in task.plan if at == point]


def step_end(tasks, steps):
    for step in range(steps):
        calls = planned(tasks, step)
        if step == steps - 1:
            calls += [task.end for task in tasks] + [task.flush for task in tasks]
        if calls:

            @pl.when(pl.program_id(0) == step)
            def _():
                for call in calls:
                    call()


def whole(shape):
    return pl.BlockSpec(shape, lambda i: (0,) * len(shape))


def per(shape):
    return pl.BlockSpec((1,) + shape, lambda i: (i,) + (0,) * len(shape))


SMEM = pl.BlockSpec(memory_space=pltpu.SMEM)


def along_model(table_ref, layer, row, rolled):
    shard = lax.axis_index("tensor") if rolled else 0
    return jnp.concatenate([table_ref[(z - shard + 4) % 4, layer, row : row + 1, :].astype(F32) for z in range(4)], 1)


def window_token(shape, axis, offset):
    s = iota(shape, axis)
    w, a = s // WP, s % WP
    r = (w // 2) * WIN + a // WIN + offset
    c = (w % 2) * WIN + a % WIN + offset
    r, c = jnp.where(r >= GRID, r - GRID, r), jnp.where(c >= GRID, c - GRID, c)
    return jnp.where(a < POS, r * GRID + c, -1)


def spread_map(offset):
    return (window_token((ROWS, 1), 0, offset) == iota((ROWS, TP), 1)).astype(F32).astype(BF)


def gather_map(offset):
    return (window_token((1, ROWS), 1, offset) == iota((TP, ROWS), 0)).astype(F32).astype(BF)


def head_mask():
    return (iota((GH * WP, GL), 0) // WP == iota((GH * WP, GL), 1) // HD).astype(F32).astype(BF)


def region_mask(w):
    def band(a, which):
        place = which * WIN + a
        return (place >= GRID - WIN).astype(jnp.int32) + (place >= GRID - SHIFT).astype(jnp.int32)

    def label(a):
        return band(a // WIN, w // 2) * 3 + band(a % WIN, w % 2)

    keys = label(iota((WP, 1), 0))
    queries = label(iota((1, GH * WP), 1) % WP)
    return jnp.where(keys != queries, MASK_VALUE, 0.0).astype(F32)


def block_diagonal(rows, mask):
    return jnp.concatenate([rows] * GH, axis=0) * mask


def query_major(pt):
    turned = pt.T
    return jnp.concatenate([turned[h * WP : (h + 1) * WP] for h in range(GH)], axis=1)


def pick_diagonal(full):
    head = iota((WP, GL), 1) // HD
    out = full[0:WP]
    for h in range(1, GH):
        out = jnp.where(head == h, full[h * WP : (h + 1) * WP], out)
    return out


def permutation(size, source_of, inverse):
    rows = iota((size, size), 1 if inverse else 0)
    cols = iota((size, size), 0 if inverse else 1)
    return (rows == source_of(cols)).astype(F32).astype(BF)


def qkv_source(col):
    return (col % GL) // HD * (3 * HD) + col // GL * HD + col % HD


def qv_source(col):
    return (col % GL) // HD * (2 * HD) + col // GL * HD + col % HD


def attn_fwd_body(
    layer, rolled, weights, keep, tasks, x_ref, table_ref, bias_ref, fw_ref, qkv_ref, p_ref, ho_ref, mid_ref,
    how_ref, wq_ref, wpt_ref, vec_ref, shift_ref, spread_ref, gather_ref, mask_ref, region_ref,
):
    begin(weights, tasks)
    wa_ref = weights.kept[0].at[0]
    first_step = pl.program_id(0) == 0

    @pl.when(first_step)
    def _():
        for n, row in enumerate((GAIN, SHIFT_ROW, BPROJ)):
            vec_ref[n : n + 1, :] = along_model(table_ref, layer, row, rolled)
        for g in range(4):
            qv = table_ref[g, layer, QV : QV + 2, :].astype(F32)
            at = 3 * GL * g
            for n, (scale, shift) in enumerate(((HD ** (-0.5), qv[0:1] * HD ** (-0.5)), (1.0, 0.0), (1.0, qv[1:2]))):
                lanes = slice(at + n * GL, at + (n + 1) * GL)
                shift_ref[0:1, lanes] = jnp.full((1, GL), scale, F32)
                shift_ref[1:2, lanes] = shift + jnp.zeros((1, GL), F32)
        spread_ref[...] = spread_map(layer * SHIFT)
        gather_ref[...] = gather_map(layer * SHIFT)
        mask_ref[...] = head_mask()
        if layer:
            for w in range(NW):
                region_ref[w] = region_mask(w)

    x = x_ref[0].astype(F32)
    normed, _ = normalize(x)
    first = (normed * vec_ref[0:1, :] + vec_ref[1:2, :]).astype(BF)
    fw = dot_nn(spread_ref[...], first).astype(BF)
    fw_ref[0] = fw

    @pl.when(first_step)
    def _():
        weights.wait_shard()
        weights.wait_rest()
        for g in range(4):
            wq_ref[:, 3 * GL * g : 3 * GL * (g + 1)] = wa_ref[g, :, : 3 * GL]
            wpt_ref[:, g * GL : (g + 1) * GL] = wa_ref[g, :, 3 * GL :]
        keep.start(wq_ref, wpt_ref)

    for n in range(3):
        lanes = slice(n * D, (n + 1) * D)
        projected = dot_nn(fw, wq_ref[:, lanes])
        qkv_ref[0, :, lanes] = (projected * shift_ref[0:1, lanes] + shift_ref[1:2, lanes]).astype(BF)

    def windows(n, carry):
        chains = [(n * AT_ONCE + w, g) for w in range(AT_ONCE) for g in range(4)]

        def rows(w):
            return pl.ds(pl.multiple_of(w * WP, WP), WP)

        def part(w, g, n):
            return qkv_ref[0, rows(w), (3 * g + n) * GL : (3 * g + n + 1) * GL]

        scores = [dot_nt(part(w, g, 1), block_diagonal(part(w, g, 0), mask_ref[...])) for w, g in chains]
        probs = []
        for (w, g), st in zip(chains, scores):
            st = st + bias_ref[0, g]
            if layer:
                st = st + region_ref[w]
            e = jnp.exp(st - jnp.max(st, 0, keepdims=True))
            pt = (e * (1.0 / jnp.sum(e, 0, keepdims=True))).astype(BF)
            p_ref[0, w, g] = pt
            probs.append(pt)
        mixed = [dot_tn(pt, part(w, g, 2)) for (w, g), pt in zip(chains, probs)]
        for (w, g), out in zip(chains, mixed):
            how_ref[rows(w), g * GL : (g + 1) * GL] = pick_diagonal(out).astype(BF)
        return carry

    lax.fori_loop(0, NW // AT_ONCE, windows, 0)
    ho = dot_nn(gather_ref[...], how_ref[...]).astype(BF)
    ho_ref[0] = ho
    mid_ref[0] = x + (dot_nt(ho, wpt_ref[...]) + vec_ref[2:3, :])
    step_end(tasks, 4)

    @pl.when(pl.program_id(0) == pl.num_programs(0) - 1)
    def _():
        keep.wait(wq_ref, wpt_ref)


def attn_fwd(layer, rolled, x, table, bias, weights, tasks=(), collective_id=None):
    n = x.shape[0]
    keep = Keep((D, 3 * D), (D, D))
    return carried_call(
        functools.partial(attn_fwd_body, layer, rolled, weights, keep, tasks),
        [keep, weights, *tasks],
        collective_id,
        grid=(n,),
        in_specs=[
            per(x.shape[1:]), whole(table.shape), pl.BlockSpec((1, 4, WP, GH * WP), lambda i: (layer, 0, 0, 0)),
        ],
        inputs=(x, table, bias),
        out_specs=[per((ROWS, D)), per((ROWS, 3 * D)), per((NW, 4, WP, GH * WP)), per((TP, D)), per((TP, D))],
        out_shape=[
            jax.ShapeDtypeStruct((n, ROWS, D), BF),
            jax.ShapeDtypeStruct((n, ROWS, 3 * D), BF),
            jax.ShapeDtypeStruct((n, NW, 4, WP, GH * WP), BF),
            jax.ShapeDtypeStruct((n, TP, D), BF),
            jax.ShapeDtypeStruct((n, TP, D), F32),
        ],
        scratch_shapes=[
            pltpu.VMEM((ROWS, D), BF), pltpu.VMEM((D, 3 * D), BF), pltpu.VMEM((D, D), BF), pltpu.VMEM((8, D), F32),
            pltpu.VMEM((8, 3 * D), F32), pltpu.VMEM((ROWS, TP), BF), pltpu.VMEM((TP, ROWS), BF), pltpu.VMEM((GH * WP, GL), BF),
            pltpu.VMEM((NW, WP, GH * WP), F32),
        ],
        name="attn_fwd",
        cost=pl.CostEstimate(flops=n * 2 * 256 * 512 * 2600, bytes_accessed=n * 2 << 20, transcendentals=0),
    )


def gelu_parts(v):
    cdf = 0.5 * (1.0 + lax.erf(v * 0.5**0.5))
    pdf = jnp.exp(-0.5 * v * v) * (2.0 * math.pi) ** (-0.5)
    return v * cdf, cdf + v * pdf


def alive_of(counts_ref, m):
    slot = lax.axis_index("tensor") * 2 + lax.axis_index("pipe")
    return (slot < counts_ref[0, m]).astype(F32)


def live_rows(counts_ref, m):
    return jnp.where(iota((TP, 1), 0) < TOK, alive_of(counts_ref, m), 0.0)


def mlp_fwd_body(
    layer, rolled, weights, keep, tasks, counts_ref, mid_ref, table_ref, second_ref, act_ref, slope_ref, y_ref, out_ref, acc_ref, hb_ref
):
    c = pl.program_id(0)
    rows_total = mid_ref.shape[0]
    begin(weights, tasks)
    wm_ref = weights.kept[0]

    @pl.when(c == 0)
    def _():
        for k in range(4):
            hb_ref[k] = jnp.concatenate([table_ref[k, layer, HB + n : HB + n + 1, :].astype(F32) for n in range(4)], 1)
        gain = along_model(table_ref, layer, MGAIN, rolled)
        shift = along_model(table_ref, layer, MSHIFT, rolled)
        mid = mid_ref[...]
        normed, _ = normalize(mid)
        second_ref[...] = (normed * gain + shift).astype(BF)
        acc_ref[...] = mid + along_model(table_ref, layer, OB, rolled)
        weights.wait_shard()

    @pl.when(c == 1)
    def _():
        weights.wait_rest()
        keep.start(wm_ref)

    def block(b, carry):
        parts = [pl.ds(pl.multiple_of(b * BLK + n * SUB_FWD, SUB_FWD), SUB_FWD) for n in range(BLK // SUB_FWD)]
        acts = []
        pre = [dot_nn(second_ref[rows, :], wm_ref[0, c]) for rows in parts]
        for rows, value in zip(parts, pre):
            act, slope = gelu_parts(value + hb_ref[c])
            act = act.astype(BF)
            act_ref[0, rows, :] = act
            slope_ref[0, rows, :] = slope.astype(BF)
            acts.append(act)
        outs = [dot_nn(act, wm_ref[1, c]) for act in acts]
        for rows, out in zip(parts, outs):
            acc_ref[rows, :] += out
        return carry

    lax.fori_loop(0, rows_total // BLK, block, 0)

    @pl.when(c == pl.num_programs(0) - 1)
    def _():
        for m in range(rows_total // TP):
            y = (acc_ref[m * TP : (m + 1) * TP, :] * live_rows(counts_ref, m)).astype(BF)
            y_ref[m] = y
            out_ref[m] = y[:TOK]
        keep.wait(wm_ref)

    step_end(tasks, 4)


def mlp_fwd(layer, rolled, counts, mid, table, weights, tasks=(), collective_id=None):
    r = mid.shape[0]
    n = r // TP
    keep = Keep((2, 4, D, D))
    return carried_call(
        functools.partial(mlp_fwd_body, layer, rolled, weights, keep, tasks),
        [keep, weights, *tasks],
        collective_id,
        grid=(4,),
        in_specs=[SMEM, whole((r, D)), whole(table.shape)],
        inputs=(counts, mid, table),
        out_specs=[whole((r, D)), per((r, D)), per((r, D)), whole((n, TP, D)), whole((n, TOK, D))],
        out_shape=[
            jax.ShapeDtypeStruct((r, D), BF),
            jax.ShapeDtypeStruct((4, r, D), BF),
            jax.ShapeDtypeStruct((4, r, D), BF),
            jax.ShapeDtypeStruct((n, TP, D), BF),
            jax.ShapeDtypeStruct((n, TOK, D), BF),
        ],
        scratch_shapes=[pltpu.VMEM((r, D), F32), pltpu.VMEM((4, 1, D), F32)],
        name="mlp_fwd",
        cost=pl.CostEstimate(flops=4 * r * D * 2048, bytes_accessed=12 << 20, transcendentals=0),
    )


def scatter_rows(place, value_ref, mine_ref, away_ref, index):
    core, dp = place
    for half, out_ref in enumerate((mine_ref, away_ref)):
        for n, j in enumerate(PLACES):
            start = (core ^ half) * 256 + (dp ^ j) * CHUNK
            out_ref[n, index] = value_ref[pl.ds(pl.multiple_of(start, CHUNK), CHUNK), :]


def where_in_plane(rolled):
    return (lax.axis_index("pipe"), lax.axis_index("dp")) if rolled else (jnp.int32(0), jnp.int32(0))


def by_shard(row):
    return jnp.concatenate([row[None, :, z * GL : (z + 1) * GL] for z in range(4)], 0)


def mlp_bwd_body(
    layer, rolled, weights, tasks, counts_ref, g_ref, act_ref, slope_ref, second_ref, mid_ref, table_ref,
    ghw_ref, ghw_away_ref, gow_ref, gow_away_ref, ghb_ref, gmid_ref, small_ref,
    gy_ref, gyt_ref, sect_ref, gp_ref, acc_ref, value_ref,
):
    c = pl.program_id(0)
    rows_total = mid_ref.shape[0]
    begin(weights, tasks)
    wm_ref = weights.kept[0]

    @pl.when(c == 0)
    def _():
        total = jnp.zeros((1, D), F32)
        for m in range(rows_total // TP):
            rows = slice(m * TP, (m + 1) * TP)
            gy = g_ref[m].astype(F32) * live_rows(counts_ref, m)
            gy_ref[rows, :] = gy.astype(BF)
            total += jnp.sum(gy, 0, keepdims=True)
        small_ref[:, 0:1] = by_shard(total)
        gyt_ref[...] = gy_ref[...].T
        sect_ref[...] = second_ref[...].T
        acc_ref[...] = jnp.zeros_like(acc_ref)
        weights.wait()

    ghb_ref[0] = jnp.zeros_like(ghb_ref[0])

    def block(b, carry):
        parts = [pl.ds(pl.multiple_of(b * BLK + n * SUB_BWD, SUB_BWD), SUB_BWD) for n in range(BLK // SUB_BWD)]
        slopes = [dot_nt(gy_ref[rows, :], wm_ref[1, c]) for rows in parts]
        pres = []
        for rows, value in zip(parts, slopes):
            gp = value * slope_ref[0, rows, :].astype(F32)
            total = jnp.sum(gp, 0, keepdims=True)
            for n in range(4):
                ghb_ref[0, n : n + 1, :] += total[:, n * GL : (n + 1) * GL]
            gp = gp.astype(BF)
            gp_ref[rows, :] = gp
            pres.append(gp)
        outs = [dot_nt(gp, wm_ref[0, c]) for gp in pres]
        for rows, out in zip(parts, outs):
            acc_ref[rows, :] += out
        return carry

    lax.fori_loop(0, rows_total // BLK, block, 0)
    place = where_in_plane(rolled)
    value_ref[0] = dot_nn(sect_ref[...], gp_ref[...]).astype(BF)
    value_ref[1] = dot_nn(gyt_ref[...], act_ref[0]).astype(BF)
    scatter_rows(place, value_ref.at[0], ghw_ref, ghw_away_ref, 0)
    scatter_rows(place, value_ref.at[1], gow_ref, gow_away_ref, 0)

    @pl.when(c == pl.num_programs(0) - 1)
    def _():
        for call in planned(tasks, LATE):
            call()
        e = acc_ref[...]
        normed, inverse = normalize(mid_ref[...])
        small_ref[:, 2:3] = by_shard(jnp.sum(e * normed, 0, keepdims=True))
        small_ref[:, 3:4] = by_shard(jnp.sum(e, 0, keepdims=True))
        gmid = gy_ref[...].astype(F32) + norm_back(e, normed, inverse, along_model(table_ref, layer, MGAIN, rolled))
        small_ref[:, 1:2] = by_shard(jnp.sum(gmid, 0, keepdims=True))
        gmid_ref[...] = gmid

    step_end(tasks, 4)


PIECES = jax.ShapeDtypeStruct((4, 4, CHUNK, D), BF)


def mlp_bwd(layer, rolled, counts, g, act, slope, second, mid, table, weights, tasks=(), collective_id=None):
    r = mid.shape[0]
    pieces = pl.BlockSpec((4, 1, CHUNK, D), lambda i: (0, i, 0, 0))
    return carried_call(
        functools.partial(mlp_bwd_body, layer, rolled, weights, tasks),
        [weights, *tasks],
        collective_id,
        grid=(4,),
        in_specs=[SMEM, whole(g.shape), per((r, D)), per((r, D)), whole((r, D)), whole((r, D)), whole(table.shape)],
        inputs=(counts, g, act, slope, second, mid, table),
        out_specs=[pieces, pieces, pieces, pieces, per((4, GL)), whole((r, D)), whole((4, 4, GL))],
        out_shape=[
            PIECES, PIECES, PIECES, PIECES,
            jax.ShapeDtypeStruct((4, 4, GL), F32),
            jax.ShapeDtypeStruct((r, D), F32),
            jax.ShapeDtypeStruct((4, 4, GL), F32),
        ],
        scratch_shapes=[
            pltpu.VMEM((r, D), BF), pltpu.VMEM((D, r), BF), pltpu.VMEM((D, r), BF), pltpu.VMEM((r, D), BF),
            pltpu.VMEM((r, D), F32), pltpu.VMEM((2, D, D), BF),
        ],
        name="mlp_bwd",
        cost=pl.CostEstimate(flops=8 * r * D * 2048, bytes_accessed=16 << 20, transcendentals=0),
    )


def attn_bwd_body(
    layer, rolled, weights, tasks, x_ref, gmid_ref, fw_ref, qkv_ref, p_ref, ho_ref, table_ref,
    gin_ref, out_ref, ga_ref, ga_away_ref, gqv_ref, gtab_ref, small_ref,
    gw_ref, dq_ref, fwt_ref, hos_ref, gms_ref, value_ref, spread_ref, gather_ref, mask_ref, gain_ref,
):
    i = pl.program_id(0)
    last = pl.num_programs(0) - 1
    begin(weights, tasks)
    wq_ref, wpt_ref = weights.kept[:2]

    @pl.when(i == 0)
    def _():
        gqv_ref[...] = jnp.zeros_like(gqv_ref)
        gtab_ref[...] = jnp.zeros_like(gtab_ref)
        small_ref[...] = jnp.zeros_like(small_ref)
        spread_ref[...] = spread_map(layer * SHIFT)
        gather_ref[...] = gather_map(layer * SHIFT)
        mask_ref[...] = head_mask()
        gain_ref[...] = along_model(table_ref, layer, GAIN, rolled)

    gmid = gmid_ref[0]
    gmb = gmid.astype(BF)
    image = pl.ds(pl.multiple_of(i * TP, 16), TP)
    gms_ref[image, :] = gmb
    hos_ref[image, :] = ho_ref[0]
    base = pl.multiple_of(i * ROWS, ROWS)
    fwt_ref[:, pl.ds(base, ROWS)] = fw_ref[0].T

    @pl.when(i == 0)
    def _():
        weights.wait()

    heads = dot_nn(gmb, wpt_ref[...]).astype(BF)
    gw_ref[...] = dot_nn(spread_ref[...], heads).astype(BF)
    scale = HD ** (-0.5)

    def windows(n, carry):
        chains = [(n * AT_ONCE + w, g) for w in range(AT_ONCE) for g in range(4)]
        mask = mask_ref[...]

        def rows(w):
            return pl.ds(pl.multiple_of(w * WP, WP), WP)

        def part(w, g, n):
            return qkv_ref[0, rows(w), (3 * g + n) * GL : (3 * g + n + 1) * GL]

        bd_grads = [block_diagonal(gw_ref[rows(w), g * GL : (g + 1) * GL], mask) for w, g in chains]
        terms = [dot_nt(part(w, g, 2), bd_grad) for (w, g), bd_grad in zip(chains, bd_grads)]
        dvs = [dot_nn(p_ref[0, w, g], bd_grad) for (w, g), bd_grad in zip(chains, bd_grads)]
        scores = []
        for (w, g), term in zip(chains, terms):
            ptf = p_ref[0, w, g].astype(F32)
            pd = term * ptf
            ds = pd - ptf * jnp.sum(pd, 0, keepdims=True)
            gtab_ref[g] += ds
            scores.append(ds.astype(BF))
        dks = [dot_nn(ds, block_diagonal(part(w, g, 0), mask)) for (w, g), ds in zip(chains, scores)]
        dqs = [dot_tn(ds, part(w, g, 1)) for (w, g), ds in zip(chains, scores)]
        for (w, g), full, dk, dv in zip(chains, dqs, dks, dvs):
            dq = pick_diagonal(full) * scale
            out_rows = pl.ds(pl.multiple_of(base + w * WP, WP), WP)
            gqv_ref[g, 0:1] += jnp.sum(dq, 0, keepdims=True)
            gqv_ref[g, 1:2] += jnp.sum(dv, 0, keepdims=True)
            for n, value in enumerate((dq, dk, dv)):
                dq_ref[out_rows, (3 * g + n) * GL : (3 * g + n + 1) * GL] = value.astype(BF)
        return carry

    lax.fori_loop(0, NW // AT_ONCE, windows, 0)
    image_rows = pl.ds(base, ROWS)
    e = dot_nt(dq_ref[image_rows, :], wq_ref[...])
    e = dot_nn(gather_ref[...], e.astype(BF))
    normed, inverse = normalize(x_ref[0].astype(F32))
    small_ref[:, 0:1] += by_shard(jnp.sum(e * normed, 0, keepdims=True))
    small_ref[:, 1:2] += by_shard(jnp.sum(e, 0, keepdims=True))
    gin = (gmid + norm_back(e, normed, inverse, gain_ref[...])).astype(BF)
    gin_ref[0] = gin
    out_ref[0] = gin[:TOK]

    @pl.when(i == last)
    def _():
        for call in planned(tasks, LATE):
            call()

        def chunk(n, carry):
            lanes = pl.ds(pl.multiple_of(n * D, D), D)
            value_ref[:, lanes] = dot_nn(fwt_ref[...], dq_ref[:, lanes]).astype(BF)
            return carry

        lax.fori_loop(0, 3, chunk, 0)
        value_ref[:, 3 * D :] = dot_nn(gms_ref[...].T, hos_ref[...]).astype(BF)
        core, dp = where_in_plane(rolled)
        for half, group_ref in enumerate((ga_ref, ga_away_ref)):
            for n, j in enumerate(PLACES):
                rows = pl.ds(pl.multiple_of((core ^ half) * 256 + (dp ^ j) * CHUNK, CHUNK), CHUNK)
                for g in range(4):
                    group_ref[n, g, :, : 3 * GL] = value_ref[rows, 3 * GL * g : 3 * GL * (g + 1)]
                    group_ref[n, g, :, 3 * GL :] = value_ref[rows, 3 * D + GL * g : 3 * D + GL * (g + 1)]

    step_end(tasks, 4)


def attn_bwd(layer, rolled, x, gmid, fw, qkv, p, ho, table, weights, tasks=(), collective_id=None):
    n = x.shape[0]
    return carried_call(
        functools.partial(attn_bwd_body, layer, rolled, weights, tasks),
        [weights, *tasks],
        collective_id,
        grid=(n,),
        in_specs=[
            per(x.shape[1:]), per((TP, D)), per((ROWS, D)), per((ROWS, 3 * D)), per((NW, 4, WP, GH * WP)), per((TP, D)),
            whole(table.shape),
        ],
        inputs=(x, gmid, fw, qkv, p, ho, table),
        out_specs=[
            per((TP, D)), per((TOK, D)), whole(PIECES.shape), whole(PIECES.shape), whole((4, 2, GL)), whole((4, WP, GH * WP)),
            whole((4, 2, GL)),
        ],
        out_shape=[
            jax.ShapeDtypeStruct((n, TP, D), BF),
            jax.ShapeDtypeStruct((n, TOK, D), BF),
            PIECES, PIECES,
            jax.ShapeDtypeStruct((4, 2, GL), F32),
            jax.ShapeDtypeStruct((4, WP, GH * WP), F32),
            jax.ShapeDtypeStruct((4, 2, GL), F32),
        ],
        scratch_shapes=[
            pltpu.VMEM((ROWS, D), BF), pltpu.VMEM((n * ROWS, 3 * D), BF), pltpu.VMEM((D, n * ROWS), BF),
            pltpu.VMEM((n * TP, D), BF), pltpu.VMEM((n * TP, D), BF), pltpu.VMEM((D, 4 * D), BF),
            pltpu.VMEM((ROWS, TP), BF), pltpu.VMEM((TP, ROWS), BF), pltpu.VMEM((GH * WP, GL), BF), pltpu.VMEM((1, D), F32),
        ],
        name="attn_bwd",
        cost=pl.CostEstimate(flops=n * 4 * 256 * 512 * 2600, bytes_accessed=n * 3 << 20, transcendentals=0),
    )


def plain_call(body, name, inputs, out_shape, scratch_shapes=(), grid=(), in_specs=None, out_specs=None, bytes_accessed=4 << 20):
    return pl.pallas_call(
        body,
        grid=grid,
        out_shape=out_shape,
        in_specs=in_specs or [pl.BlockSpec(memory_space=pltpu.VMEM)] * len(inputs),
        out_specs=out_specs or jax.tree.map(lambda _: pl.BlockSpec(memory_space=pltpu.VMEM), out_shape),
        scratch_shapes=list(scratch_shapes),
        name=name,
        compiler_params=pltpu.CompilerParams(vmem_limit_bytes=VMEM_LIMIT),
        cost_estimate=pl.CostEstimate(flops=bytes_accessed, bytes_accessed=bytes_accessed, transcendentals=0),
    )(*inputs)


def prepare_body(index, wqkv, wproj, gain, shift, qv, table, bproj, mgain, mshift, hb, ob, own_a_ref, lines_ref, index_ref, rows_ref, keys_ref):
    own_a_ref[:, : 3 * GL] = dot_nn(wqkv[...], permutation(3 * GL, qkv_source, False)).astype(BF)
    own_a_ref[:, 3 * GL :] = wproj[...].T
    rows_ref[...] = jnp.zeros_like(rows_ref)
    for row, ref in ((GAIN, gain), (SHIFT_ROW, shift), (BPROJ, bproj), (MGAIN, mgain), (MSHIFT, mshift), (OB, ob)):
        rows_ref[row : row + 1, :] = ref[...].astype(F32)
    terms = dot_nn(jnp.broadcast_to(qv[...], (16, 2 * GL)), permutation(2 * GL, qv_source, False))
    hidden, places = hb[...].astype(F32), table[...].astype(F32)
    for n in range(2):
        rows_ref[QV + n : QV + n + 1, :] = terms[0:1, n * GL : (n + 1) * GL]
    for n in range(4):
        rows_ref[HB + n : HB + n + 1, :] = hidden[:, n * GL : (n + 1) * GL]
    rows_ref[TABLE : TABLE + 4, :] = places[:, :GL]
    rows_ref[TABLE + 4 : TABLE + 8, 0 : RELS - GL] = places[:, GL:]
    lines_ref[...] = rows_ref[...].astype(BF)
    keys_ref[...] = jnp.full((GL, GL), -1.0, F32)
    keys_ref[0:POS, 0:POS] = index[...].astype(F32)
    keys_ref[...] = keys_ref[...].T
    pair = [keys_ref[pl.ds(odd, WP // 2, 2), :][:, :WP] for odd in range(2)]
    index_ref[...] = jnp.concatenate(pair, 1).astype(jnp.int32)


def prepare(rel_index, wqkv, wproj, *small):
    return plain_call(
        prepare_body, "prepare", (rel_index, wqkv, wproj, *small),
        [
            jax.ShapeDtypeStruct((D, D), BF), jax.ShapeDtypeStruct((LINES, GL), BF),
            jax.ShapeDtypeStruct((WP // 2, GL), jnp.int32),
        ],
        [pltpu.VMEM((LINES, GL), F32), pltpu.VMEM((GL, GL), F32)],
    )


class Exchange(Part):
    def __init__(self, own, lines):
        shapes = [jax.ShapeDtypeStruct(part.shape, part.dtype) for part in own]
        shapes.append(jax.ShapeDtypeStruct((4, 2) + lines.shape, lines.dtype))
        super().__init__([*own, lines], shapes, sems(4) + sems(3) + [pltpu.SemaphoreType.DMA(())])

    def swap(self, n):
        core, _, _ = place_in_mesh()
        target = self.outs[n] if n < 3 else self.outs[3].at[0, core]
        return remote(self.ins[n], target, [sem.at[n] for sem in self.kept[:2]], "pipe", 1 - core)

    def keep(self):
        core, _, _ = place_in_mesh()
        return pltpu.make_async_copy(self.ins[3], self.outs[3].at[0, core], self.kept[4])

    def spread(self, k):
        _, _, shard = place_in_mesh()
        table = self.outs[3]
        return remote(table.at[0], table.at[k], [sem.at[k - 1] for sem in self.kept[2:4]], "tensor", lax.rem(shard + 4 - k, 4))


def gather_start(own, lines, index, view):
    exchange = Exchange(own, lines)
    near_a, near_h, near_o, far_a, bias = Near(0, None, None), Near(0, None, None), Near(0, None, None), Far(None), Bias(index)
    pick = Own(view)

    def body():
        for n, task in enumerate((near_a, near_h, near_o)):
            task.ins = [exchange.ins[n], exchange.outs[n]]
        far_a.ins = [near_a.outs[0]]
        greet()
        for n in (0, 3, 1, 2):
            exchange.swap(n).start()
        exchange.keep().start()
        pick.start()
        exchange.swap(0).wait()
        near_a.start()
        exchange.keep().wait()
        exchange.swap(3).wait()
        for k in (1, 2, 3):
            exchange.spread(k).start()
        pick.pick()
        near_a.end()
        far_a.start()
        exchange.swap(1).wait()
        near_h.start()
        for k in (1, 2, 3):
            exchange.spread(k).wait()
        bias.build(exchange.outs[3])
        far_a.turn()
        exchange.swap(2).wait()
        near_o.start()
        far_a.rest()
        far_a.last()
        far_a.end()
        bias.end()
        pick.end()
        near_h.end()
        near_o.end()

    parts = [exchange, near_a, near_h, near_o, far_a, bias, pick]
    _, given = carried_call(
        body, parts, 0, grid=(), in_specs=[], inputs=(), out_specs=[], out_shape=[], scratch_shapes=[],
        name="gather_start", cost=pl.CostEstimate(flops=1 << 24, bytes_accessed=8 << 20, transcendentals=0),
    )
    others, given_a, given_h, given_o, far, *rest = given
    return others[:3], others[3], [given_a[0], *far], given_h[0], given_o[0], *[part[0] for part in rest]


def turned_index(rel_index):
    return jnp.pad(rel_index.T, ((0, WP - POS), (0, WP - POS)), constant_values=-1)


def places_of(pairs):
    return (iota((2 * GL, pairs.shape[1]), 0) == pairs).astype(F32).astype(BF)


class Own(Part):
    def __init__(self, view, plan=()):
        count = view.shape[0]
        self.count, self.plan = count, plan
        super().__init__(
            [view], [jax.ShapeDtypeStruct((count, TP, D), BF)],
            [pltpu.VMEM(view.shape, BF), pltpu.VMEM((count, TP, D), BF), pltpu.SemaphoreType.DMA((2,))],
        )

    def load(self):
        return pltpu.make_async_copy(self.ins[0], self.kept[0], self.kept[2].at[0])

    def out(self):
        return pltpu.make_async_copy(self.kept[1], self.outs[0], self.kept[2].at[1])

    def start(self):
        self.load().start()

    def pick(self):
        self.load().wait()
        first_core = lax.axis_index("pipe") == 0

        def image(m, carry):
            both = self.kept[0][m]
            self.kept[1][m] = jnp.zeros((TP, D), BF)
            self.kept[1][m, 0:TOK, :] = jnp.where(first_core, both[:, 0, :], both[:, 1, :])
            return carry

        lax.fori_loop(0, self.count, image, 0)
        self.out().start()

    def end(self):
        self.out().wait()


class Bias(Part):
    def __init__(self, index):
        super().__init__(
            [index], [jax.ShapeDtypeStruct((2, 4, WP, GH * WP), F32)],
            [pltpu.VMEM((4, 2, LINES, GL), BF), pltpu.VMEM((WP // 2, GL), jnp.int32), pltpu.VMEM((2 * H, 2 * GL), F32),
             pltpu.VMEM((WP // 2, 2 * H, GL), F32), pltpu.VMEM((WP, GL), F32), pltpu.VMEM((2, 4, WP, GH * WP), F32),
             pltpu.SemaphoreType.DMA((3,))],
        )

    def loads(self, table):
        return [pltpu.make_async_copy(table, self.kept[0], self.kept[6].at[0]), self.index()]

    def index(self):
        return pltpu.make_async_copy(self.ins[0], self.kept[1], self.kept[6].at[1])

    def out(self):
        return pltpu.make_async_copy(self.kept[5], self.outs[0], self.kept[6].at[2])

    def build(self, table):
        lines, index, rows, pairs, half, whole_ref, _ = self.kept
        for copy in self.loads(table):
            copy.start()
        for copy in self.loads(table):
            copy.wait()
        for l in range(2):
            for k in range(4):
                values = lines[k, l].astype(F32)
                at = l * H + k * GH
                rows[at : at + GH, :GL] = values[TABLE : TABLE + GH]
                rows[at : at + GH, GL:] = values[TABLE + GH : TABLE + 2 * GH]
        tables = rows[...].astype(BF)

        def product(n, carry):
            pairs[n] = dot_nn(tables, places_of(index[pl.ds(n, 1), :]))
            return carry

        lax.fori_loop(0, WP // 2, product, 0)
        shut = jnp.where(iota((WP, GL), 0) < POS, 0.0, SHUT).astype(F32)
        for l in range(2):
            for g in range(4):
                for n in range(2):
                    heads = [pairs[:, l * H + g * GH + 2 * n + m, :] for m in range(2)]
                    for odd in range(2):
                        lanes = slice(odd * WP, (odd + 1) * WP)
                        half[pl.ds(odd, WP // 2, 2), :] = jnp.concatenate([head[:, lanes] for head in heads], 1)
                    whole_ref[l, g, :, n * GL : (n + 1) * GL] = half[...] + shut
        self.out().start()

    def end(self):
        self.out().wait()


def bias_tables(table, rel_index):
    rows = table[:, :, TABLE : TABLE + 8].reshape(4, 2, 2, GH, GL).transpose(1, 0, 3, 2, 4).reshape(2 * H, 2 * GL)
    onehot = (jnp.arange(2 * GL, dtype=jnp.int32)[:, None] == turned_index(rel_index).reshape(1, -1)).astype(BF)
    flat = jnp.dot(rows, onehot, preferred_element_type=F32)
    position = flat.reshape(2, 4, GH, WP, WP).transpose(0, 1, 3, 2, 4)
    shut = jnp.where(jnp.arange(WP) < POS, 0.0, SHUT).astype(F32)[:, None, None]
    return (position + shut).reshape(2, 4, WP, GH * WP)


def table_grad(gtab, rel_index):
    rel = jnp.pad(rel_index.T, ((0, WP - POS), (0, WP - POS)), constant_values=-1).reshape(-1)
    onehot = (rel[:, None] == jnp.arange(RELS, dtype=jnp.int32)[None, :]).astype(F32)
    flat = gtab.reshape(4, WP, GH, WP).transpose(0, 2, 1, 3).reshape(H, WP * WP)
    return jnp.dot(flat, onehot, precision=lax.Precision.HIGHEST).reshape(4, GH, RELS)


class Little(Part):
    def __init__(self, rows):
        self.rows = rows
        super().__init__(
            [],
            [jax.ShapeDtypeStruct((rows, GL), F32)],
            [pltpu.VMEM((2, 4, rows, GL), F32), pltpu.VMEM((4, rows, GL), F32), pltpu.VMEM((4, rows, GL), F32),
             pltpu.VMEM((3, rows, GL), F32)]
            + sems() + sems(3) + sems(3) + [pltpu.SemaphoreType.DMA(())],
        )

    def pack(self, layers, tabs):
        _, _, shard = place_in_mesh()
        sums = self.kept[0]
        sums[...] = jnp.zeros_like(sums)
        for layer, (ghb, small_m, gqv, _, small_a) in enumerate(layers):
            for k in range(4):
                z = lax.rem(shard + k, 4)
                for row, source, n in (
                    (GAIN, small_a, 0), (SHIFT_ROW, small_a, 1), (OB, small_m, 0), (BPROJ, small_m, 1), (MGAIN, small_m, 2),
                    (MSHIFT, small_m, 3),
                ):
                    sums[layer, k, row : row + 1, :] = source[z, n : n + 1, :]
                sums[layer, k, QV : QV + 2, :] = gqv[k]
                sums[layer, k, HB : HB + 4, :] = ghb[k]
                rows = tabs[layer][GH * k : GH * (k + 1)]
                sums[layer, k, TABLE : TABLE + 4, :] = rows[:, 0:GL]
                sums[layer, k, TABLE + 4 : TABLE + 8, :] = rows[:, GL:]

    def over(self):
        core, _, _ = place_in_mesh()
        return remote(self.kept[0].at[1 - core], self.kept[1], self.kept[4:6], "pipe", 1 - core)

    def across(self, j):
        _, dp, _ = place_in_mesh()
        return remote(self.kept[2].at[0], self.kept[2].at[j], [sem.at[j - 1] for sem in self.kept[6:8]], "dp", dp ^ j)

    def along(self, k):
        _, _, shard = place_in_mesh()
        return remote(
            self.kept[1].at[k], self.kept[3].at[k - 1], [sem.at[k - 1] for sem in self.kept[8:10]], "tensor", lax.rem(shard + k, 4)
        )

    def start(self):
        self.over().start()

    def second(self):
        core, _, _ = place_in_mesh()
        self.over().wait()
        self.kept[1][...] += self.kept[0][core]
        for k in (1, 2, 3):
            self.along(k).start()

    def third(self):
        for k in (1, 2, 3):
            self.along(k).wait()
        self.kept[2][0] = self.kept[1][0] + self.kept[3][0] + self.kept[3][1] + self.kept[3][2]
        for j in (1, 2, 3):
            self.across(j).start()

    def fourth(self):
        for j in (1, 2, 3):
            self.across(j).wait()
        total = self.kept[2]
        self.kept[1][0] = total[0] + total[1] + total[2] + total[3]
        self.out().start()

    def out(self):
        return pltpu.make_async_copy(self.kept[1].at[0], self.outs[0], self.kept[10])

    def end(self):
        self.out().wait()


class Settle(Part):
    def __init__(self):
        super().__init__(
            [],
            [jax.ShapeDtypeStruct((3, D, D), BF)],
            [pltpu.VMEM((3, D, D), BF)] + sems(3) + [pltpu.SemaphoreType.DMA((3,)), pltpu.SemaphoreType.DMA((3,))],
        )

    def rows(self, core):
        return pl.ds(core * 256, 256)

    def send(self, source, n, core):
        return remote(source.at[self.rows(core)], self.outs[0].at[n, self.rows(core)], [sem.at[n] for sem in self.kept[1:3]], "pipe", 1 - core)

    def load(self, source, n, core):
        return pltpu.make_async_copy(source.at[self.rows(core)], self.kept[0].at[n, self.rows(core)], self.kept[3].at[n])

    def store(self, n, core):
        return pltpu.make_async_copy(self.kept[0].at[n, self.rows(core)], self.outs[0].at[n, self.rows(core)], self.kept[4].at[n])

    def start(self, matrices, layer, which):
        def action(core):
            for n in which:
                (self.load if core == layer else self.send)(matrices[n], n, core).start()

        by_core(action)

    def straight(self, matrix, n, layer):
        def action(core):
            if core == layer:
                rows = self.rows(core)
                pltpu.make_async_copy(matrix.at[rows], self.outs[0].at[n, rows], self.kept[4].at[n]).start()
            else:
                self.send(matrix, n, core).start()

        by_core(action)

    def pass_on(self, matrices, layer, which):
        @pl.when(lax.axis_index("pipe") == layer)
        def _():
            for n in which:
                self.load(matrices[n], n, layer).wait()
                self.store(n, layer).start()

    def end(self, matrices):
        def action(core):
            for n in range(3):
                self.store(n, core).wait()
                self.send(matrices[1 - core][n], n, core).wait()

        by_core(action)


def table_sums(gtab_ref, index_ref, half_ref, pairs_ref, out_ref):
    for g in range(4):
        for n in range(2):
            half_ref[...] = gtab_ref[g, :, n * GL : (n + 1) * GL]
            even = half_ref[pl.ds(0, WP // 2, 2), :]
            odd = half_ref[pl.ds(1, WP // 2, 2), :]
            for m in range(2):
                lanes = slice(m * WP, (m + 1) * WP)
                pairs_ref[:, g * GH + 2 * n + m, :] = jnp.concatenate([even[:, lanes], odd[:, lanes]], 1)

    def add(n, total):
        pair = pairs_ref[n]
        high = pair.astype(BF)
        low = (pair - high.astype(F32)).astype(BF)
        places = places_of(index_ref[pl.ds(n, 1), :])
        return total + (dot_nt(high, places) + dot_nt(low, places))

    out_ref[...] = lax.fori_loop(0, WP // 2, add, jnp.zeros((H, 2 * GL), F32))


def reduce_end(attention0, totals_h0, turned_o0, piece_a1, shared1, grads_in, small, index):
    halves = ((0, 32), (32, 32))
    first = [ReduceFirst(attention0, rows=rows) for rows in halves]
    second = [ReduceSecond(size=32) for _ in halves]
    share = [Share(rows=halves[0], in_vmem=True)]
    share.append(Share(rows=halves[1], target=share[0]))
    onward_o = ReduceOnward(turned_o0)
    second_m, share_m = [ReduceSecond(totals_h0), ReduceSecond()], [Share(), Share()]
    share_a1, done_m1 = Share(piece_a1), Part(shared1)
    settle, little, places = Settle(), Little(24), Stored(index)
    input_grad = Weave(grads_in)

    def body(*refs):
        layers, (tabs_ref, pairs_ref, half_ref) = (refs[:5], refs[5:10]), refs[10:]
        for n in range(2):
            second[n].ins, share[n].ins, share_m[n].ins = [first[n].total], [second[n].kept[0]], [second_m[n].kept[0]]
        second_m[1].ins = [onward_o.kept[0]]
        done = (
            [share[0].whole(), share_m[0].outs[0], share_m[1].outs[0]],
            [share_a1.outs[0], done_m1.ins[0], done_m1.ins[1]],
        )

        def tab(layer):
            table_sums(layers[layer][3], places.kept[0], half_ref, pairs_ref, tabs_ref.at[layer])

        greet()
        for task in (*first, onward_o, second_m[0]):
            task.start()
        places.load()
        places.wait()
        tab(1)
        first[0].cores()
        first[1].cores()
        settle.start(done[1], 1, (1, 2))
        input_grad.start()
        tab(0)
        little.pack(layers, tabs_ref)
        little.start()
        onward_o.close()
        second_m[1].start()
        second_m[0].close()
        share_m[0].start()
        first[0].turn()
        little.second()
        first[1].turn()
        share_a1.start()
        settle.pass_on(done[1], 1, (1, 2))
        first[0].close()
        second[0].start()
        first[1].close()
        second[1].start()
        little.third()
        second_m[1].close()
        share_m[1].start()
        input_grad.wait()
        input_grad.weave(0, 2)
        for task in (share_m[0], share_a1):
            task.end()
            task.flush()
        settle.start(done[1], 1, (0,))
        settle.start(done[0], 0, (1,))
        for n in range(2):
            second[n].close()
            share[n].start()
        input_grad.weave(2, 4)
        little.fourth()
        settle.pass_on(done[1], 1, (0,))
        settle.pass_on(done[0], 0, (1,))
        share_m[1].end()
        share_m[1].flush()
        settle.start(done[0], 0, (2,))
        settle.pass_on(done[0], 0, (2,))
        for task in share:
            task.end()
        for task in share:
            task.flush()
        settle.straight(done[0][0], 0, 0)
        little.end()
        input_grad.end()
        settle.end(done)

    parts = [
        *first, *second, *share, onward_o, *second_m, *share_m, share_a1, done_m1, settle, little, input_grad, places
    ]
    _, given = carried_call(
        body, parts, 7, grid=(), in_specs=[pl.BlockSpec(memory_space=pltpu.VMEM)] * 10, inputs=small, out_specs=[], out_shape=[],
        scratch_shapes=[pltpu.VMEM((2, H, 2 * GL), F32), pltpu.VMEM((WP // 2, H, GL), F32), pltpu.VMEM((WP, GL), F32)],
        name="reduce_end", cost=pl.CostEstimate(flops=1 << 24, bytes_accessed=8 << 20, transcendentals=0),
    )
    by_part = dict(zip(map(id, parts), given))
    return by_part[id(settle)][0], by_part[id(little)][0], by_part[id(input_grad)][0]


def finish_body(
    matrix_ref, lines_ref, gqkv_ref, gproj_ref, ghw_ref, gow_ref, gain_ref, shift_ref, qv_ref, table_ref, bproj_ref, mgain_ref,
    mshift_ref, hb_ref, ob_ref,
):
    gqkv_ref[0] = dot_nn(matrix_ref[0, :, : 3 * GL], permutation(3 * GL, qkv_source, True))
    gproj_ref[0] = matrix_ref[0, :, 3 * GL :].T.astype(F32)
    ghw_ref[0] = matrix_ref[1].astype(F32)
    gow_ref[0] = matrix_ref[2].T.astype(F32)
    lines = lines_ref[...]
    for row, ref in (
        (GAIN, gain_ref), (SHIFT_ROW, shift_ref), (BPROJ, bproj_ref), (MGAIN, mgain_ref), (MSHIFT, mshift_ref), (OB, ob_ref)
    ):
        ref[...] = lines[row : row + 1]
    qv_ref[...] = jnp.concatenate([lines[QV + n : QV + n + 1, h * HD : (h + 1) * HD] for h in range(GH) for n in range(2)], 1)
    table_ref[0] = jnp.concatenate([lines[TABLE : TABLE + 4], lines[TABLE + 4 : TABLE + 8, : RELS - GL]], 1)
    hb_ref[...] = jnp.concatenate([lines[HB + n : HB + n + 1] for n in range(4)], 1)


def finish(matrices, lines):
    shapes = [
        (1, D, 3 * GL), (1, GL, D), (1, D, D), (1, D, D), (1, GL), (1, GL), (1, 2 * GL), (1, GH, RELS), (1, GL), (1, GL), (1, GL),
        (1, D), (1, GL),
    ]
    return plain_call(finish_body, "finish", (matrices, lines), [jax.ShapeDtypeStruct(shape, F32) for shape in shapes])


def layer_forward(layer, rolled, x, counts, table, bias, weights, tasks, ids):
    (fw, qkv, p, ho, mid), given = attn_fwd(layer, rolled, x, table, bias, weights[0](), tasks[0](), ids[0])
    mid = mid.reshape(-1, D)
    kept_a, given = given[0], given[1:]
    (second, act, slope, y, out), more = mlp_fwd(layer, rolled, counts, mid, table, weights[1](given), tasks[1](given), ids[1])
    return y, out, (x, fw, qkv, p, ho, mid, second, act, slope, kept_a, more[0]), given, more[1:]


def layer_backward(layer, rolled, cot, kept, counts, table, tasks, ids):
    x, fw, qkv, p, ho, mid, second, act, slope, kept_a, kept_m = kept
    (ghw, ghw_away, gow, gow_away, ghb, gmid, small_m), given = mlp_bwd(
        layer, rolled, counts, cot, act, slope, second, mid, table, Stored(*kept_m), tasks[0](), ids[0]
    )
    big_m = ((ghw, ghw_away), (gow, gow_away))
    (gin, out, ga, ga_away, gqv, gtab, small_a), more = attn_bwd(
        layer, rolled, x, gmid.reshape(-1, TP, D), fw, qkv, p, ho, table, Stored(*kept_a), tasks[1](big_m, given), ids[1]
    )
    return gin, out, ((ga, ga_away), *big_m), (ghb, small_m, gqv, gtab, small_a), given, more


SMALL_ROWS = ((GAIN, 1), (SHIFT_ROW, 1), (QV, 2), (TABLE, 8), (BPROJ, 1), (MGAIN, 1), (MSHIFT, 1), (HB, 4), (OB, 1))


def on_lines(small_in):
    whole_of = [lax.all_gather(lax.all_gather(member[0], "tensor", axis=0, tiled=True), "pipe") for member in small_in]
    gain, shift, qv, table, bproj, mgain, mshift, hb, ob = whole_of

    def lines(member):
        return member.reshape(2, 4, -1, GL)

    qv = qv.reshape(2, 4, GH, 2, HD).transpose(0, 1, 3, 2, 4)
    table = jnp.pad(table, ((0, 0), (0, 0), (0, 2 * GL - RELS))).reshape(2, 4, GH, 2, GL).transpose(0, 1, 3, 2, 4)
    rows = jnp.concatenate([lines(part) for part in (gain, shift, qv, table, bproj, mgain, mshift, hb, ob)], 2)
    return jnp.pad(rows, ((0, 0), (0, 0), (0, LINES - rows.shape[2]), (0, 0))).transpose(1, 0, 2, 3)


def qkv_order(w):
    lead = w.shape[:-1]
    return jnp.swapaxes(w.reshape(*lead, GH, 3, HD), -3, -2).reshape(*lead, 3 * GL)


def general(core, images, cotangent, counts, rel_index, small_in, big_in):
    def both(member, axis):
        return lax.all_gather(lax.all_gather(member[0], "tensor", axis=axis, tiled=True), "pipe")

    table = on_lines(small_in)
    bias = bias_tables(table, rel_index)
    gathered = [both(member, axis) for member, axis in zip(big_in, (1, 0, 1, 0))]
    weights = []
    for l in range(2):
        wqkv, wproj, hw, ow = (pair[l] for pair in gathered)
        wqkv = qkv_order(wqkv.reshape(D, 4, 3 * GL).transpose(1, 0, 2))
        wa = jnp.concatenate([wqkv, wproj.reshape(4, GL, D).transpose(0, 2, 1)], 2)[None]
        wm = jnp.stack([hw.reshape(D, 4, -1).transpose(1, 0, 2), ow.reshape(4, -1, D)])
        weights.append((lambda *_, wa=wa: Weights(1, 0, whole=wa), lambda *_, wm=wm: Weights(2, 0, whole=wm)))
    none, back_none, ids = (lambda: [], lambda given: []), (lambda: [], lambda *_: []), (None, None)
    images, cotangent = (
        jnp.pad(lax.dynamic_index_in_dim(array, core, 1, False), ((0, 0), (0, TP - TOK), (0, 0))) for array in (images, cotangent)
    )
    y0, out0, kept0, _, _ = layer_forward(0, False, images, counts, table, bias, weights[0], none, ids)
    _, out1, kept1, _, _ = layer_forward(1, False, y0, counts, table, bias, weights[1], none, ids)
    g1, gin1, big1, small1, _, _ = layer_backward(1, False, cotangent, kept1, counts, table, back_none, ids)
    _, gin0, big0, small0, _, _ = layer_backward(0, False, g1, kept0, counts, table, back_none, ids)
    first_core = core == 0

    def deliver(mine0, mine1):
        came = lax.ppermute(jnp.where(first_core, mine1, mine0), "pipe", [(0, 1), (1, 0)])
        mine = jnp.where(first_core, mine0, mine1)
        return jnp.stack([jnp.where(first_core, mine, came), jnp.where(first_core, came, mine)], 1)[None]

    def matrix_of(pair):
        parts = [part[jnp.array([PLACES.index(j) for j in range(4)])] for part in pair]
        return jnp.concatenate(parts).transpose(1, 0, 2, 3).reshape(4, D, D)

    def full(big):
        ga, ghw, gow = (matrix_of(pair) for pair in big)
        gqkv = jnp.swapaxes(ga[:, :, : 3 * GL].reshape(4, D, 3, GH, HD), 2, 3).reshape(4, D, 3 * GL)
        return (
            gqkv.transpose(1, 0, 2).reshape(D, 3 * D), ga[:, :, 3 * GL :].transpose(0, 2, 1).reshape(D, D),
            ghw.transpose(1, 0, 2).reshape(D, -1), gow.transpose(0, 2, 1).reshape(-1, D),
        )

    def reduced(pair, axis):
        mine = lax.psum_scatter(jnp.stack(pair), "pipe", scatter_dimension=0, tiled=False)
        mine = lax.psum_scatter(mine, "tensor", scatter_dimension=axis, tiled=True)
        return lax.psum(mine, "dp").astype(F32)[None]

    gqkv, gproj, ghw, gow = (reduced(pair, axis) for pair, axis in zip(zip(full(big0), full(big1)), (1, 0, 1, 0)))

    def vectors(terms):
        ghb, small_m, gqv, gtab, small_a = terms
        qv = jnp.swapaxes(gqv.reshape(4, 2, GH, HD), 1, 2).reshape(-1)
        tab = table_grad(gtab, rel_index).reshape(H, RELS)
        parts = (small_a[:, 0], small_a[:, 1], qv, tab, small_m[:, 1], small_m[:, 2], small_m[:, 3], ghb, small_m[:, 0])
        return jnp.concatenate([part.reshape(-1) for part in parts])

    totals = lax.psum(jnp.stack([vectors(small0), vectors(small1)]), ("pipe", "dp", "tensor"))
    mine = jnp.where(first_core, totals[0], totals[1])
    outs, at = [], 0
    for member in small_in:
        shape = member.shape[1:]
        whole_shape = (shape[0] * lax.axis_size("tensor"),) + tuple(shape[1:])
        size = math.prod(whole_shape)
        piece = mine[at : at + size].reshape(whole_shape)
        outs.append(lax.dynamic_slice_in_dim(piece, lax.axis_index("tensor") * shape[0], shape[0], 0)[None])
        at += size
    return deliver(out0, out1), deliver(gin0, gin1), (gqkv, gproj, ghw, gow), outs


def four_by_four(images, cotangent, counts, rel_index, small_in, big_in):
    own_a, lines, index = prepare(rel_index, big_in[0][0], big_in[1][0], *[member[0] if member.ndim == 3 else member for member in small_in])
    own = (own_a, big_in[2][0], big_in[3][0])
    other, table, pieces_a0, near_h0, near_o0, bias, x0 = gather_start(own, lines, index, jnp.swapaxes(images, 1, 2))
    pick_cot = Own(jnp.swapaxes(cotangent, 1, 2), plan=((2, "pick"),))

    def near(n, layer, **how):
        return Near(layer, own[n], other[n], **how)

    def weights(layer, which, pieces):
        return Weights(len(which), layer, own=[own[n] for n in which], other=[other[n] for n in which], pieces=pieces)

    def mlp_tasks(near_h, near_o):
        return [Far(near_h, plan=((1, "turn"), (2, "rest"), (3, "last"))), Far(near_o, plan=((2, "turn"), (3, "rest"), (3, "last")))]

    def forward_weights(layer, pieces, near_h, near_o):
        return (
            lambda: weights(layer, (0,), [pieces]),
            lambda given: weights(layer, (1, 2), [[near_h, *given[1]], [near_o, *given[2]]]),
        )

    y0, out0, kept0, given, more = layer_forward(
        0, True, x0, counts, table, bias, forward_weights(0, pieces_a0, near_h0, near_o0),
        (lambda: [*mlp_tasks(near_h0, near_o0), near(0, 1), near(1, 1, deferred=True, plan=((1, "start"),))],
         lambda given: [Far(given[3][0], plan=((1, "turn"), (2, "rest"), (3, "last"))), near(2, 1)]),
        (1, 2),
    )
    pieces_a1, near_h1, near_o1 = [given[3][0], *more[1]], given[4][0], more[2][0]
    _, out1, kept1, given, _ = layer_forward(
        1, True, y0, counts, table, bias, forward_weights(1, pieces_a1, near_h1, near_o1),
        (lambda: [*mlp_tasks(near_h1, near_o1), pick_cot], lambda given: []), (3, None),
    )
    cot = given[3][0]

    def mlp_reduce(big_m):
        return [ReduceTurn(big_m[0], plan=((0, "cores"),)), ReduceTurn(big_m[1], plan=((1, "cores"),))]

    g1, gin1, big1, small1, given, more = layer_backward(
        1, True, cot, kept1, counts, table, (lambda: [Deliver([out0, out1])], lambda big_m, given: mlp_reduce(big_m)), (4, 5)
    )
    out_came, turned1 = given[1][0], more[1:3]

    def last_tasks(big_m, given):
        onward = ReduceOnward(given[1], plan=((1, "close"),))
        second_h = ReduceSecond(given[2][0], plan=((1, "close"),))
        second_o = ReduceSecond(given[3][0], deferred=True, plan=((1, "start"), (3, "close")))
        second_a = ReduceSecond(source=onward, deferred=True, plan=((2, "start"),))
        shares = [Share(source=second_h, plan=((1, "start"),)), Share(source=second_o, plan=((3, "start"),))]
        return [
            ReduceFirst(big_m[0], plan=((0, "cores"), (LATE, "turn"))), ReduceTurn(big_m[1], plan=((1, "cores"),)), onward, second_h,
            *shares[:1], second_o, second_a, *shares[1:], Weave([out0, out1], out_came, plan=((3, "all"),)),
        ]

    _, gin0, big0, small0, given, more = layer_backward(
        0, True, g1, kept0, counts, table,
        (
            lambda: [ReduceTurn(big1[0], plan=((0, "cores"),)), *[ReduceOnward(turned) for turned in turned1]],
            last_tasks,
        ),
        (6, 8),
    )
    totals_h0, turned_o0, piece_a1, shared1 = more[1][0], more[2], more[7][0], (more[5][0], more[8][0])
    block_out = more[9][0]
    matrices, lines, input_grad = reduce_end(
        big0[0], totals_h0, turned_o0, piece_a1, shared1, [gin0, gin1], [*small0, *small1], index
    )
    gqkv, gproj, ghw, gow, *outs = finish(matrices, lines)
    return jnp.swapaxes(block_out, 1, 2)[None], jnp.swapaxes(input_grad, 1, 2)[None], (gqkv, gproj, ghw, gow), outs


def local(
    images, cotangent, counts, rel_index, pre_attn_gain, pre_attn_bias, qkv_weight, qv_bias, bias_table, proj_weight, proj_bias,
    pre_mlp_gain, pre_mlp_bias, hidden_weight, hidden_bias, out_weight, out_bias,
):
    assert images.shape[1] == 2, images.shape
    counts = counts.T
    small_in = (pre_attn_gain, pre_attn_bias, qv_bias, bias_table, proj_bias, pre_mlp_gain, pre_mlp_bias, hidden_bias, out_bias)
    big_in = (qkv_weight, proj_weight, hidden_weight, out_weight)
    if lax.axis_size("tensor") == 4 and lax.axis_size("dp") == 4:
        block_out, input_grad, big, small = four_by_four(images, cotangent, counts, rel_index, small_in, big_in)
    else:
        block_out, input_grad, big, small = general(
            lax.axis_index("pipe"), images, cotangent, counts, rel_index, small_in, big_in
        )
    gqkv, gproj, ghw, gow = big
    gain_g, shift_g, qv_g, table_g, bproj_g, mgain_g, mshift_g, hb_g, ob_g = small
    return (
        block_out, input_grad, gain_g, shift_g, gqkv, qv_g, table_g, gproj, bproj_g, mgain_g, mshift_g, ghw, hb_g, gow, ob_g,
    )


def solution(mesh):
    return jax.shard_map(
        local,
        mesh=mesh,
        in_specs=(
            P(None, ("dp", "tensor"), None, None),
            P(None, ("dp", "tensor"), None, None),
            P(None, "dp"),
            P(),
            P("pipe", "tensor"),
            P("pipe", "tensor"),
            P("pipe", None, "tensor"),
            P("pipe", "tensor"),
            P("pipe", "tensor", None),
            P("pipe", "tensor", None),
            P("pipe", "tensor"),
            P("pipe", "tensor"),
            P("pipe", "tensor"),
            P("pipe", None, "tensor"),
            P("pipe", "tensor"),
            P("pipe", "tensor", None),
            P("pipe", "tensor"),
        ),
        out_specs=(
            P("pipe", None, ("dp", "tensor"), None, None),
            P("pipe", None, ("dp", "tensor"), None, None),
            P("pipe", "tensor"),
            P("pipe", "tensor"),
            P("pipe", None, "tensor"),
            P("pipe", "tensor"),
            P("pipe", "tensor", None),
            P("pipe", "tensor", None),
            P("pipe", "tensor"),
            P("pipe", "tensor"),
            P("pipe", "tensor"),
            P("pipe", None, "tensor"),
            P("pipe", "tensor"),
            P("pipe", "tensor", None),
            P("pipe", "tensor"),
        ),
        check_vma=False,
    )
```

```python
import functools
import math

import jax
import jax.numpy as jnp
from jax import lax
from jax.experimental import pallas as pl
from jax.experimental.pallas import tpu as pltpu
from jax.sharding import PartitionSpec as P

D = 512
H = 16
HD = 32
WIN = 7
GRID = 14
SHIFT = 3
TOK = 196
RELS = 169
POS = WIN * WIN
NW = 4
WP = 64
TP = 208
ROWS = NW * WP
GH = 4
GL = GH * HD
BLK = 832
SUB_FWD = 208
SUB_BWD = 416
CHUNK = 64
AT_ONCE = 2
LATE = "late"
LINES = 32
GAIN, SHIFT_ROW, QV, TABLE, BPROJ, MGAIN, MSHIFT, HB, OB = 0, 1, 2, 4, 12, 13, 14, 15, 19
PLACES = (1, 3, 2, 0)
EPSILON = 1e-05
MASK_VALUE = -100.0
SHUT = -1e30
F32 = jnp.float32
BF = jnp.bfloat16
ANY = pl.BlockSpec(memory_space=pl.ANY)
VMEM_LIMIT = 60 << 20


def dot_nn(a, b):
    return lax.dot_general(a, b, (((1,), (0,)), ((), ())), preferred_element_type=F32)


def dot_nt(a, b):
    return lax.dot_general(a, b, (((1,), (1,)), ((), ())), preferred_element_type=F32)


def dot_tn(a, b):
    return lax.dot_general(a, b, (((0,), (0,)), ((), ())), preferred_element_type=F32)


def iota(shape, axis):
    return lax.broadcasted_iota(jnp.int32, shape, axis)


def normalize(rows):
    center = rows - jnp.mean(rows, -1, keepdims=True)
    inverse = lax.rsqrt(jnp.mean(center * center, -1, keepdims=True) + EPSILON)
    return center * inverse, inverse


def norm_back(grad_out, normed, inverse, gain):
    scaled = grad_out * gain
    return inverse * (
        scaled
        - jnp.mean(scaled, -1, keepdims=True)
        - normed * jnp.mean(scaled * normed, -1, keepdims=True)
    )


def remote(source, target, sems, axis, index):
    return pltpu.make_async_remote_copy(
        src_ref=source, dst_ref=target, send_sem=sems[0], recv_sem=sems[1], device_id={axis: index},
        device_id_type=pl.DeviceIdType.MESH,
    )


def place_in_mesh():
    return lax.axis_index("pipe"), lax.axis_index("dp"), lax.axis_index("tensor")


def greet():
    core, dp, shard = place_in_mesh()
    barrier = pltpu.get_barrier_semaphore()

    def signal(axis, index):
        pl.semaphore_signal(barrier, inc=1, device_id={axis: index}, device_id_type=pl.DeviceIdType.MESH)

    signal("pipe", 1 - core)
    for k in (1, 2, 3):
        signal("dp", dp ^ k)
        signal("tensor", lax.rem(shard + k, 4))
    pl.semaphore_wait(barrier, 7)


def quarter(half, j):
    core, dp, _ = place_in_mesh()
    return pl.ds(pl.multiple_of((core ^ half) * 256 + (dp ^ j) * CHUNK, CHUNK), CHUNK)


def by_core(action):
    for which in (0, 1):

        @pl.when(lax.axis_index("pipe") == which)
        def _():
            action(which)


def sems(*shape):
    return [pltpu.SemaphoreType.DMA(shape), pltpu.SemaphoreType.DMA(shape)]


class Part:
    plan = ()
    deferred = False

    def flush(self):
        pass

    def __init__(self, inputs=(), outputs=(), scratch=()):
        self.inputs, self.outputs, self.scratch = list(inputs), list(outputs), list(scratch)

    def bind(self, ins, outs, kept):
        self.ins, self.outs, self.kept = ins, outs, kept


class Weights(Part):
    def __init__(self, count, layer, whole=None, own=None, other=None, pieces=None):
        self.count, self.layer, self.whole = count, layer, whole
        inputs = [whole] if whole is not None else [*own, *other, *[piece for group in pieces for piece in group]]
        super().__init__(inputs, (), [pltpu.VMEM((count, 4, D, D), BF), pltpu.SemaphoreType.DMA((9 * count,))])

    def shard(self, mine, b):
        store, sem = self.kept
        if self.whole is not None:
            return pltpu.make_async_copy(self.ins[0].at[b, 0], store.at[b, 0], sem.at[b * 9])
        owns, others = self.ins[: self.count], self.ins[self.count : 2 * self.count]
        return pltpu.make_async_copy((owns if mine else others)[b], store.at[b, 0], sem.at[b * 9])

    def rest(self):
        store, sem = self.kept
        if self.whole is not None:
            return [
                pltpu.make_async_copy(self.ins[0].at[b, pl.ds(1, 3)], store.at[b, pl.ds(1, 3)], sem.at[b * 9 + 1])
                for b in range(self.count)
            ]
        return [
            pltpu.make_async_copy(
                self.ins[2 * self.count + b * 8 + half * 4 + j], store.at[b, pl.ds(1, 3), quarter(half, j), :],
                sem.at[b * 9 + half * 4 + j + 1],
            )
            for b in range(self.count)
            for half in range(2)
            for j in range(4)
        ]

    def load(self):
        if self.whole is not None:
            for b in range(self.count):
                self.shard(True, b).start()
        else:

            def shards(core):
                for b in range(self.count):
                    self.shard(core == self.layer, b).start()

            by_core(shards)
        if self.count == 1:
            self.load_rest()

    def load_rest(self):
        for copy in self.rest():
            copy.start()

    def wait_shard(self):
        for b in range(self.count):
            self.shard(True, b).wait()

    def wait_rest(self):
        for copy in self.rest():
            copy.wait()


class Stored(Part):
    def __init__(self, *arrays):
        super().__init__(arrays, (), [pltpu.VMEM(a.shape, a.dtype) for a in arrays] + [pltpu.SemaphoreType.DMA((len(arrays),))])

    def copies(self):
        return [pltpu.make_async_copy(ref, kept, self.kept[-1].at[n]) for n, (ref, kept) in enumerate(zip(self.ins, self.kept))]

    def load(self):
        for copy in self.copies():
            copy.start()

    def wait(self):
        for copy in self.copies():
            copy.wait()


class Keep(Part):
    def __init__(self, *shapes):
        super().__init__((), [jax.ShapeDtypeStruct(shape, BF) for shape in shapes], [pltpu.SemaphoreType.DMA((len(shapes),))])

    def copies(self, refs):
        return [pltpu.make_async_copy(ref, out, self.kept[0].at[n]) for n, (ref, out) in enumerate(zip(refs, self.outs))]

    def start(self, *refs):
        for copy in self.copies(refs):
            copy.start()

    def wait(self, *refs):
        for copy in self.copies(refs):
            copy.wait()


class Near(Part):
    def __init__(self, layer, own, other, plan=(), deferred=False):
        self.layer, self.plan, self.deferred = layer, plan, deferred
        inputs = [] if own is None else [own, other]
        super().__init__(inputs, [jax.ShapeDtypeStruct((3, CHUNK, D), BF)], sems(3))

    def copy(self, mine, k):
        _, _, shard = place_in_mesh()
        source = self.ins[0 if mine else 1].at[quarter(0, 0), :]
        return remote(source, self.outs[0].at[k - 1], [sem.at[k - 1] for sem in self.kept], "tensor", lax.rem(shard + 4 - k, 4))

    def start(self):
        def sends(core):
            for k in (2, 1, 3):
                self.copy(core == self.layer, k).start()

        by_core(sends)

    def finish(self):
        for k in (1, 2, 3):
            self.copy(True, k).wait()

    def end(self):
        if not any(what == "finish" for _, what in self.plan):
            self.finish()


class Far(Part):
    def __init__(self, near, plan=(), source=None, deferred=False):
        self.plan, self.source, self.deferred = plan, source, deferred
        shape = jax.ShapeDtypeStruct((3, CHUNK, D), BF)
        super().__init__([] if near is None else [near], [shape] * 7, sems(2, 2) + sems(2) + sems(4))

    def rows(self, j):
        return pl.ds((j - 1) * 32, 32)

    def across(self, j, half):
        _, dp, _ = place_in_mesh()
        rows = self.rows(j if half == 0 else 3 - j)
        return remote(
            self.ins[0].at[:, rows], self.outs[j - 1].at[:, rows], [sem.at[j - 1, half] for sem in self.kept[:2]], "dp", dp ^ j
        )

    def onward(self, j):
        _, dp, _ = place_in_mesh()
        rows = self.rows(j)
        return remote(
            self.outs[j - 1].at[:, rows], self.outs[2].at[:, rows], [sem.at[j - 1] for sem in self.kept[2:4]], "dp", dp ^ (3 - j)
        )

    def over(self, j):
        core, _, _ = place_in_mesh()
        source = self.ins[0] if j == 0 else self.outs[j - 1]
        return remote(source, self.outs[3 + j], [sem.at[j] for sem in self.kept[4:]], "pipe", 1 - core)

    def start(self):
        for half in (0, 1):
            for j in (1, 2):
                self.across(j, half).start()
        self.over(0).start()

    def turn(self):
        for j in (1, 2):
            self.across(j, 0).wait()
        for j in (1, 2):
            self.onward(j).start()

    def rest(self):
        for j in (1, 2):
            self.across(j, 1).wait()
            self.over(j).start()

    def last(self):
        for j in (1, 2):
            self.onward(j).wait()
        self.over(3).start()

    def end(self):
        for j in range(4):
            self.over(j).wait()


class ReduceFirst(Part):
    def __init__(self, pair, plan=(), rows=(0, CHUNK)):
        self.plan, (self.start_row, self.size) = plan, rows
        size = self.size
        half = pltpu.VMEM((4, 4, size, D), BF)
        super().__init__(
            pair,
            [jax.ShapeDtypeStruct((4, size, D), BF)],
            [half, half, pltpu.VMEM((2, 2, 2, size, D), BF), pltpu.VMEM((2, 2, size, D), BF), pltpu.VMEM((4, size, D), BF)]
            + sems() + sems(2) + sems(2) + [pltpu.SemaphoreType.DMA(()), pltpu.SemaphoreType.DMA(())],
        )

    def bind(self, ins, outs, kept):
        super().bind(ins, outs, kept)
        self.mine, self.came, self.first, self.second, self.total = kept[:5]

    def over(self):
        core, _, _ = place_in_mesh()
        source = self.ins[1].at[:, :, pl.ds(self.start_row, self.size)]
        return remote(source, self.came, self.kept[5:7], "pipe", 1 - core)

    def load(self):
        return pltpu.make_async_copy(self.ins[0].at[:, :, pl.ds(self.start_row, self.size)], self.mine, self.kept[11])

    def across(self, j):
        _, dp, _ = place_in_mesh()
        source = self.mine.at[pl.ds(j - 1, 2), pl.ds(2 * j - 2, 2)]
        return remote(source, self.first.at[j - 1], [sem.at[j - 1] for sem in self.kept[7:9]], "dp", dp ^ j)

    def onward(self, j):
        _, dp, _ = place_in_mesh()
        source = self.mine.at[2 if j == 1 else 0, pl.ds(2 * j - 2, 2)]
        return remote(source, self.second.at[j - 1], [sem.at[j - 1] for sem in self.kept[9:11]], "dp", dp ^ (3 - j))

    def start(self):
        self.over().start()
        self.load().start()

    def cores(self):
        self.over().wait()
        self.load().wait()

        def add(place, k):
            self.mine[place, k] += self.came[place, k]

        def sent(n, carry):
            add(n // 2, n % 2)
            add(n // 2 + 1, n % 2 + 2)
            return carry

        def kept(n, carry):
            add(3, n)
            add(2 - n // 2 * 2, n)
            return carry

        lax.fori_loop(0, 4, sent, 0)
        for j in (1, 2):
            self.across(j).start()
        lax.fori_loop(0, 4, kept, 0)

    def turn(self):
        for j in (1, 2):
            self.across(j).wait()

        def add(n, carry):
            self.mine[2, n] += self.first[0, 1, n]
            self.mine[0, n + 2] += self.first[1, 0, n]
            return carry

        lax.fori_loop(0, 2, add, 0)
        for j in (1, 2):
            self.onward(j).start()

    def close(self):
        for j in (1, 2):
            self.onward(j).wait()

        def add(n, carry):
            for j in (1, 2):
                k = n + 2 * j - 2
                total = self.mine[3, k].astype(F32) + self.first[j - 1, j - 1, n].astype(F32)
                self.total[k] = (total + self.second[j - 1, n].astype(F32)).astype(BF)
            return carry

        lax.fori_loop(0, 2, add, 0)

    def out(self):
        return pltpu.make_async_copy(self.total, self.outs[0], self.kept[12])

    def end(self):
        self.close()
        self.out().start()

    def flush(self):
        self.out().wait()


class ReduceTurn(ReduceFirst):
    def __init__(self, pair, plan=()):
        super().__init__(pair, plan)
        self.outputs = [jax.ShapeDtypeStruct((2, 2, CHUNK, D), BF), jax.ShapeDtypeStruct((4, CHUNK, D), BF)]
        self.scratch.append(pltpu.SemaphoreType.DMA((3,)))

    def end(self):
        for j in (1, 2):
            self.across(j).wait()

        def add(n, carry):
            self.mine[2, n] += self.first[0, 1, n]
            self.mine[0, n + 2] += self.first[1, 0, n]
            for j in (1, 2):
                self.mine[3, n + 2 * j - 2] += self.first[j - 1, j - 1, n]
            return carry

        lax.fori_loop(0, 2, add, 0)
        for copy in self.copies():
            copy.start()

    def copies(self):
        sem = self.kept[13]
        return [
            pltpu.make_async_copy(self.mine.at[2, pl.ds(0, 2)], self.outs[0].at[0], sem.at[0]),
            pltpu.make_async_copy(self.mine.at[0, pl.ds(2, 2)], self.outs[0].at[1], sem.at[1]),
            pltpu.make_async_copy(self.mine.at[3], self.outs[1], sem.at[2]),
        ]

    def flush(self):
        for copy in self.copies():
            copy.wait()


class ReduceOnward(Part):
    def __init__(self, given, plan=()):
        self.plan = plan
        base = pltpu.VMEM((4, CHUNK, D), BF)
        super().__init__(
            given, [jax.ShapeDtypeStruct((4, CHUNK, D), BF)],
            [base, pltpu.VMEM((2, 2, CHUNK, D), BF)] + sems(2) + [pltpu.SemaphoreType.DMA(()), pltpu.SemaphoreType.DMA(())],
        )

    def onward(self, j):
        _, dp, _ = place_in_mesh()
        return remote(self.ins[0].at[j - 1], self.kept[1].at[j - 1], [sem.at[j - 1] for sem in self.kept[2:4]], "dp", dp ^ (3 - j))

    def load(self):
        return pltpu.make_async_copy(self.ins[1], self.kept[0], self.kept[4])

    def start(self):
        for j in (1, 2):
            self.onward(j).start()
        self.load().start()

    def close(self):
        self.load().wait()
        for j in (1, 2):
            self.onward(j).wait()
        total = self.kept[0]

        def add(n, carry):
            for j in (1, 2):
                total[n + 2 * j - 2] += self.kept[1][j - 1, n]
            return carry

        lax.fori_loop(0, 2, add, 0)

    def out(self):
        return pltpu.make_async_copy(self.kept[0], self.outs[0], self.kept[5])

    def end(self):
        if not any(what == "close" for _, what in self.plan):
            self.close()
        self.out().start()

    def flush(self):
        self.out().wait()


class ReduceSecond(Part):
    def __init__(self, totals=None, size=CHUNK, plan=(), source=None, deferred=False):
        self.plan, self.after, self.deferred = plan, source, deferred
        line = pltpu.VMEM((size, D), BF)
        super().__init__(
            [totals] if totals is not None else [],
            [jax.ShapeDtypeStruct((size, D), BF)],
            [line, pltpu.VMEM((3, size, D), BF)] + sems(3) + [pltpu.SemaphoreType.DMA(()), pltpu.SemaphoreType.DMA(())],
        )

    def own(self):
        return pltpu.make_async_copy(self.ins[0].at[0], self.kept[0], self.kept[4])

    def along(self, k):
        _, _, shard = place_in_mesh()
        return remote(
            self.ins[0].at[k], self.kept[1].at[k - 1], [sem.at[k - 1] for sem in self.kept[2:4]], "tensor", lax.rem(shard + k, 4)
        )

    def start(self):
        if self.after is not None:
            self.ins = [self.after.kept[0]]
        for k in (2, 1, 3):
            self.along(k).start()
        self.own().start()

    def close(self):
        self.own().wait()
        for k in (1, 2, 3):
            self.along(k).wait()
        total = self.kept[0][...].astype(F32)
        for k in range(3):
            total += self.kept[1][k].astype(F32)
        self.kept[0][...] = total.astype(BF)

    def end(self):
        if not any(what == "close" for _, what in self.plan):
            self.close()
        self.out().start()

    def out(self):
        return pltpu.make_async_copy(self.kept[0], self.outs[0], self.kept[5])

    def flush(self):
        self.out().wait()


class Share(Part):
    def __init__(self, piece=None, rows=(0, CHUNK), target=None, source=None, plan=(), in_vmem=False):
        self.start_row, self.size = rows
        self.target, self.after, self.plan, self.deferred = target, source, plan, source is not None
        super().__init__(
            [piece] if piece is not None else [],
            [jax.ShapeDtypeStruct((D, D), BF)] if target is None and not in_vmem else [],
            [pltpu.VMEM((self.size, D), BF)] + sems(3) + [pltpu.SemaphoreType.DMA(()), pltpu.SemaphoreType.DMA(())]
            + ([pltpu.VMEM((D, D), BF)] if in_vmem else []),
        )
        self.in_vmem = in_vmem

    def whole(self):
        return self.kept[5] if self.in_vmem else self.outs[0]

    def place(self):
        core, dp, _ = place_in_mesh()
        start = pl.multiple_of(core * 256 + dp * CHUNK, CHUNK) + self.start_row
        out = (self.target or self).whole()
        return out.at[pl.ds(pl.multiple_of(start, self.size), self.size), :]

    def across(self, j):
        _, dp, _ = place_in_mesh()
        return remote(self.ins[0], self.place(), [sem.at[j - 1] for sem in self.kept[1:3]], "dp", dp ^ j)

    def load(self):
        return pltpu.make_async_copy(self.ins[0], self.kept[0], self.kept[3])

    def keep(self):
        return pltpu.make_async_copy(self.kept[0], self.place(), self.kept[4])

    def start(self):
        if self.after is not None:
            self.ins = [self.after.kept[0]]
        for j in (3, 1, 2):
            self.across(j).start()
        self.load().start()

    def end(self):
        self.load().wait()
        self.keep().start()
        for j in (1, 2, 3):
            self.across(j).wait()

    def flush(self):
        self.keep().wait()


class Deliver(Part):
    def __init__(self, of_layers):
        super().__init__(of_layers, [jax.ShapeDtypeStruct(of_layers[0].shape, BF)], sems())

    def send(self, core):
        return remote(self.ins[1 - core], self.outs[0], self.kept, "pipe", 1 - core)

    def start(self):
        by_core(lambda core: self.send(core).start())

    def end(self):
        self.send(0).wait()


class Weave(Part):
    def __init__(self, of_layers, came=None, plan=()):
        self.plan = plan
        count = of_layers[0].shape[0]
        images = pltpu.VMEM((count, TOK, D), BF)
        self.count = count
        super().__init__(
            [*of_layers] + ([] if came is None else [came]), [jax.ShapeDtypeStruct((count, TOK, 2, D), BF)],
            [images, images, pltpu.VMEM((count, TOK, 2, D), BF)] + sems()
            + [pltpu.SemaphoreType.DMA(()), pltpu.SemaphoreType.DMA(()), pltpu.SemaphoreType.DMA((count,))],
        )

    def send(self, core):
        return remote(self.ins[1 - core], self.kept[1], self.kept[3:5], "pipe", 1 - core)

    def own(self, core):
        return pltpu.make_async_copy(self.ins[core], self.kept[0], self.kept[5])

    def came(self):
        return pltpu.make_async_copy(self.ins[2], self.kept[1], self.kept[6])

    def store(self, m):
        return pltpu.make_async_copy(self.kept[2].at[m], self.outs[0].at[m], self.kept[7].at[m])

    def start(self):
        by_core(lambda core: self.own(core).start())
        if len(self.ins) > 2:
            self.came().start()
        else:
            by_core(lambda core: self.send(core).start())

    def wait(self):
        self.own(0).wait()
        (self.came() if len(self.ins) > 2 else self.send(0)).wait()

    def weave(self, first, last):
        first_core = lax.axis_index("pipe") == 0

        def image(m, carry):
            mine, theirs = self.kept[0][m], self.kept[1][m]
            pair = [jnp.where(first_core, mine, theirs), jnp.where(first_core, theirs, mine)]
            self.kept[2][m] = jnp.stack(pair, axis=1)
            return carry

        lax.fori_loop(first, last, image, 0)
        for m in range(first, last):
            self.store(m).start()

    def all(self):
        self.wait()
        self.weave(0, self.count)

    def end(self):
        for m in range(self.count):
            self.store(m).wait()


def carried_call(body, parts, collective_id, *, grid, in_specs, inputs, out_specs, out_shape, scratch_shapes, name, cost):
    n_in, n_out, n_scratch = len(inputs), len(out_shape), len(scratch_shapes)
    counts = [(len(part.inputs), len(part.outputs), len(part.scratch)) for part in parts]

    def whole_body(*refs):
        refs = list(refs)

        def take(count, groups):
            mine = [refs.pop(0) for _ in range(count)]
            return mine, [[refs.pop(0) for _ in range(n)] for n in groups]

        mine, part_ins = take(n_in, [n for n, _, _ in counts])
        outs, part_outs = take(n_out, [n for _, n, _ in counts])
        kept, part_kept = take(n_scratch, [n for _, _, n in counts])
        for part, a, b, c in zip(parts, part_ins, part_outs, part_kept):
            part.bind(a, b, c)
        for part in parts:
            if getattr(part, "source", None) is not None:
                part.ins = [part.source.outs[0]]
        body(*mine, *outs, *kept)

    extra_in = [x for part in parts for x in part.inputs]
    extra_out = [x for part in parts for x in part.outputs]
    params = dict(vmem_limit_bytes=VMEM_LIMIT)
    if collective_id is not None:
        params.update(collective_id=collective_id, has_side_effects=True)
    results = pl.pallas_call(
        whole_body,
        grid_spec=pltpu.PrefetchScalarGridSpec(
            num_scalar_prefetch=0,
            grid=grid,
            in_specs=list(in_specs) + [ANY] * len(extra_in),
            out_specs=list(out_specs) + [ANY] * len(extra_out),
            scratch_shapes=list(scratch_shapes) + [x for part in parts for x in part.scratch],
        ),
        out_shape=list(out_shape) + extra_out,
        name=name,
        compiler_params=pltpu.CompilerParams(**params),
        cost_estimate=cost,
    )(*inputs, *extra_in)
    own, rest = results[:n_out], results[n_out:]
    given = []
    for _, n, _ in counts:
        given.append(rest[:n])
        rest = rest[n:]
    return own, given


def begin(weights, tasks):
    pl.when(pl.program_id(0) == 0)(weights.load)
    if tasks:

        @pl.when(pl.program_id(0) == 0)
        def _():
            greet()
            for task in tasks:
                if not task.deferred:
                    task.start()

    if isinstance(weights, Weights) and weights.count > 1:
        pl.when(pl.program_id(0) == 0)(weights.load_rest)


def planned(tasks, point):
    return [getattr(task, what) for task in tasks for at, what in task.plan if at == point]


def step_end(tasks, steps):
    for step in range(steps):
        calls = planned(tasks, step)
        if step == steps - 1:
            calls += [task.end for task in tasks] + [task.flush for task in tasks]
        if calls:

            @pl.when(pl.program_id(0) == step)
            def _():
                for call in calls:
                    call()


def whole(shape):
    return pl.BlockSpec(shape, lambda i: (0,) * len(shape))


def per(shape):
    return pl.BlockSpec((1,) + shape, lambda i: (i,) + (0,) * len(shape))


SMEM = pl.BlockSpec(memory_space=pltpu.SMEM)


def along_model(table_ref, layer, row, rolled):
    shard = lax.axis_index("tensor") if rolled else 0
    return jnp.concatenate([table_ref[(z - shard + 4) % 4, layer, row : row + 1, :].astype(F32) for z in range(4)], 1)


def window_token(shape, axis, offset):
    s = iota(shape, axis)
    w, a = s // WP, s % WP
    r = (w // 2) * WIN + a // WIN + offset
    c = (w % 2) * WIN + a % WIN + offset
    r, c = jnp.where(r >= GRID, r - GRID, r), jnp.where(c >= GRID, c - GRID, c)
    return jnp.where(a < POS, r * GRID + c, -1)


def spread_map(offset):
    return (window_token((ROWS, 1), 0, offset) == iota((ROWS, TP), 1)).astype(F32).astype(BF)


def gather_map(offset):
    return (window_token((1, ROWS), 1, offset) == iota((TP, ROWS), 0)).astype(F32).astype(BF)


def head_mask():
    return (iota((GH * WP, GL), 0) // WP == iota((GH * WP, GL), 1) // HD).astype(F32).astype(BF)


def region_mask(w):
    def band(a, which):
        place = which * WIN + a
        return (place >= GRID - WIN).astype(jnp.int32) + (place >= GRID - SHIFT).astype(jnp.int32)

    def label(a):
        return band(a // WIN, w // 2) * 3 + band(a % WIN, w % 2)

    keys = label(iota((WP, 1), 0))
    queries = label(iota((1, GH * WP), 1) % WP)
    return jnp.where(keys != queries, MASK_VALUE, 0.0).astype(F32)


def block_diagonal(rows, mask):
    return jnp.concatenate([rows] * GH, axis=0) * mask


def query_major(pt):
    turned = pt.T
    return jnp.concatenate([turned[h * WP : (h + 1) * WP] for h in range(GH)], axis=1)


def pick_diagonal(full):
    head = iota((WP, GL), 1) // HD
    out = full[0:WP]
    for h in range(1, GH):
        out = jnp.where(head == h, full[h * WP : (h + 1) * WP], out)
    return out


def permutation(size, source_of, inverse):
    rows = iota((size, size), 1 if inverse else 0)
    cols = iota((size, size), 0 if inverse else 1)
    return (rows == source_of(cols)).astype(F32).astype(BF)


def qkv_source(col):
    return (col % GL) // HD * (3 * HD) + col // GL * HD + col % HD


def qv_source(col):
    return (col % GL) // HD * (2 * HD) + col // GL * HD + col % HD


def attn_fwd_body(
    layer, rolled, weights, keep, tasks, x_ref, table_ref, bias_ref, fw_ref, qkv_ref, p_ref, ho_ref, mid_ref,
    how_ref, wq_ref, wpt_ref, vec_ref, shift_ref, spread_ref, gather_ref, mask_ref, region_ref,
):
    begin(weights, tasks)
    wa_ref = weights.kept[0].at[0]
    first_step = pl.program_id(0) == 0

    @pl.when(first_step)
    def _():
        for n, row in enumerate((GAIN, SHIFT_ROW, BPROJ)):
            vec_ref[n : n + 1, :] = along_model(table_ref, layer, row, rolled)
        for g in range(4):
            qv = table_ref[g, layer, QV : QV + 2, :].astype(F32)
            at = 3 * GL * g
            for n, (scale, shift) in enumerate(((HD ** (-0.5), qv[0:1] * HD ** (-0.5)), (1.0, 0.0), (1.0, qv[1:2]))):
                lanes = slice(at + n * GL, at + (n + 1) * GL)
                shift_ref[0:1, lanes] = jnp.full((1, GL), scale, F32)
                shift_ref[1:2, lanes] = shift + jnp.zeros((1, GL), F32)
        spread_ref[...] = spread_map(layer * SHIFT)
        gather_ref[...] = gather_map(layer * SHIFT)
        mask_ref[...] = head_mask()
        if layer:
            for w in range(NW):
                region_ref[w] = region_mask(w)

    x = x_ref[0].astype(F32)
    normed, _ = normalize(x)
    first = (normed * vec_ref[0:1, :] + vec_ref[1:2, :]).astype(BF)
    fw = dot_nn(spread_ref[...], first).astype(BF)
    fw_ref[0] = fw

    @pl.when(first_step)
    def _():
        weights.wait_shard()
        weights.wait_rest()
        for g in range(4):
            wq_ref[:, 3 * GL * g : 3 * GL * (g + 1)] = wa_ref[g, :, : 3 * GL]
            wpt_ref[:, g * GL : (g + 1) * GL] = wa_ref[g, :, 3 * GL :]
        keep.start(wq_ref, wpt_ref)

    for n in range(3):
        lanes = slice(n * D, (n + 1) * D)
        projected = dot_nn(fw, wq_ref[:, lanes])
        qkv_ref[0, :, lanes] = (projected * shift_ref[0:1, lanes] + shift_ref[1:2, lanes]).astype(BF)

    def windows(n, carry):
        chains = [(n * AT_ONCE + w, g) for w in range(AT_ONCE) for g in range(4)]

        def rows(w):
            return pl.ds(pl.multiple_of(w * WP, WP), WP)

        def part(w, g, n):
            return qkv_ref[0, rows(w), (3 * g + n) * GL : (3 * g + n + 1) * GL]

        scores = [dot_nt(part(w, g, 1), block_diagonal(part(w, g, 0), mask_ref[...])) for w, g in chains]
        probs = []
        for (w, g), st in zip(chains, scores):
            st = st + bias_ref[0, g]
            if layer:
                st = st + region_ref[w]
            e = jnp.exp(st - jnp.max(st, 0, keepdims=True))
            pt = (e * (1.0 / jnp.sum(e, 0, keepdims=True))).astype(BF)
            p_ref[0, w, g] = pt
            probs.append(pt)
        mixed = [dot_tn(pt, part(w, g, 2)) for (w, g), pt in zip(chains, probs)]
        for (w, g), out in zip(chains, mixed):
            how_ref[rows(w), g * GL : (g + 1) * GL] = pick_diagonal(out).astype(BF)
        return carry

    lax.fori_loop(0, NW // AT_ONCE, windows, 0)
    ho = dot_nn(gather_ref[...], how_ref[...]).astype(BF)
    ho_ref[0] = ho
    mid_ref[0] = x + (dot_nt(ho, wpt_ref[...]) + vec_ref[2:3, :])
    step_end(tasks, 4)

    @pl.when(pl.program_id(0) == pl.num_programs(0) - 1)
    def _():
        keep.wait(wq_ref, wpt_ref)


def attn_fwd(layer, rolled, x, table, bias, weights, tasks=(), collective_id=None):
    n = x.shape[0]
    keep = Keep((D, 3 * D), (D, D))
    return carried_call(
        functools.partial(attn_fwd_body, layer, rolled, weights, keep, tasks),
        [keep, weights, *tasks],
        collective_id,
        grid=(n,),
        in_specs=[
            per(x.shape[1:]), whole(table.shape), pl.BlockSpec((1, 4, WP, GH * WP), lambda i: (layer, 0, 0, 0)),
        ],
        inputs=(x, table, bias),
        out_specs=[per((ROWS, D)), per((ROWS, 3 * D)), per((NW, 4, WP, GH * WP)), per((TP, D)), per((TP, D))],
        out_shape=[
            jax.ShapeDtypeStruct((n, ROWS, D), BF),
            jax.ShapeDtypeStruct((n, ROWS, 3 * D), BF),
            jax.ShapeDtypeStruct((n, NW, 4, WP, GH * WP), BF),
            jax.ShapeDtypeStruct((n, TP, D), BF),
            jax.ShapeDtypeStruct((n, TP, D), F32),
        ],
        scratch_shapes=[
            pltpu.VMEM((ROWS, D), BF), pltpu.VMEM((D, 3 * D), BF), pltpu.VMEM((D, D), BF), pltpu.VMEM((8, D), F32),
            pltpu.VMEM((8, 3 * D), F32), pltpu.VMEM((ROWS, TP), BF), pltpu.VMEM((TP, ROWS), BF), pltpu.VMEM((GH * WP, GL), BF),
            pltpu.VMEM((NW, WP, GH * WP), F32),
        ],
        name="attn_fwd",
        cost=pl.CostEstimate(flops=n * 2 * 256 * 512 * 2600, bytes_accessed=n * 2 << 20, transcendentals=0),
    )


def gelu_parts(v):
    cdf = 0.5 * (1.0 + lax.erf(v * 0.5**0.5))
    pdf = jnp.exp(-0.5 * v * v) * (2.0 * math.pi) ** (-0.5)
    return v * cdf, cdf + v * pdf


def alive_of(counts_ref, m):
    slot = lax.axis_index("tensor") * 2 + lax.axis_index("pipe")
    return (slot < counts_ref[0, m]).astype(F32)


def live_rows(counts_ref, m):
    return jnp.where(iota((TP, 1), 0) < TOK, alive_of(counts_ref, m), 0.0)


def mlp_fwd_body(
    layer, rolled, weights, keep, tasks, counts_ref, mid_ref, table_ref, second_ref, act_ref, slope_ref, y_ref, out_ref, acc_ref, hb_ref
):
    c = pl.program_id(0)
    rows_total = mid_ref.shape[0]
    begin(weights, tasks)
    wm_ref = weights.kept[0]

    @pl.when(c == 0)
    def _():
        for k in range(4):
            hb_ref[k] = jnp.concatenate([table_ref[k, layer, HB + n : HB + n + 1, :].astype(F32) for n in range(4)], 1)
        gain = along_model(table_ref, layer, MGAIN, rolled)
        shift = along_model(table_ref, layer, MSHIFT, rolled)
        mid = mid_ref[...]
        normed, _ = normalize(mid)
        second_ref[...] = (normed * gain + shift).astype(BF)
        acc_ref[...] = mid + along_model(table_ref, layer, OB, rolled)
        weights.wait_shard()

    @pl.when(c == 1)
    def _():
        weights.wait_rest()
        keep.start(wm_ref)

    def block(b, carry):
        parts = [pl.ds(pl.multiple_of(b * BLK + n * SUB_FWD, SUB_FWD), SUB_FWD) for n in range(BLK // SUB_FWD)]
        acts = []
        pre = [dot_nn(second_ref[rows, :], wm_ref[0, c]) for rows in parts]
        for rows, value in zip(parts, pre):
            act, slope = gelu_parts(value + hb_ref[c])
            act = act.astype(BF)
            act_ref[0, rows, :] = act
            slope_ref[0, rows, :] = slope.astype(BF)
            acts.append(act)
        outs = [dot_nn(act, wm_ref[1, c]) for act in acts]
        for rows, out in zip(parts, outs):
            acc_ref[rows, :] += out
        return carry

    lax.fori_loop(0, rows_total // BLK, block, 0)

    @pl.when(c == pl.num_programs(0) - 1)
    def _():
        for m in range(rows_total // TP):
            y = (acc_ref[m * TP : (m + 1) * TP, :] * live_rows(counts_ref, m)).astype(BF)
            y_ref[m] = y
            out_ref[m] = y[:TOK]
        keep.wait(wm_ref)

    step_end(tasks, 4)


def mlp_fwd(layer, rolled, counts, mid, table, weights, tasks=(), collective_id=None):
    r = mid.shape[0]
    n = r // TP
    keep = Keep((2, 4, D, D))
    return carried_call(
        functools.partial(mlp_fwd_body, layer, rolled, weights, keep, tasks),
        [keep, weights, *tasks],
        collective_id,
        grid=(4,),
        in_specs=[SMEM, whole((r, D)), whole(table.shape)],
        inputs=(counts, mid, table),
        out_specs=[whole((r, D)), per((r, D)), per((r, D)), whole((n, TP, D)), whole((n, TOK, D))],
        out_shape=[
            jax.ShapeDtypeStruct((r, D), BF),
            jax.ShapeDtypeStruct((4, r, D), BF),
            jax.ShapeDtypeStruct((4, r, D), BF),
            jax.ShapeDtypeStruct((n, TP, D), BF),
            jax.ShapeDtypeStruct((n, TOK, D), BF),
        ],
        scratch_shapes=[pltpu.VMEM((r, D), F32), pltpu.VMEM((4, 1, D), F32)],
        name="mlp_fwd",
        cost=pl.CostEstimate(flops=4 * r * D * 2048, bytes_accessed=12 << 20, transcendentals=0),
    )


def scatter_rows(place, value_ref, mine_ref, away_ref, index):
    core, dp = place
    for half, out_ref in enumerate((mine_ref, away_ref)):
        for n, j in enumerate(PLACES):
            start = (core ^ half) * 256 + (dp ^ j) * CHUNK
            out_ref[n, index] = value_ref[pl.ds(pl.multiple_of(start, CHUNK), CHUNK), :]


def where_in_plane(rolled):
    return (lax.axis_index("pipe"), lax.axis_index("dp")) if rolled else (jnp.int32(0), jnp.int32(0))


def by_shard(row):
    return jnp.concatenate([row[None, :, z * GL : (z + 1) * GL] for z in range(4)], 0)


def mlp_bwd_body(
    layer, rolled, weights, tasks, counts_ref, g_ref, act_ref, slope_ref, second_ref, mid_ref, table_ref,
    ghw_ref, ghw_away_ref, gow_ref, gow_away_ref, ghb_ref, gmid_ref, small_ref,
    gy_ref, gyt_ref, sect_ref, gp_ref, acc_ref, value_ref,
):
    c = pl.program_id(0)
    rows_total = mid_ref.shape[0]
    begin(weights, tasks)
    wm_ref = weights.kept[0]

    @pl.when(c == 0)
    def _():
        total = jnp.zeros((1, D), F32)
        for m in range(rows_total // TP):
            rows = slice(m * TP, (m + 1) * TP)
            gy = g_ref[m].astype(F32) * live_rows(counts_ref, m)
            gy_ref[rows, :] = gy.astype(BF)
            total += jnp.sum(gy, 0, keepdims=True)
        small_ref[:, 0:1] = by_shard(total)
        gyt_ref[...] = gy_ref[...].T
        sect_ref[...] = second_ref[...].T
        acc_ref[...] = jnp.zeros_like(acc_ref)
        weights.wait()

    ghb_ref[0] = jnp.zeros_like(ghb_ref[0])

    def block(b, carry):
        parts = [pl.ds(pl.multiple_of(b * BLK + n * SUB_BWD, SUB_BWD), SUB_BWD) for n in range(BLK // SUB_BWD)]
        slopes = [dot_nt(gy_ref[rows, :], wm_ref[1, c]) for rows in parts]
        pres = []
        for rows, value in zip(parts, slopes):
            gp = value * slope_ref[0, rows, :].astype(F32)
            total = jnp.sum(gp, 0, keepdims=True)
            for n in range(4):
                ghb_ref[0, n : n + 1, :] += total[:, n * GL : (n + 1) * GL]
            gp = gp.astype(BF)
            gp_ref[rows, :] = gp
            pres.append(gp)
        outs = [dot_nt(gp, wm_ref[0, c]) for gp in pres]
        for rows, out in zip(parts, outs):
            acc_ref[rows, :] += out
        return carry

    lax.fori_loop(0, rows_total // BLK, block, 0)
    place = where_in_plane(rolled)
    value_ref[0] = dot_nn(sect_ref[...], gp_ref[...]).astype(BF)
    value_ref[1] = dot_nn(gyt_ref[...], act_ref[0]).astype(BF)
    scatter_rows(place, value_ref.at[0], ghw_ref, ghw_away_ref, 0)
    scatter_rows(place, value_ref.at[1], gow_ref, gow_away_ref, 0)

    @pl.when(c == pl.num_programs(0) - 1)
    def _():
        for call in planned(tasks, LATE):
            call()
        e = acc_ref[...]
        normed, inverse = normalize(mid_ref[...])
        small_ref[:, 2:3] = by_shard(jnp.sum(e * normed, 0, keepdims=True))
        small_ref[:, 3:4] = by_shard(jnp.sum(e, 0, keepdims=True))
        gmid = gy_ref[...].astype(F32) + norm_back(e, normed, inverse, along_model(table_ref, layer, MGAIN, rolled))
        small_ref[:, 1:2] = by_shard(jnp.sum(gmid, 0, keepdims=True))
        gmid_ref[...] = gmid

    step_end(tasks, 4)


PIECES = jax.ShapeDtypeStruct((4, 4, CHUNK, D), BF)


def mlp_bwd(layer, rolled, counts, g, act, slope, second, mid, table, weights, tasks=(), collective_id=None):
    r = mid.shape[0]
    pieces = pl.BlockSpec((4, 1, CHUNK, D), lambda i: (0, i, 0, 0))
    return carried_call(
        functools.partial(mlp_bwd_body, layer, rolled, weights, tasks),
        [weights, *tasks],
        collective_id,
        grid=(4,),
        in_specs=[SMEM, whole(g.shape), per((r, D)), per((r, D)), whole((r, D)), whole((r, D)), whole(table.shape)],
        inputs=(counts, g, act, slope, second, mid, table),
        out_specs=[pieces, pieces, pieces, pieces, per((4, GL)), whole((r, D)), whole((4, 4, GL))],
        out_shape=[
            PIECES, PIECES, PIECES, PIECES,
            jax.ShapeDtypeStruct((4, 4, GL), F32),
            jax.ShapeDtypeStruct((r, D), F32),
            jax.ShapeDtypeStruct((4, 4, GL), F32),
        ],
        scratch_shapes=[
            pltpu.VMEM((r, D), BF), pltpu.VMEM((D, r), BF), pltpu.VMEM((D, r), BF), pltpu.VMEM((r, D), BF),
            pltpu.VMEM((r, D), F32), pltpu.VMEM((2, D, D), BF),
        ],
        name="mlp_bwd",
        cost=pl.CostEstimate(flops=8 * r * D * 2048, bytes_accessed=16 << 20, transcendentals=0),
    )


def attn_bwd_body(
    layer, rolled, weights, tasks, x_ref, gmid_ref, fw_ref, qkv_ref, p_ref, ho_ref, table_ref,
    gin_ref, out_ref, ga_ref, ga_away_ref, gqv_ref, gtab_ref, small_ref,
    gw_ref, dq_ref, fwt_ref, hos_ref, gms_ref, value_ref, spread_ref, gather_ref, mask_ref, gain_ref,
):
    i = pl.program_id(0)
    last = pl.num_programs(0) - 1
    begin(weights, tasks)
    wq_ref, wpt_ref = weights.kept[:2]

    @pl.when(i == 0)
    def _():
        gqv_ref[...] = jnp.zeros_like(gqv_ref)
        gtab_ref[...] = jnp.zeros_like(gtab_ref)
        small_ref[...] = jnp.zeros_like(small_ref)
        spread_ref[...] = spread_map(layer * SHIFT)
        gather_ref[...] = gather_map(layer * SHIFT)
        mask_ref[...] = head_mask()
        gain_ref[...] = along_model(table_ref, layer, GAIN, rolled)

    gmid = gmid_ref[0]
    gmb = gmid.astype(BF)
    image = pl.ds(pl.multiple_of(i * TP, 16), TP)
    gms_ref[image, :] = gmb
    hos_ref[image, :] = ho_ref[0]
    base = pl.multiple_of(i * ROWS, ROWS)
    fwt_ref[:, pl.ds(base, ROWS)] = fw_ref[0].T

    @pl.when(i == 0)
    def _():
        weights.wait()

    heads = dot_nn(gmb, wpt_ref[...]).astype(BF)
    gw_ref[...] = dot_nn(spread_ref[...], heads).astype(BF)
    scale = HD ** (-0.5)

    def windows(n, carry):
        chains = [(n * AT_ONCE + w, g) for w in range(AT_ONCE) for g in range(4)]
        mask = mask_ref[...]

        def rows(w):
            return pl.ds(pl.multiple_of(w * WP, WP), WP)

        def part(w, g, n):
            return qkv_ref[0, rows(w), (3 * g + n) * GL : (3 * g + n + 1) * GL]

        bd_grads = [block_diagonal(gw_ref[rows(w), g * GL : (g + 1) * GL], mask) for w, g in chains]
        terms = [dot_nt(part(w, g, 2), bd_grad) for (w, g), bd_grad in zip(chains, bd_grads)]
        dvs = [dot_nn(p_ref[0, w, g], bd_grad) for (w, g), bd_grad in zip(chains, bd_grads)]
        scores = []
        for (w, g), term in zip(chains, terms):
            ptf = p_ref[0, w, g].astype(F32)
            pd = term * ptf
            ds = pd - ptf * jnp.sum(pd, 0, keepdims=True)
            gtab_ref[g] += ds
            scores.append(ds.astype(BF))
        dks = [dot_nn(ds, block_diagonal(part(w, g, 0), mask)) for (w, g), ds in zip(chains, scores)]
        dqs = [dot_tn(ds, part(w, g, 1)) for (w, g), ds in zip(chains, scores)]
        for (w, g), full, dk, dv in zip(chains, dqs, dks, dvs):
            dq = pick_diagonal(full) * scale
            out_rows = pl.ds(pl.multiple_of(base + w * WP, WP), WP)
            gqv_ref[g, 0:1] += jnp.sum(dq, 0, keepdims=True)
            gqv_ref[g, 1:2] += jnp.sum(dv, 0, keepdims=True)
            for n, value in enumerate((dq, dk, dv)):
                dq_ref[out_rows, (3 * g + n) * GL : (3 * g + n + 1) * GL] = value.astype(BF)
        return carry

    lax.fori_loop(0, NW // AT_ONCE, windows, 0)
    image_rows = pl.ds(base, ROWS)
    e = dot_nt(dq_ref[image_rows, :], wq_ref[...])
    e = dot_nn(gather_ref[...], e.astype(BF))
    normed, inverse = normalize(x_ref[0].astype(F32))
    small_ref[:, 0:1] += by_shard(jnp.sum(e * normed, 0, keepdims=True))
    small_ref[:, 1:2] += by_shard(jnp.sum(e, 0, keepdims=True))
    gin = (gmid + norm_back(e, normed, inverse, gain_ref[...])).astype(BF)
    gin_ref[0] = gin
    out_ref[0] = gin[:TOK]

    @pl.when(i == last)
    def _():
        for call in planned(tasks, LATE):
            call()

        def chunk(n, carry):
            lanes = pl.ds(pl.multiple_of(n * D, D), D)
            value_ref[:, lanes] = dot_nn(fwt_ref[...], dq_ref[:, lanes]).astype(BF)
            return carry

        lax.fori_loop(0, 3, chunk, 0)
        value_ref[:, 3 * D :] = dot_nn(gms_ref[...].T, hos_ref[...]).astype(BF)
        core, dp = where_in_plane(rolled)
        for half, group_ref in enumerate((ga_ref, ga_away_ref)):
            for n, j in enumerate(PLACES):
                rows = pl.ds(pl.multiple_of((core ^ half) * 256 + (dp ^ j) * CHUNK, CHUNK), CHUNK)
                for g in range(4):
                    group_ref[n, g, :, : 3 * GL] = value_ref[rows, 3 * GL * g : 3 * GL * (g + 1)]
                    group_ref[n, g, :, 3 * GL :] = value_ref[rows, 3 * D + GL * g : 3 * D + GL * (g + 1)]

    step_end(tasks, 4)


def attn_bwd(layer, rolled, x, gmid, fw, qkv, p, ho, table, weights, tasks=(), collective_id=None):
    n = x.shape[0]
    return carried_call(
        functools.partial(attn_bwd_body, layer, rolled, weights, tasks),
        [weights, *tasks],
        collective_id,
        grid=(n,),
        in_specs=[
            per(x.shape[1:]), per((TP, D)), per((ROWS, D)), per((ROWS, 3 * D)), per((NW, 4, WP, GH * WP)), per((TP, D)),
            whole(table.shape),
        ],
        inputs=(x, gmid, fw, qkv, p, ho, table),
        out_specs=[
            per((TP, D)), per((TOK, D)), whole(PIECES.shape), whole(PIECES.shape), whole((4, 2, GL)), whole((4, WP, GH * WP)),
            whole((4, 2, GL)),
        ],
        out_shape=[
            jax.ShapeDtypeStruct((n, TP, D), BF),
            jax.ShapeDtypeStruct((n, TOK, D), BF),
            PIECES, PIECES,
            jax.ShapeDtypeStruct((4, 2, GL), F32),
            jax.ShapeDtypeStruct((4, WP, GH * WP), F32),
            jax.ShapeDtypeStruct((4, 2, GL), F32),
        ],
        scratch_shapes=[
            pltpu.VMEM((ROWS, D), BF), pltpu.VMEM((n * ROWS, 3 * D), BF), pltpu.VMEM((D, n * ROWS), BF),
            pltpu.VMEM((n * TP, D), BF), pltpu.VMEM((n * TP, D), BF), pltpu.VMEM((D, 4 * D), BF),
            pltpu.VMEM((ROWS, TP), BF), pltpu.VMEM((TP, ROWS), BF), pltpu.VMEM((GH * WP, GL), BF), pltpu.VMEM((1, D), F32),
        ],
        name="attn_bwd",
        cost=pl.CostEstimate(flops=n * 4 * 256 * 512 * 2600, bytes_accessed=n * 3 << 20, transcendentals=0),
    )


def plain_call(body, name, inputs, out_shape, scratch_shapes=(), grid=(), in_specs=None, out_specs=None, bytes_accessed=4 << 20):
    return pl.pallas_call(
        body,
        grid=grid,
        out_shape=out_shape,
        in_specs=in_specs or [pl.BlockSpec(memory_space=pltpu.VMEM)] * len(inputs),
        out_specs=out_specs or jax.tree.map(lambda _: pl.BlockSpec(memory_space=pltpu.VMEM), out_shape),
        scratch_shapes=list(scratch_shapes),
        name=name,
        compiler_params=pltpu.CompilerParams(vmem_limit_bytes=VMEM_LIMIT),
        cost_estimate=pl.CostEstimate(flops=bytes_accessed, bytes_accessed=bytes_accessed, transcendentals=0),
    )(*inputs)


def prepare_body(index, wqkv, wproj, gain, shift, qv, table, bproj, mgain, mshift, hb, ob, own_a_ref, lines_ref, index_ref, rows_ref, keys_ref):
    own_a_ref[:, : 3 * GL] = dot_nn(wqkv[...], permutation(3 * GL, qkv_source, False)).astype(BF)
    own_a_ref[:, 3 * GL :] = wproj[...].T
    rows_ref[...] = jnp.zeros_like(rows_ref)
    for row, ref in ((GAIN, gain), (SHIFT_ROW, shift), (BPROJ, bproj), (MGAIN, mgain), (MSHIFT, mshift), (OB, ob)):
        rows_ref[row : row + 1, :] = ref[...].astype(F32)
    terms = dot_nn(jnp.broadcast_to(qv[...], (16, 2 * GL)), permutation(2 * GL, qv_source, False))
    hidden, places = hb[...].astype(F32), table[...].astype(F32)
    for n in range(2):
        rows_ref[QV + n : QV + n + 1, :] = terms[0:1, n * GL : (n + 1) * GL]
    for n in range(4):
        rows_ref[HB + n : HB + n + 1, :] = hidden[:, n * GL : (n + 1) * GL]
    rows_ref[TABLE : TABLE + 4, :] = places[:, :GL]
    rows_ref[TABLE + 4 : TABLE + 8, 0 : RELS - GL] = places[:, GL:]
    lines_ref[...] = rows_ref[...].astype(BF)
    keys_ref[...] = jnp.full((GL, GL), -1.0, F32)
    keys_ref[0:POS, 0:POS] = index[...].astype(F32)
    keys_ref[...] = keys_ref[...].T
    pair = [keys_ref[pl.ds(odd, WP // 2, 2), :][:, :WP] for odd in range(2)]
    index_ref[...] = jnp.concatenate(pair, 1).astype(jnp.int32)


def prepare(rel_index, wqkv, wproj, *small):
    return plain_call(
        prepare_body, "prepare", (rel_index, wqkv, wproj, *small),
        [
            jax.ShapeDtypeStruct((D, D), BF), jax.ShapeDtypeStruct((LINES, GL), BF),
            jax.ShapeDtypeStruct((WP // 2, GL), jnp.int32),
        ],
        [pltpu.VMEM((LINES, GL), F32), pltpu.VMEM((GL, GL), F32)],
    )


class Exchange(Part):
    def __init__(self, own, lines):
        shapes = [jax.ShapeDtypeStruct(part.shape, part.dtype) for part in own]
        shapes.append(jax.ShapeDtypeStruct((4, 2) + lines.shape, lines.dtype))
        super().__init__([*own, lines], shapes, sems(4) + sems(3) + [pltpu.SemaphoreType.DMA(())])

    def swap(self, n):
        core, _, _ = place_in_mesh()
        target = self.outs[n] if n < 3 else self.outs[3].at[0, core]
        return remote(self.ins[n], target, [sem.at[n] for sem in self.kept[:2]], "pipe", 1 - core)

    def keep(self):
        core, _, _ = place_in_mesh()
        return pltpu.make_async_copy(self.ins[3], self.outs[3].at[0, core], self.kept[4])

    def spread(self, k):
        _, _, shard = place_in_mesh()
        table = self.outs[3]
        return remote(table.at[0], table.at[k], [sem.at[k - 1] for sem in self.kept[2:4]], "tensor", lax.rem(shard + 4 - k, 4))


def gather_start(own, lines, index, view):
    exchange = Exchange(own, lines)
    near_a, near_h, near_o, far_a, bias = Near(0, None, None), Near(0, None, None), Near(0, None, None), Far(None), Bias(index)
    pick = Own(view)

    def body():
        for n, task in enumerate((near_a, near_h, near_o)):
            task.ins = [exchange.ins[n], exchange.outs[n]]
        far_a.ins = [near_a.outs[0]]
        greet()
        for n in (0, 3, 1, 2):
            exchange.swap(n).start()
        exchange.keep().start()
        pick.start()
        exchange.swap(0).wait()
        near_a.start()
        exchange.keep().wait()
        exchange.swap(3).wait()
        for k in (1, 2, 3):
            exchange.spread(k).start()
        pick.pick()
        near_a.end()
        far_a.start()
        exchange.swap(1).wait()
        near_h.start()
        for k in (1, 2, 3):
            exchange.spread(k).wait()
        bias.build(exchange.outs[3])
        far_a.turn()
        exchange.swap(2).wait()
        near_o.start()
        far_a.rest()
        far_a.last()
        far_a.end()
        bias.end()
        pick.end()
        near_h.end()
        near_o.end()

    parts = [exchange, near_a, near_h, near_o, far_a, bias, pick]
    _, given = carried_call(
        body, parts, 0, grid=(), in_specs=[], inputs=(), out_specs=[], out_shape=[], scratch_shapes=[],
        name="gather_start", cost=pl.CostEstimate(flops=1 << 24, bytes_accessed=8 << 20, transcendentals=0),
    )
    others, given_a, given_h, given_o, far, *rest = given
    return others[:3], others[3], [given_a[0], *far], given_h[0], given_o[0], *[part[0] for part in rest]


def turned_index(rel_index):
    return jnp.pad(rel_index.T, ((0, WP - POS), (0, WP - POS)), constant_values=-1)


def places_of(pairs):
    return (iota((2 * GL, pairs.shape[1]), 0) == pairs).astype(F32).astype(BF)


class Own(Part):
    def __init__(self, view, plan=()):
        count = view.shape[0]
        self.count, self.plan = count, plan
        super().__init__(
            [view], [jax.ShapeDtypeStruct((count, TP, D), BF)],
            [pltpu.VMEM(view.shape, BF), pltpu.VMEM((count, TP, D), BF), pltpu.SemaphoreType.DMA((2,))],
        )

    def load(self):
        return pltpu.make_async_copy(self.ins[0], self.kept[0], self.kept[2].at[0])

    def out(self):
        return pltpu.make_async_copy(self.kept[1], self.outs[0], self.kept[2].at[1])

    def start(self):
        self.load().start()

    def pick(self):
        self.load().wait()
        first_core = lax.axis_index("pipe") == 0

        def image(m, carry):
            both = self.kept[0][m]
            self.kept[1][m] = jnp.zeros((TP, D), BF)
            self.kept[1][m, 0:TOK, :] = jnp.where(first_core, both[:, 0, :], both[:, 1, :])
            return carry

        lax.fori_loop(0, self.count, image, 0)
        self.out().start()

    def end(self):
        self.out().wait()


class Bias(Part):
    def __init__(self, index):
        super().__init__(
            [index], [jax.ShapeDtypeStruct((2, 4, WP, GH * WP), F32)],
            [pltpu.VMEM((4, 2, LINES, GL), BF), pltpu.VMEM((WP // 2, GL), jnp.int32), pltpu.VMEM((2 * H, 2 * GL), F32),
             pltpu.VMEM((WP // 2, 2 * H, GL), F32), pltpu.VMEM((WP, GL), F32), pltpu.VMEM((2, 4, WP, GH * WP), F32),
             pltpu.SemaphoreType.DMA((3,))],
        )

    def loads(self, table):
        return [pltpu.make_async_copy(table, self.kept[0], self.kept[6].at[0]), self.index()]

    def index(self):
        return pltpu.make_async_copy(self.ins[0], self.kept[1], self.kept[6].at[1])

    def out(self):
        return pltpu.make_async_copy(self.kept[5], self.outs[0], self.kept[6].at[2])

    def build(self, table):
        lines, index, rows, pairs, half, whole_ref, _ = self.kept
        for copy in self.loads(table):
            copy.start()
        for copy in self.loads(table):
            copy.wait()
        for l in range(2):
            for k in range(4):
                values = lines[k, l].astype(F32)
                at = l * H + k * GH
                rows[at : at + GH, :GL] = values[TABLE : TABLE + GH]
                rows[at : at + GH, GL:] = values[TABLE + GH : TABLE + 2 * GH]
        tables = rows[...].astype(BF)

        def product(n, carry):
            pairs[n] = dot_nn(tables, places_of(index[pl.ds(n, 1), :]))
            return carry

        lax.fori_loop(0, WP // 2, product, 0)
        shut = jnp.where(iota((WP, GL), 0) < POS, 0.0, SHUT).astype(F32)
        for l in range(2):
            for g in range(4):
                for n in range(2):
                    heads = [pairs[:, l * H + g * GH + 2 * n + m, :] for m in range(2)]
                    for odd in range(2):
                        lanes = slice(odd * WP, (odd + 1) * WP)
                        half[pl.ds(odd, WP // 2, 2), :] = jnp.concatenate([head[:, lanes] for head in heads], 1)
                    whole_ref[l, g, :, n * GL : (n + 1) * GL] = half[...] + shut
        self.out().start()

    def end(self):
        self.out().wait()


def bias_tables(table, rel_index):
    rows = table[:, :, TABLE : TABLE + 8].reshape(4, 2, 2, GH, GL).transpose(1, 0, 3, 2, 4).reshape(2 * H, 2 * GL)
    onehot = (jnp.arange(2 * GL, dtype=jnp.int32)[:, None] == turned_index(rel_index).reshape(1, -1)).astype(BF)
    flat = jnp.dot(rows, onehot, preferred_element_type=F32)
    position = flat.reshape(2, 4, GH, WP, WP).transpose(0, 1, 3, 2, 4)
    shut = jnp.where(jnp.arange(WP) < POS, 0.0, SHUT).astype(F32)[:, None, None]
    return (position + shut).reshape(2, 4, WP, GH * WP)


def table_grad(gtab, rel_index):
    rel = jnp.pad(rel_index.T, ((0, WP - POS), (0, WP - POS)), constant_values=-1).reshape(-1)
    onehot = (rel[:, None] == jnp.arange(RELS, dtype=jnp.int32)[None, :]).astype(F32)
    flat = gtab.reshape(4, WP, GH, WP).transpose(0, 2, 1, 3).reshape(H, WP * WP)
    return jnp.dot(flat, onehot, precision=lax.Precision.HIGHEST).reshape(4, GH, RELS)


class Little(Part):
    def __init__(self, rows):
        self.rows = rows
        super().__init__(
            [],
            [jax.ShapeDtypeStruct((rows, GL), F32)],
            [pltpu.VMEM((2, 4, rows, GL), F32), pltpu.VMEM((4, rows, GL), F32), pltpu.VMEM((4, rows, GL), F32),
             pltpu.VMEM((3, rows, GL), F32)]
            + sems() + sems(3) + sems(3) + [pltpu.SemaphoreType.DMA(())],
        )

    def pack(self, layers, tabs):
        _, _, shard = place_in_mesh()
        sums = self.kept[0]
        sums[...] = jnp.zeros_like(sums)
        for layer, (ghb, small_m, gqv, _, small_a) in enumerate(layers):
            for k in range(4):
                z = lax.rem(shard + k, 4)
                for row, source, n in (
                    (GAIN, small_a, 0), (SHIFT_ROW, small_a, 1), (OB, small_m, 0), (BPROJ, small_m, 1), (MGAIN, small_m, 2),
                    (MSHIFT, small_m, 3),
                ):
                    sums[layer, k, row : row + 1, :] = source[z, n : n + 1, :]
                sums[layer, k, QV : QV + 2, :] = gqv[k]
                sums[layer, k, HB : HB + 4, :] = ghb[k]
                rows = tabs[layer][GH * k : GH * (k + 1)]
                sums[layer, k, TABLE : TABLE + 4, :] = rows[:, 0:GL]
                sums[layer, k, TABLE + 4 : TABLE + 8, :] = rows[:, GL:]

    def over(self):
        core, _, _ = place_in_mesh()
        return remote(self.kept[0].at[1 - core], self.kept[1], self.kept[4:6], "pipe", 1 - core)

    def across(self, j):
        _, dp, _ = place_in_mesh()
        return remote(self.kept[2].at[0], self.kept[2].at[j], [sem.at[j - 1] for sem in self.kept[6:8]], "dp", dp ^ j)

    def along(self, k):
        _, _, shard = place_in_mesh()
        return remote(
            self.kept[1].at[k], self.kept[3].at[k - 1], [sem.at[k - 1] for sem in self.kept[8:10]], "tensor", lax.rem(shard + k, 4)
        )

    def start(self):
        self.over().start()

    def second(self):
        core, _, _ = place_in_mesh()
        self.over().wait()
        self.kept[1][...] += self.kept[0][core]
        for k in (1, 2, 3):
            self.along(k).start()

    def third(self):
        for k in (1, 2, 3):
            self.along(k).wait()
        self.kept[2][0] = self.kept[1][0] + self.kept[3][0] + self.kept[3][1] + self.kept[3][2]
        for j in (1, 2, 3):
            self.across(j).start()

    def fourth(self):
        for j in (1, 2, 3):
            self.across(j).wait()
        total = self.kept[2]
        self.kept[1][0] = total[0] + total[1] + total[2] + total[3]
        self.out().start()

    def out(self):
        return pltpu.make_async_copy(self.kept[1].at[0], self.outs[0], self.kept[10])

    def end(self):
        self.out().wait()


class Settle(Part):
    def __init__(self):
        super().__init__(
            [],
            [jax.ShapeDtypeStruct((3, D, D), BF)],
            [pltpu.VMEM((3, D, D), BF)] + sems(3) + [pltpu.SemaphoreType.DMA((3,)), pltpu.SemaphoreType.DMA((3,))],
        )

    def rows(self, core):
        return pl.ds(core * 256, 256)

    def send(self, source, n, core):
        return remote(source.at[self.rows(core)], self.outs[0].at[n, self.rows(core)], [sem.at[n] for sem in self.kept[1:3]], "pipe", 1 - core)

    def load(self, source, n, core):
        return pltpu.make_async_copy(source.at[self.rows(core)], self.kept[0].at[n, self.rows(core)], self.kept[3].at[n])

    def store(self, n, core):
        return pltpu.make_async_copy(self.kept[0].at[n, self.rows(core)], self.outs[0].at[n, self.rows(core)], self.kept[4].at[n])

    def start(self, matrices, layer, which):
        def action(core):
            for n in which:
                (self.load if core == layer else self.send)(matrices[n], n, core).start()

        by_core(action)

    def straight(self, matrix, n, layer):
        def action(core):
            if core == layer:
                rows = self.rows(core)
                pltpu.make_async_copy(matrix.at[rows], self.outs[0].at[n, rows], self.kept[4].at[n]).start()
            else:
                self.send(matrix, n, core).start()

        by_core(action)

    def pass_on(self, matrices, layer, which):
        @pl.when(lax.axis_index("pipe") == layer)
        def _():
            for n in which:
                self.load(matrices[n], n, layer).wait()
                self.store(n, layer).start()

    def end(self, matrices):
        def action(core):
            for n in range(3):
                self.store(n, core).wait()
                self.send(matrices[1 - core][n], n, core).wait()

        by_core(action)


def table_sums(gtab_ref, index_ref, half_ref, pairs_ref, out_ref):
    for g in range(4):
        for n in range(2):
            half_ref[...] = gtab_ref[g, :, n * GL : (n + 1) * GL]
            even = half_ref[pl.ds(0, WP // 2, 2), :]
            odd = half_ref[pl.ds(1, WP // 2, 2), :]
            for m in range(2):
                lanes = slice(m * WP, (m + 1) * WP)
                pairs_ref[:, g * GH + 2 * n + m, :] = jnp.concatenate([even[:, lanes], odd[:, lanes]], 1)

    def add(n, total):
        pair = pairs_ref[n]
        high = pair.astype(BF)
        low = (pair - high.astype(F32)).astype(BF)
        places = places_of(index_ref[pl.ds(n, 1), :])
        return total + (dot_nt(high, places) + dot_nt(low, places))

    out_ref[...] = lax.fori_loop(0, WP // 2, add, jnp.zeros((H, 2 * GL), F32))


def reduce_end(attention0, totals_h0, turned_o0, pieces1, shared_h1, grads_in, small, index):
    halves = ((0, 32), (32, 32))
    first = [ReduceFirst(attention0, rows=rows) for rows in halves]
    second = [ReduceSecond(size=32) for _ in halves]
    share = [Share(rows=halves[0], in_vmem=True)]
    share.append(Share(rows=halves[1], target=share[0]))
    onward_o = ReduceOnward(turned_o0)
    second_m, share_m = [ReduceSecond(totals_h0), ReduceSecond()], [Share(), Share()]
    share_a1, share_o1, done_h1 = Share(pieces1[0]), Share(pieces1[1]), Part([shared_h1])
    settle, little, places = Settle(), Little(24), Stored(index)
    input_grad = Weave(grads_in)

    def body(*refs):
        layers, (tabs_ref, pairs_ref, half_ref) = (refs[:5], refs[5:10]), refs[10:]
        for n in range(2):
            second[n].ins, share[n].ins, share_m[n].ins = [first[n].total], [second[n].kept[0]], [second_m[n].kept[0]]
        second_m[1].ins = [onward_o.kept[0]]
        done = (
            [share[0].whole(), share_m[0].outs[0], share_m[1].outs[0]],
            [share_a1.outs[0], done_h1.ins[0], share_o1.outs[0]],
        )

        def tab(layer):
            table_sums(layers[layer][3], places.kept[0], half_ref, pairs_ref, tabs_ref.at[layer])

        greet()
        for task in (*first, onward_o, second_m[0]):
            task.start()
        places.load()
        places.wait()
        tab(1)
        first[0].cores()
        first[1].cores()
        share_o1.start()
        settle.start(done[1], 1, (1,))
        input_grad.start()
        tab(0)
        little.pack(layers, tabs_ref)
        little.start()
        onward_o.close()
        second_m[1].start()
        second_m[0].close()
        share_m[0].start()
        first[0].turn()
        little.second()
        first[1].turn()
        share_a1.start()
        settle.pass_on(done[1], 1, (1,))
        first[0].close()
        second[0].start()
        first[1].close()
        second[1].start()
        little.third()
        second_m[1].close()
        share_m[1].start()
        input_grad.wait()
        input_grad.weave(0, 2)
        for task in (share_m[0], share_a1, share_o1):
            task.end()
            task.flush()
        settle.start(done[1], 1, (0, 2))
        settle.start(done[0], 0, (1,))
        for n in range(2):
            second[n].close()
            share[n].start()
        input_grad.weave(2, 4)
        little.fourth()
        settle.pass_on(done[1], 1, (0, 2))
        settle.pass_on(done[0], 0, (1,))
        share_m[1].end()
        share_m[1].flush()
        settle.start(done[0], 0, (2,))
        settle.pass_on(done[0], 0, (2,))
        for task in share:
            task.end()
        for task in share:
            task.flush()
        settle.straight(done[0][0], 0, 0)
        little.end()
        input_grad.end()
        settle.end(done)

    parts = [
        *first, *second, *share, onward_o, *second_m, *share_m, share_a1, share_o1, done_h1, settle, little, input_grad, places
    ]
    _, given = carried_call(
        body, parts, 7, grid=(), in_specs=[pl.BlockSpec(memory_space=pltpu.VMEM)] * 10, inputs=small, out_specs=[], out_shape=[],
        scratch_shapes=[pltpu.VMEM((2, H, 2 * GL), F32), pltpu.VMEM((WP // 2, H, GL), F32), pltpu.VMEM((WP, GL), F32)],
        name="reduce_end", cost=pl.CostEstimate(flops=1 << 24, bytes_accessed=8 << 20, transcendentals=0),
    )
    by_part = dict(zip(map(id, parts), given))
    return by_part[id(settle)][0], by_part[id(little)][0], by_part[id(input_grad)][0]


def finish_body(
    matrix_ref, lines_ref, gqkv_ref, gproj_ref, ghw_ref, gow_ref, gain_ref, shift_ref, qv_ref, table_ref, bproj_ref, mgain_ref,
    mshift_ref, hb_ref, ob_ref,
):
    gqkv_ref[0] = dot_nn(matrix_ref[0, :, : 3 * GL], permutation(3 * GL, qkv_source, True))
    gproj_ref[0] = matrix_ref[0, :, 3 * GL :].T.astype(F32)
    ghw_ref[0] = matrix_ref[1].astype(F32)
    gow_ref[0] = matrix_ref[2].T.astype(F32)
    lines = lines_ref[...]
    for row, ref in (
        (GAIN, gain_ref), (SHIFT_ROW, shift_ref), (BPROJ, bproj_ref), (MGAIN, mgain_ref), (MSHIFT, mshift_ref), (OB, ob_ref)
    ):
        ref[...] = lines[row : row + 1]
    qv_ref[...] = jnp.concatenate([lines[QV + n : QV + n + 1, h * HD : (h + 1) * HD] for h in range(GH) for n in range(2)], 1)
    table_ref[0] = jnp.concatenate([lines[TABLE : TABLE + 4], lines[TABLE + 4 : TABLE + 8, : RELS - GL]], 1)
    hb_ref[...] = jnp.concatenate([lines[HB + n : HB + n + 1] for n in range(4)], 1)


def finish(matrices, lines):
    shapes = [
        (1, D, 3 * GL), (1, GL, D), (1, D, D), (1, D, D), (1, GL), (1, GL), (1, 2 * GL), (1, GH, RELS), (1, GL), (1, GL), (1, GL),
        (1, D), (1, GL),
    ]
    return plain_call(finish_body, "finish", (matrices, lines), [jax.ShapeDtypeStruct(shape, F32) for shape in shapes])


def layer_forward(layer, rolled, x, counts, table, bias, weights, tasks, ids):
    (fw, qkv, p, ho, mid), given = attn_fwd(layer, rolled, x, table, bias, weights[0](), tasks[0](), ids[0])
    mid = mid.reshape(-1, D)
    kept_a, given = given[0], given[1:]
    (second, act, slope, y, out), more = mlp_fwd(layer, rolled, counts, mid, table, weights[1](given), tasks[1](given), ids[1])
    return y, out, (x, fw, qkv, p, ho, mid, second, act, slope, kept_a, more[0]), given, more[1:]


def layer_backward(layer, rolled, cot, kept, counts, table, tasks, ids):
    x, fw, qkv, p, ho, mid, second, act, slope, kept_a, kept_m = kept
    (ghw, ghw_away, gow, gow_away, ghb, gmid, small_m), given = mlp_bwd(
        layer, rolled, counts, cot, act, slope, second, mid, table, Stored(*kept_m), tasks[0](), ids[0]
    )
    big_m = ((ghw, ghw_away), (gow, gow_away))
    (gin, out, ga, ga_away, gqv, gtab, small_a), more = attn_bwd(
        layer, rolled, x, gmid.reshape(-1, TP, D), fw, qkv, p, ho, table, Stored(*kept_a), tasks[1](big_m, given), ids[1]
    )
    return gin, out, ((ga, ga_away), *big_m), (ghb, small_m, gqv, gtab, small_a), given, more


SMALL_ROWS = ((GAIN, 1), (SHIFT_ROW, 1), (QV, 2), (TABLE, 8), (BPROJ, 1), (MGAIN, 1), (MSHIFT, 1), (HB, 4), (OB, 1))


def on_lines(small_in):
    whole_of = [lax.all_gather(lax.all_gather(member[0], "tensor", axis=0, tiled=True), "pipe") for member in small_in]
    gain, shift, qv, table, bproj, mgain, mshift, hb, ob = whole_of

    def lines(member):
        return member.reshape(2, 4, -1, GL)

    qv = qv.reshape(2, 4, GH, 2, HD).transpose(0, 1, 3, 2, 4)
    table = jnp.pad(table, ((0, 0), (0, 0), (0, 2 * GL - RELS))).reshape(2, 4, GH, 2, GL).transpose(0, 1, 3, 2, 4)
    rows = jnp.concatenate([lines(part) for part in (gain, shift, qv, table, bproj, mgain, mshift, hb, ob)], 2)
    return jnp.pad(rows, ((0, 0), (0, 0), (0, LINES - rows.shape[2]), (0, 0))).transpose(1, 0, 2, 3)


def qkv_order(w):
    lead = w.shape[:-1]
    return jnp.swapaxes(w.reshape(*lead, GH, 3, HD), -3, -2).reshape(*lead, 3 * GL)


def general(core, images, cotangent, counts, rel_index, small_in, big_in):
    def both(member, axis):
        return lax.all_gather(lax.all_gather(member[0], "tensor", axis=axis, tiled=True), "pipe")

    table = on_lines(small_in)
    bias = bias_tables(table, rel_index)
    gathered = [both(member, axis) for member, axis in zip(big_in, (1, 0, 1, 0))]
    weights = []
    for l in range(2):
        wqkv, wproj, hw, ow = (pair[l] for pair in gathered)
        wqkv = qkv_order(wqkv.reshape(D, 4, 3 * GL).transpose(1, 0, 2))
        wa = jnp.concatenate([wqkv, wproj.reshape(4, GL, D).transpose(0, 2, 1)], 2)[None]
        wm = jnp.stack([hw.reshape(D, 4, -1).transpose(1, 0, 2), ow.reshape(4, -1, D)])
        weights.append((lambda *_, wa=wa: Weights(1, 0, whole=wa), lambda *_, wm=wm: Weights(2, 0, whole=wm)))
    none, back_none, ids = (lambda: [], lambda given: []), (lambda: [], lambda *_: []), (None, None)
    images, cotangent = (
        jnp.pad(lax.dynamic_index_in_dim(array, core, 1, False), ((0, 0), (0, TP - TOK), (0, 0))) for array in (images, cotangent)
    )
    y0, out0, kept0, _, _ = layer_forward(0, False, images, counts, table, bias, weights[0], none, ids)
    _, out1, kept1, _, _ = layer_forward(1, False, y0, counts, table, bias, weights[1], none, ids)
    g1, gin1, big1, small1, _, _ = layer_backward(1, False, cotangent, kept1, counts, table, back_none, ids)
    _, gin0, big0, small0, _, _ = layer_backward(0, False, g1, kept0, counts, table, back_none, ids)
    first_core = core == 0

    def deliver(mine0, mine1):
        came = lax.ppermute(jnp.where(first_core, mine1, mine0), "pipe", [(0, 1), (1, 0)])
        mine = jnp.where(first_core, mine0, mine1)
        return jnp.stack([jnp.where(first_core, mine, came), jnp.where(first_core, came, mine)], 1)[None]

    def matrix_of(pair):
        parts = [part[jnp.array([PLACES.index(j) for j in range(4)])] for part in pair]
        return jnp.concatenate(parts).transpose(1, 0, 2, 3).reshape(4, D, D)

    def full(big):
        ga, ghw, gow = (matrix_of(pair) for pair in big)
        gqkv = jnp.swapaxes(ga[:, :, : 3 * GL].reshape(4, D, 3, GH, HD), 2, 3).reshape(4, D, 3 * GL)
        return (
            gqkv.transpose(1, 0, 2).reshape(D, 3 * D), ga[:, :, 3 * GL :].transpose(0, 2, 1).reshape(D, D),
            ghw.transpose(1, 0, 2).reshape(D, -1), gow.transpose(0, 2, 1).reshape(-1, D),
        )

    def reduced(pair, axis):
        mine = lax.psum_scatter(jnp.stack(pair), "pipe", scatter_dimension=0, tiled=False)
        mine = lax.psum_scatter(mine, "tensor", scatter_dimension=axis, tiled=True)
        return lax.psum(mine, "dp").astype(F32)[None]

    gqkv, gproj, ghw, gow = (reduced(pair, axis) for pair, axis in zip(zip(full(big0), full(big1)), (1, 0, 1, 0)))

    def vectors(terms):
        ghb, small_m, gqv, gtab, small_a = terms
        qv = jnp.swapaxes(gqv.reshape(4, 2, GH, HD), 1, 2).reshape(-1)
        tab = table_grad(gtab, rel_index).reshape(H, RELS)
        parts = (small_a[:, 0], small_a[:, 1], qv, tab, small_m[:, 1], small_m[:, 2], small_m[:, 3], ghb, small_m[:, 0])
        return jnp.concatenate([part.reshape(-1) for part in parts])

    totals = lax.psum(jnp.stack([vectors(small0), vectors(small1)]), ("pipe", "dp", "tensor"))
    mine = jnp.where(first_core, totals[0], totals[1])
    outs, at = [], 0
    for member in small_in:
        shape = member.shape[1:]
        whole_shape = (shape[0] * lax.axis_size("tensor"),) + tuple(shape[1:])
        size = math.prod(whole_shape)
        piece = mine[at : at + size].reshape(whole_shape)
        outs.append(lax.dynamic_slice_in_dim(piece, lax.axis_index("tensor") * shape[0], shape[0], 0)[None])
        at += size
    return deliver(out0, out1), deliver(gin0, gin1), (gqkv, gproj, ghw, gow), outs


def four_by_four(images, cotangent, counts, rel_index, small_in, big_in):
    own_a, lines, index = prepare(rel_index, big_in[0][0], big_in[1][0], *[member[0] if member.ndim == 3 else member for member in small_in])
    own = (own_a, big_in[2][0], big_in[3][0])
    other, table, pieces_a0, near_h0, near_o0, bias, x0 = gather_start(own, lines, index, jnp.swapaxes(images, 1, 2))
    pick_cot = Own(jnp.swapaxes(cotangent, 1, 2), plan=((2, "pick"),))

    def near(n, layer, **how):
        return Near(layer, own[n], other[n], **how)

    def weights(layer, which, pieces):
        return Weights(len(which), layer, own=[own[n] for n in which], other=[other[n] for n in which], pieces=pieces)

    def mlp_tasks(near_h, near_o):
        return [Far(near_h, plan=((1, "turn"), (2, "rest"), (3, "last"))), Far(near_o, plan=((2, "turn"), (3, "rest"), (3, "last")))]

    def forward_weights(layer, pieces, near_h, near_o):
        return (
            lambda: weights(layer, (0,), [pieces]),
            lambda given: weights(layer, (1, 2), [[near_h, *given[1]], [near_o, *given[2]]]),
        )

    y0, out0, kept0, given, more = layer_forward(
        0, True, x0, counts, table, bias, forward_weights(0, pieces_a0, near_h0, near_o0),
        (lambda: [*mlp_tasks(near_h0, near_o0), near(0, 1), near(1, 1, deferred=True, plan=((1, "start"),))],
         lambda given: [Far(given[3][0], plan=((1, "turn"), (2, "rest"), (3, "last"))), near(2, 1)]),
        (1, 2),
    )
    pieces_a1, near_h1, near_o1 = [given[3][0], *more[1]], given[4][0], more[2][0]
    _, out1, kept1, given, _ = layer_forward(
        1, True, y0, counts, table, bias, forward_weights(1, pieces_a1, near_h1, near_o1),
        (lambda: [*mlp_tasks(near_h1, near_o1), pick_cot], lambda given: []), (3, None),
    )
    cot = given[3][0]

    def mlp_reduce(big_m):
        return [ReduceTurn(big_m[0], plan=((0, "cores"),)), ReduceTurn(big_m[1], plan=((1, "cores"),))]

    g1, gin1, big1, small1, given, more = layer_backward(
        1, True, cot, kept1, counts, table, (lambda: [Deliver([out0, out1])], lambda big_m, given: mlp_reduce(big_m)), (4, 5)
    )
    out_came, turned1 = given[1][0], more[1:3]

    def last_tasks(big_m, given):
        onward = ReduceOnward(given[1], plan=((1, "close"),))
        second_h = ReduceSecond(given[2][0], plan=((1, "close"),))
        second_o = ReduceSecond(given[3][0], deferred=True, plan=((1, "start"),))
        second_a = ReduceSecond(source=onward, deferred=True, plan=((2, "start"),))
        share_h = Share(source=second_h, plan=((1, "start"),))
        return [
            ReduceFirst(big_m[0], plan=((0, "cores"), (LATE, "turn"))), ReduceTurn(big_m[1], plan=((1, "cores"),)), onward, second_h,
            share_h, second_o, second_a, Weave([out0, out1], out_came, plan=((3, "all"),)),
        ]

    _, gin0, big0, small0, given, more = layer_backward(
        0, True, g1, kept0, counts, table,
        (
            lambda: [ReduceTurn(big1[0], plan=((0, "cores"),)), *[ReduceOnward(turned) for turned in turned1]],
            last_tasks,
        ),
        (6, 8),
    )
    totals_h0, turned_o0, pieces1, shared_h1 = more[1][0], more[2], (more[7][0], more[6][0]), more[5][0]
    block_out = more[8][0]
    matrices, lines, input_grad = reduce_end(
        big0[0], totals_h0, turned_o0, pieces1, shared_h1, [gin0, gin1], [*small0, *small1], index
    )
    gqkv, gproj, ghw, gow, *outs = finish(matrices, lines)
    return jnp.swapaxes(block_out, 1, 2)[None], jnp.swapaxes(input_grad, 1, 2)[None], (gqkv, gproj, ghw, gow), outs


def local(
    images, cotangent, counts, rel_index, pre_attn_gain, pre_attn_bias, qkv_weight, qv_bias, bias_table, proj_weight, proj_bias,
    pre_mlp_gain, pre_mlp_bias, hidden_weight, hidden_bias, out_weight, out_bias,
):
    assert images.shape[1] == 2, images.shape
    counts = counts.T
    small_in = (pre_attn_gain, pre_attn_bias, qv_bias, bias_table, proj_bias, pre_mlp_gain, pre_mlp_bias, hidden_bias, out_bias)
    big_in = (qkv_weight, proj_weight, hidden_weight, out_weight)
    if lax.axis_size("tensor") == 4 and lax.axis_size("dp") == 4:
        block_out, input_grad, big, small = four_by_four(images, cotangent, counts, rel_index, small_in, big_in)
    else:
        block_out, input_grad, big, small = general(
            lax.axis_index("pipe"), images, cotangent, counts, rel_index, small_in, big_in
        )
    gqkv, gproj, ghw, gow = big
    gain_g, shift_g, qv_g, table_g, bproj_g, mgain_g, mshift_g, hb_g, ob_g = small
    return (
        block_out, input_grad, gain_g, shift_g, gqkv, qv_g, table_g, gproj, bproj_g, mgain_g, mshift_g, ghw, hb_g, gow, ob_g,
    )


def solution(mesh):
    return jax.shard_map(
        local,
        mesh=mesh,
        in_specs=(
            P(None, ("dp", "tensor"), None, None),
            P(None, ("dp", "tensor"), None, None),
            P(None, "dp"),
            P(),
            P("pipe", "tensor"),
            P("pipe", "tensor"),
            P("pipe", None, "tensor"),
            P("pipe", "tensor"),
            P("pipe", "tensor", None),
            P("pipe", "tensor", None),
            P("pipe", "tensor"),
            P("pipe", "tensor"),
            P("pipe", "tensor"),
            P("pipe", None, "tensor"),
            P("pipe", "tensor"),
            P("pipe", "tensor", None),
            P("pipe", "tensor"),
        ),
        out_specs=(
            P("pipe", None, ("dp", "tensor"), None, None),
            P("pipe", None, ("dp", "tensor"), None, None),
            P("pipe", "tensor"),
            P("pipe", "tensor"),
            P("pipe", None, "tensor"),
            P("pipe", "tensor"),
            P("pipe", "tensor", None),
            P("pipe", "tensor", None),
            P("pipe", "tensor"),
            P("pipe", "tensor"),
            P("pipe", "tensor"),
            P("pipe", None, "tensor"),
            P("pipe", "tensor"),
            P("pipe", "tensor", None),
            P("pipe", "tensor"),
        ),
        check_vma=False,
    )
```
